128 devices in a mesh: subj: 4 (over y_lo, core), vox: 32 (over z, x, y_hi).
Axes of the slice: x: 4, y: 4 (y_hi: 2, y_lo: 2; y = y_hi * 2 + y_lo), z: 4, core: 2. Of those that a mesh axis runs over, the one named last changes fastest.
Arguments:
- series: bfloat16 [16, 256, 16384], P('subj', None, 'vox'), may hold values from -6 to 6
- offsets: int32 [16, 12], replicated, may hold values from 0 to 240
- selected: int32 [64], replicated, may hold values from 0 to 16383, as said below
Outputs:
- kernel: float32 [64, 192, 192], P('vox', 'subj')
The draws below stay inside these ranges and needn't reach their ends.
Inputs may be any that keep to these rules, and one draw needn't show every extreme that they name: `offsets`: each epoch lies inside its subject's run; epochs may intersect. `selected`: the ids are distinct.
All inputs are finite; a program needn't handle non-finite values.
Results may differ from the reference program's by a relative error of at most 0.00035.
Values may be sent and summed in bfloat16 or wider, within the bound.
A program may use at most 128 MiB of HBM per device.

```python
import jax
import jax.numpy as jnp
from jax import lax

VOX = 16384
TR = 16
EP = 12
RUN_TR = 256
SUBJECTS = 16
SEL = 64


def draw_selected(key, part):
    first_key = jax.random.fold_in(key, 11)
    second_key = jax.random.fold_in(key, 12)
    middle = jax.random.permutation(first_key, VOX - 2)[:SEL - 2] + 1
    ends = jnp.array([0, VOX - 1], dtype=jnp.int32)
    joined = jnp.concatenate([ends, middle.astype(jnp.int32)])
    return jax.random.permutation(second_key, joined).astype(jnp.int32)


def plant(entries, stream_key, least, high):
    extent = entries.shape
    place = [jax.random.randint(jax.random.fold_in(stream_key, axis), (), 0, extent[axis]) for axis in range(len(extent))]
    entries = entries.at[tuple(place)].set(least)
    longest = extent.index(max(extent))
    place[longest] = (place[longest] + 1) % extent[longest]
    return entries.at[tuple(place)].set(high)


def block_levels(key, shape, cuts, smallest, top_value):
    def one(position, parts):
        steps = jax.random.uniform(jax.random.fold_in(jax.random.fold_in(key, 6), position), (parts,), jnp.float32, smallest / len(cuts), top_value / len(cuts))
        return jnp.repeat(jnp.exp(steps), shape[position] // parts).reshape((-1,) + (1,) * (len(shape) - position - 1))

    gain = one(*cuts[0])
    for cut in cuts[1:]:
        gain = gain * one(*cut)
    return gain


def bell_draw(key, dims, scale, reach, cuts=(), held_as=jnp.bfloat16):
    entries = scale * jax.random.normal(key, dims, jnp.float32)
    if cuts:
        entries = entries * block_levels(key, dims, cuts, -0.22, 0.18)
    return jnp.clip(entries, -reach, reach).astype(held_as)


def setup_inputs(seed: int = 0) -> dict:
    keys = jax.random.split(jax.random.key(seed), 4)
    return {
        "series": bell_draw(keys[0], (SUBJECTS, RUN_TR, VOX), 1.0, 6.0, ((0, 4), (2, 32))),
        "offsets": plant(jax.random.randint(keys[1], (SUBJECTS, EP), 0, RUN_TR - TR + 1), jax.random.fold_in(keys[1], 1), 0, RUN_TR - TR).astype(jnp.int32),
        "selected": draw_selected(jax.random.fold_in(keys[3], 71), 0),
    }


series_floor = 1.0
spread_floor = 0.05
shrink_factor = 0.9

def windows(block, starts):

    def subject_windows(subject_row, subject_offsets):
        return jax.vmap(lambda offset: lax.dynamic_slice_in_dim(subject_row, offset, TR, 0))(subject_offsets)
    return jax.vmap(subject_windows)(block, starts)

def standardize(values):
    centred = values - lax.optimization_barrier(jnp.mean(values, axis=2, keepdims=True))
    return centred / jnp.sqrt(lax.optimization_barrier(jnp.sum(centred * centred, axis=2, keepdims=True)) + series_floor)

def fisher_transform(correlation):
    shrunk = shrink_factor * correlation
    return 0.5 * jnp.log((1.0 + shrunk) / (1.0 - shrunk))

def scores(slab_std, voxel_std):
    correlation = jnp.einsum('setk,setv->ksev', slab_std, voxel_std, precision=lax.Precision.HIGHEST)
    fisher = fisher_transform(correlation)
    centred = fisher - lax.optimization_barrier(jnp.mean(fisher, axis=2, keepdims=True))
    variance = lax.optimization_barrier(jnp.mean(centred * centred, axis=2, keepdims=True))
    zscored = (centred / jnp.sqrt(variance + spread_floor)).astype(jnp.bfloat16)
    return zscored.reshape(zscored.shape[0], zscored.shape[1] * zscored.shape[2], zscored.shape[3])

def reference(series, offsets, selected):
    epochs = windows(series, offsets)
    voxel_std = standardize(epochs.astype(jnp.float32))
    slab_std = standardize(jnp.take(epochs, selected, axis=3).astype(jnp.float32))
    block_width = 8
    blocks = jnp.moveaxis(slab_std.reshape(slab_std.shape[:3] + (SEL // block_width, block_width)), 3, 0)

    def kernel_block(slab_block):
        zscored = scores(slab_block, voxel_std).astype(jnp.float32)
        return jnp.einsum('kev,kfv->kef', zscored, zscored, precision=lax.Precision.HIGHEST) * (1.0 / VOX)
    mapped = lax.map(kernel_block, blocks)
    return mapped.reshape(SEL, mapped.shape[2], mapped.shape[3])
```

```python
import functools

import jax
import jax.numpy as jnp
from jax import lax
from jax.experimental import pallas as pl
from jax.experimental.pallas import tpu as pltpu
from jax.sharding import PartitionSpec as P

MESH = pl.DeviceIdType.MESH
F32, BF16, I32 = jnp.float32, jnp.bfloat16, jnp.int32
HIGH = lax.Precision.HIGHEST

SUBJ, SHARDS = 4, 32
TR, EP, RUN = 16, 12, 256
LOCAL = 4
QUADS = 3
SEL, OWN = 64, 16
VOX = 512
ROWS = SUBJ * EP * LOCAL
NT = (((1,), (1,)), ((), ()))
series_floor = 1.0
spread_floor = 0.05
shrink_factor = 0.9


def copy_to(src, dst, send_sem, recv_sem, subj, vox):
    return pltpu.make_async_remote_copy(
        src_ref=src,
        dst_ref=dst,
        send_sem=send_sem,
        recv_sem=recv_sem,
        device_id={"subj": subj, "vox": vox},
        device_id_type=MESH,
    )


def await_bytes(ref, sem):
    pltpu.make_async_copy(ref, ref, sem).wait()


def fold(x):
    return x + pltpu.roll(x, 4, 0)


def main_kernel(
    series_hbm,
    offsets,
    selected,
    out_ref,
    series,
    choose,
    epochs,
    scale,
    slab_out,
    slab_in,
    slab_sum,
    slab,
    raw,
    lhs_hi,
    lhs_lo,
    std_hi,
    std_lo,
    corr,
    score,
    gram,
    parts,
    total,
    final,
    load_sem,
    slab_send,
    slab_recv,
    share_send,
    share_recv,
    near_send,
    near_recv,
    far_send,
    far_recv,
    relay_send,
    relay_recv,
    part_send,
    part_recv,
    final_send,
    final_recv,
):
    j = lax.axis_index("subj")
    v = lax.axis_index("vox")
    near, far = j ^ 1, j ^ 2

    load = pltpu.make_async_copy(series_hbm, series, load_sem)
    load.start()

    barrier = pltpu.get_barrier_semaphore()

    def greet(step, carry):
        index = lax.rem(j * SHARDS + v + step, SUBJ * SHARDS)
        pl.semaphore_signal(
            barrier,
            inc=1,
            device_id={"subj": index // SHARDS, "vox": lax.rem(index, SHARDS)},
            device_id_type=MESH,
        )
        return carry

    lax.fori_loop(1, SUBJ * SHARDS, greet, 0)

    row16 = lax.broadcasted_iota(I32, (16, 128), 0)
    scan = lax.broadcasted_iota(I32, (16, LOCAL * RUN), 1)

    for q in range(QUADS):
        start = jnp.zeros((16, 128), I32)
        for r in range(16):
            first = offsets[j * LOCAL + r % 4, q * 4 + r // 4] + (r % 4) * RUN
            start = jnp.where(row16 == r, first, start)
        ahead = scan - jnp.concatenate([start] * (LOCAL * RUN // 128), axis=1)
        for t in range(TR):
            choose[pl.ds(q * 256 + t * 16, 16), :] = jnp.where(ahead == t, 1.0, 0.0).astype(BF16)

    id_rows = []
    row8 = lax.broadcasted_iota(I32, (8, 128), 0)
    for block in range(SEL // 8):
        ids = jnp.zeros((8, 128), I32)
        for r in range(8):
            place = block * 8 + r
            ids = jnp.where(row8 == r, selected[4 * (place % OWN) + place // OWN], ids)
        id_rows.append(ids)
    ids = jnp.concatenate(id_rows, axis=0)
    columns = lax.broadcasted_iota(I32, (SEL, VOX), 1) + v * VOX
    picker = jnp.where(columns == jnp.concatenate([ids] * (VOX // 128), axis=1), 1.0, 0.0).astype(BF16)

    load.wait()
    runs = series[...].reshape(LOCAL * RUN, VOX)
    for q in range(QUADS):
        chosen = jnp.dot(choose[pl.ds(q * 256, 256), :], runs, preferred_element_type=F32).astype(BF16)
        epochs[0, q] = chosen
        slab_out[:, 0, pl.ds(q * 256, 256)] = lax.dot_general(picker, chosen, NT, preferred_element_type=F32)

    pl.semaphore_wait(barrier, SUBJ * SHARDS - 1)

    def send_slab(step, carry):
        piece = lax.rem(v + step, SHARDS)
        to_j, to_v = piece // 8, j * 8 + lax.rem(piece, 8)

        @pl.when(jnp.logical_or(to_j != j, to_v != v))
        def _():
            copy_to(slab_out.at[pl.ds(piece * 2, 2)], slab_in.at[v], slab_send, slab_recv, to_j, to_v).start()

        return carry

    lax.fori_loop(0, SHARDS, send_slab, 0)

    for q in range(QUADS):
        copy_to(epochs.at[0, q], epochs.at[1, q], near_send.at[q], near_recv.at[q], near, v).start()
        copy_to(epochs.at[0, q], epochs.at[2, q], far_send.at[q], far_recv.at[q], far, v).start()

    def scales(r, carry):
        for q in range(QUADS):
            y = epochs[r, q].astype(F32).reshape(TR, 16, VOX)
            centred = y - (jnp.sum(y, axis=0) * (1.0 / TR))[None]
            scale[r, q] = lax.rsqrt(jnp.sum(centred * centred, axis=0) + series_floor)
        return carry

    lax.fori_loop(0, 1, scales, 0)

    own_group = v // 8 == j

    @pl.when(own_group)
    def _():
        slab_in[v] = slab_out[pl.ds((j * 8 + lax.rem(v, 8)) * 2, 2)]
        await_bytes(slab_in.at[pl.ds(0, SHARDS - 1)], slab_recv)
        await_bytes(slab_in.at[pl.ds(0, SHARDS - 1)], slab_send)

    @pl.when(jnp.logical_not(own_group))
    def _():
        await_bytes(slab_in, slab_recv)
        await_bytes(slab_in, slab_send)

    slab_sum[...] = jnp.sum(slab_in[...], axis=0)

    def share_slab(step, carry):
        to_v = lax.rem(v + step, SHARDS)
        copy_to(slab_sum, slab.at[v], share_send, share_recv, j, to_v).start()
        return carry

    lax.fori_loop(1, SHARDS, share_slab, 0)
    slab[v] = slab_sum[...]

    for q in range(QUADS):
        copy_to(epochs.at[0, q], epochs.at[1, q], near_send.at[q], near_recv.at[q], near, v).wait_recv()
    lax.fori_loop(1, 2, scales, 0)

    def relay(q):
        copy_to(epochs.at[0, q], epochs.at[2, q], far_send.at[q], far_recv.at[q], far, v).wait_recv()
        copy_to(epochs.at[2, q], epochs.at[3, q], relay_send.at[q], relay_recv.at[q], near, v).start()

    relay(0)
    await_bytes(slab.at[pl.ds(0, SHARDS - 1)], share_recv)
    await_bytes(slab.at[pl.ds(0, SHARDS - 1)], share_send)

    for r in range(SUBJ):
        group = (j ^ r) if r else j
        for kk in range(8):
            for i in range(2):
                for q in range(QUADS):
                    raw[r * QUADS + q, pl.ds(kk * 2 + i, 1), :] = slab[group * 8 + kk, i, :, pl.ds(q * 256, 256)]
    x = raw[...].reshape(SUBJ * QUADS * OWN, 256)
    same = jnp.where(
        lax.rem(lax.broadcasted_iota(I32, (256, 256), 0), 16) == lax.rem(lax.broadcasted_iota(I32, (256, 256), 1), 16),
        1.0,
        0.0,
    )
    centred = x - jnp.dot(x, same, precision=HIGH, preferred_element_type=F32) * (1.0 / TR)
    spread = jnp.dot(centred * centred, same, precision=HIGH, preferred_element_type=F32)
    x_std = centred * lax.rsqrt(spread + series_floor) * shrink_factor
    x_hi = x_std.astype(BF16).astype(F32)
    std_hi[...] = x_hi.reshape(SUBJ * QUADS, OWN, 256)
    std_lo[...] = (x_std - x_hi).reshape(SUBJ * QUADS, OWN, 256)

    own_row = lax.rem(lax.broadcasted_iota(I32, (16, 256), 1), 16) == lax.broadcasted_iota(I32, (16, 256), 0)

    def group_scores(r, carry):
        def correlate(q, carry):
            for k in range(OWN):
                for std, lhs in ((std_hi, lhs_hi), (std_lo, lhs_lo)):
                    line = jnp.broadcast_to(std[r * QUADS + q, pl.ds(k, 1), :], (16, 256))
                    lhs[pl.ds(k * 16, 16), :] = jnp.where(own_row, line, 0.0).astype(BF16)
            y = epochs[r, q]
            corr[q] = jnp.dot(lhs_hi[...], y, preferred_element_type=F32) + jnp.dot(
                lhs_lo[...], y, preferred_element_type=F32
            )
            return carry

        lax.fori_loop(0, QUADS, correlate, 0)

        def standard(k, carry):
            rows = pl.ds(pl.multiple_of(k * 16, 16), 16)
            twice = []
            for q in range(QUADS):
                shrunk = corr[q, rows, :] * scale[r, q]
                twice.append(jnp.log(1.0 + shrunk) - jnp.log(1.0 - shrunk))
            halves = [f[h * 8 : h * 8 + 8] for f in twice for h in range(2)]
            mean = fold(functools.reduce(jnp.add, halves)) * (1.0 / EP)
            halves = [f - mean for f in halves]
            spread = fold(functools.reduce(jnp.add, [f * f for f in halves])) * (1.0 / EP)
            gain = lax.rsqrt(spread + 4.0 * spread_floor)
            for q in range(QUADS):
                both = jnp.concatenate([halves[2 * q] * gain, halves[2 * q + 1] * gain], axis=0).astype(BF16)
                at = pl.multiple_of(r * 48 + q * 16, 16)
                score[k, pl.ds(at, 16), :] = both

                @pl.when(at < 64)
                def _():
                    score[k, pl.ds(pl.multiple_of(ROWS + lax.rem(at, 64), 16), 16), :] = both

            return carry

        lax.fori_loop(0, OWN, standard, 0)
        return carry

    lax.fori_loop(0, 1, group_scores, 0)
    relay(1)
    lax.fori_loop(1, 2, group_scores, 0)
    relay(2)
    lax.fori_loop(2, 3, scales, 0)
    lax.fori_loop(2, 3, group_scores, 0)
    for q in range(QUADS):
        copy_to(epochs.at[2, q], epochs.at[3, q], relay_send.at[q], relay_recv.at[q], near, v).wait_recv()
    lax.fori_loop(3, 4, scales, 0)
    lax.fori_loop(3, 4, group_scores, 0)

    def kernels(step, carry):
        m = lax.rem(v // 2 + step, OWN)
        for i in range(3):
            gram[m, pl.ds(i * 64, 64), :] = lax.dot_general(
                score[m, pl.ds(i * 64, 64), :], score[m, pl.ds(i * 64, 128), :], NT, preferred_element_type=F32
            )
        for h in range(2):
            to_v = m * 2 + h

            @pl.when(to_v != v)
            def _():
                copy_to(gram.at[m, pl.ds(h * 96, 96)], parts.at[v], part_send, part_recv, j, to_v).start()

        return carry

    lax.fori_loop(0, OWN, kernels, 0)

    parts[v] = gram[v // 2, pl.ds(pl.multiple_of(lax.rem(v, 2) * 96, 8), 96), :]
    await_bytes(parts.at[pl.ds(0, SHARDS - 1)], part_recv)

    def add(i, acc):
        return acc + parts[i]

    total[...] = lax.fori_loop(0, SHARDS, add, jnp.zeros((96, 128), F32)) * (1.0 / (VOX * SHARDS))

    half = lax.rem(v, 2)
    owner_v = v - half + j // 2
    place = lax.rem(j, 2)
    for s in range(SUBJ):

        @pl.when(jnp.logical_or(j != s, owner_v != v))
        def _():
            copy_to(total, final.at[place * 2 + half], final_send, final_recv, s, owner_v).start()

    @pl.when(owner_v == v)
    def _():
        final[place * 2 + half] = total[...]
        await_bytes(final.at[pl.ds(0, SUBJ - 1)], final_recv)
        await_bytes(final.at[pl.ds(0, SUBJ - 1)], final_send)

    @pl.when(owner_v != v)
    def _():
        await_bytes(final, final_recv)
        await_bytes(final, final_send)

    for i in range(2):
        for h in range(2):
            out_ref[i, pl.ds(h * 96, 96), :] = final[i * 2 + h]

    await_bytes(parts.at[pl.ds(0, SHARDS - 1)], part_send)
    for q in range(QUADS):
        copy_to(epochs.at[0, q], epochs.at[1, q], near_send.at[q], near_recv.at[q], near, v).wait_send()
        copy_to(epochs.at[0, q], epochs.at[2, q], far_send.at[q], far_recv.at[q], far, v).wait_send()
        copy_to(epochs.at[2, q], epochs.at[3, q], relay_send.at[q], relay_recv.at[q], near, v).wait_send()


def line_of(group, epoch, subject):
    return group * (EP * LOCAL) + epoch * LOCAL + subject


def place_kernel(cyclic_ref, out_ref):
    j = lax.axis_index("subj")
    v = lax.axis_index("vox")

    def column_line(b, taker):
        s = b // EP
        return line_of((s // LOCAL) ^ taker, lax.rem(b, EP), lax.rem(s, LOCAL))

    for i in range(2):
        taker = lax.rem(v, 2) * 2 + i
        out = jnp.zeros((EP * LOCAL, ROWS), F32)
        for block in range(3):
            part = cyclic_ref[i, pl.ds(block * 64, 64), :]
            c = lax.broadcasted_iota(I32, (128, ROWS), 0)
            to = column_line(lax.broadcasted_iota(I32, (128, ROWS), 1), taker)
            weight = jnp.where(c < 64, 0.5, 1.0)
            wide = jnp.where(lax.rem(block * 64 + c, ROWS) == to, weight, 0.0)
            c = lax.broadcasted_iota(I32, (64, ROWS), 0)
            to = column_line(lax.broadcasted_iota(I32, (64, ROWS), 1), taker)
            tall = jnp.where(block * 64 + c == to, 1.0, 0.0)
            p = lax.broadcasted_iota(I32, (EP * LOCAL, 64), 0)
            line = line_of(j ^ taker, lax.rem(p, EP), p // EP)
            rows = jnp.where(block * 64 + lax.broadcasted_iota(I32, (EP * LOCAL, 64), 1) == line, 1.0, 0.0)
            p = lax.broadcasted_iota(I32, (EP * LOCAL, 128), 0)
            line = line_of(j ^ taker, lax.rem(p, EP), p // EP)
            c = lax.broadcasted_iota(I32, (EP * LOCAL, 128), 1)
            weight = jnp.where(c < 64, 0.5, 1.0)
            turned = jnp.where(lax.rem(block * 64 + c, ROWS) == line, weight, 0.0)
            dot = functools.partial(jnp.dot, precision=HIGH, preferred_element_type=F32)
            out += dot(dot(rows, part), wide)
            out += dot(lax.dot_general(turned, part, NT, precision=HIGH, preferred_element_type=F32), tall)
        out_ref[i] = out


def body(series, offsets, selected):
    vmem = pltpu.VMEM
    dma = pltpu.SemaphoreType.DMA
    cyclic = pl.pallas_call(
        main_kernel,
        out_shape=jax.ShapeDtypeStruct((2, ROWS, 128), F32),
        in_specs=[
            pl.BlockSpec(memory_space=pl.ANY),
            pl.BlockSpec(memory_space=pltpu.SMEM),
            pl.BlockSpec(memory_space=pltpu.SMEM),
        ],
        out_specs=pl.BlockSpec(memory_space=pltpu.VMEM),
        scratch_shapes=[
            vmem((LOCAL, RUN, VOX), BF16),
            vmem((QUADS * 256, LOCAL * RUN), BF16),
            vmem((SUBJ, QUADS, 256, VOX), BF16),
            vmem((SUBJ, QUADS, 16, VOX), F32),
            vmem((SEL, 1, QUADS * 256), F32),
            vmem((SHARDS, 2, 1, QUADS * 256), F32),
            vmem((2, 1, QUADS * 256), F32),
            vmem((SHARDS, 2, 1, QUADS * 256), F32),
            vmem((SUBJ * QUADS, OWN, 256), F32),
            vmem((256, 256), BF16),
            vmem((256, 256), BF16),
            vmem((SUBJ * QUADS, OWN, 256), F32),
            vmem((SUBJ * QUADS, OWN, 256), F32),
            vmem((QUADS, 256, VOX), F32),
            vmem((OWN, 256, VOX), BF16),
            vmem((OWN, ROWS, 128), F32),
            vmem((SHARDS, 96, 128), F32),
            vmem((96, 128), F32),
            vmem((SUBJ, 96, 128), F32),
            dma,
            dma,
            dma,
            dma,
            dma,
            dma((QUADS,)),
            dma((QUADS,)),
            dma((QUADS,)),
            dma((QUADS,)),
            dma((QUADS,)),
            dma((QUADS,)),
            dma,
            dma,
            dma,
            dma,
        ],
        compiler_params=pltpu.CompilerParams(collective_id=0, has_side_effects=True),
        cost_estimate=pl.CostEstimate(flops=10**9, bytes_accessed=10**7, transcendentals=10**6),
    )(series, offsets, selected)
    return pl.pallas_call(
        place_kernel,
        out_shape=jax.ShapeDtypeStruct((2, EP * LOCAL, ROWS), F32),
        in_specs=[pl.BlockSpec(memory_space=pltpu.VMEM)],
        out_specs=pl.BlockSpec(memory_space=pltpu.VMEM),
    )(cyclic)


def solution(mesh):
    placed = (P("subj", None, "vox"), P(), P())
    return jax.shard_map(
        body, mesh=mesh, in_specs=placed, out_specs=P("vox", "subj", None), check_vma=False
    )
```

```python
import functools

import jax
import jax.numpy as jnp
from jax import lax
from jax.experimental import pallas as pl
from jax.experimental.pallas import tpu as pltpu
from jax.sharding import PartitionSpec as P

MESH = pl.DeviceIdType.MESH
F32, BF16, I32 = jnp.float32, jnp.bfloat16, jnp.int32
HIGH = lax.Precision.HIGHEST

SUBJ, SHARDS = 4, 32
TR, EP, RUN = 16, 12, 256
LOCAL = 4
QUADS = 3
SEL, OWN = 64, 16
VOX = 512
ROWS = SUBJ * EP * LOCAL
NT = (((1,), (1,)), ((), ()))
series_floor = 1.0
spread_floor = 0.05
shrink_factor = 0.9


def copy_to(src, dst, send_sem, recv_sem, subj, vox):
    return pltpu.make_async_remote_copy(
        src_ref=src,
        dst_ref=dst,
        send_sem=send_sem,
        recv_sem=recv_sem,
        device_id={"subj": subj, "vox": vox},
        device_id_type=MESH,
    )


def await_bytes(ref, sem):
    pltpu.make_async_copy(ref, ref, sem).wait()


def fold(x):
    return x + pltpu.roll(x, 4, 0)


def main_kernel(
    series_hbm,
    offsets,
    selected,
    out_ref,
    series,
    choose,
    epochs,
    scale,
    slab_out,
    slab_in,
    slab_sum,
    slab,
    raw,
    lhs_hi,
    lhs_lo,
    std_hi,
    std_lo,
    corr,
    score,
    gram,
    z_parts,
    x_parts,
    z_sums,
    x_sums,
    last_parts,
    total,
    final,
    load_sem,
    slab_send,
    slab_recv,
    share_send,
    share_recv,
    near_send,
    near_recv,
    far_send,
    far_recv,
    relay_send,
    relay_recv,
    part_send,
    z_recv,
    x_recv,
    sum_send,
    sum_recv,
    final_send,
    final_recv,
):
    j = lax.axis_index("subj")
    v = lax.axis_index("vox")
    near, far = j ^ 1, j ^ 2

    load = pltpu.make_async_copy(series_hbm, series, load_sem)
    load.start()

    barrier = pltpu.get_barrier_semaphore()

    def greet(step, carry):
        for other in range(SUBJ):
            pl.semaphore_signal(
                barrier,
                inc=1,
                device_id={"subj": j ^ other, "vox": (v + step) & (SHARDS - 1)},
                device_id_type=MESH,
            )
        return carry

    with jax.named_scope("greet"):
        lax.fori_loop(1, SHARDS, greet, 0, unroll=4)
        for other in range(1, SUBJ):
            pl.semaphore_signal(barrier, inc=1, device_id={"subj": j ^ other, "vox": v}, device_id_type=MESH)

    row16 = lax.broadcasted_iota(I32, (16, 128), 0)
    scan = lax.broadcasted_iota(I32, (16, LOCAL * RUN), 1)

    with jax.named_scope("choose"):
        for q in range(QUADS):
            start = jnp.zeros((16, 128), I32)
            for r in range(16):
                first = offsets[j * LOCAL + r % 4, q * 4 + r // 4] + (r % 4) * RUN
                start = jnp.where(row16 == r, first, start)
            ahead = scan - jnp.concatenate([start] * (LOCAL * RUN // 128), axis=1)
            for t in range(TR):
                choose[pl.ds(q * 256 + t * 16, 16), :] = jnp.where(ahead == t, 1.0, 0.0).astype(BF16)

    id_rows = []
    row8 = lax.broadcasted_iota(I32, (8, 128), 0)
    for block in range(SEL // 8):
        ids = jnp.zeros((8, 128), I32)
        for r in range(8):
            place = block * 8 + r
            ids = jnp.where(row8 == r, selected[4 * (place % OWN) + place // OWN], ids)
        id_rows.append(ids)
    ids = jnp.concatenate(id_rows, axis=0)
    columns = lax.broadcasted_iota(I32, (SEL, VOX), 1) + v * VOX
    picker = jnp.where(columns == jnp.concatenate([ids] * (VOX // 128), axis=1), 1.0, 0.0).astype(BF16)

    with jax.named_scope("pick_epochs"):
        load.wait()
        runs = series[...].reshape(LOCAL * RUN, VOX)
        for q in range(QUADS):
            chosen = jnp.dot(choose[pl.ds(q * 256, 256), :], runs, preferred_element_type=F32).astype(BF16)
            epochs[0, q] = chosen
            slab_out[:, 0, pl.ds(q * 256, 256)] = lax.dot_general(picker, chosen, NT, preferred_element_type=F32)

    with jax.named_scope("barrier"):
        pl.semaphore_wait(barrier, SUBJ * SHARDS - 1)

    def send_slab(step, carry):
        piece = lax.rem(v + step, SHARDS)
        to_j, to_v = piece // 8, j * 8 + lax.rem(piece, 8)

        @pl.when(jnp.logical_or(to_j != j, to_v != v))
        def _():
            copy_to(slab_out.at[pl.ds(piece * 2, 2)], slab_in.at[v], slab_send, slab_recv, to_j, to_v).start()

        return carry

    with jax.named_scope("send_slab"):
        lax.fori_loop(0, SHARDS, send_slab, 0)

    for q in range(QUADS):
        copy_to(epochs.at[0, q], epochs.at[1, q], near_send.at[q], near_recv.at[q], near, v).start()

    def send_far(q):
        copy_to(epochs.at[0, q], epochs.at[2, q], far_send.at[q], far_recv.at[q], far, v).start()

    send_far(0)

    def scales(r, carry):
        for q in range(QUADS):
            y = epochs[r, q].astype(F32).reshape(TR, 16, VOX)
            centred = y - (jnp.sum(y, axis=0) * (1.0 / TR))[None]
            scale[r, q] = lax.rsqrt(jnp.sum(centred * centred, axis=0) + series_floor)
        return carry

    with jax.named_scope("scale0"):
        lax.fori_loop(0, 1, scales, 0)

    own_group = v // 8 == j

    with jax.named_scope("slab_wait"):
        @pl.when(own_group)
        def _():
            slab_in[v] = slab_out[pl.ds((j * 8 + lax.rem(v, 8)) * 2, 2)]
            await_bytes(slab_in.at[pl.ds(0, SHARDS - 1)], slab_recv)
            await_bytes(slab_in.at[pl.ds(0, SHARDS - 1)], slab_send)

        @pl.when(jnp.logical_not(own_group))
        def _():
            await_bytes(slab_in, slab_recv)
            await_bytes(slab_in, slab_send)

    with jax.named_scope("slab_sum"):
        slab_sum[...] = jnp.sum(slab_in[...], axis=0)

    def share_slab(step, carry):
        to_v = lax.rem(v + step, SHARDS)
        copy_to(slab_sum, slab.at[v], share_send, share_recv, j, to_v).start()
        return carry

    with jax.named_scope("share_slab"):
        lax.fori_loop(1, SHARDS, share_slab, 0)
        slab[v] = slab_sum[...]

    send_far(1)
    send_far(2)

    with jax.named_scope("near_wait"):
        for q in range(QUADS):
            copy_to(epochs.at[0, q], epochs.at[1, q], near_send.at[q], near_recv.at[q], near, v).wait_recv()
    with jax.named_scope("scale1"):
        lax.fori_loop(1, 2, scales, 0)

    def relay(q):
        copy_to(epochs.at[0, q], epochs.at[2, q], far_send.at[q], far_recv.at[q], far, v).wait_recv()
        copy_to(epochs.at[2, q], epochs.at[3, q], relay_send.at[q], relay_recv.at[q], near, v).start()

    with jax.named_scope("relay0"):
        relay(0)
    with jax.named_scope("share_wait"):
        await_bytes(slab.at[pl.ds(0, SHARDS - 1)], share_recv)
        await_bytes(slab.at[pl.ds(0, SHARDS - 1)], share_send)

    with jax.named_scope("standard_slab"):
        for r in range(SUBJ):
            group = (j ^ r) if r else j
            for kk in range(8):
                for i in range(2):
                    for q in range(QUADS):
                        raw[r * QUADS + q, pl.ds(kk * 2 + i, 1), :] = slab[group * 8 + kk, i, :, pl.ds(q * 256, 256)]
        x = raw[...].reshape(SUBJ * QUADS * OWN, 256)
        same = jnp.where(
            lax.rem(lax.broadcasted_iota(I32, (256, 256), 0), 16) == lax.rem(lax.broadcasted_iota(I32, (256, 256), 1), 16),
            1.0,
            0.0,
        )
        centred = x - jnp.dot(x, same, precision=HIGH, preferred_element_type=F32) * (1.0 / TR)
        spread = jnp.dot(centred * centred, same, precision=HIGH, preferred_element_type=F32)
        x_std = centred * lax.rsqrt(spread + series_floor) * shrink_factor
        x_hi = x_std.astype(BF16).astype(F32)
        std_hi[...] = x_hi.reshape(SUBJ * QUADS, OWN, 256)
        std_lo[...] = (x_std - x_hi).reshape(SUBJ * QUADS, OWN, 256)

    own_row = lax.rem(lax.broadcasted_iota(I32, (16, 256), 1), 16) == lax.broadcasted_iota(I32, (16, 256), 0)

    def group_scores(r, carry):
        def correlate(q, carry):
            for k in range(OWN):
                for std, lhs in ((std_hi, lhs_hi), (std_lo, lhs_lo)):
                    line = jnp.broadcast_to(std[r * QUADS + q, pl.ds(k, 1), :], (16, 256))
                    lhs[pl.ds(k * 16, 16), :] = jnp.where(own_row, line, 0.0).astype(BF16)
            y = epochs[r, q]
            corr[q] = jnp.dot(lhs_hi[...], y, preferred_element_type=F32) + jnp.dot(
                lhs_lo[...], y, preferred_element_type=F32
            )
            return carry

        lax.fori_loop(0, QUADS, correlate, 0)

        def standard(k, carry):
            rows = pl.ds(pl.multiple_of(k * 16, 16), 16)
            twice = []
            for q in range(QUADS):
                shrunk = corr[q, rows, :] * scale[r, q]
                twice.append(jnp.log(1.0 + shrunk) - jnp.log(1.0 - shrunk))
            halves = [f[h * 8 : h * 8 + 8] for f in twice for h in range(2)]
            mean = fold(functools.reduce(jnp.add, halves)) * (1.0 / EP)
            halves = [f - mean for f in halves]
            spread = fold(functools.reduce(jnp.add, [f * f for f in halves])) * (1.0 / EP)
            gain = lax.rsqrt(spread + 4.0 * spread_floor)
            for q in range(QUADS):
                both = jnp.concatenate([halves[2 * q] * gain, halves[2 * q + 1] * gain], axis=0).astype(BF16)
                at = pl.multiple_of(r * 48 + q * 16, 16)
                score[k, pl.ds(at, 16), :] = both

                @pl.when(at < 64)
                def _():
                    score[k, pl.ds(pl.multiple_of(ROWS + lax.rem(at, 64), 16), 16), :] = both

            return carry

        lax.fori_loop(0, OWN, standard, 0)
        return carry

    with jax.named_scope("scores0"):
        lax.fori_loop(0, 1, group_scores, 0)
    with jax.named_scope("relay1"):
        relay(1)
    with jax.named_scope("scores1"):
        lax.fori_loop(1, 2, group_scores, 0)
    with jax.named_scope("relay2"):
        relay(2)
    with jax.named_scope("scores2"):
        lax.fori_loop(2, 3, scales, 0)
        lax.fori_loop(2, 3, group_scores, 0)
    with jax.named_scope("relay_wait"):
        for q in range(QUADS):
            copy_to(epochs.at[2, q], epochs.at[3, q], relay_send.at[q], relay_recv.at[q], near, v).wait_recv()
    with jax.named_scope("scores3"):
        lax.fori_loop(3, 4, scales, 0)
        lax.fori_loop(3, 4, group_scores, 0)

    z, x, y = v // 8, lax.rem(v // 2, 4), lax.rem(v, 2)

    def ahead_of(place, step):
        return (place + step) & 3

    def shard_at(z, x, y):
        return z * 8 + x * 2 + y

    def rows_of(m, first, last):
        for top in (first, 64 if first == 0 else 128):
            bottom = {0: 64, 64: 96, 96: 128, 128: 192}[top]
            block = top // 64 * 64
            gram[m, top:bottom, :] = lax.dot_general(
                score[m, top:bottom, :], score[m, block : block + 128, :], NT, preferred_element_type=F32
            )

    def kernels(step, carry):
        major, minor = step // 4, step & 3
        m = ahead_of(z, minor) * 4 + ahead_of(x, major)
        rows_of(m, 0, 96)

        @pl.when(minor == 0)
        def _():
            z_parts[major, 0] = gram[m, 0:96, :]

        @pl.when(minor > 0)
        def _():
            to_v = shard_at(ahead_of(z, minor), x, y)
            copy_to(gram.at[m, pl.ds(0, 96)], z_parts.at[major, minor], part_send, z_recv.at[major], j, to_v).start()

        m = ahead_of(z, major) * 4 + ahead_of(x, minor)
        rows_of(m, 96, 192)

        @pl.when(minor == 0)
        def _():
            x_parts[major, 0] = gram[m, 96:192, :]

        @pl.when(minor > 0)
        def _():
            to_v = shard_at(z, ahead_of(x, minor), y)
            copy_to(gram.at[m, pl.ds(96, 96)], x_parts.at[major, minor], part_send, x_recv.at[major], j, to_v).start()

        return carry

    with jax.named_scope("kernels"):
        lax.fori_loop(0, OWN, kernels, 0)

    for step in range(4):
        for half_of, parts, recv, sums, to_v in (
            (0, z_parts, z_recv, z_sums, shard_at(z, ahead_of(x, step), 0)),
            (1, x_parts, x_recv, x_sums, shard_at(ahead_of(z, step), x, 1)),
        ):
            with jax.named_scope("part_wait"):
                await_bytes(parts.at[step, pl.ds(1, 3)], recv.at[step])
            sums[step] = (parts[step, 0] + parts[step, 1]) + (parts[step, 2] + parts[step, 3])
            if step:
                slot = step * 2 + (y ^ half_of)
                copy_to(sums.at[step], last_parts.at[slot], sum_send, sum_recv, j, to_v).start()
            else:

                @pl.when(y == half_of)
                def _():
                    last_parts[0] = sums[0]

                @pl.when(y != half_of)
                def _():
                    copy_to(sums.at[0], last_parts.at[1], sum_send, sum_recv, j, to_v).start()

    with jax.named_scope("last_wait"):
        await_bytes(last_parts.at[pl.ds(1, 7)], sum_recv)

    total[...] = jnp.sum(last_parts[...], axis=0) * (1.0 / (VOX * SHARDS))

    with jax.named_scope("final"):
        half = lax.rem(v, 2)
        owner_v = v - half + j // 2
        place = lax.rem(j, 2)
        for s in range(SUBJ):

            @pl.when(jnp.logical_or(j != s, owner_v != v))
            def _():
                copy_to(total, final.at[place * 2 + half], final_send, final_recv, s, owner_v).start()

        @pl.when(owner_v == v)
        def _():
            final[place * 2 + half] = total[...]
            await_bytes(final.at[pl.ds(0, SUBJ - 1)], final_recv)
            await_bytes(final.at[pl.ds(0, SUBJ - 1)], final_send)

        @pl.when(owner_v != v)
        def _():
            await_bytes(final, final_recv)
            await_bytes(final, final_send)

    for i in range(2):
        for h in range(2):
            out_ref[i, pl.ds(h * 96, 96), :] = final[i * 2 + h]

    with jax.named_scope("drain"):
        for _ in range(2):
            await_bytes(z_parts.at[pl.ds(0, 3)], part_send)
        await_bytes(last_parts.at[pl.ds(1, 7)], sum_send)
        for q in range(QUADS):
            copy_to(epochs.at[0, q], epochs.at[1, q], near_send.at[q], near_recv.at[q], near, v).wait_send()
            copy_to(epochs.at[0, q], epochs.at[2, q], far_send.at[q], far_recv.at[q], far, v).wait_send()
            copy_to(epochs.at[2, q], epochs.at[3, q], relay_send.at[q], relay_recv.at[q], near, v).wait_send()


def line_of(group, epoch, subject):
    return group * (EP * LOCAL) + epoch * LOCAL + subject


def place_kernel(cyclic_ref, out_ref):
    j = lax.axis_index("subj")
    v = lax.axis_index("vox")

    def column_line(b, taker):
        s = b // EP
        return line_of((s // LOCAL) ^ taker, lax.rem(b, EP), lax.rem(s, LOCAL))

    for i in range(2):
        taker = lax.rem(v, 2) * 2 + i
        out = jnp.zeros((EP * LOCAL, ROWS), F32)
        for block in range(3):
            part = cyclic_ref[i, pl.ds(block * 64, 64), :]
            c = lax.broadcasted_iota(I32, (128, ROWS), 0)
            to = column_line(lax.broadcasted_iota(I32, (128, ROWS), 1), taker)
            weight = jnp.where(c < 64, 0.5, 1.0)
            wide = jnp.where(lax.rem(block * 64 + c, ROWS) == to, weight, 0.0)
            c = lax.broadcasted_iota(I32, (64, ROWS), 0)
            to = column_line(lax.broadcasted_iota(I32, (64, ROWS), 1), taker)
            tall = jnp.where(block * 64 + c == to, 1.0, 0.0)
            p = lax.broadcasted_iota(I32, (EP * LOCAL, 64), 0)
            line = line_of(j ^ taker, lax.rem(p, EP), p // EP)
            rows = jnp.where(block * 64 + lax.broadcasted_iota(I32, (EP * LOCAL, 64), 1) == line, 1.0, 0.0)
            p = lax.broadcasted_iota(I32, (EP * LOCAL, 128), 0)
            line = line_of(j ^ taker, lax.rem(p, EP), p // EP)
            c = lax.broadcasted_iota(I32, (EP * LOCAL, 128), 1)
            weight = jnp.where(c < 64, 0.5, 1.0)
            turned = jnp.where(lax.rem(block * 64 + c, ROWS) == line, weight, 0.0)
            dot = functools.partial(jnp.dot, precision=HIGH, preferred_element_type=F32)
            out += dot(dot(rows, part), wide)
            out += dot(lax.dot_general(turned, part, NT, precision=HIGH, preferred_element_type=F32), tall)
        out_ref[i] = out


def body(series, offsets, selected):
    vmem = pltpu.VMEM
    dma = pltpu.SemaphoreType.DMA
    cyclic = pl.pallas_call(
        main_kernel,
        out_shape=jax.ShapeDtypeStruct((2, ROWS, 128), F32),
        in_specs=[
            pl.BlockSpec(memory_space=pl.ANY),
            pl.BlockSpec(memory_space=pltpu.SMEM),
            pl.BlockSpec(memory_space=pltpu.SMEM),
        ],
        out_specs=pl.BlockSpec(memory_space=pltpu.VMEM),
        scratch_shapes=[
            vmem((LOCAL, RUN, VOX), BF16),
            vmem((QUADS * 256, LOCAL * RUN), BF16),
            vmem((SUBJ, QUADS, 256, VOX), BF16),
            vmem((SUBJ, QUADS, 16, VOX), F32),
            vmem((SEL, 1, QUADS * 256), F32),
            vmem((SHARDS, 2, 1, QUADS * 256), F32),
            vmem((2, 1, QUADS * 256), F32),
            vmem((SHARDS, 2, 1, QUADS * 256), F32),
            vmem((SUBJ * QUADS, OWN, 256), F32),
            vmem((256, 256), BF16),
            vmem((256, 256), BF16),
            vmem((SUBJ * QUADS, OWN, 256), F32),
            vmem((SUBJ * QUADS, OWN, 256), F32),
            vmem((QUADS, 256, VOX), F32),
            vmem((OWN, 256, VOX), BF16),
            vmem((OWN, ROWS, 128), F32),
            vmem((4, 4, 96, 128), F32),
            vmem((4, 4, 96, 128), F32),
            vmem((4, 96, 128), F32),
            vmem((4, 96, 128), F32),
            vmem((8, 96, 128), F32),
            vmem((96, 128), F32),
            vmem((SUBJ, 96, 128), F32),
            dma,
            dma,
            dma,
            dma,
            dma,
            dma((QUADS,)),
            dma((QUADS,)),
            dma((QUADS,)),
            dma((QUADS,)),
            dma((QUADS,)),
            dma((QUADS,)),
            dma,
            dma((4,)),
            dma((4,)),
            dma,
            dma,
            dma,
            dma,
        ],
        compiler_params=pltpu.CompilerParams(collective_id=0, has_side_effects=True),
        cost_estimate=pl.CostEstimate(flops=10**9, bytes_accessed=10**7, transcendentals=10**6),
    )(series, offsets, selected)
    return pl.pallas_call(
        place_kernel,
        out_shape=jax.ShapeDtypeStruct((2, EP * LOCAL, ROWS), F32),
        in_specs=[pl.BlockSpec(memory_space=pltpu.VMEM)],
        out_specs=pl.BlockSpec(memory_space=pltpu.VMEM),
    )(cyclic)


def solution(mesh):
    placed = (P("subj", None, "vox"), P(), P())
    return jax.shard_map(
        body, mesh=mesh, in_specs=placed, out_specs=P("vox", "subj", None), check_vma=False
    )
```

```python
import functools

import jax
import jax.numpy as jnp
from jax import lax
from jax.experimental import pallas as pl
from jax.experimental.pallas import tpu as pltpu
from jax.sharding import PartitionSpec as P

MESH = pl.DeviceIdType.MESH
F32, BF16, I32 = jnp.float32, jnp.bfloat16, jnp.int32
HIGH = lax.Precision.HIGHEST

SUBJ, SHARDS = 4, 32
TR, EP, RUN = 16, 12, 256
LOCAL = 4
QUADS = 3
SEL, OWN = 64, 16
VOX = 512
ROWS = SUBJ * EP * LOCAL
NT = (((1,), (1,)), ((), ()))
series_floor = 1.0
spread_floor = 0.05
shrink_factor = 0.9


def copy_to(src, dst, send_sem, recv_sem, subj, vox):
    return pltpu.make_async_remote_copy(
        src_ref=src,
        dst_ref=dst,
        send_sem=send_sem,
        recv_sem=recv_sem,
        device_id={"subj": subj, "vox": vox},
        device_id_type=MESH,
    )


def await_bytes(ref, sem):
    pltpu.make_async_copy(ref, ref, sem).wait()


def fold(x):
    return x + pltpu.roll(x, 4, 0)


def exact_terms(x):
    first = x.astype(BF16)
    rest = x - first.astype(F32)
    second = rest.astype(BF16)
    return first, second, (rest - second.astype(F32)).astype(BF16)


def line_of(group, epoch, subject):
    return group * (EP * LOCAL) + epoch * LOCAL + subject


def main_kernel(
    series_hbm,
    offsets,
    selected,
    out_ref,
    series,
    choose,
    epochs,
    scale,
    slab_out,
    slab_in,
    slab_sum,
    slab,
    raw,
    lhs_hi,
    lhs_lo,
    std_hi,
    std_lo,
    corr,
    score,
    gram,
    z_parts,
    x_parts,
    y_parts,
    z_sums,
    x_sums,
    y_sums,
    last,
    total,
    final,
    pick_rows,
    pick_turned,
    put_columns,
    load_sem,
    slab_send,
    slab_recv,
    share_send,
    share_recv,
    near_send,
    near_recv,
    far_send,
    far_recv,
    relay_send,
    relay_recv,
    part_send,
    z_recv,
    x_recv,
    y_recv,
    sum_send,
    sum_recv,
    final_send,
    final_recv,
):
    j = lax.axis_index("subj")
    v = lax.axis_index("vox")
    near, far = j ^ 1, j ^ 2
    z, x, y = v // 8, (v // 2) & 3, v & 1

    def ahead_of(place, step):
        return (place + step) & 3

    def shard_at(z, x, y):
        return z * 8 + x * 2 + y

    load = pltpu.make_async_copy(series_hbm, series, load_sem)
    load.start()

    barrier = pltpu.get_barrier_semaphore()

    def greet(step, carry):
        for other in range(SUBJ):
            pl.semaphore_signal(
                barrier,
                inc=1,
                device_id={"subj": j ^ other, "vox": (v + step) & (SHARDS - 1)},
                device_id_type=MESH,
            )
        return carry

    with jax.named_scope("greet"):
        lax.fori_loop(1, SHARDS, greet, 0, unroll=4)
        for other in range(1, SUBJ):
            pl.semaphore_signal(barrier, inc=1, device_id={"subj": j ^ other, "vox": v}, device_id_type=MESH)

    with jax.named_scope("choose"):
        row16 = lax.broadcasted_iota(I32, (16, 128), 0)
        scan = lax.broadcasted_iota(I32, (16, LOCAL * RUN), 1)
        for q in range(QUADS):
            start = jnp.zeros((16, 128), I32)
            for r in range(16):
                first = offsets[j * LOCAL + r % 4, q * 4 + r // 4] + (r % 4) * RUN
                start = jnp.where(row16 == r, first, start)
            ahead = scan - jnp.concatenate([start] * (LOCAL * RUN // 128), axis=1)
            for t in range(TR):
                choose[pl.ds(q * 256 + t * 16, 16), :] = jnp.where(ahead == t, 1.0, 0.0).astype(BF16)

    id_rows = []
    row8 = lax.broadcasted_iota(I32, (8, 128), 0)
    for block in range(SEL // 8):
        ids = jnp.zeros((8, 128), I32)
        for r in range(8):
            place = block * 8 + r
            ids = jnp.where(row8 == r, selected[4 * (place % OWN) + place // OWN], ids)
        id_rows.append(ids)
    ids = jnp.concatenate(id_rows, axis=0)
    columns = lax.broadcasted_iota(I32, (SEL, VOX), 1) + v * VOX
    picker = jnp.where(columns == jnp.concatenate([ids] * (VOX // 128), axis=1), 1.0, 0.0).astype(BF16)

    with jax.named_scope("pick_epochs"):
        load.wait()
        runs = series[...].reshape(LOCAL * RUN, VOX)
        for q in range(QUADS):
            chosen = jnp.dot(choose[pl.ds(q * 256, 256), :], runs, preferred_element_type=F32).astype(BF16)
            epochs[0, q] = chosen
            picked = lax.dot_general(picker, chosen, NT, preferred_element_type=F32)
            slab_out[:, :, pl.ds(q * 256, 256)] = picked.astype(BF16).reshape(SHARDS, 2, 256)

    with jax.named_scope("barrier"):
        pl.semaphore_wait(barrier, SUBJ * SHARDS - 1)

    def send_slab(step, carry):
        piece = (v + step) & (SHARDS - 1)
        to_j, to_v = piece // 8, j * 8 + (piece & 7)

        @pl.when(jnp.logical_or(to_j != j, to_v != v))
        def _():
            copy_to(slab_out.at[piece], slab_in.at[v], slab_send, slab_recv, to_j, to_v).start()

        return carry

    with jax.named_scope("send_slab"):
        lax.fori_loop(0, SHARDS, send_slab, 0)

    def near_copy(q):
        return copy_to(epochs.at[0, q], epochs.at[1, q], near_send.at[q], near_recv.at[q], near, v)

    def half_of(r, h, q):
        return epochs.at[r, q, :, pl.ds(h * 256, 256)]

    def far_copy(h, q):
        at = h * QUADS + q
        return copy_to(half_of(0, h, q), half_of(2, h, q), far_send.at[at], far_recv.at[at], far, v)

    def relay_copy(h, q):
        at = h * QUADS + q
        return copy_to(half_of(2, h, q), half_of(3, h, q), relay_send.at[at], relay_recv.at[at], near, v)

    def relay(h, q):
        with jax.named_scope("relay"):
            far_copy(h, q).wait_recv()
            relay_copy(h, q).start()

    for q in range(QUADS):
        near_copy(q).start()
    far_copy(0, 0).start()
    far_copy(0, 1).start()

    def scales(r, h):
        lanes = pl.ds(h * 256, 256)
        for q in range(QUADS):
            seen = epochs[r, q, :, lanes].astype(F32).reshape(TR, 16, 256)
            centred = seen - (jnp.sum(seen, axis=0) * (1.0 / TR))[None]
            scale[r, q, :, lanes] = lax.rsqrt(jnp.sum(centred * centred, axis=0) + series_floor)

    for h in range(2):
        scales(0, h)

    own_group = v // 8 == j

    with jax.named_scope("slab_wait"):

        @pl.when(own_group)
        def _():
            slab_in[v] = slab_out[j * 8 + (v & 7)]
            await_bytes(slab_in.at[pl.ds(0, SHARDS - 1)], slab_recv)

        @pl.when(jnp.logical_not(own_group))
        def _():
            await_bytes(slab_in, slab_recv)

    with jax.named_scope("slab_sum"):
        slab_sum[...] = jnp.sum(slab_in[...].astype(F32), axis=0).astype(BF16)

    def share_slab(step, carry):
        copy_to(slab_sum, slab.at[v], share_send, share_recv, j, (v + step) & (SHARDS - 1)).start()
        return carry

    with jax.named_scope("share_slab"):
        lax.fori_loop(1, SHARDS, share_slab, 0)
        slab[v] = slab_sum[...]

    far_copy(0, 2).start()
    for q in range(QUADS):
        far_copy(1, q).start()

    with jax.named_scope("places"):
        b = lax.broadcasted_iota(I32, (1, ROWS), 1)
        p = lax.broadcasted_iota(I32, (EP * LOCAL, 1), 0)
        for i in range(2):
            taker = y * 2 + i
            s = b // EP
            to = line_of((s // LOCAL) ^ taker, b - s * EP, s & 3)
            s = p // EP
            line = line_of(j ^ taker, p - s * EP, s)
            c = lax.broadcasted_iota(I32, (ROWS, 1), 0)
            put_columns[i, pl.ds(3 * 128, ROWS), :] = jnp.where(c == to, 1.0, 0.0).astype(BF16)
            for block in range(3):
                c = lax.broadcasted_iota(I32, (128, 1), 0) + block * 64
                c = jnp.where(c < ROWS, c, c - ROWS)
                weight = jnp.where(lax.broadcasted_iota(I32, (128, ROWS), 0) < 64, 0.5, 1.0)
                put_columns[i, pl.ds(block * 128, 128), :] = jnp.where(c == to, weight, 0.0).astype(BF16)
                c = lax.broadcasted_iota(I32, (1, 128), 1) + block * 64
                c = jnp.where(c < ROWS, c, c - ROWS)
                weight = jnp.where(lax.broadcasted_iota(I32, (EP * LOCAL, 128), 1) < 64, 0.5, 1.0)
                pick_turned[i, block] = jnp.where(c == line, weight, 0.0).astype(BF16)
                c = lax.broadcasted_iota(I32, (1, 64), 1) + block * 64
                pick_rows[i, block] = jnp.where(c == line, 1.0, 0.0).astype(BF16)

    with jax.named_scope("near_wait"):
        for q in range(QUADS):
            near_copy(q).wait_recv()
    for h in range(2):
        scales(1, h)

    relay(0, 0)
    relay(0, 1)
    with jax.named_scope("share_wait"):
        await_bytes(slab.at[pl.ds(0, SHARDS - 1)], share_recv)

    with jax.named_scope("standard_slab"):
        for r in range(SUBJ):
            group = (j ^ r) if r else j
            for kk in range(8):
                for q in range(QUADS):
                    raw[r * QUADS + q, pl.ds(kk * 2, 2), :] = slab[group * 8 + kk, :, pl.ds(q * 256, 256)].astype(F32)
        seen = raw[...].reshape(SUBJ * QUADS * OWN, 256)
        same = jnp.where(
            (lax.broadcasted_iota(I32, (256, 256), 0) & 15) == (lax.broadcasted_iota(I32, (256, 256), 1) & 15), 1.0, 0.0
        )
        centred = seen - jnp.dot(seen, same, precision=HIGH, preferred_element_type=F32) * (1.0 / TR)
        spread = jnp.dot(centred * centred, same, precision=HIGH, preferred_element_type=F32)
        x_std = centred * lax.rsqrt(spread + series_floor) * shrink_factor
        x_hi = x_std.astype(BF16).astype(F32)
        std_hi[...] = x_hi.reshape(SUBJ * QUADS, OWN, 256)
        std_lo[...] = (x_std - x_hi).reshape(SUBJ * QUADS, OWN, 256)

    own_row = (lax.broadcasted_iota(I32, (16, 256), 1) & 15) == lax.broadcasted_iota(I32, (16, 256), 0)

    def group_scores(r, h):
        lanes = pl.ds(h * 256, 256)

        def correlate(q, carry):
            for k in range(OWN):
                for std, lhs in ((std_hi, lhs_hi), (std_lo, lhs_lo)):
                    line = jnp.broadcast_to(std[r * QUADS + q, pl.ds(k, 1), :], (16, 256))
                    lhs[pl.ds(k * 16, 16), :] = jnp.where(own_row, line, 0.0).astype(BF16)
            seen = epochs[r, q, :, lanes]
            corr[q] = jnp.dot(lhs_hi[...], seen, preferred_element_type=F32) + jnp.dot(
                lhs_lo[...], seen, preferred_element_type=F32
            )
            return carry

        lax.fori_loop(0, QUADS, correlate, 0)

        def standard(k, carry):
            rows = pl.ds(pl.multiple_of(k * 16, 16), 16)
            halves = []
            for q in range(QUADS):
                shrunk = corr[q, rows, :] * scale[r, q, :, lanes]
                twice = jnp.log(1.0 + shrunk) - jnp.log(1.0 - shrunk)
                halves += [twice[0:8], twice[8:16]]
            mean = fold(functools.reduce(jnp.add, halves)) * (1.0 / EP)
            halves = [f - mean for f in halves]
            spread = fold(functools.reduce(jnp.add, [f * f for f in halves])) * (1.0 / EP)
            gain = lax.rsqrt(spread + 4.0 * spread_floor)
            for q in range(QUADS):
                both = jnp.concatenate([halves[2 * q] * gain, halves[2 * q + 1] * gain], axis=0).astype(BF16)
                at = r * 48 + q * 16
                score[k, pl.ds(at, 16), lanes] = both
                if at < 64:
                    score[k, pl.ds(ROWS + at, 16), lanes] = both
            return carry

        lax.fori_loop(0, OWN, standard, 0, unroll=2)

    with jax.named_scope("scores0"):
        group_scores(0, 0)
        group_scores(0, 1)
    relay(0, 2)
    with jax.named_scope("scores1"):
        group_scores(1, 0)
    relay(1, 0)
    with jax.named_scope("scores1"):
        group_scores(1, 1)
    with jax.named_scope("scores2"):
        scales(2, 0)
        group_scores(2, 0)
    relay(1, 1)
    for q in range(QUADS):
        relay_copy(0, q).wait_recv()
    with jax.named_scope("scores3"):
        scales(3, 0)
        group_scores(3, 0)
    relay(1, 2)
    with jax.named_scope("scores4"):
        scales(2, 1)
        group_scores(2, 1)
    for q in range(QUADS):
        relay_copy(1, q).wait_recv()
    with jax.named_scope("scores5"):
        scales(3, 1)
        group_scores(3, 1)

    def block_of(m, block):
        gram[m, pl.ds(block * 64, 64), :] = lax.dot_general(
            score[m, pl.ds(block * 64, 64), :], score[m, pl.ds(block * 64, 128), :], NT, preferred_element_type=F32
        )

    def kernels(step, carry):
        major, minor = step // 4, step & 3
        m = ahead_of(z, minor) * 4 + ahead_of(x, major)
        block_of(m, 0)

        @pl.when(minor == 0)
        def _():
            z_parts[major, 0] = gram[m, 0:64, :]

        @pl.when(minor > 0)
        def _():
            to_v = shard_at(ahead_of(z, minor), x, y)
            copy_to(gram.at[m, pl.ds(0, 64)], z_parts.at[major, minor], part_send, z_recv.at[major], j, to_v).start()

        m = ahead_of(z, major) * 4 + ahead_of(x, minor)
        block_of(m, 1)

        @pl.when(minor == 0)
        def _():
            x_parts[major, 0] = gram[m, 64:128, :]

        @pl.when(minor > 0)
        def _():
            to_v = shard_at(z, ahead_of(x, minor), y)
            copy_to(gram.at[m, pl.ds(64, 64)], x_parts.at[major, minor], part_send, x_recv.at[major], j, to_v).start()

        block_of(m, 2)
        rows = pl.ds(pl.multiple_of(128 + 32 * (y ^ 1), 32), 32)
        copy_to(gram.at[m, rows], y_parts.at[step], part_send, y_recv.at[major], j, v ^ 1).start()
        return carry

    with jax.named_scope("kernels"):
        lax.fori_loop(0, OWN, kernels, 0)

    for major in range(4):
        for block, parts, recv, sums in ((0, z_parts, z_recv, z_sums), (1, x_parts, x_recv, x_sums)):
            with jax.named_scope("part_wait"):
                await_bytes(parts.at[major, pl.ds(1, 3)], recv.at[major])
            sums[major] = (parts[major, 0] + parts[major, 1]) + (parts[major, 2] + parts[major, 3])
            for other in range(2):
                side = y ^ other
                rows = pl.ds(pl.multiple_of(side * 32, 32), 32)
                slot = major * 2 + other
                to_v = shard_at(ahead_of(z, major), x, side) if block else shard_at(z, ahead_of(x, major), side)
                if slot:
                    copy_to(sums.at[major, rows], last.at[block * 8 + slot], sum_send, sum_recv, j, to_v).start()
                else:
                    last[block * 8] = sums[0, rows, :]
        with jax.named_scope("part_wait"):
            await_bytes(y_parts.at[pl.ds(major * 4, 4)], y_recv.at[major])
        for minor in range(4):
            step = major * 4 + minor
            to_z, to_x = ahead_of(z, major), ahead_of(x, minor)
            rows = pl.ds(pl.multiple_of(128 + 32 * y, 32), 32)
            added = y_parts[step] + gram[to_z * 4 + to_x, rows, :]
            if step:
                y_sums[step] = added
                copy_to(y_sums.at[step], last.at[16 + step], sum_send, sum_recv, j, shard_at(to_z, to_x, y)).start()
            else:
                last[16] = added

    with jax.named_scope("last_wait"):
        await_bytes(last.at[pl.ds(0, 29)], sum_recv)

    mean = 1.0 / (VOX * SHARDS)
    total[0:32, :] = jnp.sum(last[0:8], axis=0) * mean
    total[32:64, :] = jnp.sum(last[8:16], axis=0) * mean
    total[64:96, :] = jnp.sum(last[16:32], axis=0) * mean

    owner_v = v - y + j // 2
    place = (j & 1) * 2 + y
    with jax.named_scope("final"):
        for other in range(SUBJ):
            to_j = (j ^ other) if other else j
            if other:
                copy_to(total, final.at[place], final_send, final_recv, to_j, owner_v).start()
            else:

                @pl.when(owner_v != v)
                def _():
                    copy_to(total, final.at[place], final_send, final_recv, j, owner_v).start()

        @pl.when(owner_v == v)
        def _():
            final[place] = total[...]
            await_bytes(final.at[pl.ds(0, SUBJ - 1)], final_recv)

        @pl.when(owner_v != v)
        def _():
            await_bytes(final, final_recv)

    with jax.named_scope("place"):
        for i in range(2):
            taken = []
            for block in range(3):
                rows = pl.ds(block * 32, 32)
                terms = exact_terms(jnp.concatenate([final[2 * i, rows, :], final[2 * i + 1, rows, :]], axis=0))
                wide = [jnp.dot(pick_rows[i, block], t, preferred_element_type=F32) for t in terms]
                tall = [lax.dot_general(pick_turned[i, block], t, NT, preferred_element_type=F32) for t in terms]
                taken.append((wide[0] + wide[1] + wide[2], tall[0] + tall[1] + tall[2]))
            lines = jnp.concatenate([t[0] for t in taken] + [t[1] for t in taken], axis=1)
            terms = [jnp.dot(t, put_columns[i], preferred_element_type=F32) for t in exact_terms(lines)]
            out_ref[i] = terms[0] + terms[1] + terms[2]

    with jax.named_scope("drain"):
        await_bytes(slab_in.at[pl.ds(0, SHARDS - 1)], share_send)

        @pl.when(own_group)
        def _():
            await_bytes(slab_in.at[pl.ds(0, SHARDS - 1)], slab_send)

        @pl.when(jnp.logical_not(own_group))
        def _():
            await_bytes(slab_in, slab_send)

        for _ in range(2):
            await_bytes(z_parts.at[pl.ds(0, 3)], part_send)
        await_bytes(y_parts, part_send)
        await_bytes(last.at[pl.ds(0, 29)], sum_send)

        @pl.when(owner_v == v)
        def _():
            await_bytes(final.at[pl.ds(0, SUBJ - 1)], final_send)

        @pl.when(owner_v != v)
        def _():
            await_bytes(final, final_send)

        for q in range(QUADS):
            near_copy(q).wait_send()
            for h in range(2):
                far_copy(h, q).wait_send()
                relay_copy(h, q).wait_send()


def body(series, offsets, selected):
    vmem = pltpu.VMEM
    dma = pltpu.SemaphoreType.DMA
    return pl.pallas_call(
        main_kernel,
        out_shape=jax.ShapeDtypeStruct((2, EP * LOCAL, ROWS), F32),
        in_specs=[
            pl.BlockSpec(memory_space=pl.ANY),
            pl.BlockSpec(memory_space=pltpu.SMEM),
            pl.BlockSpec(memory_space=pltpu.SMEM),
        ],
        out_specs=pl.BlockSpec(memory_space=pltpu.VMEM),
        scratch_shapes=[
            vmem((LOCAL, RUN, VOX), BF16),
            vmem((QUADS * 256, LOCAL * RUN), BF16),
            vmem((SUBJ, QUADS, 256, VOX), BF16),
            vmem((SUBJ, QUADS, 16, VOX), F32),
            vmem((SHARDS, 2, QUADS * 256), BF16),
            vmem((SHARDS, 2, QUADS * 256), BF16),
            vmem((2, QUADS * 256), BF16),
            vmem((SHARDS, 2, QUADS * 256), BF16),
            vmem((SUBJ * QUADS, OWN, 256), F32),
            vmem((256, 256), BF16),
            vmem((256, 256), BF16),
            vmem((SUBJ * QUADS, OWN, 256), F32),
            vmem((SUBJ * QUADS, OWN, 256), F32),
            vmem((QUADS, 256, 256), F32),
            vmem((OWN, 256, VOX), BF16),
            vmem((OWN, ROWS, 128), F32),
            vmem((4, 4, 64, 128), F32),
            vmem((4, 4, 64, 128), F32),
            vmem((OWN, 32, 128), F32),
            vmem((4, 64, 128), F32),
            vmem((4, 64, 128), F32),
            vmem((OWN, 32, 128), F32),
            vmem((32, 32, 128), F32),
            vmem((96, 128), F32),
            vmem((SUBJ, 96, 128), F32),
            vmem((2, 3, EP * LOCAL, 64), BF16),
            vmem((2, 3, EP * LOCAL, 128), BF16),
            vmem((2, 3 * 128 + ROWS, ROWS), BF16),
            dma,
            dma,
            dma,
            dma,
            dma,
            dma((QUADS,)),
            dma((QUADS,)),
            dma((2 * QUADS,)),
            dma((2 * QUADS,)),
            dma((2 * QUADS,)),
            dma((2 * QUADS,)),
            dma,
            dma((4,)),
            dma((4,)),
            dma((4,)),
            dma,
            dma,
            dma,
            dma,
        ],
        compiler_params=pltpu.CompilerParams(collective_id=0, has_side_effects=True),
    )(series, offsets, selected)


def solution(mesh):
    placed = (P("subj", None, "vox"), P(), P())
    return jax.shard_map(
        body, mesh=mesh, in_specs=placed, out_specs=P("vox", "subj", None), check_vma=False
    )
```

```python
import functools

import jax
import jax.numpy as jnp
from jax import lax
from jax.experimental import pallas as pl
from jax.experimental.pallas import tpu as pltpu
from jax.sharding import PartitionSpec as P

MESH = pl.DeviceIdType.MESH
F32, BF16, I32 = jnp.float32, jnp.bfloat16, jnp.int32
HIGH = lax.Precision.HIGHEST

SUBJ, SHARDS = 4, 32
TR, EP, RUN = 16, 12, 256
LOCAL = 4
QUADS = 3
SEL, OWN = 64, 16
VOX = 512
ROWS = SUBJ * EP * LOCAL
NT = (((1,), (1,)), ((), ()))
series_floor = 1.0
spread_floor = 0.05
shrink_factor = 0.9


def copy_to(src, dst, send_sem, recv_sem, subj, vox):
    return pltpu.make_async_remote_copy(
        src_ref=src,
        dst_ref=dst,
        send_sem=send_sem,
        recv_sem=recv_sem,
        device_id={"subj": subj, "vox": vox},
        device_id_type=MESH,
    )


def await_bytes(ref, sem):
    pltpu.make_async_copy(ref, ref, sem).wait()


def fold(x):
    return x + pltpu.roll(x, 4, 0)


def exact_terms(x):
    first = x.astype(BF16)
    rest = x - first.astype(F32)
    second = rest.astype(BF16)
    return first, second, (rest - second.astype(F32)).astype(BF16)


def line_of(group, epoch, subject):
    return group * (EP * LOCAL) + epoch * LOCAL + subject


def main_kernel(
    series_hbm,
    offsets_hbm,
    selected_hbm,
    out_ref,
    offsets,
    selected,
    series,
    choose,
    epochs,
    scale,
    slab_out,
    slab_in,
    slab_sum,
    slab,
    raw,
    lhs_hi,
    lhs_lo,
    std_hi,
    std_lo,
    corr_even,
    corr_odd,
    score,
    gram,
    z_parts,
    x_parts,
    y_parts,
    z_sums,
    x_sums,
    y_sums,
    last,
    total,
    final,
    pick_rows,
    pick_turned,
    put_columns,
    load_sem,
    slab_send,
    slab_recv,
    share_send,
    share_recv,
    near_send,
    near_recv,
    far_send,
    far_recv,
    relay_send,
    relay_recv,
    part_send,
    z_recv,
    x_recv,
    y_recv,
    sum_send,
    sum_recv,
    final_send,
    final_recv,
):
    corr = (corr_even, corr_odd)
    j = lax.axis_index("subj")
    v = lax.axis_index("vox")
    near, far = j ^ 1, j ^ 2
    z, x, y = v // 8, (v // 2) & 3, v & 1

    def ahead_of(place, step):
        return (place + step) & 3

    def shard_at(z, x, y):
        return z * 8 + x * 2 + y

    loads = [
        pltpu.make_async_copy(source, target, load_sem.at[i])
        for i, (source, target) in enumerate(
            ((offsets_hbm, offsets), (selected_hbm, selected), (series_hbm, series))
        )
    ]
    for load in loads:
        load.start()

    barrier = pltpu.get_barrier_semaphore()

    def greet(step, carry):
        for other in range(SUBJ):
            pl.semaphore_signal(
                barrier,
                inc=1,
                device_id={"subj": j ^ other, "vox": (v + step) & (SHARDS - 1)},
                device_id_type=MESH,
            )
        return carry

    with jax.named_scope("greet"):
        lax.fori_loop(1, SHARDS, greet, 0, unroll=4)
        for other in range(1, SUBJ):
            pl.semaphore_signal(barrier, inc=1, device_id={"subj": j ^ other, "vox": v}, device_id_type=MESH)

    loads[0].wait()
    loads[1].wait()

    with jax.named_scope("choose"):
        row16 = lax.broadcasted_iota(I32, (16, 128), 0)
        scan = lax.broadcasted_iota(I32, (16, LOCAL * RUN), 1)
        for q in range(QUADS):
            start = jnp.zeros((16, 128), I32)
            for r in range(16):
                first = offsets[j * LOCAL + r % 4, q * 4 + r // 4] + (r % 4) * RUN
                start = jnp.where(row16 == r, first, start)
            ahead = scan - jnp.concatenate([start] * (LOCAL * RUN // 128), axis=1)
            for t in range(TR):
                choose[pl.ds(q * 256 + t * 16, 16), :] = jnp.where(ahead == t, 1.0, 0.0).astype(BF16)

    id_rows = []
    row8 = lax.broadcasted_iota(I32, (8, 128), 0)
    for block in range(SEL // 8):
        ids = jnp.zeros((8, 128), I32)
        for r in range(8):
            place = block * 8 + r
            ids = jnp.where(row8 == r, selected[4 * (place % OWN) + place // OWN], ids)
        id_rows.append(ids)
    ids = jnp.concatenate(id_rows, axis=0)
    columns = lax.broadcasted_iota(I32, (SEL, VOX), 1) + v * VOX
    picker = jnp.where(columns == jnp.concatenate([ids] * (VOX // 128), axis=1), 1.0, 0.0).astype(BF16)

    with jax.named_scope("pick_epochs"):
        loads[2].wait()
        runs = series[...].reshape(LOCAL * RUN, VOX)
        for q in range(QUADS):
            chosen = jnp.dot(choose[pl.ds(q * 256, 256), :], runs, preferred_element_type=F32).astype(BF16)
            epochs[0, q] = chosen
            picked = lax.dot_general(picker, chosen, NT, preferred_element_type=F32)
            slab_out[:, :, pl.ds(q * 256, 256)] = picked.astype(BF16).reshape(SHARDS, 2, 256)

    with jax.named_scope("barrier"):
        pl.semaphore_wait(barrier, SUBJ * SHARDS - 1)

    def send_slab(step, carry):
        piece = (v + step) & (SHARDS - 1)
        to_j, to_v = piece // 8, j * 8 + (piece & 7)

        @pl.when(jnp.logical_or(to_j != j, to_v != v))
        def _():
            copy_to(slab_out.at[piece], slab_in.at[v], slab_send, slab_recv, to_j, to_v).start()

        return carry

    with jax.named_scope("send_slab"):
        lax.fori_loop(0, SHARDS, send_slab, 0)

    def near_copy(q):
        return copy_to(epochs.at[0, q], epochs.at[1, q], near_send.at[q], near_recv.at[q], near, v)

    def half_of(r, h, q):
        return epochs.at[r, q, :, pl.ds(h * 256, 256)]

    def far_copy(h, q):
        at = h * QUADS + q
        return copy_to(half_of(0, h, q), half_of(2, h, q), far_send.at[at], far_recv.at[at], far, v)

    def relay_copy(h, q):
        at = h * QUADS + q
        return copy_to(half_of(2, h, q), half_of(3, h, q), relay_send.at[at], relay_recv.at[at], near, v)

    def relay(h, q):
        with jax.named_scope("relay"):
            far_copy(h, q).wait_recv()
            relay_copy(h, q).start()

    for q in range(QUADS):
        near_copy(q).start()
    far_copy(0, 0).start()

    def scales(r, h):
        lanes = pl.ds(h * 256, 256)
        for q in range(QUADS):
            seen = epochs[r, q, :, lanes].astype(F32).reshape(TR, 16, 256)
            centred = seen - (jnp.sum(seen, axis=0) * (1.0 / TR))[None]
            scale[r, q, :, lanes] = lax.rsqrt(jnp.sum(centred * centred, axis=0) + series_floor)

    for h in range(2):
        scales(0, h)

    own_group = v // 8 == j

    with jax.named_scope("slab_wait"):

        @pl.when(own_group)
        def _():
            slab_in[v] = slab_out[j * 8 + (v & 7)]
            await_bytes(slab_in.at[pl.ds(0, SHARDS - 1)], slab_recv)

        @pl.when(jnp.logical_not(own_group))
        def _():
            await_bytes(slab_in, slab_recv)

    with jax.named_scope("slab_sum"):
        slab_sum[...] = jnp.sum(slab_in[...].astype(F32), axis=0).astype(BF16)

    def share_slab(step, carry):
        copy_to(slab_sum, slab.at[v], share_send, share_recv, j, (v + step) & (SHARDS - 1)).start()
        return carry

    with jax.named_scope("share_slab"):
        lax.fori_loop(1, SHARDS, share_slab, 0)
        slab[v] = slab_sum[...]

    far_copy(0, 1).start()
    far_copy(0, 2).start()
    for q in range(QUADS):
        far_copy(1, q).start()

    with jax.named_scope("places"):
        b = lax.broadcasted_iota(I32, (1, ROWS), 1)
        p = lax.broadcasted_iota(I32, (EP * LOCAL, 1), 0)
        for i in range(2):
            taker = y * 2 + i
            s = b // EP
            to = line_of((s // LOCAL) ^ taker, b - s * EP, s & 3)
            s = p // EP
            line = line_of(j ^ taker, p - s * EP, s)
            c = lax.broadcasted_iota(I32, (ROWS, 1), 0)
            put_columns[i, pl.ds(3 * 128, ROWS), :] = jnp.where(c == to, 1.0, 0.0).astype(BF16)
            for block in range(3):
                c = lax.broadcasted_iota(I32, (128, 1), 0) + block * 64
                c = jnp.where(c < ROWS, c, c - ROWS)
                weight = jnp.where(lax.broadcasted_iota(I32, (128, ROWS), 0) < 64, 0.5, 1.0)
                put_columns[i, pl.ds(block * 128, 128), :] = jnp.where(c == to, weight, 0.0).astype(BF16)
                c = lax.broadcasted_iota(I32, (1, 128), 1) + block * 64
                c = jnp.where(c < ROWS, c, c - ROWS)
                weight = jnp.where(lax.broadcasted_iota(I32, (EP * LOCAL, 128), 1) < 64, 0.5, 1.0)
                pick_turned[i, block] = jnp.where(c == line, weight, 0.0).astype(BF16)
                c = lax.broadcasted_iota(I32, (1, 64), 1) + block * 64
                pick_rows[i, block] = jnp.where(c == line, 1.0, 0.0).astype(BF16)

    with jax.named_scope("near_wait"):
        for q in range(QUADS):
            near_copy(q).wait_recv()
    for h in range(2):
        scales(1, h)

    relay(0, 0)
    relay(0, 1)
    with jax.named_scope("share_wait"):
        await_bytes(slab.at[pl.ds(0, SHARDS - 1)], share_recv)

    with jax.named_scope("standard_slab"):
        for r in range(SUBJ):
            group = (j ^ r) if r else j
            for kk in range(8):
                for q in range(QUADS):
                    raw[r * QUADS + q, pl.ds(kk * 2, 2), :] = slab[group * 8 + kk, :, pl.ds(q * 256, 256)].astype(F32)
        seen = raw[...].reshape(SUBJ * QUADS * OWN, 256)
        same = jnp.where(
            (lax.broadcasted_iota(I32, (256, 256), 0) & 15) == (lax.broadcasted_iota(I32, (256, 256), 1) & 15), 1.0, 0.0
        ).astype(BF16)
        centred = seen - jnp.dot(seen.astype(BF16), same, preferred_element_type=F32) * (1.0 / TR)
        terms = exact_terms(centred * centred)
        spread = [jnp.dot(t, same, preferred_element_type=F32) for t in terms]
        spread = spread[0] + spread[1] + spread[2]
        x_std = centred * lax.rsqrt(spread + series_floor) * shrink_factor
        x_hi = x_std.astype(BF16).astype(F32)
        std_hi[...] = x_hi.reshape(SUBJ * QUADS, OWN, 256)
        std_lo[...] = (x_std - x_hi).reshape(SUBJ * QUADS, OWN, 256)

    own_row = (lax.broadcasted_iota(I32, (16, 256), 1) & 15) == lax.broadcasted_iota(I32, (16, 256), 0)

    units = ((0, 0), (0, 1), (1, 0), (1, 1), (2, 0), (3, 0), (2, 1), (3, 1))

    def correlate(unit):
        r, h = units[unit]
        lanes = pl.ds(h * 256, 256)
        if r >= 2:
            scales(r, h)
        for q in range(QUADS):
            at = r * QUADS + q
            if h == 0:
                for k in range(OWN):
                    for std, lhs in ((std_hi, lhs_hi), (std_lo, lhs_lo)):
                        line = jnp.broadcast_to(std[at, pl.ds(k, 1), :], (16, 256))
                        lhs[at, pl.ds(k * 16, 16), :] = jnp.where(own_row, line, 0.0).astype(BF16)
            seen = epochs[r, q, :, lanes]
            corr[unit % 2][q] = jnp.dot(lhs_hi[at], seen, preferred_element_type=F32) + jnp.dot(
                lhs_lo[at], seen, preferred_element_type=F32
            )

    def standard(unit):
        r, h = units[unit]
        lanes = pl.ds(h * 256, 256)
        for k in range(OWN):
            halves = []
            for q in range(QUADS):
                shrunk = corr[unit % 2][q, pl.ds(k * 16, 16), :] * scale[r, q, :, lanes]
                twice = jnp.log(1.0 + shrunk) - jnp.log(1.0 - shrunk)
                halves += [twice[0:8], twice[8:16]]
            mean = fold(functools.reduce(jnp.add, halves)) * (1.0 / EP)
            halves = [f - mean for f in halves]
            spread = fold(functools.reduce(jnp.add, [f * f for f in halves])) * (1.0 / EP)
            gain = lax.rsqrt(spread + 4.0 * spread_floor)
            for q in range(QUADS):
                both = jnp.concatenate([halves[2 * q] * gain, halves[2 * q + 1] * gain], axis=0).astype(BF16)
                at = r * 48 + q * 16
                score[k, pl.ds(at, 16), lanes] = both
                if at < 64:
                    score[k, pl.ds(ROWS + at, 16), lanes] = both

    before = {
        1: lambda: relay(0, 2),
        2: lambda: relay(1, 0),
        4: lambda: relay(1, 1),
        5: lambda: [relay_copy(0, q).wait_recv() for q in range(QUADS)],
        6: lambda: relay(1, 2),
        7: lambda: [relay_copy(1, q).wait_recv() for q in range(QUADS)],
    }
    with jax.named_scope("scores"):
        correlate(0)
    for unit in range(1, len(units) + 1):
        if unit in before:
            before[unit]()
        with jax.named_scope("scores"):
            if unit < len(units):
                correlate(unit)
            standard(unit - 1)

    def block_of(m, block):
        gram[m, pl.ds(block * 64, 64), :] = lax.dot_general(
            score[m, pl.ds(block * 64, 64), :], score[m, pl.ds(block * 64, 128), :], NT, preferred_element_type=F32
        )

    def kernels(pair, carry):
        steps = []
        for step in (pair * 2, pair * 2 + 1):
            major, minor = step // 4, step & 3
            by_z = ahead_of(z, minor) * 4 + ahead_of(x, major)
            by_x = ahead_of(z, major) * 4 + ahead_of(x, minor)
            steps.append((step, major, minor, by_z, by_x))
        for _, _, _, by_z, by_x in steps:
            block_of(by_z, 0)
            block_of(by_x, 1)
            block_of(by_x, 2)
        for step, major, minor, by_z, by_x in steps:

            @pl.when(minor > 0)
            def _():
                to_v = shard_at(ahead_of(z, minor), x, y)
                copy_to(gram.at[by_z, pl.ds(0, 64)], z_parts.at[major, minor], part_send, z_recv.at[major], j, to_v).start()
                to_v = shard_at(z, ahead_of(x, minor), y)
                copy_to(gram.at[by_x, pl.ds(64, 64)], x_parts.at[major, minor], part_send, x_recv.at[major], j, to_v).start()

            rows = pl.ds(pl.multiple_of(128 + 32 * (y ^ 1), 32), 32)
            copy_to(gram.at[by_x, rows], y_parts.at[step], part_send, y_recv.at[major], j, v ^ 1).start()
        return carry

    with jax.named_scope("kernels"):
        lax.fori_loop(0, OWN // 2, kernels, 0)

    for major in range(4):
        for block, parts, recv, sums in ((0, z_parts, z_recv, z_sums), (1, x_parts, x_recv, x_sums)):
            with jax.named_scope("part_wait"):
                await_bytes(parts.at[major, pl.ds(1, 3)], recv.at[major])
            own = (ahead_of(z, major) * 4 + x) if block else (z * 4 + ahead_of(x, major))
            own = gram[own, pl.ds(block * 64, 64), :]
            sums[major] = (own + parts[major, 1]) + (parts[major, 2] + parts[major, 3])
            for other in range(2):
                side = y ^ other
                rows = pl.ds(pl.multiple_of(side * 32, 32), 32)
                slot = major * 2 + other
                to_v = shard_at(ahead_of(z, major), x, side) if block else shard_at(z, ahead_of(x, major), side)
                if slot:
                    copy_to(sums.at[major, rows], last.at[block * 8 + slot], sum_send, sum_recv, j, to_v).start()
                else:
                    last[block * 8] = sums[0, rows, :]
        with jax.named_scope("part_wait"):
            await_bytes(y_parts.at[pl.ds(major * 4, 4)], y_recv.at[major])
        for minor in range(4):
            step = major * 4 + minor
            to_z, to_x = ahead_of(z, major), ahead_of(x, minor)
            rows = pl.ds(pl.multiple_of(128 + 32 * y, 32), 32)
            added = y_parts[step] + gram[to_z * 4 + to_x, rows, :]
            if step:
                y_sums[step] = added
                copy_to(y_sums.at[step], last.at[16 + step], sum_send, sum_recv, j, shard_at(to_z, to_x, y)).start()
            else:
                last[16] = added

    with jax.named_scope("last_wait"):
        await_bytes(last.at[pl.ds(0, 29)], sum_recv)

    mean = 1.0 / (VOX * SHARDS)
    total[0:32, :] = jnp.sum(last[0:8], axis=0) * mean
    total[32:64, :] = jnp.sum(last[8:16], axis=0) * mean
    total[64:96, :] = jnp.sum(last[16:32], axis=0) * mean

    owner_v = v - y + j // 2
    place = (j & 1) * 2 + y
    with jax.named_scope("final"):
        for other in range(SUBJ):
            to_j = (j ^ other) if other else j
            if other:
                copy_to(total, final.at[place], final_send, final_recv, to_j, owner_v).start()
            else:

                @pl.when(owner_v != v)
                def _():
                    copy_to(total, final.at[place], final_send, final_recv, j, owner_v).start()

        @pl.when(owner_v == v)
        def _():
            final[place] = total[...]
            await_bytes(final.at[pl.ds(0, SUBJ - 1)], final_recv)

        @pl.when(owner_v != v)
        def _():
            await_bytes(final, final_recv)

    with jax.named_scope("place"):
        for i in range(2):
            taken = []
            for block in range(3):
                rows = pl.ds(block * 32, 32)
                terms = exact_terms(jnp.concatenate([final[2 * i, rows, :], final[2 * i + 1, rows, :]], axis=0))
                wide = [jnp.dot(pick_rows[i, block], t, preferred_element_type=F32) for t in terms]
                tall = [lax.dot_general(pick_turned[i, block], t, NT, preferred_element_type=F32) for t in terms]
                taken.append((wide[0] + wide[1] + wide[2], tall[0] + tall[1] + tall[2]))
            lines = jnp.concatenate([t[0] for t in taken] + [t[1] for t in taken], axis=1)
            terms = [jnp.dot(t, put_columns[i], preferred_element_type=F32) for t in exact_terms(lines)]
            out_ref[i] = terms[0] + terms[1] + terms[2]

    with jax.named_scope("drain"):
        await_bytes(slab_in.at[pl.ds(0, SHARDS - 1)], share_send)

        @pl.when(own_group)
        def _():
            await_bytes(slab_in.at[pl.ds(0, SHARDS - 1)], slab_send)

        @pl.when(jnp.logical_not(own_group))
        def _():
            await_bytes(slab_in, slab_send)

        for _ in range(2):
            await_bytes(z_parts.at[pl.ds(0, 3)], part_send)
        await_bytes(y_parts, part_send)
        await_bytes(last.at[pl.ds(0, 29)], sum_send)

        @pl.when(owner_v == v)
        def _():
            await_bytes(final.at[pl.ds(0, SUBJ - 1)], final_send)

        @pl.when(owner_v != v)
        def _():
            await_bytes(final, final_send)

        for q in range(QUADS):
            near_copy(q).wait_send()
            for h in range(2):
                far_copy(h, q).wait_send()
                relay_copy(h, q).wait_send()


def body(series, offsets, selected):
    vmem = pltpu.VMEM
    dma = pltpu.SemaphoreType.DMA
    return pl.pallas_call(
        main_kernel,
        out_shape=jax.ShapeDtypeStruct((2, EP * LOCAL, ROWS), F32),
        in_specs=[
            pl.BlockSpec(memory_space=pl.ANY),
            pl.BlockSpec(memory_space=pl.ANY),
            pl.BlockSpec(memory_space=pl.ANY),
        ],
        out_specs=pl.BlockSpec(memory_space=pltpu.VMEM),
        scratch_shapes=[
            pltpu.SMEM((SUBJ * LOCAL, EP), I32),
            pltpu.SMEM((SEL,), I32),
            vmem((LOCAL, RUN, VOX), BF16),
            vmem((QUADS * 256, LOCAL * RUN), BF16),
            vmem((SUBJ, QUADS, 256, VOX), BF16),
            vmem((SUBJ, QUADS, 16, VOX), F32),
            vmem((SHARDS, 2, QUADS * 256), BF16),
            vmem((SHARDS, 2, QUADS * 256), BF16),
            vmem((2, QUADS * 256), BF16),
            vmem((SHARDS, 2, QUADS * 256), BF16),
            vmem((SUBJ * QUADS, OWN, 256), F32),
            vmem((SUBJ * QUADS, 256, 256), BF16),
            vmem((SUBJ * QUADS, 256, 256), BF16),
            vmem((SUBJ * QUADS, OWN, 256), F32),
            vmem((SUBJ * QUADS, OWN, 256), F32),
            vmem((QUADS, 256, 256), F32),
            vmem((QUADS, 256, 256), F32),
            vmem((OWN, 256, VOX), BF16),
            vmem((OWN, ROWS, 128), F32),
            vmem((4, 4, 64, 128), F32),
            vmem((4, 4, 64, 128), F32),
            vmem((OWN, 32, 128), F32),
            vmem((4, 64, 128), F32),
            vmem((4, 64, 128), F32),
            vmem((OWN, 32, 128), F32),
            vmem((32, 32, 128), F32),
            vmem((96, 128), F32),
            vmem((SUBJ, 96, 128), F32),
            vmem((2, 3, EP * LOCAL, 64), BF16),
            vmem((2, 3, EP * LOCAL, 128), BF16),
            vmem((2, 3 * 128 + ROWS, ROWS), BF16),
            dma((3,)),
            dma,
            dma,
            dma,
            dma,
            dma((QUADS,)),
            dma((QUADS,)),
            dma((2 * QUADS,)),
            dma((2 * QUADS,)),
            dma((2 * QUADS,)),
            dma((2 * QUADS,)),
            dma,
            dma((4,)),
            dma((4,)),
            dma((4,)),
            dma,
            dma,
            dma,
            dma,
        ],
        compiler_params=pltpu.CompilerParams(collective_id=0, has_side_effects=True),
    )(series, offsets, selected)


def solution(mesh):
    placed = (P("subj", None, "vox"), P(), P())
    return jax.shard_map(
        body, mesh=mesh, in_specs=placed, out_specs=P("vox", "subj", None), check_vma=False
    )
```

```python
import functools

import jax
import jax.numpy as jnp
from jax import lax
from jax.experimental import pallas as pl
from jax.experimental.pallas import tpu as pltpu
from jax.sharding import PartitionSpec as P

MESH = pl.DeviceIdType.MESH
F32, BF16, I32 = jnp.float32, jnp.bfloat16, jnp.int32
HIGH = lax.Precision.HIGHEST

SUBJ, SHARDS = 4, 32
TR, EP, RUN = 16, 12, 256
LOCAL = 4
QUADS = 3
SEL, OWN = 64, 16
VOX = 512
ROWS = SUBJ * EP * LOCAL
NT = (((1,), (1,)), ((), ()))
series_floor = 1.0
spread_floor = 0.05
shrink_factor = 0.9


def copy_to(src, dst, send_sem, recv_sem, subj, vox):
    return pltpu.make_async_remote_copy(
        src_ref=src,
        dst_ref=dst,
        send_sem=send_sem,
        recv_sem=recv_sem,
        device_id={"subj": subj, "vox": vox},
        device_id_type=MESH,
    )


def await_bytes(ref, sem):
    pltpu.make_async_copy(ref, ref, sem).wait()


def fold(x):
    return x + pltpu.roll(x, 4, 0)


def exact_terms(x):
    first = x.astype(BF16)
    rest = x - first.astype(F32)
    second = rest.astype(BF16)
    return first, second, (rest - second.astype(F32)).astype(BF16)


def slot_of(group, taker):
    return jnp.where((group ^ taker) < 2, group ^ taker, 2 + (group & 1))


def line_of(slot, epoch, subject):
    return slot * (EP * LOCAL) + epoch * LOCAL + subject


def main_kernel(
    series_hbm,
    offsets_hbm,
    selected_hbm,
    out_ref,
    offsets,
    selected,
    series,
    choose,
    epochs,
    scale,
    slab_out,
    slab_in,
    slab_sum,
    slab,
    raw,
    lhs_hi,
    lhs_lo,
    std_hi,
    std_lo,
    corr_even,
    corr_odd,
    score,
    gram,
    z_parts_first,
    z_parts_second,
    x_parts_first,
    x_parts_second,
    y_parts,
    z_sums_first,
    z_sums_second,
    x_sums_first,
    x_sums_second,
    y_sums,
    last_first,
    last_second,
    total,
    final,
    pick_rows,
    pick_turned,
    put_columns,
    load_sem,
    slab_send,
    slab_recv,
    share_send,
    share_recv,
    near_send,
    near_recv,
    far_send,
    far_recv,
    relay_send,
    relay_recv,
    part_send,
    z_recv,
    x_recv,
    y_recv,
    sum_send,
    sum_recv,
    final_send,
    final_recv,
):
    corr = (corr_even, corr_odd)
    z_parts = (z_parts_first, z_parts_second)
    x_parts = (x_parts_first, x_parts_second)
    z_sums = (z_sums_first, z_sums_second)
    x_sums = (x_sums_first, x_sums_second)
    last = (last_first, last_second)
    j = lax.axis_index("subj")
    v = lax.axis_index("vox")
    near, far, core = j ^ 1, j ^ 2, j & 1
    z, x, y = v // 8, (v // 2) & 3, v & 1

    def ahead_of(place, step):
        return (place + step) & 3

    def shard_at(z, x, y):
        return z * 8 + x * 2 + y

    loads = [
        pltpu.make_async_copy(source, target, load_sem.at[i])
        for i, (source, target) in enumerate(
            ((offsets_hbm, offsets), (selected_hbm, selected), (series_hbm, series))
        )
    ]
    for load in loads:
        load.start()

    barrier = pltpu.get_barrier_semaphore()

    def greet(step, carry):
        for other in range(SUBJ):
            pl.semaphore_signal(
                barrier,
                inc=1,
                device_id={"subj": j ^ other, "vox": (v + step) & (SHARDS - 1)},
                device_id_type=MESH,
            )
        return carry

    with jax.named_scope("greet"):
        lax.fori_loop(1, SHARDS, greet, 0, unroll=4)
        for other in range(1, SUBJ):
            pl.semaphore_signal(barrier, inc=1, device_id={"subj": j ^ other, "vox": v}, device_id_type=MESH)

    loads[0].wait()
    loads[1].wait()

    with jax.named_scope("choose"):
        row16 = lax.broadcasted_iota(I32, (16, 128), 0)
        scan = lax.broadcasted_iota(I32, (16, LOCAL * RUN), 1)
        for q in range(QUADS):
            start = jnp.zeros((16, 128), I32)
            for r in range(16):
                first = offsets[j * LOCAL + r % 4, q * 4 + r // 4] + (r % 4) * RUN
                start = jnp.where(row16 == r, first, start)
            ahead = scan - jnp.concatenate([start] * (LOCAL * RUN // 128), axis=1)
            for t in range(TR):
                choose[pl.ds(q * 256 + t * 16, 16), :] = jnp.where(ahead == t, 1.0, 0.0).astype(BF16)

    id_rows = []
    row8 = lax.broadcasted_iota(I32, (8, 128), 0)
    for block in range(SEL // 8):
        ids = jnp.zeros((8, 128), I32)
        for r in range(8):
            place = block * 8 + r
            ids = jnp.where(row8 == r, selected[4 * (place % OWN) + place // OWN], ids)
        id_rows.append(ids)
    ids = jnp.concatenate(id_rows, axis=0)
    columns = lax.broadcasted_iota(I32, (SEL, VOX), 1) + v * VOX
    picker = jnp.where(columns == jnp.concatenate([ids] * (VOX // 128), axis=1), 1.0, 0.0).astype(BF16)

    with jax.named_scope("pick_epochs"):
        loads[2].wait()
        runs = series[...].reshape(LOCAL * RUN, VOX)
        for q in range(QUADS):
            chosen = jnp.dot(choose[pl.ds(q * 256, 256), :], runs, preferred_element_type=F32).astype(BF16)
            epochs[0, q] = chosen
            picked = lax.dot_general(picker, chosen, NT, preferred_element_type=F32)
            slab_out[:, :, pl.ds(q * 256, 256)] = picked.astype(BF16).reshape(SHARDS, 2, 256)

    with jax.named_scope("barrier"):
        pl.semaphore_wait(barrier, SUBJ * SHARDS - 1)

    def send_slab(step, carry):
        piece = (v + step) & (SHARDS - 1)
        to_j, to_v = piece // 8, j * 8 + (piece & 7)

        @pl.when(jnp.logical_or(to_j != j, to_v != v))
        def _():
            copy_to(slab_out.at[piece], slab_in.at[v], slab_send, slab_recv, to_j, to_v).start()

        return carry

    with jax.named_scope("send_slab"):
        lax.fori_loop(0, SHARDS, send_slab, 0)

    def near_copy(q):
        return copy_to(epochs.at[0, q], epochs.at[1, q], near_send.at[q], near_recv.at[q], near, v)

    half = pl.ds(pl.multiple_of(core * 256, 256), 256)

    def far_copy(g, q):
        at = g * QUADS + q
        source, target = epochs.at[core ^ g, q, :, half], epochs.at[2 + g, q, :, half]
        return copy_to(source, target, far_send.at[at], far_recv.at[at], far, v)

    def relay_copy(g, q):
        at = g * QUADS + q
        ref = epochs.at[2 + g, q, :, half]
        return copy_to(ref, ref, relay_send.at[at], relay_recv.at[at], near, v)

    def relay(g, q):
        with jax.named_scope("relay"):
            far_copy(g, q).wait_recv()
            relay_copy(g, q).start()

    for q in range(QUADS):
        near_copy(q).start()

    @pl.when(core == 0)
    def _():
        far_copy(0, 0).start()

    def scales(r, h):
        lanes = pl.ds(h * 256, 256)
        for q in range(QUADS):
            seen = epochs[r, q, :, lanes].astype(F32).reshape(TR, 16, 256)
            centred = seen - (jnp.sum(seen, axis=0) * (1.0 / TR))[None]
            scale[r, q, :, lanes] = lax.rsqrt(jnp.sum(centred * centred, axis=0) + series_floor)

    for h in range(2):
        scales(0, h)

    with jax.named_scope("near_wait"):
        for q in range(QUADS):
            near_copy(q).wait_recv()

    @pl.when(core == 1)
    def _():
        far_copy(0, 0).start()

    far_copy(0, 1).start()

    own_group = v // 8 == j

    with jax.named_scope("slab_wait"):

        @pl.when(own_group)
        def _():
            slab_in[v] = slab_out[j * 8 + (v & 7)]
            await_bytes(slab_in.at[pl.ds(0, SHARDS - 1)], slab_recv)

        @pl.when(jnp.logical_not(own_group))
        def _():
            await_bytes(slab_in, slab_recv)

    with jax.named_scope("slab_sum"):
        slab_sum[...] = jnp.sum(slab_in[...].astype(F32), axis=0).astype(BF16)

    def share_slab(step, carry):
        copy_to(slab_sum, slab.at[v], share_send, share_recv, j, (v + step) & (SHARDS - 1)).start()
        return carry

    with jax.named_scope("share_slab"):
        lax.fori_loop(1, SHARDS, share_slab, 0)
        slab[v] = slab_sum[...]

    far_copy(0, 2).start()
    for q in range(QUADS):
        far_copy(1, q).start()

    with jax.named_scope("places"):
        b = lax.broadcasted_iota(I32, (1, ROWS), 1)
        p = lax.broadcasted_iota(I32, (EP * LOCAL, 1), 0)
        for i in range(2):
            taker = y * 2 + i
            s = b // EP
            to = line_of(slot_of(s // LOCAL, taker), b - s * EP, s & 3)
            s = p // EP
            line = line_of(slot_of(j, taker), p - s * EP, s)

            def put(first, rows, lines):
                put_columns[i, pl.ds(first, rows), :] = jnp.where(lines == to, 1.0, 0.0).astype(BF16)

            across = lax.broadcasted_iota(I32, (1, 128), 1)
            down = lax.broadcasted_iota(I32, (128, 1), 0)
            for n in range(2):
                put(n * 256, 128, down)
                put(n * 256 + 128, 128, (down & 63) + (n + 1) * 64)
                put(512 + n * 64, 64, lax.broadcasted_iota(I32, (64, 1), 0) + n * 128)
                rows = lax.broadcasted_iota(I32, (1, 64), 1)
                pick_rows[i, 2 * n] = jnp.where(rows + n * 128 == line, 1.0, 0.0).astype(BF16)
                pick_rows[i, 2 * n + 1] = jnp.where(rows + (n + 1) * 64 == line, 1.0, 0.0).astype(BF16)
                turned = across if n else jnp.where(across < 64, -1, across)
                pick_turned[i, n] = jnp.where(turned == line, 1.0, 0.0).astype(BF16)

    for h in range(2):
        scales(1, h)

    relay(0, 0)
    relay(0, 1)
    with jax.named_scope("share_wait"):
        await_bytes(slab.at[pl.ds(0, SHARDS - 1)], share_recv)

    with jax.named_scope("standard_slab"):
        for r in range(SUBJ):
            group = (j, near, far & 2, far | 1)[r]
            for kk in range(8):
                for q in range(QUADS):
                    raw[r * QUADS + q, pl.ds(kk * 2, 2), :] = slab[group * 8 + kk, :, pl.ds(q * 256, 256)].astype(F32)
        seen = raw[...].reshape(SUBJ * QUADS * OWN, 256)
        same = jnp.where(
            (lax.broadcasted_iota(I32, (256, 256), 0) & 15) == (lax.broadcasted_iota(I32, (256, 256), 1) & 15), 1.0, 0.0
        ).astype(BF16)
        centred = seen - jnp.dot(seen.astype(BF16), same, preferred_element_type=F32) * (1.0 / TR)
        terms = exact_terms(centred * centred)
        spread = [jnp.dot(t, same, preferred_element_type=F32) for t in terms]
        spread = spread[0] + spread[1] + spread[2]
        x_std = centred * lax.rsqrt(spread + series_floor) * shrink_factor
        x_hi = x_std.astype(BF16).astype(F32)
        std_hi[...] = x_hi.reshape(SUBJ * QUADS, OWN, 256)
        std_lo[...] = (x_std - x_hi).reshape(SUBJ * QUADS, OWN, 256)

    own_row = (lax.broadcasted_iota(I32, (16, 256), 1) & 15) == lax.broadcasted_iota(I32, (16, 256), 0)

    units = ((0, 0), (0, 1), (1, 0), (1, 1), (2, 0), (2, 1), (3, 0), (3, 1))

    def correlate(unit):
        r, h = units[unit]
        lanes = pl.ds(h * 256, 256)
        if r >= 2:
            scales(r, h)
        for q in range(QUADS):
            at = r * QUADS + q
            if h == 0:
                for k in range(OWN):
                    for std, lhs in ((std_hi, lhs_hi), (std_lo, lhs_lo)):
                        line = jnp.broadcast_to(std[at, pl.ds(k, 1), :], (16, 256))
                        lhs[at, pl.ds(k * 16, 16), :] = jnp.where(own_row, line, 0.0).astype(BF16)
            seen = epochs[r, q, :, lanes]
            corr[unit % 2][q] = jnp.dot(lhs_hi[at], seen, preferred_element_type=F32) + jnp.dot(
                lhs_lo[at], seen, preferred_element_type=F32
            )

    def standard(unit):
        r, h = units[unit]
        lanes = pl.ds(h * 256, 256)
        for k in range(OWN):
            halves = []
            for q in range(QUADS):
                shrunk = corr[unit % 2][q, pl.ds(k * 16, 16), :] * scale[r, q, :, lanes]
                twice = jnp.log(1.0 + shrunk) - jnp.log(1.0 - shrunk)
                halves += [twice[0:8], twice[8:16]]
            mean = fold(functools.reduce(jnp.add, halves)) * (1.0 / EP)
            halves = [f - mean for f in halves]
            spread = fold(functools.reduce(jnp.add, [f * f for f in halves])) * (1.0 / EP)
            gain = lax.rsqrt(spread + 4.0 * spread_floor)
            for q in range(QUADS):
                both = jnp.concatenate([halves[2 * q] * gain, halves[2 * q + 1] * gain], axis=0).astype(BF16)
                at = r * 48 + q * 16
                score[k, pl.ds(at, 16), lanes] = both

    split = ((48, 48, 0), (32, 32, 32))

    def block_of(n, m):
        top = pl.ds(n * 128, 64)
        gram[n, m, 0:64, :] = lax.dot_general(
            score[m, top, :], score[m, pl.ds(0, 128), :], NT, preferred_element_type=F32
        )
        rows = score[m, pl.ds((n + 1) * 64, 64), :]
        square = lax.dot_general(rows, rows, NT, preferred_element_type=F32)
        gram[n, m, 64:96, :] = jnp.concatenate([square[0:32], square[32:64]], axis=1)

    def kernels(n):
        z_rows, x_rows, y_rows = split[n]

        def pair(index, carry):
            for step in (index * 2, index * 2 + 1):
                block_of(n, ahead_of(z, step // 4) * 4 + ahead_of(x, step & 3))
            for step in (index * 2, index * 2 + 1):
                major, minor = step // 4, step & 3
                m = ahead_of(z, major) * 4 + ahead_of(x, minor)

                @pl.when(major > 0)
                def _():
                    source = gram.at[n, m, pl.ds(0, z_rows)]
                    to_v = shard_at(ahead_of(z, major), x, y)
                    copy_to(source, z_parts[n].at[minor, major], part_send.at[n], z_recv.at[n, minor], j, to_v).start()

                @pl.when(minor > 0)
                def _():
                    source = gram.at[n, m, pl.ds(z_rows, x_rows)]
                    to_v = shard_at(z, ahead_of(x, minor), y)
                    copy_to(source, x_parts[n].at[major, minor], part_send.at[n], x_recv.at[n, major], j, to_v).start()

                if y_rows:
                    rows = pl.ds(pl.multiple_of(z_rows + x_rows + y_rows // 2 * (y ^ 1), 8), y_rows // 2)
                    copy_to(
                        gram.at[n, m, rows], y_parts.at[step], part_send.at[n], y_recv.at[major], j, v ^ 1
                    ).start()
            return carry

        with jax.named_scope("kernels"):
            lax.fori_loop(0, OWN // 2, pair, 0)

    def second_sums(n):
        z_rows, x_rows, y_rows = split[n]

        def along(step, block):
            parts, recv, sums = ((z_parts, z_recv, z_sums), (x_parts, x_recv, x_sums))[block]
            with jax.named_scope("part_wait"):
                await_bytes(parts[n].at[step, pl.ds(1, 3)], recv.at[n, step])
            own = (ahead_of(z, step) * 4 + x) if block else (z * 4 + ahead_of(x, step))
            own = gram[n, own, pl.ds(z_rows, x_rows) if block else pl.ds(0, z_rows), :]
            sums[n][step] = (own + parts[n][step, 1]) + (parts[n][step, 2] + parts[n][step, 3])
            for other in range(2):
                side = y ^ other
                count = (z_rows, x_rows)[block] // 2
                rows = pl.ds(pl.multiple_of(side * count, 8), count)
                slot = step * 2 + other
                to_v = shard_at(ahead_of(z, step), x, side) if block else shard_at(z, ahead_of(x, step), side)
                if slot:
                    copy_to(
                        sums[n].at[step, rows], last[n].at[block * 8 + slot], sum_send.at[n], sum_recv.at[n], j, to_v
                    ).start()
                else:
                    last[n][block * 8] = sums[n][0, rows, :]

        def from_side(major):
            with jax.named_scope("part_wait"):
                await_bytes(y_parts.at[pl.ds(major * 4, 4)], y_recv.at[major])
            for minor in range(4):
                step = major * 4 + minor
                to_z, to_x = ahead_of(z, major), ahead_of(x, minor)
                rows = pl.ds(pl.multiple_of(z_rows + x_rows + y_rows // 2 * y, 8), y_rows // 2)
                added = y_parts[step] + gram[n, to_z * 4 + to_x, rows, :]
                if step:
                    y_sums[step] = added
                    copy_to(
                        y_sums.at[step], last[n].at[16 + step], sum_send.at[n], sum_recv.at[n], j, shard_at(to_z, to_x, y)
                    ).start()
                else:
                    last[n][16] = added

        if y_rows:
            for major in range(4):
                along(major, 1)
                from_side(major)
            for step in range(4):
                along(step, 0)
        else:
            for step in range(4):
                along(step, 1)
            for step in range(4):
                along(step, 0)

    owner_v = v - y + j // 2
    place = core * 2 + y
    remote_sums = (14, 29)

    def hand_over(n):
        with jax.named_scope("last_wait"):
            await_bytes(last[n].at[pl.ds(0, remote_sums[n])], sum_recv.at[n])
        mean = 1.0 / (VOX * SHARDS)
        first = 0
        for block, rows in enumerate(split[n]):
            if rows:
                slots = last[n][block * 8 : (block + (2 if block == 2 else 1)) * 8]
                total[n, pl.ds(first, rows // 2), :] = jnp.sum(slots, axis=0) * mean
                first += rows // 2
        for other in range(SUBJ):
            copy = copy_to(
                total.at[n], final.at[n, place], final_send.at[n], final_recv.at[n], (j ^ other) if other else j, owner_v
            )
            if other:
                copy.start()
            else:

                @pl.when(owner_v != v)
                def _():
                    copy.start()

        @pl.when(owner_v == v)
        def _():
            final[n, place] = total[n]

    def await_final(n, sem):
        @pl.when(owner_v == v)
        def _():
            await_bytes(final.at[n, pl.ds(0, SUBJ - 1)], sem.at[n])

        @pl.when(owner_v != v)
        def _():
            await_bytes(final.at[n], sem.at[n])

    def scores_of(correlated, finished):
        with jax.named_scope("scores"):
            if correlated is not None:
                correlate(correlated)
            if finished is not None:
                standard(finished)

    def relayed(g):
        with jax.named_scope("relay_wait"):
            for q in range(QUADS):
                relay_copy(g, q).wait_recv()

    scores_of(0, None)
    scores_of(1, 0)
    relay(0, 2)
    scores_of(2, 1)
    scores_of(3, 2)
    relayed(0)
    scores_of(4, 3)
    scores_of(5, 4)
    scores_of(None, 5)
    relay(1, 0)
    kernels(0)
    relay(1, 1)
    relay(1, 2)
    relayed(1)
    scores_of(6, None)
    scores_of(7, 6)
    scores_of(None, 7)
    kernels(1)
    second_sums(0)
    second_sums(1)
    hand_over(0)
    hand_over(1)
    with jax.named_scope("final"):
        await_final(0, final_recv)
        await_final(1, final_recv)

    with jax.named_scope("place"):
        beside = lax.broadcasted_iota(I32, (EP * LOCAL, 128), 1) < 64

        def picked_by(pick, terms, dims):
            parts = [lax.dot_general(pick, t, dims, preferred_element_type=F32) for t in terms]
            return parts[0] + parts[1] + parts[2]

        for i in range(2):
            lines, turned = [], []
            for n in range(2):
                pieces, first = [], 0
                for rows in split[n]:
                    if rows:
                        here = pl.ds(first, rows // 2)
                        pieces += [final[n, 2 * i, here, :], final[n, 2 * i + 1, here, :]]
                        first += rows // 2
                both = jnp.concatenate(pieces, axis=0)
                wide, square = exact_terms(both[0:64]), exact_terms(both[64:96])
                lines.append(picked_by(pick_rows[i, 2 * n], wide, (((1,), (0,)), ((), ()))))
                halves = [
                    picked_by(pick_rows[i, 2 * n + 1, :, h * 32 : h * 32 + 32], square, (((1,), (0,)), ((), ())))
                    for h in range(2)
                ]
                lines.append(jnp.where(beside, halves[0], halves[1]))
                turned.append(picked_by(pick_turned[i, n], wide, NT))
            lines = jnp.concatenate(lines + turned, axis=1)
            terms = [jnp.dot(t, put_columns[i], preferred_element_type=F32) for t in exact_terms(lines)]
            out_ref[i] = terms[0] + terms[1] + terms[2]

    with jax.named_scope("drain"):
        await_bytes(slab_in.at[pl.ds(0, SHARDS - 1)], share_send)

        @pl.when(own_group)
        def _():
            await_bytes(slab_in.at[pl.ds(0, SHARDS - 1)], slab_send)

        @pl.when(jnp.logical_not(own_group))
        def _():
            await_bytes(slab_in, slab_send)

        for n in range(2):
            await_bytes(z_parts[n].at[pl.ds(0, 3)], part_send.at[n])
            await_bytes(x_parts[n].at[pl.ds(0, 3)], part_send.at[n])
            await_bytes(last[n].at[pl.ds(0, remote_sums[n])], sum_send.at[n])
            await_final(n, final_send)
        await_bytes(y_parts, part_send.at[1])
        for q in range(QUADS):
            near_copy(q).wait_send()
            for h in range(2):
                far_copy(h, q).wait_send()
                relay_copy(h, q).wait_send()


def body(series, offsets, selected):
    vmem = pltpu.VMEM
    dma = pltpu.SemaphoreType.DMA
    return pl.pallas_call(
        main_kernel,
        out_shape=jax.ShapeDtypeStruct((2, EP * LOCAL, ROWS), F32),
        in_specs=[
            pl.BlockSpec(memory_space=pl.ANY),
            pl.BlockSpec(memory_space=pl.ANY),
            pl.BlockSpec(memory_space=pl.ANY),
        ],
        out_specs=pl.BlockSpec(memory_space=pltpu.VMEM),
        scratch_shapes=[
            pltpu.SMEM((SUBJ * LOCAL, EP), I32),
            pltpu.SMEM((SEL,), I32),
            vmem((LOCAL, RUN, VOX), BF16),
            vmem((QUADS * 256, LOCAL * RUN), BF16),
            vmem((SUBJ, QUADS, 256, VOX), BF16),
            vmem((SUBJ, QUADS, 16, VOX), F32),
            vmem((SHARDS, 2, QUADS * 256), BF16),
            vmem((SHARDS, 2, QUADS * 256), BF16),
            vmem((2, QUADS * 256), BF16),
            vmem((SHARDS, 2, QUADS * 256), BF16),
            vmem((SUBJ * QUADS, OWN, 256), F32),
            vmem((SUBJ * QUADS, 256, 256), BF16),
            vmem((SUBJ * QUADS, 256, 256), BF16),
            vmem((SUBJ * QUADS, OWN, 256), F32),
            vmem((SUBJ * QUADS, OWN, 256), F32),
            vmem((QUADS, 256, 256), F32),
            vmem((QUADS, 256, 256), F32),
            vmem((OWN, ROWS, VOX), BF16),
            vmem((2, OWN, 96, 128), F32),
            vmem((4, 4, 48, 128), F32),
            vmem((4, 4, 32, 128), F32),
            vmem((4, 4, 48, 128), F32),
            vmem((4, 4, 32, 128), F32),
            vmem((OWN, 16, 128), F32),
            vmem((4, 48, 128), F32),
            vmem((4, 32, 128), F32),
            vmem((4, 48, 128), F32),
            vmem((4, 32, 128), F32),
            vmem((OWN, 16, 128), F32),
            vmem((16, 24, 128), F32),
            vmem((32, 16, 128), F32),
            vmem((2, 48, 128), F32),
            vmem((2, SUBJ, 48, 128), F32),
            vmem((2, 4, EP * LOCAL, 64), BF16),
            vmem((2, 2, EP * LOCAL, 128), BF16),
            vmem((2, 5 * 128, ROWS), BF16),
            dma((3,)),
            dma,
            dma,
            dma,
            dma,
            dma((QUADS,)),
            dma((QUADS,)),
            dma((2 * QUADS,)),
            dma((2 * QUADS,)),
            dma((2 * QUADS,)),
            dma((2 * QUADS,)),
            dma((2,)),
            dma((2, 4)),
            dma((2, 4)),
            dma((4,)),
            dma((2,)),
            dma((2,)),
            dma((2,)),
            dma((2,)),
        ],
        compiler_params=pltpu.CompilerParams(collective_id=0, has_side_effects=True),
    )(series, offsets, selected)


def solution(mesh):
    placed = (P("subj", None, "vox"), P(), P())
    return jax.shard_map(
        body, mesh=mesh, in_specs=placed, out_specs=P("vox", "subj", None), check_vma=False
    )
```

```python
import functools

import jax
import jax.numpy as jnp
from jax import lax
from jax.experimental import pallas as pl
from jax.experimental.pallas import tpu as pltpu
from jax.sharding import PartitionSpec as P

MESH = pl.DeviceIdType.MESH
F32, BF16, I32 = jnp.float32, jnp.bfloat16, jnp.int32
HIGH = lax.Precision.HIGHEST

SUBJ, SHARDS = 4, 32
TR, EP, RUN = 16, 12, 256
LOCAL = 4
QUADS = 3
SEL, OWN = 64, 16
VOX = 512
ROWS = SUBJ * EP * LOCAL
NT = (((1,), (1,)), ((), ()))
series_floor = 1.0
spread_floor = 0.05
shrink_factor = 0.9


def copy_to(src, dst, send_sem, recv_sem, subj, vox):
    return pltpu.make_async_remote_copy(
        src_ref=src,
        dst_ref=dst,
        send_sem=send_sem,
        recv_sem=recv_sem,
        device_id={"subj": subj, "vox": vox},
        device_id_type=MESH,
    )


def await_bytes(ref, sem):
    pltpu.make_async_copy(ref, ref, sem).wait()


def fold(x):
    return x + pltpu.roll(x, 4, 0)


def exact_terms(x):
    first = x.astype(BF16)
    rest = x - first.astype(F32)
    second = rest.astype(BF16)
    return first, second, (rest - second.astype(F32)).astype(BF16)


def slot_of(group, taker):
    return jnp.where((group ^ taker) < 2, group ^ taker, 2 + (group & 1))


def line_of(slot, epoch, subject):
    return slot * (EP * LOCAL) + epoch * LOCAL + subject


def main_kernel(
    series_hbm,
    offsets_hbm,
    selected_hbm,
    out_ref,
    offsets,
    selected,
    series,
    choose,
    epochs,
    scale,
    slab_out,
    slab_in,
    slab_sum,
    slab,
    raw,
    lhs_hi,
    lhs_lo,
    std_hi,
    std_lo,
    corr_even,
    corr_odd,
    score,
    gram,
    z_parts_first,
    z_parts_second,
    x_parts_first,
    x_parts_second,
    y_parts,
    z_sums_first,
    z_sums_second,
    x_sums_first,
    x_sums_second,
    y_sums,
    last_first,
    last_second,
    total,
    final,
    pick_rows,
    pick_turned,
    put_columns,
    load_sem,
    slab_send,
    slab_recv,
    share_send,
    share_recv,
    near_send,
    near_recv,
    far_send,
    far_recv,
    relay_send,
    relay_recv,
    part_send,
    z_recv,
    x_recv,
    y_recv,
    sum_send,
    sum_recv,
    final_send,
    final_recv,
):
    corr = (corr_even, corr_odd)
    z_parts = (z_parts_first, z_parts_second)
    x_parts = (x_parts_first, x_parts_second)
    z_sums = (z_sums_first, z_sums_second)
    x_sums = (x_sums_first, x_sums_second)
    last = (last_first, last_second)
    j = lax.axis_index("subj")
    v = lax.axis_index("vox")
    near, far, core = j ^ 1, j ^ 2, j & 1
    z, x, y = v // 8, (v // 2) & 3, v & 1

    def ahead_of(place, step):
        return (place + step) & 3

    def shard_at(z, x, y):
        return z * 8 + x * 2 + y

    loads = [
        pltpu.make_async_copy(source, target, load_sem.at[i])
        for i, (source, target) in enumerate(
            ((offsets_hbm, offsets), (selected_hbm, selected), (series_hbm, series))
        )
    ]
    for load in loads:
        load.start()

    barrier = pltpu.get_barrier_semaphore()

    def greet(step, carry):
        to = step ^ 21
        to_v = shard_at(ahead_of(z, to // 8), ahead_of(x, (to // 2) & 3), y ^ (to & 1))
        for other in range(SUBJ):
            pl.semaphore_signal(barrier, inc=1, device_id={"subj": j ^ other, "vox": to_v}, device_id_type=MESH)
        return carry

    with jax.named_scope("greet"):
        lax.fori_loop(0, 21, greet, 0, unroll=3)
        lax.fori_loop(22, SHARDS, greet, 0, unroll=2)
        for other in range(1, SUBJ):
            pl.semaphore_signal(barrier, inc=1, device_id={"subj": j ^ other, "vox": v}, device_id_type=MESH)

    loads[0].wait()
    loads[1].wait()

    with jax.named_scope("choose"):
        row16 = lax.broadcasted_iota(I32, (16, 128), 0)
        scan = lax.broadcasted_iota(I32, (16, LOCAL * RUN), 1)
        for q in range(QUADS):
            start = jnp.zeros((16, 128), I32)
            for r in range(16):
                first = offsets[j * LOCAL + r % 4, q * 4 + r // 4] + (r % 4) * RUN
                start = jnp.where(row16 == r, first, start)
            ahead = scan - jnp.concatenate([start] * (LOCAL * RUN // 128), axis=1)
            for t in range(TR):
                choose[pl.ds(q * 256 + t * 16, 16), :] = jnp.where(ahead == t, 1.0, 0.0).astype(BF16)

    id_rows = []
    row8 = lax.broadcasted_iota(I32, (8, 128), 0)
    for block in range(SEL // 8):
        ids = jnp.zeros((8, 128), I32)
        for r in range(8):
            place = block * 8 + r
            ids = jnp.where(row8 == r, selected[4 * (place % OWN) + place // OWN], ids)
        id_rows.append(ids)
    ids = jnp.concatenate(id_rows, axis=0)
    columns = lax.broadcasted_iota(I32, (SEL, VOX), 1) + v * VOX
    picker = jnp.where(columns == jnp.concatenate([ids] * (VOX // 128), axis=1), 1.0, 0.0).astype(BF16)

    with jax.named_scope("pick_epochs"):
        loads[2].wait()
        runs = series[...].reshape(LOCAL * RUN, VOX)
        for q in range(QUADS):
            chosen = jnp.dot(choose[pl.ds(q * 256, 256), :], runs, preferred_element_type=F32).astype(BF16)
            epochs[0, q] = chosen
            picked = lax.dot_general(picker, chosen, NT, preferred_element_type=F32)
            slab_out[:, :, pl.ds(q * 256, 256)] = picked.astype(BF16).reshape(SHARDS, 2, 256)

    with jax.named_scope("barrier"):
        pl.semaphore_wait(barrier, SUBJ * SHARDS - 1)

    def send_slab(step, carry):
        piece = (v + step) & (SHARDS - 1)
        to_j, to_v = piece // 8, j * 8 + (piece & 7)

        @pl.when(jnp.logical_or(to_j != j, to_v != v))
        def _():
            copy_to(slab_out.at[piece], slab_in.at[v], slab_send, slab_recv, to_j, to_v).start()

        return carry

    with jax.named_scope("send_slab"):
        lax.fori_loop(0, SHARDS, send_slab, 0)

    def near_copy(q):
        return copy_to(epochs.at[0, q], epochs.at[1, q], near_send.at[q], near_recv.at[q], near, v)

    half = pl.ds(pl.multiple_of(core * 256, 256), 256)

    def far_copy(g, q):
        at = g * QUADS + q
        source, target = epochs.at[core ^ g, q, :, half], epochs.at[2 + g, q, :, half]
        return copy_to(source, target, far_send.at[at], far_recv.at[at], far, v)

    def relay_copy(g, q):
        at = g * QUADS + q
        ref = epochs.at[2 + g, q, :, half]
        return copy_to(ref, ref, relay_send.at[at], relay_recv.at[at], near, v)

    def relay(g, q):
        with jax.named_scope("relay"):
            far_copy(g, q).wait_recv()
            relay_copy(g, q).start()

    for q in range(QUADS):
        near_copy(q).start()

    @pl.when(core == 0)
    def _():
        far_copy(0, 0).start()

    def scales(r, h):
        lanes = pl.ds(h * 256, 256)
        for q in range(QUADS):
            seen = epochs[r, q, :, lanes].astype(F32).reshape(TR, 16, 256)
            centred = seen - (jnp.sum(seen, axis=0) * (1.0 / TR))[None]
            scale[r, q, :, lanes] = lax.rsqrt(jnp.sum(centred * centred, axis=0) + series_floor)

    for h in range(2):
        scales(0, h)

    with jax.named_scope("near_wait"):
        for q in range(QUADS):
            near_copy(q).wait_recv()

    @pl.when(core == 1)
    def _():
        far_copy(0, 0).start()

    far_copy(0, 1).start()

    own_group = v // 8 == j

    with jax.named_scope("slab_wait"):

        @pl.when(own_group)
        def _():
            slab_in[v] = slab_out[j * 8 + (v & 7)]
            await_bytes(slab_in.at[pl.ds(0, SHARDS - 1)], slab_recv)

        @pl.when(jnp.logical_not(own_group))
        def _():
            await_bytes(slab_in, slab_recv)

    with jax.named_scope("slab_sum"):
        slab_sum[...] = jnp.sum(slab_in[...].astype(F32), axis=0).astype(BF16)

    def share_slab(step, carry):
        copy_to(slab_sum, slab.at[v], share_send, share_recv, j, (v + step) & (SHARDS - 1)).start()
        return carry

    with jax.named_scope("share_slab"):
        lax.fori_loop(1, SHARDS, share_slab, 0)
        slab[v] = slab_sum[...]

    far_copy(0, 2).start()
    for q in range(QUADS):
        far_copy(1, q).start()

    with jax.named_scope("places"):
        b = lax.broadcasted_iota(I32, (1, ROWS), 1)
        p = lax.broadcasted_iota(I32, (EP * LOCAL, 1), 0)
        for i in range(2):
            taker = y * 2 + i
            s = b // EP
            to = line_of(slot_of(s // LOCAL, taker), b - s * EP, s & 3)
            s = p // EP
            line = line_of(slot_of(j, taker), p - s * EP, s)

            def put(first, rows, lines):
                put_columns[i, pl.ds(first, rows), :] = jnp.where(lines == to, 1.0, 0.0).astype(BF16)

            across = lax.broadcasted_iota(I32, (1, 128), 1)
            down = lax.broadcasted_iota(I32, (128, 1), 0)
            for n in range(2):
                put(n * 320, 128, down)
                put(n * 320 + 128, 128, (down & 63) + (n + 1) * 64)
                put(n * 320 + 256, 64, lax.broadcasted_iota(I32, (64, 1), 0) + n * 128)
                rows = lax.broadcasted_iota(I32, (1, 64), 1)
                pick_rows[i, 2 * n] = jnp.where(rows + n * 128 == line, 1.0, 0.0).astype(BF16)
                pick_rows[i, 2 * n + 1] = jnp.where(rows + (n + 1) * 64 == line, 1.0, 0.0).astype(BF16)
                turned = across if n else jnp.where(across < 64, -1, across)
                pick_turned[i, n] = jnp.where(turned == line, 1.0, 0.0).astype(BF16)

    for h in range(2):
        scales(1, h)

    relay(0, 0)
    relay(0, 1)
    with jax.named_scope("share_wait"):
        await_bytes(slab.at[pl.ds(0, SHARDS - 1)], share_recv)

    with jax.named_scope("standard_slab"):
        for r in range(SUBJ):
            group = (j, near, far & 2, far | 1)[r]
            for kk in range(8):
                for q in range(QUADS):
                    raw[r * QUADS + q, pl.ds(kk * 2, 2), :] = slab[group * 8 + kk, :, pl.ds(q * 256, 256)].astype(F32)
        seen = raw[...].reshape(SUBJ * QUADS * OWN, 256)
        same = jnp.where(
            (lax.broadcasted_iota(I32, (256, 256), 0) & 15) == (lax.broadcasted_iota(I32, (256, 256), 1) & 15), 1.0, 0.0
        ).astype(BF16)
        centred = seen - jnp.dot(seen.astype(BF16), same, preferred_element_type=F32) * (1.0 / TR)
        terms = exact_terms(centred * centred)
        spread = [jnp.dot(t, same, preferred_element_type=F32) for t in terms]
        spread = spread[0] + spread[1] + spread[2]
        x_std = centred * lax.rsqrt(spread + series_floor) * shrink_factor
        x_hi = x_std.astype(BF16).astype(F32)
        std_hi[...] = x_hi.reshape(SUBJ * QUADS, OWN, 256)
        std_lo[...] = (x_std - x_hi).reshape(SUBJ * QUADS, OWN, 256)

    own_row = (lax.broadcasted_iota(I32, (16, 256), 1) & 15) == lax.broadcasted_iota(I32, (16, 256), 0)

    units = ((0, 0), (0, 1), (1, 0), (1, 1), (2, 0), (2, 1), (3, 0), (3, 1))

    def correlate(unit):
        r, h = units[unit]
        lanes = pl.ds(h * 256, 256)
        if r >= 2:
            scales(r, h)
        for q in range(QUADS):
            at = r * QUADS + q
            if h == 0:
                for k in range(OWN):
                    for std, lhs in ((std_hi, lhs_hi), (std_lo, lhs_lo)):
                        line = jnp.broadcast_to(std[at, pl.ds(k, 1), :], (16, 256))
                        lhs[at, pl.ds(k * 16, 16), :] = jnp.where(own_row, line, 0.0).astype(BF16)
            seen = epochs[r, q, :, lanes]
            corr[unit % 2][q] = jnp.dot(lhs_hi[at], seen, preferred_element_type=F32) + jnp.dot(
                lhs_lo[at], seen, preferred_element_type=F32
            )

    def standard(unit, ids=range(OWN)):
        r, h = units[unit]
        lanes = pl.ds(h * 256, 256)
        for k in ids:
            rows = pl.ds(k * 16 if isinstance(k, int) else pl.multiple_of(k * 16, 16), 16)
            halves = []
            for q in range(QUADS):
                shrunk = corr[unit % 2][q, rows, :] * scale[r, q, :, lanes]
                twice = jnp.log(1.0 + shrunk) - jnp.log(1.0 - shrunk)
                halves += [twice[0:8], twice[8:16]]
            mean = fold(functools.reduce(jnp.add, halves)) * (1.0 / EP)
            halves = [f - mean for f in halves]
            spread = fold(functools.reduce(jnp.add, [f * f for f in halves])) * (1.0 / EP)
            gain = lax.rsqrt(spread + 4.0 * spread_floor)
            for q in range(QUADS):
                both = jnp.concatenate([halves[2 * q] * gain, halves[2 * q + 1] * gain], axis=0).astype(BF16)
                at = r * 48 + q * 16
                score[k, pl.ds(at, 16), lanes] = both

    split = ((48, 48, 0), (32, 32, 32))

    def block_of(n, m):
        top = pl.ds(n * 128, 64)
        gram[n, m, 0:64, :] = lax.dot_general(
            score[m, top, :], score[m, pl.ds(0, 128), :], NT, preferred_element_type=F32
        )
        rows = score[m, pl.ds((n + 1) * 64, 64), :]
        square = lax.dot_general(rows, rows, NT, preferred_element_type=F32)
        gram[n, m, 64:96, :] = jnp.concatenate([square[0:32], square[32:64]], axis=1)

    def kernels(n, unfinished=None):
        z_rows, x_rows, y_rows = split[n]

        def id_at(step):
            return ahead_of(z, step // 4) * 4 + ahead_of(x, step & 3)

        def pair(index, carry):
            for step in (index * 2, index * 2 + 1):
                block_of(n, id_at(step))
            if unfinished is not None:
                standard(unfinished, [id_at((index * 2 + more) & 15) for more in (2, 3)])
            for step in (index * 2, index * 2 + 1):
                major, minor = step // 4, step & 3
                m = ahead_of(z, major) * 4 + ahead_of(x, minor)

                @pl.when(major > 0)
                def _():
                    source = gram.at[n, m, pl.ds(0, z_rows)]
                    to_v = shard_at(ahead_of(z, major), x, y)
                    copy_to(source, z_parts[n].at[minor, major], part_send.at[n], z_recv.at[n, minor], j, to_v).start()

                @pl.when(minor > 0)
                def _():
                    source = gram.at[n, m, pl.ds(z_rows, x_rows)]
                    to_v = shard_at(z, ahead_of(x, minor), y)
                    copy_to(source, x_parts[n].at[major, minor], part_send.at[n], x_recv.at[n, major], j, to_v).start()

                if y_rows:
                    rows = pl.ds(pl.multiple_of(z_rows + x_rows + y_rows // 2 * (y ^ 1), 8), y_rows // 2)
                    copy_to(
                        gram.at[n, m, rows], y_parts.at[step], part_send.at[n], y_recv.at[major], j, v ^ 1
                    ).start()
            return carry

        with jax.named_scope("kernels"):
            if unfinished is not None:
                standard(unfinished, [id_at(0), id_at(1)])
            lax.fori_loop(0, OWN // 2, pair, 0)

    def second_sums(n):
        z_rows, x_rows, y_rows = split[n]

        def along(step, block):
            parts, recv, sums = ((z_parts, z_recv, z_sums), (x_parts, x_recv, x_sums))[block]
            with jax.named_scope("part_wait"):
                await_bytes(parts[n].at[step, pl.ds(1, 3)], recv.at[n, step])
            own = (ahead_of(z, step) * 4 + x) if block else (z * 4 + ahead_of(x, step))
            own = gram[n, own, pl.ds(z_rows, x_rows) if block else pl.ds(0, z_rows), :]
            sums[n][step] = (own + parts[n][step, 1]) + (parts[n][step, 2] + parts[n][step, 3])
            for other in range(2):
                side = y ^ other
                count = (z_rows, x_rows)[block] // 2
                rows = pl.ds(pl.multiple_of(side * count, 8), count)
                slot = step * 2 + other
                to_v = shard_at(ahead_of(z, step), x, side) if block else shard_at(z, ahead_of(x, step), side)
                if slot:
                    copy_to(
                        sums[n].at[step, rows], last[n].at[block * 8 + slot], sum_send.at[n], sum_recv.at[n], j, to_v
                    ).start()
                else:
                    last[n][block * 8] = sums[n][0, rows, :]

        def from_side(major):
            with jax.named_scope("part_wait"):
                await_bytes(y_parts.at[pl.ds(major * 4, 4)], y_recv.at[major])
            for minor in range(4):
                step = major * 4 + minor
                to_z, to_x = ahead_of(z, major), ahead_of(x, minor)
                rows = pl.ds(pl.multiple_of(z_rows + x_rows + y_rows // 2 * y, 8), y_rows // 2)
                added = y_parts[step] + gram[n, to_z * 4 + to_x, rows, :]
                if step:
                    y_sums[step] = added
                    copy_to(
                        y_sums.at[step], last[n].at[16 + step], sum_send.at[n], sum_recv.at[n], j, shard_at(to_z, to_x, y)
                    ).start()
                else:
                    last[n][16] = added

        if y_rows:
            for major in range(4):
                along(major, 1)
                from_side(major)
            for step in range(4):
                along(step, 0)
        else:
            for step in range(4):
                along(step, 1)
            for step in range(4):
                along(step, 0)

    owner_v = v - y + j // 2
    place = core * 2 + y
    remote_sums = (14, 29)

    def hand_over(n):
        with jax.named_scope("last_wait"):
            await_bytes(last[n].at[pl.ds(0, remote_sums[n])], sum_recv.at[n])
        mean = 1.0 / (VOX * SHARDS)
        first = 0
        for block, rows in enumerate(split[n]):
            if rows:
                slots = last[n][block * 8 : (block + (2 if block == 2 else 1)) * 8]
                total[n, pl.ds(first, rows // 2), :] = jnp.sum(slots, axis=0) * mean
                first += rows // 2
        for other in range(SUBJ):
            copy = copy_to(
                total.at[n], final.at[n, place], final_send.at[n], final_recv.at[n], (j ^ other) if other else j, owner_v
            )
            if other:
                copy.start()
            else:

                @pl.when(owner_v != v)
                def _():
                    copy.start()

        @pl.when(owner_v == v)
        def _():
            final[n, place] = total[n]

    def await_final(n, sem):
        @pl.when(owner_v == v)
        def _():
            await_bytes(final.at[n, pl.ds(0, SUBJ - 1)], sem.at[n])

        @pl.when(owner_v != v)
        def _():
            await_bytes(final.at[n], sem.at[n])

    def scores_of(correlated, finished):
        with jax.named_scope("scores"):
            if correlated is not None:
                correlate(correlated)
            if finished is not None:
                standard(finished)

    def relayed(g):
        with jax.named_scope("relay_wait"):
            for q in range(QUADS):
                relay_copy(g, q).wait_recv()

    scores_of(0, None)
    scores_of(1, 0)
    relay(0, 2)
    scores_of(2, 1)
    scores_of(3, 2)
    relayed(0)
    scores_of(4, 3)
    scores_of(5, 4)
    scores_of(None, 5)
    relay(1, 0)
    kernels(0)
    relay(1, 1)
    relay(1, 2)
    second_sums(0)
    relayed(1)
    scores_of(6, None)
    scores_of(7, 6)
    kernels(1, 7)
    second_sums(1)
    hand_over(0)
    hand_over(1)

    beside = lax.broadcasted_iota(I32, (EP * LOCAL, 128), 1) < 64

    def picked_by(pick, terms, dims):
        parts = [lax.dot_general(pick, t, dims, preferred_element_type=F32) for t in terms]
        return parts[0] + parts[1] + parts[2]

    def placed(n, i):
        pieces, first = [], 0
        for rows in split[n]:
            if rows:
                here = pl.ds(first, rows // 2)
                pieces += [final[n, 2 * i, here, :], final[n, 2 * i + 1, here, :]]
                first += rows // 2
        both = jnp.concatenate(pieces, axis=0)
        wide, square = exact_terms(both[0:64]), exact_terms(both[64:96])
        halves = [
            picked_by(pick_rows[i, 2 * n + 1, :, h * 32 : h * 32 + 32], square, (((1,), (0,)), ((), ())))
            for h in range(2)
        ]
        lines = [
            picked_by(pick_rows[i, 2 * n], wide, (((1,), (0,)), ((), ()))),
            jnp.where(beside, halves[0], halves[1]),
            picked_by(pick_turned[i, n], wide, NT),
        ]
        put = put_columns[i, pl.ds(n * 320, 320), :]
        terms = [jnp.dot(t, put, preferred_element_type=F32) for t in exact_terms(jnp.concatenate(lines, axis=1))]
        return terms[0] + terms[1] + terms[2]

    with jax.named_scope("final"):
        await_final(0, final_recv)
    with jax.named_scope("place"):
        for i in range(2):
            out_ref[i] = placed(0, i)
    with jax.named_scope("final"):
        await_final(1, final_recv)
    with jax.named_scope("place"):
        for i in range(2):
            out_ref[i] += placed(1, i)

    with jax.named_scope("drain"):
        await_bytes(slab_in.at[pl.ds(0, SHARDS - 1)], share_send)

        @pl.when(own_group)
        def _():
            await_bytes(slab_in.at[pl.ds(0, SHARDS - 1)], slab_send)

        @pl.when(jnp.logical_not(own_group))
        def _():
            await_bytes(slab_in, slab_send)

        for n in range(2):
            await_bytes(z_parts[n].at[pl.ds(0, 3)], part_send.at[n])
            await_bytes(x_parts[n].at[pl.ds(0, 3)], part_send.at[n])
            await_bytes(last[n].at[pl.ds(0, remote_sums[n])], sum_send.at[n])
            await_final(n, final_send)
        await_bytes(y_parts, part_send.at[1])
        for q in range(QUADS):
            near_copy(q).wait_send()
            for h in range(2):
                far_copy(h, q).wait_send()
                relay_copy(h, q).wait_send()


def body(series, offsets, selected):
    vmem = pltpu.VMEM
    dma = pltpu.SemaphoreType.DMA
    return pl.pallas_call(
        main_kernel,
        out_shape=pltpu.VMEM((2, EP * LOCAL, ROWS), F32),
        in_specs=[
            pl.BlockSpec(memory_space=pl.ANY),
            pl.BlockSpec(memory_space=pl.ANY),
            pl.BlockSpec(memory_space=pl.ANY),
        ],
        out_specs=pl.BlockSpec(memory_space=pltpu.VMEM),
        scratch_shapes=[
            pltpu.SMEM((SUBJ * LOCAL, EP), I32),
            pltpu.SMEM((SEL,), I32),
            vmem((LOCAL, RUN, VOX), BF16),
            vmem((QUADS * 256, LOCAL * RUN), BF16),
            vmem((SUBJ, QUADS, 256, VOX), BF16),
            vmem((SUBJ, QUADS, 16, VOX), F32),
            vmem((SHARDS, 2, QUADS * 256), BF16),
            vmem((SHARDS, 2, QUADS * 256), BF16),
            vmem((2, QUADS * 256), BF16),
            vmem((SHARDS, 2, QUADS * 256), BF16),
            vmem((SUBJ * QUADS, OWN, 256), F32),
            vmem((SUBJ * QUADS, 256, 256), BF16),
            vmem((SUBJ * QUADS, 256, 256), BF16),
            vmem((SUBJ * QUADS, OWN, 256), F32),
            vmem((SUBJ * QUADS, OWN, 256), F32),
            vmem((QUADS, 256, 256), F32),
            vmem((QUADS, 256, 256), F32),
            vmem((OWN, ROWS, VOX), BF16),
            vmem((2, OWN, 96, 128), F32),
            vmem((4, 4, 48, 128), F32),
            vmem((4, 4, 32, 128), F32),
            vmem((4, 4, 48, 128), F32),
            vmem((4, 4, 32, 128), F32),
            vmem((OWN, 16, 128), F32),
            vmem((4, 48, 128), F32),
            vmem((4, 32, 128), F32),
            vmem((4, 48, 128), F32),
            vmem((4, 32, 128), F32),
            vmem((OWN, 16, 128), F32),
            vmem((16, 24, 128), F32),
            vmem((32, 16, 128), F32),
            vmem((2, 48, 128), F32),
            vmem((2, SUBJ, 48, 128), F32),
            vmem((2, 4, EP * LOCAL, 64), BF16),
            vmem((2, 2, EP * LOCAL, 128), BF16),
            vmem((2, 5 * 128, ROWS), BF16),
            dma((3,)),
            dma,
            dma,
            dma,
            dma,
            dma((QUADS,)),
            dma((QUADS,)),
            dma((2 * QUADS,)),
            dma((2 * QUADS,)),
            dma((2 * QUADS,)),
            dma((2 * QUADS,)),
            dma((2,)),
            dma((2, 4)),
            dma((2, 4)),
            dma((4,)),
            dma((2,)),
            dma((2,)),
            dma((2,)),
            dma((2,)),
        ],
        compiler_params=pltpu.CompilerParams(collective_id=0, has_side_effects=True),
    )(series, offsets, selected)


def solution(mesh):
    placed = (P("subj", None, "vox"), P(), P())
    return jax.shard_map(
        body, mesh=mesh, in_specs=placed, out_specs=P("vox", "subj", None), check_vma=False
    )
```

```python
import functools

import jax
import jax.numpy as jnp
from jax import lax
from jax.experimental import pallas as pl
from jax.experimental.pallas import tpu as pltpu
from jax.sharding import PartitionSpec as P

MESH = pl.DeviceIdType.MESH
F32, BF16, I32 = jnp.float32, jnp.bfloat16, jnp.int32
HIGH = lax.Precision.HIGHEST

SUBJ, SHARDS = 4, 32
TR, EP, RUN = 16, 12, 256
LOCAL = 4
QUADS = 3
SEL, OWN = 64, 16
VOX = 512
ROWS = SUBJ * EP * LOCAL
NT = (((1,), (1,)), ((), ()))
series_floor = 1.0
spread_floor = 0.05
shrink_factor = 0.9


def copy_to(src, dst, send_sem, recv_sem, subj, vox):
    return pltpu.make_async_remote_copy(
        src_ref=src,
        dst_ref=dst,
        send_sem=send_sem,
        recv_sem=recv_sem,
        device_id={"subj": subj, "vox": vox},
        device_id_type=MESH,
    )


def await_bytes(ref, sem):
    pltpu.make_async_copy(ref, ref, sem).wait()


def fold(x):
    return x + pltpu.roll(x, 4, 0)


def exact_terms(x):
    first = x.astype(BF16)
    rest = x - first.astype(F32)
    second = rest.astype(BF16)
    return first, second, (rest - second.astype(F32)).astype(BF16)


def slot_of(group, taker):
    return jnp.where((group ^ taker) < 2, group ^ taker, 2 + (group & 1))


def line_of(slot, epoch, subject):
    return slot * (EP * LOCAL) + epoch * LOCAL + subject


def main_kernel(
    series_hbm,
    offsets_hbm,
    selected_hbm,
    out_ref,
    offsets,
    selected,
    series,
    choose,
    epochs,
    scale,
    slab_out,
    slab_in,
    slab_sum,
    slab,
    raw,
    lhs_hi,
    lhs_lo,
    std_hi,
    std_lo,
    corr_even,
    corr_odd,
    score,
    gram,
    z_parts_first,
    z_parts_second,
    x_parts_first,
    x_parts_second,
    y_parts,
    z_sums_first,
    z_sums_second,
    x_sums_first,
    x_sums_second,
    y_sums,
    last_first,
    last_second,
    total,
    final,
    pick_rows,
    pick_turned,
    put_columns,
    load_sem,
    slab_send,
    slab_recv,
    share_send,
    share_recv,
    near_send,
    near_recv,
    far_send,
    far_recv,
    relay_send,
    relay_recv,
    part_send,
    z_recv,
    x_recv,
    y_recv,
    sum_send,
    sum_recv,
    final_send,
    final_recv,
):
    corr = (corr_even, corr_odd)
    z_parts = (z_parts_first, z_parts_second)
    x_parts = (x_parts_first, x_parts_second)
    z_sums = (z_sums_first, z_sums_second)
    x_sums = (x_sums_first, x_sums_second)
    last = (last_first, last_second)
    j = lax.axis_index("subj")
    v = lax.axis_index("vox")
    near, far, core = j ^ 1, j ^ 2, j & 1
    z, x, y = v // 8, (v // 2) & 3, v & 1

    def ahead_of(place, step):
        return (place + step) & 3

    def shard_at(z, x, y):
        return z * 8 + x * 2 + y

    loads = [
        pltpu.make_async_copy(source, target, load_sem.at[i])
        for i, (source, target) in enumerate(
            ((offsets_hbm, offsets), (selected_hbm, selected), (series_hbm, series))
        )
    ]
    for load in loads:
        load.start()

    barrier = pltpu.get_barrier_semaphore()

    def greet(step, carry):
        for other in range(SUBJ):
            pl.semaphore_signal(
                barrier,
                inc=1,
                device_id={"subj": j ^ other, "vox": (v + step) & (SHARDS - 1)},
                device_id_type=MESH,
            )
        return carry

    with jax.named_scope("greet"):
        lax.fori_loop(1, SHARDS, greet, 0, unroll=4)
        for other in range(1, SUBJ):
            pl.semaphore_signal(barrier, inc=1, device_id={"subj": j ^ other, "vox": v}, device_id_type=MESH)

    loads[0].wait()
    loads[1].wait()

    with jax.named_scope("choose"):
        row16 = lax.broadcasted_iota(I32, (16, 128), 0)
        scan = lax.broadcasted_iota(I32, (16, LOCAL * RUN), 1)
        for q in range(QUADS):
            start = jnp.zeros((16, 128), I32)
            for r in range(16):
                first = offsets[j * LOCAL + r % 4, q * 4 + r // 4] + (r % 4) * RUN
                start = jnp.where(row16 == r, first, start)
            ahead = scan - jnp.concatenate([start] * (LOCAL * RUN // 128), axis=1)
            for t in range(TR):
                choose[pl.ds(q * 256 + t * 16, 16), :] = jnp.where(ahead == t, 1.0, 0.0).astype(BF16)

    id_rows = []
    row8 = lax.broadcasted_iota(I32, (8, 128), 0)
    for block in range(SEL // 8):
        ids = jnp.zeros((8, 128), I32)
        for r in range(8):
            place = block * 8 + r
            ids = jnp.where(row8 == r, selected[4 * (place % OWN) + place // OWN], ids)
        id_rows.append(ids)
    ids = jnp.concatenate(id_rows, axis=0)
    columns = lax.broadcasted_iota(I32, (SEL, VOX), 1) + v * VOX
    picker = jnp.where(columns == jnp.concatenate([ids] * (VOX // 128), axis=1), 1.0, 0.0).astype(BF16)

    with jax.named_scope("pick_epochs"):
        loads[2].wait()
        runs = series[...].reshape(LOCAL * RUN, VOX)
        for q in range(QUADS):
            chosen = jnp.dot(choose[pl.ds(q * 256, 256), :], runs, preferred_element_type=F32).astype(BF16)
            epochs[0, q] = chosen
            picked = lax.dot_general(picker, chosen, NT, preferred_element_type=F32)
            slab_out[:, :, pl.ds(q * 256, 256)] = picked.astype(BF16).reshape(SHARDS, 2, 256)

    with jax.named_scope("barrier"):
        pl.semaphore_wait(barrier, SUBJ * SHARDS - 1)

    def send_slab(step, carry):
        piece = (v + step) & (SHARDS - 1)
        to_j, to_v = piece // 8, j * 8 + (piece & 7)

        @pl.when(jnp.logical_or(to_j != j, to_v != v))
        def _():
            copy_to(slab_out.at[piece], slab_in.at[v], slab_send, slab_recv, to_j, to_v).start()

        return carry

    with jax.named_scope("send_slab"):
        lax.fori_loop(0, SHARDS, send_slab, 0)

    def near_copy(q):
        return copy_to(epochs.at[0, q], epochs.at[1, q], near_send.at[q], near_recv.at[q], near, v)

    half = pl.ds(pl.multiple_of(core * 256, 256), 256)

    def far_copy(g, q):
        at = g * QUADS + q
        source, target = epochs.at[core ^ g, q, :, half], epochs.at[2 + g, q, :, half]
        return copy_to(source, target, far_send.at[at], far_recv.at[at], far, v)

    def relay_copy(g, q):
        at = g * QUADS + q
        ref = epochs.at[2 + g, q, :, half]
        return copy_to(ref, ref, relay_send.at[at], relay_recv.at[at], near, v)

    def relay(g, q):
        with jax.named_scope("relay"):
            far_copy(g, q).wait_recv()
            relay_copy(g, q).start()

    for q in range(QUADS):
        near_copy(q).start()

    @pl.when(core == 0)
    def _():
        far_copy(0, 0).start()

    def scales(r, h):
        lanes = pl.ds(h * 256, 256)
        for q in range(QUADS):
            seen = epochs[r, q, :, lanes].astype(F32).reshape(TR, 16, 256)
            centred = seen - (jnp.sum(seen, axis=0) * (1.0 / TR))[None]
            scale[r, q, :, lanes] = lax.rsqrt(jnp.sum(centred * centred, axis=0) + series_floor)

    for h in range(2):
        scales(0, h)

    with jax.named_scope("near_wait"):
        for q in range(QUADS):
            near_copy(q).wait_recv()

    @pl.when(core == 1)
    def _():
        far_copy(0, 0).start()

    far_copy(0, 1).start()

    own_group = v // 8 == j

    with jax.named_scope("slab_wait"):

        @pl.when(own_group)
        def _():
            slab_in[v] = slab_out[j * 8 + (v & 7)]
            await_bytes(slab_in.at[pl.ds(0, SHARDS - 1)], slab_recv)

        @pl.when(jnp.logical_not(own_group))
        def _():
            await_bytes(slab_in, slab_recv)

    with jax.named_scope("slab_sum"):
        slab_sum[...] = jnp.sum(slab_in[...].astype(F32), axis=0).astype(BF16)

    def share_slab(step, carry):
        copy_to(slab_sum, slab.at[v], share_send, share_recv, j, (v + step) & (SHARDS - 1)).start()
        return carry

    with jax.named_scope("share_slab"):
        lax.fori_loop(1, SHARDS, share_slab, 0)
        slab[v] = slab_sum[...]

    far_copy(0, 2).start()
    for q in range(QUADS):
        far_copy(1, q).start()

    with jax.named_scope("places"):
        b = lax.broadcasted_iota(I32, (1, ROWS), 1)
        p = lax.broadcasted_iota(I32, (EP * LOCAL, 1), 0)
        for i in range(2):
            taker = y * 2 + i
            s = b // EP
            to = line_of(slot_of(s // LOCAL, taker), b - s * EP, s & 3)
            s = p // EP
            line = line_of(slot_of(j, taker), p - s * EP, s)

            def put(first, rows, lines):
                put_columns[i, pl.ds(first, rows), :] = jnp.where(lines == to, 1.0, 0.0).astype(BF16)

            across = lax.broadcasted_iota(I32, (1, 128), 1)
            down = lax.broadcasted_iota(I32, (128, 1), 0)
            for n in range(2):
                put(n * 320, 128, down)
                put(n * 320 + 128, 128, (down & 63) + (n + 1) * 64)
                put(n * 320 + 256, 64, lax.broadcasted_iota(I32, (64, 1), 0) + n * 128)
                rows = lax.broadcasted_iota(I32, (1, 64), 1)
                pick_rows[i, 2 * n] = jnp.where(rows + n * 128 == line, 1.0, 0.0).astype(BF16)
                pick_rows[i, 2 * n + 1] = jnp.where(rows + (n + 1) * 64 == line, 1.0, 0.0).astype(BF16)
                turned = across if n else jnp.where(across < 64, -1, across)
                pick_turned[i, n] = jnp.where(turned == line, 1.0, 0.0).astype(BF16)

    for h in range(2):
        scales(1, h)

    relay(0, 0)
    relay(0, 1)
    with jax.named_scope("share_wait"):
        await_bytes(slab.at[pl.ds(0, SHARDS - 1)], share_recv)
    relay(0, 2)

    with jax.named_scope("standard_slab"):
        for r in range(SUBJ):
            group = (j, near, far & 2, far | 1)[r]
            for kk in range(8):
                for q in range(QUADS):
                    raw[r * QUADS + q, pl.ds(kk * 2, 2), :] = slab[group * 8 + kk, :, pl.ds(q * 256, 256)].astype(F32)
        seen = raw[...].reshape(SUBJ * QUADS * OWN, 256)
        same = jnp.where(
            (lax.broadcasted_iota(I32, (256, 256), 0) & 15) == (lax.broadcasted_iota(I32, (256, 256), 1) & 15), 1.0, 0.0
        ).astype(BF16)
        centred = seen - jnp.dot(seen.astype(BF16), same, preferred_element_type=F32) * (1.0 / TR)
        terms = exact_terms(centred * centred)
        spread = [jnp.dot(t, same, preferred_element_type=F32) for t in terms]
        spread = spread[0] + spread[1] + spread[2]
        x_std = centred * lax.rsqrt(spread + series_floor) * shrink_factor
        x_hi = x_std.astype(BF16).astype(F32)
        std_hi[...] = x_hi.reshape(SUBJ * QUADS, OWN, 256)
        std_lo[...] = (x_std - x_hi).reshape(SUBJ * QUADS, OWN, 256)

    own_row = (lax.broadcasted_iota(I32, (16, 256), 1) & 15) == lax.broadcasted_iota(I32, (16, 256), 0)

    units = ((0, 0), (0, 1), (1, 0), (1, 1), (2, 0), (2, 1), (3, 0), (3, 1))

    def correlate(unit):
        r, h = units[unit]
        lanes = pl.ds(h * 256, 256)
        if r >= 2:
            scales(r, h)
        for q in range(QUADS):
            at = r * QUADS + q
            if h == 0:
                for k in range(OWN):
                    for std, lhs in ((std_hi, lhs_hi), (std_lo, lhs_lo)):
                        line = jnp.broadcast_to(std[at, pl.ds(k, 1), :], (16, 256))
                        lhs[at, pl.ds(k * 16, 16), :] = jnp.where(own_row, line, 0.0).astype(BF16)
            seen = epochs[r, q, :, lanes]
            corr[unit % 2][q] = jnp.dot(lhs_hi[at], seen, preferred_element_type=F32) + jnp.dot(
                lhs_lo[at], seen, preferred_element_type=F32
            )

    def standard(unit, ids=range(OWN)):
        r, h = units[unit]
        lanes = pl.ds(h * 256, 256)
        for k in ids:
            rows = pl.ds(k * 16 if isinstance(k, int) else pl.multiple_of(k * 16, 16), 16)
            halves = []
            for q in range(QUADS):
                shrunk = corr[unit % 2][q, rows, :] * scale[r, q, :, lanes]
                twice = jnp.log(1.0 + shrunk) - jnp.log(1.0 - shrunk)
                halves += [twice[0:8], twice[8:16]]
            mean = fold(functools.reduce(jnp.add, halves)) * (1.0 / EP)
            halves = [f - mean for f in halves]
            spread = fold(functools.reduce(jnp.add, [f * f for f in halves])) * (1.0 / EP)
            gain = lax.rsqrt(spread + 4.0 * spread_floor)
            for q in range(QUADS):
                both = jnp.concatenate([halves[2 * q] * gain, halves[2 * q + 1] * gain], axis=0).astype(BF16)
                at = r * 48 + q * 16
                score[k, pl.ds(at, 16), lanes] = both

    split = ((48, 48, 0), (32, 32, 32))

    def block_of(n, m):
        top = pl.ds(n * 128, 64)
        gram[n, m, 0:64, :] = lax.dot_general(
            score[m, top, :], score[m, pl.ds(0, 128), :], NT, preferred_element_type=F32
        )
        rows = score[m, pl.ds((n + 1) * 64, 64), :]
        square = lax.dot_general(rows, rows, NT, preferred_element_type=F32)
        gram[n, m, 64:96, :] = jnp.concatenate([square[0:32], square[32:64]], axis=1)

    def kernels(n, unfinished=None):
        z_rows, x_rows, y_rows = split[n]

        def id_at(step):
            return ahead_of(z, step // 4) * 4 + ahead_of(x, step & 3)

        def four(index, carry):
            steps = [index * 4 + more for more in range(8)]
            for step in steps[:4]:
                block_of(n, id_at(step))
            if unfinished is not None:
                standard(unfinished, [id_at(step & 15) for step in steps[4:]])
            for step in steps[:4]:
                major, minor = step // 4, step & 3
                m = ahead_of(z, major) * 4 + ahead_of(x, minor)

                @pl.when(major > 0)
                def _():
                    source = gram.at[n, m, pl.ds(0, z_rows)]
                    to_v = shard_at(ahead_of(z, major), x, y)
                    copy_to(source, z_parts[n].at[minor, major], part_send.at[n], z_recv.at[n, minor], j, to_v).start()

                @pl.when(minor > 0)
                def _():
                    source = gram.at[n, m, pl.ds(z_rows, x_rows)]
                    to_v = shard_at(z, ahead_of(x, minor), y)
                    copy_to(source, x_parts[n].at[major, minor], part_send.at[n], x_recv.at[n, major], j, to_v).start()

                if y_rows:
                    rows = pl.ds(pl.multiple_of(z_rows + x_rows + y_rows // 2 * (y ^ 1), 8), y_rows // 2)
                    copy_to(
                        gram.at[n, m, rows], y_parts.at[step], part_send.at[n], y_recv.at[major], j, v ^ 1
                    ).start()
            return carry

        with jax.named_scope("kernels"):
            if unfinished is not None:
                standard(unfinished, [id_at(step) for step in range(4)])
            lax.fori_loop(0, OWN // 4, four, 0)

    def second_sums(n):
        z_rows, x_rows, y_rows = split[n]

        def along(step, block):
            parts, recv, sums = ((z_parts, z_recv, z_sums), (x_parts, x_recv, x_sums))[block]
            with jax.named_scope("part_wait"):
                await_bytes(parts[n].at[step, pl.ds(1, 3)], recv.at[n, step])
            own = (ahead_of(z, step) * 4 + x) if block else (z * 4 + ahead_of(x, step))
            own = gram[n, own, pl.ds(z_rows, x_rows) if block else pl.ds(0, z_rows), :]
            sums[n][step] = (own + parts[n][step, 1]) + (parts[n][step, 2] + parts[n][step, 3])
            for other in range(2):
                side = y ^ other
                count = (z_rows, x_rows)[block] // 2
                rows = pl.ds(pl.multiple_of(side * count, 8), count)
                slot = step * 2 + other
                to_v = shard_at(ahead_of(z, step), x, side) if block else shard_at(z, ahead_of(x, step), side)
                if slot:
                    copy_to(
                        sums[n].at[step, rows], last[n].at[block * 8 + slot], sum_send.at[n], sum_recv.at[n], j, to_v
                    ).start()
                else:
                    last[n][block * 8] = sums[n][0, rows, :]

        def from_side(major):
            with jax.named_scope("part_wait"):
                await_bytes(y_parts.at[pl.ds(major * 4, 4)], y_recv.at[major])
            for minor in range(4):
                step = major * 4 + minor
                to_z, to_x = ahead_of(z, major), ahead_of(x, minor)
                rows = pl.ds(pl.multiple_of(z_rows + x_rows + y_rows // 2 * y, 8), y_rows // 2)
                added = y_parts[step] + gram[n, to_z * 4 + to_x, rows, :]
                if step:
                    y_sums[step] = added
                    copy_to(
                        y_sums.at[step], last[n].at[16 + step], sum_send.at[n], sum_recv.at[n], j, shard_at(to_z, to_x, y)
                    ).start()
                else:
                    last[n][16] = added

        if y_rows:
            for major in range(4):
                along(major, 1)
                from_side(major)
            for step in range(4):
                along(step, 0)
        else:
            for step in range(4):
                along(step, 1)
            for step in range(4):
                along(step, 0)

    owner_v = v - y + j // 2
    place = core * 2 + y
    remote_sums = (14, 29)

    def hand_over(n):
        with jax.named_scope("last_wait"):
            await_bytes(last[n].at[pl.ds(0, remote_sums[n])], sum_recv.at[n])
        mean = 1.0 / (VOX * SHARDS)
        first = 0
        for block, rows in enumerate(split[n]):
            if rows:
                slots = last[n][block * 8 : (block + (2 if block == 2 else 1)) * 8]
                total[n, pl.ds(first, rows // 2), :] = jnp.sum(slots, axis=0) * mean
                first += rows // 2
        for other in range(SUBJ):
            copy = copy_to(
                total.at[n], final.at[n, place], final_send.at[n], final_recv.at[n], (j ^ other) if other else j, owner_v
            )
            if other:
                copy.start()
            else:

                @pl.when(owner_v != v)
                def _():
                    copy.start()

        @pl.when(owner_v == v)
        def _():
            final[n, place] = total[n]

    def await_final(n, sem):
        @pl.when(owner_v == v)
        def _():
            await_bytes(final.at[n, pl.ds(0, SUBJ - 1)], sem.at[n])

        @pl.when(owner_v != v)
        def _():
            await_bytes(final.at[n], sem.at[n])

    def scores_of(correlated, finished):
        with jax.named_scope("scores"):
            if correlated is not None:
                correlate(correlated)
            if finished is not None:
                standard(finished)

    def relayed(g):
        with jax.named_scope("relay_wait"):
            for q in range(QUADS):
                relay_copy(g, q).wait_recv()

    scores_of(0, None)
    scores_of(1, 0)
    scores_of(2, 1)
    scores_of(3, 2)
    relayed(0)
    scores_of(4, 3)
    relay(1, 0)
    scores_of(5, 4)
    scores_of(None, 5)
    relay(1, 1)
    kernels(0)
    relay(1, 2)
    relayed(1)
    scores_of(6, None)
    scores_of(7, 6)
    kernels(1, 7)
    second_sums(0)
    second_sums(1)
    hand_over(0)
    hand_over(1)

    beside = lax.broadcasted_iota(I32, (EP * LOCAL, 128), 1) < 64

    def picked_by(pick, terms, dims):
        parts = [lax.dot_general(pick, t, dims, preferred_element_type=F32) for t in terms]
        return parts[0] + parts[1] + parts[2]

    def placed(n, i):
        pieces, first = [], 0
        for rows in split[n]:
            if rows:
                here = pl.ds(first, rows // 2)
                pieces += [final[n, 2 * i, here, :], final[n, 2 * i + 1, here, :]]
                first += rows // 2
        both = jnp.concatenate(pieces, axis=0)
        wide, square = exact_terms(both[0:64]), exact_terms(both[64:96])
        halves = [
            picked_by(pick_rows[i, 2 * n + 1, :, h * 32 : h * 32 + 32], square, (((1,), (0,)), ((), ())))
            for h in range(2)
        ]
        lines = [
            picked_by(pick_rows[i, 2 * n], wide, (((1,), (0,)), ((), ()))),
            jnp.where(beside, halves[0], halves[1]),
            picked_by(pick_turned[i, n], wide, NT),
        ]
        put = put_columns[i, pl.ds(n * 320, 320), :]
        terms = [jnp.dot(t, put, preferred_element_type=F32) for t in exact_terms(jnp.concatenate(lines, axis=1))]
        return terms[0] + terms[1] + terms[2]

    with jax.named_scope("final"):
        await_final(0, final_recv)
    with jax.named_scope("place"):
        for i in range(2):
            out_ref[i] = placed(0, i)
    with jax.named_scope("final"):
        await_final(1, final_recv)
    with jax.named_scope("place"):
        for i in range(2):
            out_ref[i] += placed(1, i)

    with jax.named_scope("drain"):
        await_bytes(slab_in.at[pl.ds(0, SHARDS - 1)], share_send)

        @pl.when(own_group)
        def _():
            await_bytes(slab_in.at[pl.ds(0, SHARDS - 1)], slab_send)

        @pl.when(jnp.logical_not(own_group))
        def _():
            await_bytes(slab_in, slab_send)

        for n in range(2):
            await_bytes(z_parts[n].at[pl.ds(0, 3)], part_send.at[n])
            await_bytes(x_parts[n].at[pl.ds(0, 3)], part_send.at[n])
            await_bytes(last[n].at[pl.ds(0, remote_sums[n])], sum_send.at[n])
            await_final(n, final_send)
        await_bytes(y_parts, part_send.at[1])
        for q in range(QUADS):
            near_copy(q).wait_send()
            for h in range(2):
                far_copy(h, q).wait_send()
                relay_copy(h, q).wait_send()


def body(series, offsets, selected):
    vmem = pltpu.VMEM
    dma = pltpu.SemaphoreType.DMA
    return pl.pallas_call(
        main_kernel,
        out_shape=pltpu.VMEM((2, EP * LOCAL, ROWS), F32),
        in_specs=[
            pl.BlockSpec(memory_space=pl.ANY),
            pl.BlockSpec(memory_space=pl.ANY),
            pl.BlockSpec(memory_space=pl.ANY),
        ],
        out_specs=pl.BlockSpec(memory_space=pltpu.VMEM),
        scratch_shapes=[
            pltpu.SMEM((SUBJ * LOCAL, EP), I32),
            pltpu.SMEM((SEL,), I32),
            vmem((LOCAL, RUN, VOX), BF16),
            vmem((QUADS * 256, LOCAL * RUN), BF16),
            vmem((SUBJ, QUADS, 256, VOX), BF16),
            vmem((SUBJ, QUADS, 16, VOX), F32),
            vmem((SHARDS, 2, QUADS * 256), BF16),
            vmem((SHARDS, 2, QUADS * 256), BF16),
            vmem((2, QUADS * 256), BF16),
            vmem((SHARDS, 2, QUADS * 256), BF16),
            vmem((SUBJ * QUADS, OWN, 256), F32),
            vmem((SUBJ * QUADS, 256, 256), BF16),
            vmem((SUBJ * QUADS, 256, 256), BF16),
            vmem((SUBJ * QUADS, OWN, 256), F32),
            vmem((SUBJ * QUADS, OWN, 256), F32),
            vmem((QUADS, 256, 256), F32),
            vmem((QUADS, 256, 256), F32),
            vmem((OWN, ROWS, VOX), BF16),
            vmem((2, OWN, 96, 128), F32),
            vmem((4, 4, 48, 128), F32),
            vmem((4, 4, 32, 128), F32),
            vmem((4, 4, 48, 128), F32),
            vmem((4, 4, 32, 128), F32),
            vmem((OWN, 16, 128), F32),
            vmem((4, 48, 128), F32),
            vmem((4, 32, 128), F32),
            vmem((4, 48, 128), F32),
            vmem((4, 32, 128), F32),
            vmem((OWN, 16, 128), F32),
            vmem((16, 24, 128), F32),
            vmem((32, 16, 128), F32),
            vmem((2, 48, 128), F32),
            vmem((2, SUBJ, 48, 128), F32),
            vmem((2, 4, EP * LOCAL, 64), BF16),
            vmem((2, 2, EP * LOCAL, 128), BF16),
            vmem((2, 5 * 128, ROWS), BF16),
            dma((3,)),
            dma,
            dma,
            dma,
            dma,
            dma((QUADS,)),
            dma((QUADS,)),
            dma((2 * QUADS,)),
            dma((2 * QUADS,)),
            dma((2 * QUADS,)),
            dma((2 * QUADS,)),
            dma((2,)),
            dma((2, 4)),
            dma((2, 4)),
            dma((4,)),
            dma((2,)),
            dma((2,)),
            dma((2,)),
            dma((2,)),
        ],
        compiler_params=pltpu.CompilerParams(collective_id=0, has_side_effects=True),
    )(series, offsets, selected)


def solution(mesh):
    placed = (P("subj", None, "vox"), P(), P())
    return jax.shard_map(
        body, mesh=mesh, in_specs=placed, out_specs=P("vox", "subj", None), check_vma=False
    )
```

```python
import functools

import jax
import jax.numpy as jnp
from jax import lax
from jax.experimental import pallas as pl
from jax.experimental.pallas import tpu as pltpu
from jax.sharding import PartitionSpec as P

MESH = pl.DeviceIdType.MESH
F32, BF16, I32 = jnp.float32, jnp.bfloat16, jnp.int32
HIGH = lax.Precision.HIGHEST

SUBJ, SHARDS = 4, 32
TR, EP, RUN = 16, 12, 256
LOCAL = 4
QUADS = 3
SEL, OWN = 64, 16
VOX = 512
ROWS = SUBJ * EP * LOCAL
NT = (((1,), (1,)), ((), ()))
series_floor = 1.0
spread_floor = 0.05
shrink_factor = 0.9


def copy_to(src, dst, send_sem, recv_sem, subj, vox):
    return pltpu.make_async_remote_copy(
        src_ref=src,
        dst_ref=dst,
        send_sem=send_sem,
        recv_sem=recv_sem,
        device_id={"subj": subj, "vox": vox},
        device_id_type=MESH,
    )


def await_bytes(ref, sem):
    pltpu.make_async_copy(ref, ref, sem).wait()


def fold(x):
    return x + pltpu.roll(x, 4, 0)


def exact_terms(x):
    first = x.astype(BF16)
    rest = x - first.astype(F32)
    second = rest.astype(BF16)
    return first, second, (rest - second.astype(F32)).astype(BF16)


def two_terms(x):
    first = x.astype(BF16)
    return first, (x - first.astype(F32)).astype(BF16)


def slot_of(group, taker):
    return jnp.where((group ^ taker) < 2, group ^ taker, 2 + (group & 1))


def line_of(slot, epoch, subject):
    return slot * (EP * LOCAL) + epoch * LOCAL + subject


def main_kernel(
    series_hbm,
    offsets_hbm,
    selected_hbm,
    out_ref,
    offsets,
    selected,
    series,
    choose,
    epochs,
    scale,
    slab_out,
    slab_in,
    slab_sum,
    slab,
    raw,
    lhs_hi,
    lhs_lo,
    std_hi,
    std_lo,
    corr_even,
    corr_odd,
    score,
    gram_a,
    gram_b,
    gram_c,
    z_parts_a,
    z_parts_b,
    z_parts_c,
    x_parts_a,
    x_parts_b,
    x_parts_c,
    y_parts,
    z_sums_a,
    z_sums_b,
    z_sums_c,
    x_sums_a,
    x_sums_b,
    x_sums_c,
    y_sums,
    z_last_a,
    z_last_b,
    z_last_c,
    x_last_a,
    x_last_b,
    x_last_c,
    y_last,
    total_a,
    total_b,
    total_c,
    final_a,
    final_b,
    final_c,
    pick_a,
    pick_b,
    pick_wide,
    pick_square,
    turn_a,
    turn_b,
    turn_c,
    put_columns,
    load_sem,
    slab_send,
    slab_recv,
    share_send,
    share_recv,
    near_send,
    near_recv,
    far_send,
    far_recv,
    relay_send,
    relay_recv,
    part_send,
    z_recv,
    x_recv,
    y_recv,
    sum_send,
    sum_recv,
    final_send,
    final_recv,
):
    corr = (corr_even, corr_odd)
    z_parts, x_parts = (z_parts_a, z_parts_b, z_parts_c), (x_parts_a, x_parts_b, x_parts_c)
    z_sums, x_sums = (z_sums_a, z_sums_b, z_sums_c), (x_sums_a, x_sums_b, x_sums_c)
    last = ((z_last_a, x_last_a), (z_last_b, x_last_b), (z_last_c, x_last_c, y_last))
    gram = (gram_a, gram_b, gram_c)
    total, final = (total_a, total_b, total_c), (final_a, final_b, final_c)
    j = lax.axis_index("subj")
    v = lax.axis_index("vox")
    near, far, core = j ^ 1, j ^ 2, j & 1
    z, x, y = v // 8, (v // 2) & 3, v & 1

    def ahead_of(place, step):
        return (place + step) & 3

    def shard_at(z, x, y):
        return z * 8 + x * 2 + y

    loads = [
        pltpu.make_async_copy(source, target, load_sem.at[i])
        for i, (source, target) in enumerate(
            ((offsets_hbm, offsets), (selected_hbm, selected), (series_hbm, series))
        )
    ]
    for load in loads:
        load.start()

    barrier = pltpu.get_barrier_semaphore()

    def greet(step, carry):
        for other in range(SUBJ):
            pl.semaphore_signal(
                barrier,
                inc=1,
                device_id={"subj": j ^ other, "vox": (v + step) & (SHARDS - 1)},
                device_id_type=MESH,
            )
        return carry

    with jax.named_scope("greet"):
        lax.fori_loop(1, SHARDS, greet, 0, unroll=4)
        for other in range(1, SUBJ):
            pl.semaphore_signal(barrier, inc=1, device_id={"subj": j ^ other, "vox": v}, device_id_type=MESH)

    loads[0].wait()
    loads[1].wait()

    with jax.named_scope("choose"):
        row16 = lax.broadcasted_iota(I32, (16, 128), 0)
        scan = lax.broadcasted_iota(I32, (16, LOCAL * RUN), 1)
        for q in range(QUADS):
            start = jnp.zeros((16, 128), I32)
            for r in range(16):
                first = offsets[j * LOCAL + r % 4, q * 4 + r // 4] + (r % 4) * RUN
                start = jnp.where(row16 == r, first, start)
            ahead = scan - jnp.concatenate([start] * (LOCAL * RUN // 128), axis=1)
            for t in range(TR):
                choose[pl.ds(q * 256 + t * 16, 16), :] = jnp.where(ahead == t, 1.0, 0.0).astype(BF16)

    id_rows = []
    row8 = lax.broadcasted_iota(I32, (8, 128), 0)
    for block in range(SEL // 8):
        ids = jnp.zeros((8, 128), I32)
        for r in range(8):
            place = block * 8 + r
            ids = jnp.where(row8 == r, selected[4 * (place % OWN) + place // OWN], ids)
        id_rows.append(ids)
    ids = jnp.concatenate(id_rows, axis=0)
    columns = lax.broadcasted_iota(I32, (SEL, VOX), 1) + v * VOX
    picker = jnp.where(columns == jnp.concatenate([ids] * (VOX // 128), axis=1), 1.0, 0.0).astype(BF16)

    with jax.named_scope("pick_epochs"):
        loads[2].wait()
        runs = series[...].reshape(LOCAL * RUN, VOX)
        for q in range(QUADS):
            chosen = jnp.dot(choose[pl.ds(q * 256, 256), :], runs, preferred_element_type=F32).astype(BF16)
            epochs[0, q] = chosen
            picked = lax.dot_general(picker, chosen, NT, preferred_element_type=F32)
            slab_out[:, :, pl.ds(q * 256, 256)] = picked.astype(BF16).reshape(SHARDS, 2, 256)

    with jax.named_scope("barrier"):
        pl.semaphore_wait(barrier, SUBJ * SHARDS - 1)

    def send_slab(step, carry):
        piece = (v + step) & (SHARDS - 1)
        to_j, to_v = piece // 8, j * 8 + (piece & 7)

        @pl.when(jnp.logical_or(to_j != j, to_v != v))
        def _():
            copy_to(slab_out.at[piece], slab_in.at[v], slab_send, slab_recv, to_j, to_v).start()

        return carry

    with jax.named_scope("send_slab"):
        lax.fori_loop(0, SHARDS, send_slab, 0)

    def near_copy(q):
        return copy_to(epochs.at[0, q], epochs.at[1, q], near_send.at[q], near_recv.at[q], near, v)

    half = pl.ds(pl.multiple_of(core * 256, 256), 256)

    def far_copy(g, q):
        at = g * QUADS + q
        source, target = epochs.at[core ^ g, q, :, half], epochs.at[2 + g, q, :, half]
        return copy_to(source, target, far_send.at[at], far_recv.at[at], far, v)

    def relay_copy(g, q):
        at = g * QUADS + q
        ref = epochs.at[2 + g, q, :, half]
        return copy_to(ref, ref, relay_send.at[at], relay_recv.at[at], near, v)

    def relay(g, q):
        with jax.named_scope("relay"):
            far_copy(g, q).wait_recv()
            relay_copy(g, q).start()

    for q in range(QUADS):
        near_copy(q).start()

    @pl.when(core == 0)
    def _():
        far_copy(0, 0).start()

    def scales(r, h):
        lanes = pl.ds(h * 256, 256)
        for q in range(QUADS):
            seen = epochs[r, q, :, lanes].astype(F32).reshape(TR, 16, 256)
            centred = seen - (jnp.sum(seen, axis=0) * (1.0 / TR))[None]
            scale[r, q, :, lanes] = lax.rsqrt(jnp.sum(centred * centred, axis=0) + series_floor)

    for h in range(2):
        scales(0, h)

    with jax.named_scope("near_wait"):
        for q in range(QUADS):
            near_copy(q).wait_recv()

    @pl.when(core == 1)
    def _():
        far_copy(0, 0).start()

    far_copy(0, 1).start()

    own_group = v // 8 == j

    with jax.named_scope("slab_wait"):

        @pl.when(own_group)
        def _():
            slab_in[v] = slab_out[j * 8 + (v & 7)]
            await_bytes(slab_in.at[pl.ds(0, SHARDS - 1)], slab_recv)

        @pl.when(jnp.logical_not(own_group))
        def _():
            await_bytes(slab_in, slab_recv)

    with jax.named_scope("slab_sum"):
        slab_sum[...] = jnp.sum(slab_in[...].astype(F32), axis=0).astype(BF16)

    def share_slab(step, carry):
        copy_to(slab_sum, slab.at[v], share_send, share_recv, j, (v + step) & (SHARDS - 1)).start()
        return carry

    with jax.named_scope("share_slab"):
        lax.fori_loop(1, SHARDS, share_slab, 0)
        slab[v] = slab_sum[...]

    far_copy(0, 2).start()
    for q in range(QUADS):
        far_copy(1, q).start()

    with jax.named_scope("places"):
        b = lax.broadcasted_iota(I32, (1, ROWS), 1)
        p = lax.broadcasted_iota(I32, (EP * LOCAL, 1), 0)
        for i in range(2):
            taker = y * 2 + i
            s = b // EP
            to = line_of(slot_of(s // LOCAL, taker), b - s * EP, s & 3)
            s = p // EP
            line = line_of(slot_of(j, taker), p - s * EP, s)

            def put(first, lines):
                put_columns[i, pl.ds(first, lines.shape[0]), :] = jnp.where(lines == to, 1.0, 0.0).astype(BF16)

            def hot(lines):
                return jnp.where(lines == line, 1.0, 0.0).astype(BF16)

            def down(count):
                return lax.broadcasted_iota(I32, (count, 1), 0)

            def across(count):
                return lax.broadcasted_iota(I32, (1, count), 1)

            c, r = down(128), down(64)
            around = (c & 63) + 64
            put(0, jnp.where(c < 64, c, c - 32))
            put(128, jnp.where(around < 96, around, around - 96))
            put(256, jnp.where(r < 32, r, jnp.where(r < 48, r + 32, -1)))
            put(320, jnp.where(r < 48, jnp.where(r < 32, r + 32, r + 48), -1))
            c, r = across(128), across(64)
            around = (c & 63) + 64
            apart = (c & 32) > 0
            for piece, (lines, columns) in enumerate(
                (
                    (jnp.where(r < 32, r, -1), jnp.where(apart & (c < 64), c, -1)),
                    (jnp.where(r < 32, r + 32, -1), jnp.where(apart & (c >= 64), c - 32, -1)),
                    (jnp.where((r >= 32) & (r < 48), r + 32, -1), jnp.where(apart & (c < 64), around - 96, -1)),
                    (jnp.where((r >= 32) & (r < 48), r + 48, -1), jnp.where(apart & (c >= 64), around - 96, -1)),
                )
            ):
                pick_a[i, pl.ds(piece * 48, 48), :] = hot(lines)
                turn_a[i, pl.ds(piece * 48, 48), :] = hot(columns)
            put(384, down(128))
            put(512, down(32) + 96)
            pick_b[i] = hot(across(32) + 96)
            turn_b[i] = hot(jnp.where(c < 96, c, -1))
            put(544, down(128))
            put(672, (down(128) & 63) + 128)
            put(800, down(64) + 128)
            pick_wide[i] = hot(r + 128)
            pick_square[i] = hot(r + 128)
            turn_c[i] = hot(c)
        for k in range(OWN):
            score[k, 96:128, :] = jnp.zeros((32, VOX), BF16)

    for h in range(2):
        scales(1, h)

    relay(0, 0)
    relay(0, 1)
    with jax.named_scope("share_wait"):
        await_bytes(slab.at[pl.ds(0, SHARDS - 1)], share_recv)
    relay(0, 2)

    with jax.named_scope("standard_slab"):
        for r in range(SUBJ):
            group = (j, near, far & 2, far | 1)[r]
            for kk in range(8):
                for q in range(QUADS):
                    raw[r * QUADS + q, pl.ds(kk * 2, 2), :] = slab[group * 8 + kk, :, pl.ds(q * 256, 256)].astype(F32)
        seen = raw[...].reshape(SUBJ * QUADS * OWN, 256)
        same = jnp.where(
            (lax.broadcasted_iota(I32, (256, 256), 0) & 15) == (lax.broadcasted_iota(I32, (256, 256), 1) & 15), 1.0, 0.0
        ).astype(BF16)
        centred = seen - jnp.dot(seen.astype(BF16), same, preferred_element_type=F32) * (1.0 / TR)
        terms = exact_terms(centred * centred)
        spread = [jnp.dot(t, same, preferred_element_type=F32) for t in terms]
        spread = spread[0] + spread[1] + spread[2]
        x_std = centred * lax.rsqrt(spread + series_floor) * shrink_factor
        x_hi = x_std.astype(BF16).astype(F32)
        std_hi[...] = x_hi.reshape(SUBJ * QUADS, OWN, 256)
        std_lo[...] = (x_std - x_hi).reshape(SUBJ * QUADS, OWN, 256)

    own_row = (lax.broadcasted_iota(I32, (16, 256), 1) & 15) == lax.broadcasted_iota(I32, (16, 256), 0)

    units = ((0, 0), (0, 1), (1, 0), (1, 1), (2, 0), (2, 1), (3, 0), (3, 1))

    def correlate(unit):
        r, h = units[unit]
        lanes = pl.ds(h * 256, 256)
        if r >= 2:
            scales(r, h)
        for q in range(QUADS):
            at = r * QUADS + q
            if h == 0:
                for k in range(OWN):
                    for std, lhs in ((std_hi, lhs_hi), (std_lo, lhs_lo)):
                        line = jnp.broadcast_to(std[at, pl.ds(k, 1), :], (16, 256))
                        lhs[at, pl.ds(k * 16, 16), :] = jnp.where(own_row, line, 0.0).astype(BF16)
            seen = epochs[r, q, :, lanes]
            corr[unit % 2][q] = jnp.dot(lhs_hi[at], seen, preferred_element_type=F32) + jnp.dot(
                lhs_lo[at], seen, preferred_element_type=F32
            )

    def standard(unit, ids=range(OWN)):
        r, h = units[unit]
        lanes = pl.ds(h * 256, 256)
        for k in ids:
            rows = pl.ds(k * 16 if isinstance(k, int) else pl.multiple_of(k * 16, 16), 16)
            halves = []
            for q in range(QUADS):
                shrunk = corr[unit % 2][q, rows, :] * scale[r, q, :, lanes]
                twice = jnp.log(1.0 + shrunk) - jnp.log(1.0 - shrunk)
                halves += [twice[0:8], twice[8:16]]
            mean = fold(functools.reduce(jnp.add, halves)) * (1.0 / EP)
            halves = [f - mean for f in halves]
            spread = fold(functools.reduce(jnp.add, [f * f for f in halves])) * (1.0 / EP)
            gain = lax.rsqrt(spread + 4.0 * spread_floor)
            for q in range(QUADS):
                both = jnp.concatenate([halves[2 * q] * gain, halves[2 * q + 1] * gain], axis=0).astype(BF16)
                at = r * 48 + q * 16
                score[k, pl.ds(at, 16), lanes] = both

    split = ((32, 16, 0), (16, 16, 0), (32, 32, 32))
    lane = lax.broadcasted_iota(I32, (16, 128), 1)

    def against(m, first, count, columns=slice(0, 128)):
        return lax.dot_general(score[m, pl.ds(first, count), :], score[m, columns, :], NT, preferred_element_type=F32)

    def block_of(n, m):
        if n == 0:
            block = against(m, 0, 96)
            for top in (0, 16):
                beside = pltpu.roll(block[32 + top : 48 + top], 32, 1)
                gram[n][m, top : top + 16, :] = jnp.where(lane < 64, block[top : top + 16], beside)
            upper, lower = block[64:80], block[80:96]
            left = jnp.where(lane < 32, pltpu.roll(upper, 64, 1), pltpu.roll(upper, 32, 1))
            right = jnp.where(lane < 96, lower, pltpu.roll(lower, 96, 1))
            gram[n][m, 32:48, :] = jnp.where(lane < 64, left, right)
        elif n == 1:
            gram[n][m] = against(m, 96, 32)
        else:
            gram[n][m, 0:64, :] = against(m, 128, 64)
            square = against(m, 128, 64, slice(128, 192))
            gram[n][m, 64:96, :] = jnp.concatenate([square[0:32], square[32:64]], axis=1)

    def kernels(n, unfinished=None):
        z_rows, x_rows, y_rows = split[n]

        def id_at(step):
            return ahead_of(z, step // 4) * 4 + ahead_of(x, step & 3)

        def four(index, carry):
            steps = [index * 4 + more for more in range(8)]
            for step in steps[:4]:
                block_of(n, id_at(step))
            if unfinished is not None:
                standard(unfinished, [id_at(step & 15) for step in steps[4:]])
            for step in steps[:4]:
                major, minor = step // 4, step & 3
                m = ahead_of(z, major) * 4 + ahead_of(x, minor)

                @pl.when(major > 0)
                def _():
                    source = gram[n].at[m, pl.ds(0, z_rows)]
                    to_v = shard_at(ahead_of(z, major), x, y)
                    copy_to(source, z_parts[n].at[minor, major], part_send.at[n], z_recv.at[n, minor], j, to_v).start()

                @pl.when(minor > 0)
                def _():
                    source = gram[n].at[m, pl.ds(z_rows, x_rows)]
                    to_v = shard_at(z, ahead_of(x, minor), y)
                    copy_to(source, x_parts[n].at[major, minor], part_send.at[n], x_recv.at[n, major], j, to_v).start()

                if y_rows:
                    rows = pl.ds(pl.multiple_of(z_rows + x_rows + y_rows // 2 * (y ^ 1), 8), y_rows // 2)
                    copy_to(
                        gram[n].at[m, rows], y_parts.at[step], part_send.at[n], y_recv.at[major], j, v ^ 1
                    ).start()
            return carry

        with jax.named_scope("kernels"):
            if unfinished is not None:
                standard(unfinished, [id_at(step) for step in range(4)])
            lax.fori_loop(0, OWN // 4, four, 0)

    def second_sums(n):
        z_rows, x_rows, y_rows = split[n]

        def along(step, block):
            parts, recv, sums = ((z_parts, z_recv, z_sums), (x_parts, x_recv, x_sums))[block]
            with jax.named_scope("part_wait"):
                await_bytes(parts[n].at[step, pl.ds(1, 3)], recv.at[n, step])
            own = (ahead_of(z, step) * 4 + x) if block else (z * 4 + ahead_of(x, step))
            own = gram[n][own, pl.ds(z_rows, x_rows) if block else pl.ds(0, z_rows), :]
            sums[n][step] = (own + parts[n][step, 1]) + (parts[n][step, 2] + parts[n][step, 3])
            for other in range(2):
                side = y ^ other
                count = (z_rows, x_rows)[block] // 2
                rows = pl.ds(pl.multiple_of(side * count, 8), count)
                slot = step * 2 + other
                to_v = shard_at(ahead_of(z, step), x, side) if block else shard_at(z, ahead_of(x, step), side)
                if slot:
                    copy_to(
                        sums[n].at[step, rows], last[n][block].at[slot], sum_send.at[n], sum_recv.at[n, block], j, to_v
                    ).start()
                else:
                    last[n][block][0] = sums[n][0, rows, :]

        def from_side(major):
            with jax.named_scope("part_wait"):
                await_bytes(y_parts.at[pl.ds(major * 4, 4)], y_recv.at[major])
            for minor in range(4):
                step = major * 4 + minor
                to_z, to_x = ahead_of(z, major), ahead_of(x, minor)
                rows = pl.ds(pl.multiple_of(z_rows + x_rows + y_rows // 2 * y, 8), y_rows // 2)
                added = y_parts[step] + gram[n][to_z * 4 + to_x, rows, :]
                if step:
                    y_sums[step] = added
                    copy_to(
                        y_sums.at[step], y_last.at[step], sum_send.at[n], sum_recv.at[n, 2], j, shard_at(to_z, to_x, y)
                    ).start()
                else:
                    y_last[0] = added

        if y_rows:
            for major in range(4):
                along(major, 1)
                from_side(major)
            for step in range(4):
                along(step, 0)
        else:
            for step in range(4):
                along(step, 1)
            for step in range(4):
                along(step, 0)

    owner_v = v - y + j // 2
    place = core * 2 + y

    def hand_over(n):
        with jax.named_scope("last_wait"):
            for block, ref in enumerate(last[n]):
                await_bytes(ref.at[pl.ds(0, ref.shape[0] - 1)], sum_recv.at[n, block])
        mean = 1.0 / (VOX * SHARDS)
        first = 0
        for ref in last[n]:
            rows = ref.shape[1]
            total[n][pl.ds(first, rows), :] = jnp.sum(ref[...], axis=0) * mean
            first += rows
        for other in range(SUBJ):
            copy = copy_to(
                total[n], final[n].at[place], final_send.at[n], final_recv.at[n], (j ^ other) if other else j, owner_v
            )
            if other:
                copy.start()
            else:

                @pl.when(owner_v != v)
                def _():
                    copy.start()

        @pl.when(owner_v == v)
        def _():
            final[n][place] = total[n][...]

    def await_final(n, sem):
        @pl.when(owner_v == v)
        def _():
            await_bytes(final[n].at[pl.ds(0, SUBJ - 1)], sem.at[n])

        @pl.when(owner_v != v)
        def _():
            await_bytes(final[n], sem.at[n])

    def scores_of(correlated, finished):
        with jax.named_scope("scores"):
            if correlated is not None:
                correlate(correlated)
            if finished is not None:
                standard(finished)

    def relayed(g):
        with jax.named_scope("relay_wait"):
            for q in range(QUADS):
                relay_copy(g, q).wait_recv()

    scores_of(0, None)
    scores_of(1, 0)
    scores_of(2, 1)
    scores_of(3, 2)
    relayed(0)
    scores_of(4, 3)
    relay(1, 0)
    kernels(0)
    scores_of(5, 4)
    kernels(1, 5)
    relay(1, 1)
    second_sums(0)
    relay(1, 2)
    relayed(1)
    scores_of(6, None)
    scores_of(7, 6)
    kernels(2, 7)
    second_sums(1)
    hand_over(0)
    second_sums(2)
    hand_over(1)

    straight = (((1,), (0,)), ((), ()))
    left = lax.broadcasted_iota(I32, (EP * LOCAL, 128), 1) < 64
    upper = lax.broadcasted_iota(I32, (EP * LOCAL, 64), 1) < 32
    puts = (0, 384, 544, 864)

    def picked_by(pick, terms, dims):
        parts = [lax.dot_general(pick, t, dims, preferred_element_type=F32) for t in terms]
        return parts[0] + parts[1]

    def placed(n, i):
        pieces, first = [], 0
        for rows in split[n]:
            if rows:
                here = pl.ds(first, rows // 2)
                pieces += [final[n][2 * i, here, :], final[n][2 * i + 1, here, :]]
                first += rows // 2
        if n == 0:
            terms = two_terms(jnp.concatenate(pieces + [jnp.zeros((16, 128), F32)], axis=0))
            by_row = picked_by(pick_a[i], terms, straight)
            by_column = picked_by(turn_a[i], terms, NT)
            lines = [
                jnp.where(left, by_row[0:48], by_row[48:96]),
                jnp.where(left, by_row[96:144], by_row[144:192]),
                jnp.where(upper, by_column[0:48], by_column[96:144]),
                jnp.where(upper, by_column[48:96], by_column[144:192]),
            ]
        elif n == 1:
            terms = two_terms(jnp.concatenate(pieces, axis=0))
            lines = [picked_by(pick_b[i], terms, straight), picked_by(turn_b[i], terms, NT)]
        else:
            both = jnp.concatenate(pieces, axis=0)
            wide, square = two_terms(both[0:64]), two_terms(both[64:96])
            halves = [picked_by(pick_square[i, :, h * 32 : h * 32 + 32], square, straight) for h in range(2)]
            lines = [
                picked_by(pick_wide[i], wide, straight),
                jnp.where(left, halves[0], halves[1]),
                picked_by(turn_c[i], wide, NT),
            ]
        put = put_columns[i, puts[n] : puts[n + 1], :]
        terms = [jnp.dot(t, put, preferred_element_type=F32) for t in two_terms(jnp.concatenate(lines, axis=1))]
        return terms[0] + terms[1]

    with jax.named_scope("final"):
        await_final(0, final_recv)
    with jax.named_scope("place"):
        for i in range(2):
            out_ref[i] = placed(0, i)
    hand_over(2)
    with jax.named_scope("final"):
        await_final(1, final_recv)
    with jax.named_scope("place"):
        for i in range(2):
            out_ref[i] += placed(1, i)
    with jax.named_scope("final"):
        await_final(2, final_recv)
    with jax.named_scope("place"):
        for i in range(2):
            out_ref[i] += placed(2, i)

    with jax.named_scope("drain"):
        await_bytes(slab_in.at[pl.ds(0, SHARDS - 1)], share_send)

        @pl.when(own_group)
        def _():
            await_bytes(slab_in.at[pl.ds(0, SHARDS - 1)], slab_send)

        @pl.when(jnp.logical_not(own_group))
        def _():
            await_bytes(slab_in, slab_send)

        for n in range(3):
            await_bytes(z_parts[n].at[pl.ds(0, 3)], part_send.at[n])
            await_bytes(x_parts[n].at[pl.ds(0, 3)], part_send.at[n])
            for ref in last[n]:
                await_bytes(ref.at[pl.ds(0, ref.shape[0] - 1)], sum_send.at[n])
            await_final(n, final_send)
        await_bytes(y_parts, part_send.at[2])
        for q in range(QUADS):
            near_copy(q).wait_send()
            for h in range(2):
                far_copy(h, q).wait_send()
                relay_copy(h, q).wait_send()


def body(series, offsets, selected):
    vmem = pltpu.VMEM
    dma = pltpu.SemaphoreType.DMA
    return pl.pallas_call(
        main_kernel,
        out_shape=pltpu.VMEM((2, EP * LOCAL, ROWS), F32),
        in_specs=[
            pl.BlockSpec(memory_space=pl.ANY),
            pl.BlockSpec(memory_space=pl.ANY),
            pl.BlockSpec(memory_space=pl.ANY),
        ],
        out_specs=pl.BlockSpec(memory_space=pltpu.VMEM),
        scratch_shapes=[
            pltpu.SMEM((SUBJ * LOCAL, EP), I32),
            pltpu.SMEM((SEL,), I32),
            vmem((LOCAL, RUN, VOX), BF16),
            vmem((QUADS * 256, LOCAL * RUN), BF16),
            vmem((SUBJ, QUADS, 256, VOX), BF16),
            vmem((SUBJ, QUADS, 16, VOX), F32),
            vmem((SHARDS, 2, QUADS * 256), BF16),
            vmem((SHARDS, 2, QUADS * 256), BF16),
            vmem((2, QUADS * 256), BF16),
            vmem((SHARDS, 2, QUADS * 256), BF16),
            vmem((SUBJ * QUADS, OWN, 256), F32),
            vmem((SUBJ * QUADS, 256, 256), BF16),
            vmem((SUBJ * QUADS, 256, 256), BF16),
            vmem((SUBJ * QUADS, OWN, 256), F32),
            vmem((SUBJ * QUADS, OWN, 256), F32),
            vmem((QUADS, 256, 256), F32),
            vmem((QUADS, 256, 256), F32),
            vmem((OWN, ROWS, VOX), BF16),
            vmem((OWN, 48, 128), F32),
            vmem((OWN, 32, 128), F32),
            vmem((OWN, 96, 128), F32),
            vmem((4, 4, 32, 128), F32),
            vmem((4, 4, 16, 128), F32),
            vmem((4, 4, 32, 128), F32),
            vmem((4, 4, 16, 128), F32),
            vmem((4, 4, 16, 128), F32),
            vmem((4, 4, 32, 128), F32),
            vmem((OWN, 16, 128), F32),
            vmem((4, 32, 128), F32),
            vmem((4, 16, 128), F32),
            vmem((4, 32, 128), F32),
            vmem((4, 16, 128), F32),
            vmem((4, 16, 128), F32),
            vmem((4, 32, 128), F32),
            vmem((OWN, 16, 128), F32),
            vmem((8, 16, 128), F32),
            vmem((8, 8, 128), F32),
            vmem((8, 16, 128), F32),
            vmem((8, 8, 128), F32),
            vmem((8, 8, 128), F32),
            vmem((8, 16, 128), F32),
            vmem((OWN, 16, 128), F32),
            vmem((24, 128), F32),
            vmem((16, 128), F32),
            vmem((48, 128), F32),
            vmem((SUBJ, 24, 128), F32),
            vmem((SUBJ, 16, 128), F32),
            vmem((SUBJ, 48, 128), F32),
            vmem((2, 4 * EP * LOCAL, 64), BF16),
            vmem((2, EP * LOCAL, 32), BF16),
            vmem((2, EP * LOCAL, 64), BF16),
            vmem((2, EP * LOCAL, 64), BF16),
            vmem((2, 4 * EP * LOCAL, 128), BF16),
            vmem((2, EP * LOCAL, 128), BF16),
            vmem((2, EP * LOCAL, 128), BF16),
            vmem((2, 864, ROWS), BF16),
            dma((3,)),
            dma,
            dma,
            dma,
            dma,
            dma((QUADS,)),
            dma((QUADS,)),
            dma((2 * QUADS,)),
            dma((2 * QUADS,)),
            dma((2 * QUADS,)),
            dma((2 * QUADS,)),
            dma((3,)),
            dma((3, 4)),
            dma((3, 4)),
            dma((4,)),
            dma((3,)),
            dma((3, 3)),
            dma((3,)),
            dma((3,)),
        ],
        compiler_params=pltpu.CompilerParams(collective_id=0, has_side_effects=True),
    )(series, offsets, selected)


def solution(mesh):
    placed = (P("subj", None, "vox"), P(), P())
    return jax.shard_map(
        body, mesh=mesh, in_specs=placed, out_specs=P("vox", "subj", None), check_vma=False
    )
```

```python
import functools

import jax
import jax.numpy as jnp
from jax import lax
from jax.experimental import pallas as pl
from jax.experimental.pallas import tpu as pltpu
from jax.sharding import PartitionSpec as P

MESH = pl.DeviceIdType.MESH
F32, BF16, I32 = jnp.float32, jnp.bfloat16, jnp.int32
HIGH = lax.Precision.HIGHEST

SUBJ, SHARDS = 4, 32
TR, EP, RUN = 16, 12, 256
LOCAL = 4
QUADS = 3
SEL, OWN = 64, 16
VOX = 512
ROWS = SUBJ * EP * LOCAL
NT = (((1,), (1,)), ((), ()))
series_floor = 1.0
spread_floor = 0.05
shrink_factor = 0.9


def copy_to(src, dst, send_sem, recv_sem, subj, vox):
    return pltpu.make_async_remote_copy(
        src_ref=src,
        dst_ref=dst,
        send_sem=send_sem,
        recv_sem=recv_sem,
        device_id={"subj": subj, "vox": vox},
        device_id_type=MESH,
    )


def await_bytes(ref, sem):
    pltpu.make_async_copy(ref, ref, sem).wait()


def fold(x):
    return x + pltpu.roll(x, 4, 0)


def exact_terms(x):
    first = x.astype(BF16)
    rest = x - first.astype(F32)
    second = rest.astype(BF16)
    return first, second, (rest - second.astype(F32)).astype(BF16)


def two_terms(x):
    first = x.astype(BF16)
    return first, (x - first.astype(F32)).astype(BF16)


def slot_of(group, taker):
    return jnp.where((group ^ taker) < 2, group ^ taker, 2 + (group & 1))


def line_of(slot, epoch, subject):
    return slot * (EP * LOCAL) + epoch * LOCAL + subject


def main_kernel(
    series_hbm,
    offsets_hbm,
    selected_hbm,
    out_ref,
    offsets,
    selected,
    series,
    choose,
    epochs,
    scale,
    slab_out,
    slab_in,
    slab_sum,
    slab,
    raw,
    lhs_hi,
    lhs_lo,
    std_hi,
    std_lo,
    corr_even,
    corr_odd,
    score,
    gram_a,
    gram_b,
    gram_c,
    z_parts_a,
    z_parts_b,
    z_parts_c,
    x_parts_a,
    x_parts_b,
    x_parts_c,
    y_parts,
    z_sums_a,
    z_sums_b,
    z_sums_c,
    x_sums_a,
    x_sums_b,
    x_sums_c,
    y_sums,
    z_last_a,
    z_last_b,
    z_last_c,
    x_last_a,
    x_last_b,
    x_last_c,
    y_last,
    total_a,
    total_b,
    total_c,
    final_a,
    final_b,
    final_c,
    pick_a,
    pick_b,
    pick_wide,
    pick_square,
    turn_a,
    turn_b,
    turn_c,
    put_columns,
    load_sem,
    slab_send,
    slab_recv,
    share_send,
    share_recv,
    near_send,
    near_recv,
    far_send,
    far_recv,
    relay_send,
    relay_recv,
    part_send,
    z_recv,
    x_recv,
    y_recv,
    sum_send,
    sum_recv,
    final_send,
    final_recv,
):
    corr = (corr_even, corr_odd)
    z_parts, x_parts = (z_parts_a, z_parts_b, z_parts_c), (x_parts_a, x_parts_b, x_parts_c)
    z_sums, x_sums = (z_sums_a, z_sums_b, z_sums_c), (x_sums_a, x_sums_b, x_sums_c)
    last = ((z_last_a, x_last_a), (z_last_b, x_last_b), (z_last_c, x_last_c, y_last))
    gram = (gram_a, gram_b, gram_c)
    total, final = (total_a, total_b, total_c), (final_a, final_b, final_c)
    j = lax.axis_index("subj")
    v = lax.axis_index("vox")
    near, far, core = j ^ 1, j ^ 2, j & 1
    z, x, y = v // 8, (v // 2) & 3, v & 1

    def ahead_of(place, step):
        return (place + step) & 3

    def shard_at(z, x, y):
        return z * 8 + x * 2 + y

    loads = [
        pltpu.make_async_copy(source, target, load_sem.at[i])
        for i, (source, target) in enumerate(
            ((offsets_hbm, offsets), (selected_hbm, selected), (series_hbm, series))
        )
    ]
    for load in loads:
        load.start()

    barrier = pltpu.get_barrier_semaphore()

    def greet(step, carry):
        for other in range(SUBJ):
            pl.semaphore_signal(
                barrier,
                inc=1,
                device_id={"subj": j ^ other, "vox": (v + step) & (SHARDS - 1)},
                device_id_type=MESH,
            )
        return carry

    with jax.named_scope("greet"):
        lax.fori_loop(1, SHARDS, greet, 0, unroll=4)
        for other in range(1, SUBJ):
            pl.semaphore_signal(barrier, inc=1, device_id={"subj": j ^ other, "vox": v}, device_id_type=MESH)

    loads[0].wait()
    loads[1].wait()

    with jax.named_scope("choose"):
        row16 = lax.broadcasted_iota(I32, (16, 128), 0)
        scan = lax.broadcasted_iota(I32, (16, LOCAL * RUN), 1)
        for q in range(QUADS):
            start = jnp.zeros((16, 128), I32)
            for r in range(16):
                first = offsets[j * LOCAL + r % 4, q * 4 + r // 4] + (r % 4) * RUN
                start = jnp.where(row16 == r, first, start)
            ahead = scan - jnp.concatenate([start] * (LOCAL * RUN // 128), axis=1)
            for t in range(TR):
                choose[pl.ds(q * 256 + t * 16, 16), :] = jnp.where(ahead == t, 1.0, 0.0).astype(BF16)

    id_rows = []
    row8 = lax.broadcasted_iota(I32, (8, 128), 0)
    for block in range(SEL // 8):
        ids = jnp.zeros((8, 128), I32)
        for r in range(8):
            place = block * 8 + r
            ids = jnp.where(row8 == r, selected[4 * (place % OWN) + place // OWN], ids)
        id_rows.append(ids)
    ids = jnp.concatenate(id_rows, axis=0)
    columns = lax.broadcasted_iota(I32, (SEL, VOX), 1) + v * VOX
    picker = jnp.where(columns == jnp.concatenate([ids] * (VOX // 128), axis=1), 1.0, 0.0).astype(BF16)

    with jax.named_scope("pick_epochs"):
        loads[2].wait()
        runs = series[...].reshape(LOCAL * RUN, VOX)
        for q in range(QUADS):
            chosen = jnp.dot(choose[pl.ds(q * 256, 256), :], runs, preferred_element_type=F32).astype(BF16)
            for h in range(2):
                epochs[0, h, q] = chosen[:, h * 256 : h * 256 + 256]
            picked = lax.dot_general(picker, chosen, NT, preferred_element_type=F32)
            slab_out[:, :, pl.ds(q * 256, 256)] = picked.astype(BF16).reshape(SHARDS, 2, 256)

    with jax.named_scope("barrier"):
        pl.semaphore_wait(barrier, SUBJ * SHARDS - 1)

    def send_slab(step, carry):
        piece = (v + step) & (SHARDS - 1)
        to_j, to_v = piece // 8, j * 8 + (piece & 7)

        @pl.when(jnp.logical_or(to_j != j, to_v != v))
        def _():
            copy_to(slab_out.at[piece], slab_in.at[v], slab_send, slab_recv, to_j, to_v).start()

        return carry

    with jax.named_scope("send_slab"):
        lax.fori_loop(0, SHARDS, send_slab, 0)

    def near_copy(h):
        return copy_to(epochs.at[0, h], epochs.at[1, h], near_send.at[h], near_recv.at[h], near, v)

    def far_copy(g, q):
        at = g * QUADS + q
        source, target = epochs.at[core ^ g, core, q], epochs.at[2 + g, core, q]
        return copy_to(source, target, far_send.at[at], far_recv.at[at], far, v)

    def relay_copy(g, q):
        at = g * QUADS + q
        ref = epochs.at[2 + g, core, q]
        return copy_to(ref, ref, relay_send.at[at], relay_recv.at[at], near, v)

    def relay(g, q):
        with jax.named_scope("relay"):
            far_copy(g, q).wait_recv()
            relay_copy(g, q).start()

    for h in (1, 0):
        near_copy(h).start()

    @pl.when(core == 0)
    def _():
        far_copy(0, 0).start()

    def lanes_of(h):
        return pl.ds(h * 256 if isinstance(h, int) else pl.multiple_of(h * 256, 256), 256)

    def scales(r, h):
        lanes = lanes_of(h)
        for q in range(QUADS):
            seen = epochs[r, h, q].astype(F32).reshape(TR, 16, 256)
            centred = seen - (jnp.sum(seen, axis=0) * (1.0 / TR))[None]
            scale[r, q, :, lanes] = lax.rsqrt(jnp.sum(centred * centred, axis=0) + series_floor)

    for h in range(2):
        scales(0, h)

    with jax.named_scope("near_wait"):
        for h in range(2):
            near_copy(h).wait_recv()

    @pl.when(core == 1)
    def _():
        far_copy(0, 0).start()

    far_copy(0, 1).start()

    own_group = v // 8 == j

    with jax.named_scope("slab_wait"):

        @pl.when(own_group)
        def _():
            slab_in[v] = slab_out[j * 8 + (v & 7)]
            await_bytes(slab_in.at[pl.ds(0, SHARDS - 1)], slab_recv)

        @pl.when(jnp.logical_not(own_group))
        def _():
            await_bytes(slab_in, slab_recv)

    with jax.named_scope("slab_sum"):
        slab_sum[...] = jnp.sum(slab_in[...].astype(F32), axis=0).astype(BF16)

    def share_slab(step, carry):
        copy_to(slab_sum, slab.at[v], share_send, share_recv, j, (v + step) & (SHARDS - 1)).start()
        return carry

    with jax.named_scope("share_slab"):
        lax.fori_loop(1, SHARDS, share_slab, 0)
        slab[v] = slab_sum[...]

    far_copy(0, 2).start()
    for q in range(QUADS):
        far_copy(1, q).start()

    with jax.named_scope("places"):
        b = lax.broadcasted_iota(I32, (1, ROWS), 1)
        p = lax.broadcasted_iota(I32, (EP * LOCAL, 1), 0)
        for i in range(2):
            taker = y * 2 + i
            s = b // EP
            to = line_of(slot_of(s // LOCAL, taker), b - s * EP, s & 3)
            s = p // EP
            line = line_of(slot_of(j, taker), p - s * EP, s)

            def put(first, lines):
                put_columns[i, pl.ds(first, lines.shape[0]), :] = jnp.where(lines == to, 1.0, 0.0).astype(BF16)

            def hot(lines):
                return jnp.where(lines == line, 1.0, 0.0).astype(BF16)

            def down(count):
                return lax.broadcasted_iota(I32, (count, 1), 0)

            def across(count):
                return lax.broadcasted_iota(I32, (1, count), 1)

            c, r = down(128), down(64)
            around = (c & 63) + 64
            put(0, jnp.where(c < 64, c, c - 32))
            put(128, jnp.where(around < 96, around, around - 96))
            put(256, jnp.where(r < 32, r, jnp.where(r < 48, r + 32, -1)))
            put(320, jnp.where(r < 48, jnp.where(r < 32, r + 32, r + 48), -1))
            c, r = across(128), across(64)
            around = (c & 63) + 64
            apart = (c & 32) > 0
            for piece, (lines, columns) in enumerate(
                (
                    (jnp.where(r < 32, r, -1), jnp.where(apart & (c < 64), c, -1)),
                    (jnp.where(r < 32, r + 32, -1), jnp.where(apart & (c >= 64), c - 32, -1)),
                    (jnp.where((r >= 32) & (r < 48), r + 32, -1), jnp.where(apart & (c < 64), around - 96, -1)),
                    (jnp.where((r >= 32) & (r < 48), r + 48, -1), jnp.where(apart & (c >= 64), around - 96, -1)),
                )
            ):
                pick_a[i, pl.ds(piece * 48, 48), :] = hot(lines)
                turn_a[i, pl.ds(piece * 48, 48), :] = hot(columns)
            put(384, down(128))
            put(512, down(32) + 96)
            pick_b[i] = hot(across(32) + 96)
            turn_b[i] = hot(jnp.where(c < 96, c, -1))
            put(544, down(128))
            put(672, (down(128) & 63) + 128)
            put(800, down(64) + 128)
            pick_wide[i] = hot(r + 128)
            pick_square[i] = hot(r + 128)
            turn_c[i] = hot(c)
        for k in range(OWN):
            score[k, 96:128, :] = jnp.zeros((32, VOX), BF16)

    for h in range(2):
        scales(1, h)

    relay(0, 0)
    relay(0, 1)
    with jax.named_scope("share_wait"):
        await_bytes(slab.at[pl.ds(0, SHARDS - 1)], share_recv)
    relay(0, 2)

    with jax.named_scope("standard_slab"):
        for r in range(SUBJ):
            group = (j, near, far & 2, far | 1)[r]
            for kk in range(8):
                for q in range(QUADS):
                    raw[r * QUADS + q, pl.ds(kk * 2, 2), :] = slab[group * 8 + kk, :, pl.ds(q * 256, 256)].astype(F32)
        seen = raw[...].reshape(SUBJ * QUADS * OWN, 256)
        same = jnp.where(
            (lax.broadcasted_iota(I32, (256, 256), 0) & 15) == (lax.broadcasted_iota(I32, (256, 256), 1) & 15), 1.0, 0.0
        ).astype(BF16)
        centred = seen - jnp.dot(seen.astype(BF16), same, preferred_element_type=F32) * (1.0 / TR)
        terms = exact_terms(centred * centred)
        spread = [jnp.dot(t, same, preferred_element_type=F32) for t in terms]
        spread = spread[0] + spread[1] + spread[2]
        x_std = centred * lax.rsqrt(spread + series_floor) * shrink_factor
        x_hi = x_std.astype(BF16).astype(F32)
        std_hi[...] = x_hi.reshape(SUBJ * QUADS, OWN, 256)
        std_lo[...] = (x_std - x_hi).reshape(SUBJ * QUADS, OWN, 256)

    own_row = (lax.broadcasted_iota(I32, (16, 256), 1) & 15) == lax.broadcasted_iota(I32, (16, 256), 0)

    units = ((0, 0), (0, 1), (1, 0), (1, 1), (2, 0), (2, 1), (3, core), (3, 1 - core))

    def correlate(unit):
        r, h = units[unit]
        lanes = lanes_of(h)
        if r >= 2:
            scales(r, h)
        for q in range(QUADS):
            at = r * QUADS + q
            if unit % 2 == 0:
                for k in range(OWN):
                    for std, lhs in ((std_hi, lhs_hi), (std_lo, lhs_lo)):
                        line = jnp.broadcast_to(std[at, pl.ds(k, 1), :], (16, 256))
                        lhs[at, pl.ds(k * 16, 16), :] = jnp.where(own_row, line, 0.0).astype(BF16)
            seen = epochs[r, h, q]
            corr[unit % 2][q] = jnp.dot(lhs_hi[at], seen, preferred_element_type=F32) + jnp.dot(
                lhs_lo[at], seen, preferred_element_type=F32
            )

    def standard(unit, ids=range(OWN)):
        r, h = units[unit]
        lanes = lanes_of(h)
        for k in ids:
            rows = pl.ds(k * 16 if isinstance(k, int) else pl.multiple_of(k * 16, 16), 16)
            halves = []
            for q in range(QUADS):
                shrunk = corr[unit % 2][q, rows, :] * scale[r, q, :, lanes]
                twice = jnp.log(1.0 + shrunk) - jnp.log(1.0 - shrunk)
                halves += [twice[0:8], twice[8:16]]
            mean = fold(functools.reduce(jnp.add, halves)) * (1.0 / EP)
            halves = [f - mean for f in halves]
            spread = fold(functools.reduce(jnp.add, [f * f for f in halves])) * (1.0 / EP)
            gain = lax.rsqrt(spread + 4.0 * spread_floor)
            for q in range(QUADS):
                both = jnp.concatenate([halves[2 * q] * gain, halves[2 * q + 1] * gain], axis=0).astype(BF16)
                at = r * 48 + q * 16
                score[k, pl.ds(at, 16), lanes] = both

    split = ((32, 16, 0), (16, 16, 0), (32, 32, 32))
    lane = lax.broadcasted_iota(I32, (16, 128), 1)

    def against(m, first, count, columns=slice(0, 128)):
        return lax.dot_general(score[m, pl.ds(first, count), :], score[m, columns, :], NT, preferred_element_type=F32)

    def block_of(n, m):
        if n == 0:
            block = against(m, 0, 96)
            for top in (0, 16):
                beside = pltpu.roll(block[32 + top : 48 + top], 32, 1)
                gram[n][m, top : top + 16, :] = jnp.where(lane < 64, block[top : top + 16], beside)
            upper, lower = block[64:80], block[80:96]
            left = jnp.where(lane < 32, pltpu.roll(upper, 64, 1), pltpu.roll(upper, 32, 1))
            right = jnp.where(lane < 96, lower, pltpu.roll(lower, 96, 1))
            gram[n][m, 32:48, :] = jnp.where(lane < 64, left, right)
        elif n == 1:
            gram[n][m] = against(m, 96, 32)
        else:
            gram[n][m, 0:64, :] = against(m, 128, 64)
            square = against(m, 128, 64, slice(128, 192))
            gram[n][m, 64:96, :] = jnp.concatenate([square[0:32], square[32:64]], axis=1)

    def kernels(n, unfinished=None):
        z_rows, x_rows, y_rows = split[n]

        def id_at(step):
            return ahead_of(z, step // 4) * 4 + ahead_of(x, step & 3)

        def four(index, carry):
            steps = [index * 4 + more for more in range(8)]
            for step in steps[:4]:
                block_of(n, id_at(step))
            if unfinished is not None:
                standard(unfinished, [id_at(step & 15) for step in steps[4:]])
            for step in steps[:4]:
                major, minor = step // 4, step & 3
                m = ahead_of(z, major) * 4 + ahead_of(x, minor)

                @pl.when(major > 0)
                def _():
                    source = gram[n].at[m, pl.ds(0, z_rows)]
                    to_v = shard_at(ahead_of(z, major), x, y)
                    copy_to(source, z_parts[n].at[minor, major], part_send.at[n], z_recv.at[n, minor], j, to_v).start()

                @pl.when(minor > 0)
                def _():
                    source = gram[n].at[m, pl.ds(z_rows, x_rows)]
                    to_v = shard_at(z, ahead_of(x, minor), y)
                    copy_to(source, x_parts[n].at[major, minor], part_send.at[n], x_recv.at[n, major], j, to_v).start()

                if y_rows:
                    rows = pl.ds(pl.multiple_of(z_rows + x_rows + y_rows // 2 * (y ^ 1), 8), y_rows // 2)
                    copy_to(
                        gram[n].at[m, rows], y_parts.at[step], part_send.at[n], y_recv.at[major], j, v ^ 1
                    ).start()
            return carry

        with jax.named_scope("kernels"):
            if unfinished is not None:
                standard(unfinished, [id_at(step) for step in range(4)])
            lax.fori_loop(0, OWN // 4, four, 0)

    def second_sums(n):
        z_rows, x_rows, y_rows = split[n]

        def along(step, block):
            parts, recv, sums = ((z_parts, z_recv, z_sums), (x_parts, x_recv, x_sums))[block]
            with jax.named_scope("part_wait"):
                await_bytes(parts[n].at[step, pl.ds(1, 3)], recv.at[n, step])
            own = (ahead_of(z, step) * 4 + x) if block else (z * 4 + ahead_of(x, step))
            own = gram[n][own, pl.ds(z_rows, x_rows) if block else pl.ds(0, z_rows), :]
            sums[n][step] = (own + parts[n][step, 1]) + (parts[n][step, 2] + parts[n][step, 3])
            for other in range(2):
                side = y ^ other
                count = (z_rows, x_rows)[block] // 2
                rows = pl.ds(pl.multiple_of(side * count, 8), count)
                slot = step * 2 + other
                to_v = shard_at(ahead_of(z, step), x, side) if block else shard_at(z, ahead_of(x, step), side)
                if slot:
                    copy_to(
                        sums[n].at[step, rows], last[n][block].at[slot], sum_send.at[n], sum_recv.at[n, block], j, to_v
                    ).start()
                else:
                    last[n][block][0] = sums[n][0, rows, :]

        def from_side(major):
            with jax.named_scope("part_wait"):
                await_bytes(y_parts.at[pl.ds(major * 4, 4)], y_recv.at[major])
            for minor in range(4):
                step = major * 4 + minor
                to_z, to_x = ahead_of(z, major), ahead_of(x, minor)
                rows = pl.ds(pl.multiple_of(z_rows + x_rows + y_rows // 2 * y, 8), y_rows // 2)
                added = y_parts[step] + gram[n][to_z * 4 + to_x, rows, :]
                if step:
                    y_sums[step] = added
                    copy_to(
                        y_sums.at[step], y_last.at[step], sum_send.at[n], sum_recv.at[n, 2], j, shard_at(to_z, to_x, y)
                    ).start()
                else:
                    y_last[0] = added

        if y_rows:
            for major in range(4):
                along(major, 1)
                from_side(major)
            for step in range(4):
                along(step, 0)
        else:
            for step in range(4):
                along(step, 1)
            for step in range(4):
                along(step, 0)

    owner_v = v - y + j // 2
    place = core * 2 + y

    def hand_over(n):
        with jax.named_scope("last_wait"):
            for block, ref in enumerate(last[n]):
                await_bytes(ref.at[pl.ds(0, ref.shape[0] - 1)], sum_recv.at[n, block])
        mean = 1.0 / (VOX * SHARDS)
        first = 0
        for ref in last[n]:
            rows = ref.shape[1]
            total[n][pl.ds(first, rows), :] = jnp.sum(ref[...], axis=0) * mean
            first += rows
        for other in range(SUBJ):
            copy = copy_to(
                total[n], final[n].at[place], final_send.at[n], final_recv.at[n], (j ^ other) if other else j, owner_v
            )
            if other:
                copy.start()
            else:

                @pl.when(owner_v != v)
                def _():
                    copy.start()

        @pl.when(owner_v == v)
        def _():
            final[n][place] = total[n][...]

    def await_final(n, sem):
        @pl.when(owner_v == v)
        def _():
            await_bytes(final[n].at[pl.ds(0, SUBJ - 1)], sem.at[n])

        @pl.when(owner_v != v)
        def _():
            await_bytes(final[n], sem.at[n])

    def scores_of(correlated, finished):
        with jax.named_scope("scores"):
            if correlated is not None:
                correlate(correlated)
            if finished is not None:
                standard(finished)

    def relayed(g):
        with jax.named_scope("relay_wait"):
            for q in range(QUADS):
                relay_copy(g, q).wait_recv()

    scores_of(0, None)
    scores_of(1, 0)
    scores_of(2, 1)
    scores_of(3, 2)
    relayed(0)
    scores_of(4, 3)
    relay(1, 0)
    kernels(0)
    scores_of(5, 4)
    kernels(1, 5)
    relay(1, 1)
    relay(1, 2)
    scores_of(6, None)
    scores_of(None, 6)
    second_sums(0)
    relayed(1)
    scores_of(7, None)
    kernels(2, 7)
    second_sums(1)
    hand_over(0)
    second_sums(2)
    hand_over(1)

    straight = (((1,), (0,)), ((), ()))
    left = lax.broadcasted_iota(I32, (EP * LOCAL, 128), 1) < 64
    upper = lax.broadcasted_iota(I32, (EP * LOCAL, 64), 1) < 32
    puts = (0, 384, 544, 864)

    def picked_by(pick, terms, dims):
        parts = [lax.dot_general(pick, t, dims, preferred_element_type=F32) for t in terms]
        return parts[0] + parts[1]

    def placed(n, i):
        pieces, first = [], 0
        for rows in split[n]:
            if rows:
                here = pl.ds(first, rows // 2)
                pieces += [final[n][2 * i, here, :], final[n][2 * i + 1, here, :]]
                first += rows // 2
        if n == 0:
            terms = two_terms(jnp.concatenate(pieces + [jnp.zeros((16, 128), F32)], axis=0))
            by_row = picked_by(pick_a[i], terms, straight)
            by_column = picked_by(turn_a[i], terms, NT)
            lines = [
                jnp.where(left, by_row[0:48], by_row[48:96]),
                jnp.where(left, by_row[96:144], by_row[144:192]),
                jnp.where(upper, by_column[0:48], by_column[96:144]),
                jnp.where(upper, by_column[48:96], by_column[144:192]),
            ]
        elif n == 1:
            terms = two_terms(jnp.concatenate(pieces, axis=0))
            lines = [picked_by(pick_b[i], terms, straight), picked_by(turn_b[i], terms, NT)]
        else:
            both = jnp.concatenate(pieces, axis=0)
            wide, square = two_terms(both[0:64]), two_terms(both[64:96])
            halves = [picked_by(pick_square[i, :, h * 32 : h * 32 + 32], square, straight) for h in range(2)]
            lines = [
                picked_by(pick_wide[i], wide, straight),
                jnp.where(left, halves[0], halves[1]),
                picked_by(turn_c[i], wide, NT),
            ]
        put = put_columns[i, puts[n] : puts[n + 1], :]
        terms = [jnp.dot(t, put, preferred_element_type=F32) for t in two_terms(jnp.concatenate(lines, axis=1))]
        return terms[0] + terms[1]

    with jax.named_scope("final"):
        await_final(0, final_recv)
    with jax.named_scope("place"):
        for i in range(2):
            out_ref[i] = placed(0, i)
    hand_over(2)
    with jax.named_scope("final"):
        await_final(1, final_recv)
    with jax.named_scope("place"):
        for i in range(2):
            out_ref[i] += placed(1, i)
    with jax.named_scope("final"):
        await_final(2, final_recv)
    with jax.named_scope("place"):
        for i in range(2):
            out_ref[i] += placed(2, i)

    with jax.named_scope("drain"):
        await_bytes(slab_in.at[pl.ds(0, SHARDS - 1)], share_send)

        @pl.when(own_group)
        def _():
            await_bytes(slab_in.at[pl.ds(0, SHARDS - 1)], slab_send)

        @pl.when(jnp.logical_not(own_group))
        def _():
            await_bytes(slab_in, slab_send)

        for n in range(3):
            await_bytes(z_parts[n].at[pl.ds(0, 3)], part_send.at[n])
            await_bytes(x_parts[n].at[pl.ds(0, 3)], part_send.at[n])
            for ref in last[n]:
                await_bytes(ref.at[pl.ds(0, ref.shape[0] - 1)], sum_send.at[n])
            await_final(n, final_send)
        await_bytes(y_parts, part_send.at[2])
        for h in range(2):
            near_copy(h).wait_send()
            for q in range(QUADS):
                far_copy(h, q).wait_send()
                relay_copy(h, q).wait_send()


def body(series, offsets, selected):
    vmem = pltpu.VMEM
    dma = pltpu.SemaphoreType.DMA
    return pl.pallas_call(
        main_kernel,
        out_shape=pltpu.VMEM((2, EP * LOCAL, ROWS), F32),
        in_specs=[
            pl.BlockSpec(memory_space=pl.ANY),
            pl.BlockSpec(memory_space=pl.ANY),
            pl.BlockSpec(memory_space=pl.ANY),
        ],
        out_specs=pl.BlockSpec(memory_space=pltpu.VMEM),
        scratch_shapes=[
            pltpu.SMEM((SUBJ * LOCAL, EP), I32),
            pltpu.SMEM((SEL,), I32),
            vmem((LOCAL, RUN, VOX), BF16),
            vmem((QUADS * 256, LOCAL * RUN), BF16),
            vmem((SUBJ, 2, QUADS, 256, 256), BF16),
            vmem((SUBJ, QUADS, 16, VOX), F32),
            vmem((SHARDS, 2, QUADS * 256), BF16),
            vmem((SHARDS, 2, QUADS * 256), BF16),
            vmem((2, QUADS * 256), BF16),
            vmem((SHARDS, 2, QUADS * 256), BF16),
            vmem((SUBJ * QUADS, OWN, 256), F32),
            vmem((SUBJ * QUADS, 256, 256), BF16),
            vmem((SUBJ * QUADS, 256, 256), BF16),
            vmem((SUBJ * QUADS, OWN, 256), F32),
            vmem((SUBJ * QUADS, OWN, 256), F32),
            vmem((QUADS, 256, 256), F32),
            vmem((QUADS, 256, 256), F32),
            vmem((OWN, ROWS, VOX), BF16),
            vmem((OWN, 48, 128), F32),
            vmem((OWN, 32, 128), F32),
            vmem((OWN, 96, 128), F32),
            vmem((4, 4, 32, 128), F32),
            vmem((4, 4, 16, 128), F32),
            vmem((4, 4, 32, 128), F32),
            vmem((4, 4, 16, 128), F32),
            vmem((4, 4, 16, 128), F32),
            vmem((4, 4, 32, 128), F32),
            vmem((OWN, 16, 128), F32),
            vmem((4, 32, 128), F32),
            vmem((4, 16, 128), F32),
            vmem((4, 32, 128), F32),
            vmem((4, 16, 128), F32),
            vmem((4, 16, 128), F32),
            vmem((4, 32, 128), F32),
            vmem((OWN, 16, 128), F32),
            vmem((8, 16, 128), F32),
            vmem((8, 8, 128), F32),
            vmem((8, 16, 128), F32),
            vmem((8, 8, 128), F32),
            vmem((8, 8, 128), F32),
            vmem((8, 16, 128), F32),
            vmem((OWN, 16, 128), F32),
            vmem((24, 128), F32),
            vmem((16, 128), F32),
            vmem((48, 128), F32),
            vmem((SUBJ, 24, 128), F32),
            vmem((SUBJ, 16, 128), F32),
            vmem((SUBJ, 48, 128), F32),
            vmem((2, 4 * EP * LOCAL, 64), BF16),
            vmem((2, EP * LOCAL, 32), BF16),
            vmem((2, EP * LOCAL, 64), BF16),
            vmem((2, EP * LOCAL, 64), BF16),
            vmem((2, 4 * EP * LOCAL, 128), BF16),
            vmem((2, EP * LOCAL, 128), BF16),
            vmem((2, EP * LOCAL, 128), BF16),
            vmem((2, 864, ROWS), BF16),
            dma((3,)),
            dma,
            dma,
            dma,
            dma,
            dma((2,)),
            dma((2,)),
            dma((2 * QUADS,)),
            dma((2 * QUADS,)),
            dma((2 * QUADS,)),
            dma((2 * QUADS,)),
            dma((3,)),
            dma((3, 4)),
            dma((3, 4)),
            dma((4,)),
            dma((3,)),
            dma((3, 3)),
            dma((3,)),
            dma((3,)),
        ],
        compiler_params=pltpu.CompilerParams(collective_id=0, has_side_effects=True),
    )(series, offsets, selected)


def solution(mesh):
    placed = (P("subj", None, "vox"), P(), P())
    return jax.shard_map(
        body, mesh=mesh, in_specs=placed, out_specs=P("vox", "subj", None), check_vma=False
    )
```

```python
import functools

import jax
import jax.numpy as jnp
from jax import lax
from jax.experimental import pallas as pl
from jax.experimental.pallas import tpu as pltpu
from jax.sharding import PartitionSpec as P

MESH = pl.DeviceIdType.MESH
F32, BF16, I32 = jnp.float32, jnp.bfloat16, jnp.int32
HIGH = lax.Precision.HIGHEST

SUBJ, SHARDS = 4, 32
TR, EP, RUN = 16, 12, 256
LOCAL = 4
QUADS = 3
SEL, OWN = 64, 16
VOX = 512
ROWS = SUBJ * EP * LOCAL
NT = (((1,), (1,)), ((), ()))
series_floor = 1.0
spread_floor = 0.05
shrink_factor = 0.9


def copy_to(src, dst, send_sem, recv_sem, subj, vox):
    return pltpu.make_async_remote_copy(
        src_ref=src,
        dst_ref=dst,
        send_sem=send_sem,
        recv_sem=recv_sem,
        device_id={"subj": subj, "vox": vox},
        device_id_type=MESH,
    )


def await_bytes(ref, sem):
    pltpu.make_async_copy(ref, ref, sem).wait()


def fold(x):
    return x + pltpu.roll(x, 4, 0)


def exact_terms(x):
    first = x.astype(BF16)
    rest = x - first.astype(F32)
    second = rest.astype(BF16)
    return first, second, (rest - second.astype(F32)).astype(BF16)


def two_terms(x):
    first = x.astype(BF16)
    return first, (x - first.astype(F32)).astype(BF16)


def slot_of(group, taker):
    return jnp.where((group ^ taker) < 2, group ^ taker, 2 + (group & 1))


def line_of(slot, epoch, subject):
    return slot * (EP * LOCAL) + epoch * LOCAL + subject


def main_kernel(
    series_hbm,
    offsets_hbm,
    selected_hbm,
    out_ref,
    offsets,
    selected,
    series,
    choose,
    epochs,
    scale,
    slab_out,
    slab_in,
    slab_sum,
    slab,
    raw,
    lhs_hi,
    lhs_lo,
    std_hi,
    std_lo,
    corr_even,
    corr_odd,
    score,
    gram_a,
    gram_b,
    gram_c,
    z_parts_a,
    z_parts_b,
    z_parts_c,
    x_parts_a,
    x_parts_b,
    x_parts_c,
    y_parts,
    z_sums_a,
    z_sums_b,
    z_sums_c,
    x_sums_a,
    x_sums_b,
    x_sums_c,
    y_sums,
    z_last_a,
    z_last_b,
    z_last_c,
    x_last_a,
    x_last_b,
    x_last_c,
    y_last,
    total_a,
    total_b,
    total_c,
    final_a,
    final_b,
    final_c,
    pick_a,
    pick_b,
    pick_wide,
    pick_square,
    turn_a,
    turn_b,
    turn_c,
    put_columns,
    load_sem,
    slab_send,
    slab_recv,
    share_send,
    share_recv,
    near_send,
    near_recv,
    far_send,
    far_recv,
    relay_send,
    relay_recv,
    part_send,
    z_recv,
    x_recv,
    y_recv,
    sum_send,
    sum_recv,
    final_send,
    final_recv,
):
    corr = (corr_even, corr_odd)
    z_parts, x_parts = (z_parts_a, z_parts_b, z_parts_c), (x_parts_a, x_parts_b, x_parts_c)
    z_sums, x_sums = (z_sums_a, z_sums_b, z_sums_c), (x_sums_a, x_sums_b, x_sums_c)
    last = ((z_last_a, x_last_a), (z_last_b, x_last_b), (z_last_c, x_last_c, y_last))
    gram = (gram_a, gram_b, gram_c)
    total, final = (total_a, total_b, total_c), (final_a, final_b, final_c)
    j = lax.axis_index("subj")
    v = lax.axis_index("vox")
    near, far, core = j ^ 1, j ^ 2, j & 1
    z, x, y = v // 8, (v // 2) & 3, v & 1

    def ahead_of(place, step):
        return (place + step) & 3

    def shard_at(z, x, y):
        return z * 8 + x * 2 + y

    loads = [
        pltpu.make_async_copy(source, target, load_sem.at[i])
        for i, (source, target) in enumerate(
            ((offsets_hbm, offsets), (selected_hbm, selected), (series_hbm, series))
        )
    ]
    for load in loads:
        load.start()

    barrier = pltpu.get_barrier_semaphore()

    def greet(step, carry):
        for other in range(SUBJ):
            pl.semaphore_signal(
                barrier,
                inc=1,
                device_id={"subj": j ^ other, "vox": (v + step) & (SHARDS - 1)},
                device_id_type=MESH,
            )
        return carry

    with jax.named_scope("greet"):
        lax.fori_loop(1, SHARDS, greet, 0, unroll=4)
        for other in range(1, SUBJ):
            pl.semaphore_signal(barrier, inc=1, device_id={"subj": j ^ other, "vox": v}, device_id_type=MESH)

    loads[0].wait()
    loads[1].wait()

    with jax.named_scope("choose"):
        row16 = lax.broadcasted_iota(I32, (16, 128), 0)
        scan = lax.broadcasted_iota(I32, (16, LOCAL * RUN), 1)
        for q in range(QUADS):
            start = jnp.zeros((16, 128), I32)
            for r in range(16):
                first = offsets[j * LOCAL + r % 4, q * 4 + r // 4] + (r % 4) * RUN
                start = jnp.where(row16 == r, first, start)
            ahead = scan - jnp.concatenate([start] * (LOCAL * RUN // 128), axis=1)
            for t in range(TR):
                choose[pl.ds(q * 256 + t * 16, 16), :] = jnp.where(ahead == t, 1.0, 0.0).astype(BF16)

    id_rows = []
    row8 = lax.broadcasted_iota(I32, (8, 128), 0)
    for block in range(SEL // 8):
        ids = jnp.zeros((8, 128), I32)
        for r in range(8):
            place = block * 8 + r
            ids = jnp.where(row8 == r, selected[4 * (place % OWN) + place // OWN], ids)
        id_rows.append(ids)
    ids = jnp.concatenate(id_rows, axis=0)
    columns = lax.broadcasted_iota(I32, (SEL, VOX), 1) + v * VOX
    picker = jnp.where(columns == jnp.concatenate([ids] * (VOX // 128), axis=1), 1.0, 0.0).astype(BF16)

    with jax.named_scope("pick_epochs"):
        loads[2].wait()
        runs = series[...].reshape(LOCAL * RUN, VOX)
        all_chosen = jnp.dot(choose[...], runs, preferred_element_type=F32).astype(BF16)
        for q in range(QUADS):
            chosen = all_chosen[q * 256 : q * 256 + 256]
            for h in range(2):
                epochs[0, h, q] = chosen[:, h * 256 : h * 256 + 256]
            picked = lax.dot_general(picker, chosen, NT, preferred_element_type=F32)
            slab_out[:, :, pl.ds(q * 256, 256)] = picked.astype(BF16).reshape(SHARDS, 2, 256)

    with jax.named_scope("barrier"):
        pl.semaphore_wait(barrier, SUBJ * SHARDS - 1)

    def send_slab(step, carry):
        piece = (v + step) & (SHARDS - 1)
        to_j, to_v = piece // 8, j * 8 + (piece & 7)

        @pl.when(jnp.logical_or(to_j != j, to_v != v))
        def _():
            copy_to(slab_out.at[piece], slab_in.at[v], slab_send, slab_recv, to_j, to_v).start()

        return carry

    with jax.named_scope("send_slab"):
        lax.fori_loop(0, SHARDS, send_slab, 0)

    def near_copy(h):
        return copy_to(epochs.at[0, h], epochs.at[1, h], near_send.at[h], near_recv.at[h], near, v)

    def far_copy(g, q):
        at = g * QUADS + q
        source, target = epochs.at[core ^ g, core, q], epochs.at[2 + g, core, q]
        return copy_to(source, target, far_send.at[at], far_recv.at[at], far, v)

    def relay_copy(g, q):
        at = g * QUADS + q
        ref = epochs.at[2 + g, core, q]
        return copy_to(ref, ref, relay_send.at[at], relay_recv.at[at], near, v)

    def relay(g, q):
        with jax.named_scope("relay"):
            far_copy(g, q).wait_recv()
            relay_copy(g, q).start()

    for h in (1, 0):
        near_copy(h).start()

    @pl.when(core == 0)
    def _():
        far_copy(0, 0).start()

    def lanes_of(h):
        return pl.ds(h * 256 if isinstance(h, int) else pl.multiple_of(h * 256, 256), 256)

    def scales(r, h):
        lanes = lanes_of(h)
        for q in range(QUADS):
            seen = epochs[r, h, q].astype(F32).reshape(TR, 16, 256)
            centred = seen - (jnp.sum(seen, axis=0) * (1.0 / TR))[None]
            scale[r, q, :, lanes] = lax.rsqrt(jnp.sum(centred * centred, axis=0) + series_floor)

    for h in range(2):
        scales(0, h)

    with jax.named_scope("near_wait"):
        for h in range(2):
            near_copy(h).wait_recv()

    @pl.when(core == 1)
    def _():
        far_copy(0, 0).start()

    far_copy(0, 1).start()

    own_group = v // 8 == j

    with jax.named_scope("slab_wait"):

        @pl.when(own_group)
        def _():
            slab_in[v] = slab_out[j * 8 + (v & 7)]
            await_bytes(slab_in.at[pl.ds(0, SHARDS - 1)], slab_recv)

        @pl.when(jnp.logical_not(own_group))
        def _():
            await_bytes(slab_in, slab_recv)

    with jax.named_scope("slab_sum"):
        slab_sum[...] = jnp.sum(slab_in[...].astype(F32), axis=0).astype(BF16)

    def share_slab(step, carry):
        copy_to(slab_sum, slab.at[v], share_send, share_recv, j, (v + step) & (SHARDS - 1)).start()
        return carry

    with jax.named_scope("share_slab"):
        lax.fori_loop(1, SHARDS, share_slab, 0)
        slab[v] = slab_sum[...]

    far_copy(0, 2).start()
    for q in range(QUADS):
        far_copy(1, q).start()

    with jax.named_scope("places"):
        b = lax.broadcasted_iota(I32, (1, ROWS), 1)
        p = lax.broadcasted_iota(I32, (EP * LOCAL, 1), 0)
        for i in range(2):
            taker = y * 2 + i
            s = b // EP
            to = line_of(slot_of(s // LOCAL, taker), b - s * EP, s & 3)
            s = p // EP
            line = line_of(slot_of(j, taker), p - s * EP, s)

            def put(first, lines):
                put_columns[i, pl.ds(first, lines.shape[0]), :] = jnp.where(lines == to, 1.0, 0.0).astype(BF16)

            def hot(lines):
                return jnp.where(lines == line, 1.0, 0.0).astype(BF16)

            def down(count):
                return lax.broadcasted_iota(I32, (count, 1), 0)

            def across(count):
                return lax.broadcasted_iota(I32, (1, count), 1)

            c, r = down(128), down(64)
            around = (c & 63) + 64
            put(0, jnp.where(c < 64, c, c - 32))
            put(128, jnp.where(around < 96, around, around - 96))
            put(256, jnp.where(r < 32, r, jnp.where(r < 48, r + 32, -1)))
            put(320, jnp.where(r < 48, jnp.where(r < 32, r + 32, r + 48), -1))
            c, r = across(128), across(64)
            around = (c & 63) + 64
            apart = (c & 32) > 0
            for piece, (lines, columns) in enumerate(
                (
                    (jnp.where(r < 32, r, -1), jnp.where(apart & (c < 64), c, -1)),
                    (jnp.where(r < 32, r + 32, -1), jnp.where(apart & (c >= 64), c - 32, -1)),
                    (jnp.where((r >= 32) & (r < 48), r + 32, -1), jnp.where(apart & (c < 64), around - 96, -1)),
                    (jnp.where((r >= 32) & (r < 48), r + 48, -1), jnp.where(apart & (c >= 64), around - 96, -1)),
                )
            ):
                pick_a[i, pl.ds(piece * 48, 48), :] = hot(lines)
                turn_a[i, pl.ds(piece * 48, 48), :] = hot(columns)
            put(384, down(128))
            put(512, down(32) + 96)
            pick_b[i] = hot(across(32) + 96)
            turn_b[i] = hot(jnp.where(c < 96, c, -1))
            put(544, down(128))
            put(672, (down(128) & 63) + 128)
            put(800, down(64) + 128)
            pick_wide[i] = hot(r + 128)
            pick_square[i] = hot(r + 128)
            turn_c[i] = hot(c)
        for k in range(OWN):
            score[k, 96:128, :] = jnp.zeros((32, VOX), BF16)

    for h in range(2):
        scales(1, h)

    relay(0, 0)
    relay(0, 1)
    with jax.named_scope("share_wait"):
        await_bytes(slab.at[pl.ds(0, SHARDS - 1)], share_recv)
    relay(0, 2)

    with jax.named_scope("standard_slab"):
        for r in range(SUBJ):
            group = (j, near, far & 2, far | 1)[r]
            for kk in range(8):
                for q in range(QUADS):
                    raw[r * QUADS + q, pl.ds(kk * 2, 2), :] = slab[group * 8 + kk, :, pl.ds(q * 256, 256)].astype(F32)
        seen = raw[...].reshape(SUBJ * QUADS * OWN, 256)
        same = jnp.where(
            (lax.broadcasted_iota(I32, (256, 256), 0) & 15) == (lax.broadcasted_iota(I32, (256, 256), 1) & 15), 1.0, 0.0
        ).astype(BF16)
        centred = seen - jnp.dot(seen.astype(BF16), same, preferred_element_type=F32) * (1.0 / TR)
        terms = exact_terms(centred * centred)
        spread = [jnp.dot(t, same, preferred_element_type=F32) for t in terms]
        spread = spread[0] + spread[1] + spread[2]
        x_std = centred * lax.rsqrt(spread + series_floor) * shrink_factor
        x_hi = x_std.astype(BF16).astype(F32)
        std_hi[...] = x_hi.reshape(SUBJ * QUADS, OWN, 256)
        std_lo[...] = (x_std - x_hi).reshape(SUBJ * QUADS, OWN, 256)

    own_row = (lax.broadcasted_iota(I32, (16, 256), 1) & 15) == lax.broadcasted_iota(I32, (16, 256), 0)

    units = ((0, 0), (0, 1), (1, 0), (1, 1), (2, 0), (2, 1), (3, core), (3, 1 - core))

    def correlate(unit):
        r, h = units[unit]
        lanes = lanes_of(h)
        if r >= 2:
            scales(r, h)
        for q in range(QUADS):
            at = r * QUADS + q
            if unit % 2 == 0:
                for k in range(OWN):
                    for std, lhs in ((std_hi, lhs_hi), (std_lo, lhs_lo)):
                        line = jnp.broadcast_to(std[at, pl.ds(k, 1), :], (16, 256))
                        lhs[at, pl.ds(k * 16, 16), :] = jnp.where(own_row, line, 0.0).astype(BF16)
            seen = epochs[r, h, q]
            corr[unit % 2][q] = jnp.dot(lhs_hi[at], seen, preferred_element_type=F32) + jnp.dot(
                lhs_lo[at], seen, preferred_element_type=F32
            )

    def standard(unit, ids=range(OWN)):
        r, h = units[unit]
        lanes = lanes_of(h)
        for k in ids:
            rows = pl.ds(k * 16 if isinstance(k, int) else pl.multiple_of(k * 16, 16), 16)
            halves = []
            for q in range(QUADS):
                shrunk = corr[unit % 2][q, rows, :] * scale[r, q, :, lanes]
                twice = jnp.log(1.0 + shrunk) - jnp.log(1.0 - shrunk)
                halves += [twice[0:8], twice[8:16]]
            mean = fold(functools.reduce(jnp.add, halves)) * (1.0 / EP)
            halves = [f - mean for f in halves]
            spread = fold(functools.reduce(jnp.add, [f * f for f in halves])) * (1.0 / EP)
            gain = lax.rsqrt(spread + 4.0 * spread_floor)
            for q in range(QUADS):
                both = jnp.concatenate([halves[2 * q] * gain, halves[2 * q + 1] * gain], axis=0).astype(BF16)
                at = r * 48 + q * 16
                score[k, pl.ds(at, 16), lanes] = both

    split = ((32, 16, 0), (16, 16, 0), (32, 32, 32))
    lane = lax.broadcasted_iota(I32, (16, 128), 1)

    def against(m, first, count, columns=slice(0, 128)):
        return lax.dot_general(score[m, pl.ds(first, count), :], score[m, columns, :], NT, preferred_element_type=F32)

    def block_of(n, m):
        if n == 0:
            block = against(m, 0, 96)
            for top in (0, 16):
                beside = pltpu.roll(block[32 + top : 48 + top], 32, 1)
                gram[n][m, top : top + 16, :] = jnp.where(lane < 64, block[top : top + 16], beside)
            upper, lower = block[64:80], block[80:96]
            left = jnp.where(lane < 32, pltpu.roll(upper, 64, 1), pltpu.roll(upper, 32, 1))
            right = jnp.where(lane < 96, lower, pltpu.roll(lower, 96, 1))
            gram[n][m, 32:48, :] = jnp.where(lane < 64, left, right)
        elif n == 1:
            gram[n][m] = against(m, 96, 32)
        else:
            gram[n][m, 0:64, :] = against(m, 128, 64)
            square = against(m, 128, 64, slice(128, 192))
            gram[n][m, 64:96, :] = jnp.concatenate([square[0:32], square[32:64]], axis=1)

    def kernels(n, unfinished=None):
        z_rows, x_rows, y_rows = split[n]

        def offsets_at(step):
            slow, fast = (step // 4 + 1) & 3, (step + 1) & 3
            return slow ^ (slow >> 1), fast ^ (fast >> 1)

        def id_at(step):
            major, minor = offsets_at(step)
            return ahead_of(z, major) * 4 + ahead_of(x, minor)

        def four(index, carry):
            steps = [index * 4 + more for more in range(8)]
            for step in steps[:4]:
                block_of(n, id_at(step))
            if unfinished is not None:
                standard(unfinished, [id_at(step & 15) for step in steps[4:]])
            for step in steps[:4]:
                major, minor = offsets_at(step)
                m = ahead_of(z, major) * 4 + ahead_of(x, minor)

                @pl.when(major > 0)
                def _():
                    source = gram[n].at[m, pl.ds(0, z_rows)]
                    to_v = shard_at(ahead_of(z, major), x, y)
                    copy_to(source, z_parts[n].at[minor, major], part_send.at[n], z_recv.at[n, minor], j, to_v).start()

                @pl.when(minor > 0)
                def _():
                    source = gram[n].at[m, pl.ds(z_rows, x_rows)]
                    to_v = shard_at(z, ahead_of(x, minor), y)
                    copy_to(source, x_parts[n].at[major, minor], part_send.at[n], x_recv.at[n, major], j, to_v).start()

                if y_rows:
                    rows = pl.ds(pl.multiple_of(z_rows + x_rows + y_rows // 2 * (y ^ 1), 8), y_rows // 2)
                    copy_to(
                        gram[n].at[m, rows], y_parts.at[major * 4 + minor], part_send.at[n], y_recv.at[major], j, v ^ 1
                    ).start()
            return carry

        with jax.named_scope("kernels"):
            if unfinished is not None:
                standard(unfinished, [id_at(step) for step in range(4)])
            lax.fori_loop(0, OWN // 4, four, 0)

    def second_sums(n):
        z_rows, x_rows, y_rows = split[n]

        def along(step, block):
            parts, recv, sums = ((z_parts, z_recv, z_sums), (x_parts, x_recv, x_sums))[block]
            with jax.named_scope("part_wait"):
                await_bytes(parts[n].at[step, pl.ds(1, 3)], recv.at[n, step])
            own = (ahead_of(z, step) * 4 + x) if block else (z * 4 + ahead_of(x, step))
            own = gram[n][own, pl.ds(z_rows, x_rows) if block else pl.ds(0, z_rows), :]
            sums[n][step] = (own + parts[n][step, 1]) + (parts[n][step, 2] + parts[n][step, 3])
            for other in range(2):
                side = y ^ other
                count = (z_rows, x_rows)[block] // 2
                rows = pl.ds(pl.multiple_of(side * count, 8), count)
                slot = step * 2 + other
                to_v = shard_at(ahead_of(z, step), x, side) if block else shard_at(z, ahead_of(x, step), side)
                if slot:
                    copy_to(
                        sums[n].at[step, rows], last[n][block].at[slot], sum_send.at[n], sum_recv.at[n, block], j, to_v
                    ).start()
                else:
                    last[n][block][0] = sums[n][0, rows, :]

        def from_side(major):
            with jax.named_scope("part_wait"):
                await_bytes(y_parts.at[pl.ds(major * 4, 4)], y_recv.at[major])
            for minor in range(4):
                step = major * 4 + minor
                to_z, to_x = ahead_of(z, major), ahead_of(x, minor)
                rows = pl.ds(pl.multiple_of(z_rows + x_rows + y_rows // 2 * y, 8), y_rows // 2)
                added = y_parts[step] + gram[n][to_z * 4 + to_x, rows, :]
                if step:
                    y_sums[step] = added
                    copy_to(
                        y_sums.at[step], y_last.at[step], sum_send.at[n], sum_recv.at[n, 2], j, shard_at(to_z, to_x, y)
                    ).start()
                else:
                    y_last[0] = added

        if y_rows:
            for major in (1, 3, 2, 0):
                along(major, 1)
                from_side(major)
        else:
            for step in (1, 3, 2, 0):
                along(step, 1)
        for step in (1, 3, 2, 0):
            along(step, 0)

    owner_v = v - y + j // 2
    place = core * 2 + y

    def hand_over(n):
        with jax.named_scope("last_wait"):
            for block, ref in enumerate(last[n]):
                await_bytes(ref.at[pl.ds(0, ref.shape[0] - 1)], sum_recv.at[n, block])
        mean = 1.0 / (VOX * SHARDS)
        first = 0
        for ref in last[n]:
            rows = ref.shape[1]
            total[n][pl.ds(first, rows), :] = jnp.sum(ref[...], axis=0) * mean
            first += rows
        for other in range(SUBJ):
            copy = copy_to(
                total[n], final[n].at[place], final_send.at[n], final_recv.at[n], (j ^ other) if other else j, owner_v
            )
            if other:
                copy.start()
            else:

                @pl.when(owner_v != v)
                def _():
                    copy.start()

        @pl.when(owner_v == v)
        def _():
            final[n][place] = total[n][...]

    def await_final(n, sem):
        @pl.when(owner_v == v)
        def _():
            await_bytes(final[n].at[pl.ds(0, SUBJ - 1)], sem.at[n])

        @pl.when(owner_v != v)
        def _():
            await_bytes(final[n], sem.at[n])

    def scores_of(correlated, finished):
        with jax.named_scope("scores"):
            if correlated is not None:
                correlate(correlated)
            if finished is not None:
                standard(finished)

    def relayed(g):
        with jax.named_scope("relay_wait"):
            for q in range(QUADS):
                relay_copy(g, q).wait_recv()

    scores_of(0, None)
    scores_of(1, 0)
    scores_of(2, 1)
    scores_of(3, 2)
    relayed(0)
    scores_of(4, 3)
    relay(1, 0)
    kernels(0)
    scores_of(5, 4)
    kernels(1, 5)
    relay(1, 1)
    relay(1, 2)
    scores_of(6, None)
    scores_of(None, 6)
    second_sums(0)
    relayed(1)
    scores_of(7, None)
    kernels(2, 7)
    second_sums(1)
    second_sums(2)
    hand_over(0)
    hand_over(1)

    straight = (((1,), (0,)), ((), ()))
    left = lax.broadcasted_iota(I32, (EP * LOCAL, 128), 1) < 64
    upper = lax.broadcasted_iota(I32, (EP * LOCAL, 64), 1) < 32
    puts = (0, 384, 544, 864)

    def picked_by(pick, terms, dims):
        parts = [lax.dot_general(pick, t, dims, preferred_element_type=F32) for t in terms]
        return parts[0] + parts[1]

    def placed(n, i):
        pieces, first = [], 0
        for rows in split[n]:
            if rows:
                here = pl.ds(first, rows // 2)
                pieces += [final[n][2 * i, here, :], final[n][2 * i + 1, here, :]]
                first += rows // 2
        if n == 0:
            terms = two_terms(jnp.concatenate(pieces + [jnp.zeros((16, 128), F32)], axis=0))
            by_row = picked_by(pick_a[i], terms, straight)
            by_column = picked_by(turn_a[i], terms, NT)
            lines = [
                jnp.where(left, by_row[0:48], by_row[48:96]),
                jnp.where(left, by_row[96:144], by_row[144:192]),
                jnp.where(upper, by_column[0:48], by_column[96:144]),
                jnp.where(upper, by_column[48:96], by_column[144:192]),
            ]
        elif n == 1:
            terms = two_terms(jnp.concatenate(pieces, axis=0))
            lines = [picked_by(pick_b[i], terms, straight), picked_by(turn_b[i], terms, NT)]
        else:
            both = jnp.concatenate(pieces, axis=0)
            wide, square = two_terms(both[0:64]), two_terms(both[64:96])
            halves = [picked_by(pick_square[i, :, h * 32 : h * 32 + 32], square, straight) for h in range(2)]
            lines = [
                picked_by(pick_wide[i], wide, straight),
                jnp.where(left, halves[0], halves[1]),
                picked_by(turn_c[i], wide, NT),
            ]
        put = put_columns[i, puts[n] : puts[n + 1], :]
        terms = [jnp.dot(t, put, preferred_element_type=F32) for t in two_terms(jnp.concatenate(lines, axis=1))]
        return terms[0] + terms[1]

    with jax.named_scope("final"):
        await_final(0, final_recv)
    with jax.named_scope("place"):
        for i in range(2):
            out_ref[i] = placed(0, i)
    hand_over(2)
    with jax.named_scope("final"):
        await_final(1, final_recv)
    with jax.named_scope("place"):
        for i in range(2):
            out_ref[i] += placed(1, i)
    with jax.named_scope("final"):
        await_final(2, final_recv)
    with jax.named_scope("place"):
        for i in range(2):
            out_ref[i] += placed(2, i)

    with jax.named_scope("drain"):
        await_bytes(slab_in.at[pl.ds(0, SHARDS - 1)], share_send)

        @pl.when(own_group)
        def _():
            await_bytes(slab_in.at[pl.ds(0, SHARDS - 1)], slab_send)

        @pl.when(jnp.logical_not(own_group))
        def _():
            await_bytes(slab_in, slab_send)

        for n in range(3):
            await_bytes(z_parts[n].at[pl.ds(0, 3)], part_send.at[n])
            await_bytes(x_parts[n].at[pl.ds(0, 3)], part_send.at[n])
            for ref in last[n]:
                await_bytes(ref.at[pl.ds(0, ref.shape[0] - 1)], sum_send.at[n])
            await_final(n, final_send)
        await_bytes(y_parts, part_send.at[2])
        for h in range(2):
            near_copy(h).wait_send()
            for q in range(QUADS):
                far_copy(h, q).wait_send()
                relay_copy(h, q).wait_send()


def body(series, offsets, selected):
    vmem = pltpu.VMEM
    dma = pltpu.SemaphoreType.DMA
    return pl.pallas_call(
        main_kernel,
        out_shape=pltpu.VMEM((2, EP * LOCAL, ROWS), F32),
        in_specs=[
            pl.BlockSpec(memory_space=pl.ANY),
            pl.BlockSpec(memory_space=pl.ANY),
            pl.BlockSpec(memory_space=pl.ANY),
        ],
        out_specs=pl.BlockSpec(memory_space=pltpu.VMEM),
        scratch_shapes=[
            pltpu.SMEM((SUBJ * LOCAL, EP), I32),
            pltpu.SMEM((SEL,), I32),
            vmem((LOCAL, RUN, VOX), BF16),
            vmem((QUADS * 256, LOCAL * RUN), BF16),
            vmem((SUBJ, 2, QUADS, 256, 256), BF16),
            vmem((SUBJ, QUADS, 16, VOX), F32),
            vmem((SHARDS, 2, QUADS * 256), BF16),
            vmem((SHARDS, 2, QUADS * 256), BF16),
            vmem((2, QUADS * 256), BF16),
            vmem((SHARDS, 2, QUADS * 256), BF16),
            vmem((SUBJ * QUADS, OWN, 256), F32),
            vmem((SUBJ * QUADS, 256, 256), BF16),
            vmem((SUBJ * QUADS, 256, 256), BF16),
            vmem((SUBJ * QUADS, OWN, 256), F32),
            vmem((SUBJ * QUADS, OWN, 256), F32),
            vmem((QUADS, 256, 256), F32),
            vmem((QUADS, 256, 256), F32),
            vmem((OWN, ROWS, VOX), BF16),
            vmem((OWN, 48, 128), F32),
            vmem((OWN, 32, 128), F32),
            vmem((OWN, 96, 128), F32),
            vmem((4, 4, 32, 128), F32),
            vmem((4, 4, 16, 128), F32),
            vmem((4, 4, 32, 128), F32),
            vmem((4, 4, 16, 128), F32),
            vmem((4, 4, 16, 128), F32),
            vmem((4, 4, 32, 128), F32),
            vmem((OWN, 16, 128), F32),
            vmem((4, 32, 128), F32),
            vmem((4, 16, 128), F32),
            vmem((4, 32, 128), F32),
            vmem((4, 16, 128), F32),
            vmem((4, 16, 128), F32),
            vmem((4, 32, 128), F32),
            vmem((OWN, 16, 128), F32),
            vmem((8, 16, 128), F32),
            vmem((8, 8, 128), F32),
            vmem((8, 16, 128), F32),
            vmem((8, 8, 128), F32),
            vmem((8, 8, 128), F32),
            vmem((8, 16, 128), F32),
            vmem((OWN, 16, 128), F32),
            vmem((24, 128), F32),
            vmem((16, 128), F32),
            vmem((48, 128), F32),
            vmem((SUBJ, 24, 128), F32),
            vmem((SUBJ, 16, 128), F32),
            vmem((SUBJ, 48, 128), F32),
            vmem((2, 4 * EP * LOCAL, 64), BF16),
            vmem((2, EP * LOCAL, 32), BF16),
            vmem((2, EP * LOCAL, 64), BF16),
            vmem((2, EP * LOCAL, 64), BF16),
            vmem((2, 4 * EP * LOCAL, 128), BF16),
            vmem((2, EP * LOCAL, 128), BF16),
            vmem((2, EP * LOCAL, 128), BF16),
            vmem((2, 864, ROWS), BF16),
            dma((3,)),
            dma,
            dma,
            dma,
            dma,
            dma((2,)),
            dma((2,)),
            dma((2 * QUADS,)),
            dma((2 * QUADS,)),
            dma((2 * QUADS,)),
            dma((2 * QUADS,)),
            dma((3,)),
            dma((3, 4)),
            dma((3, 4)),
            dma((4,)),
            dma((3,)),
            dma((3, 3)),
            dma((3,)),
            dma((3,)),
        ],
        compiler_params=pltpu.CompilerParams(collective_id=0, has_side_effects=True),
    )(series, offsets, selected)


def solution(mesh):
    placed = (P("subj", None, "vox"), P(), P())
    return jax.shard_map(
        body, mesh=mesh, in_specs=placed, out_specs=P("vox", "subj", None), check_vma=False
    )
```

```python
import functools

import jax
import jax.numpy as jnp
from jax import lax
from jax.experimental import pallas as pl
from jax.experimental.pallas import tpu as pltpu
from jax.sharding import PartitionSpec as P

MESH = pl.DeviceIdType.MESH
F32, BF16, I32 = jnp.float32, jnp.bfloat16, jnp.int32
HIGH = lax.Precision.HIGHEST

SUBJ, SHARDS = 4, 32
TR, EP, RUN = 16, 12, 256
LOCAL = 4
QUADS = 3
SEL, OWN = 64, 16
VOX = 512
ROWS = SUBJ * EP * LOCAL
NT = (((1,), (1,)), ((), ()))
series_floor = 1.0
spread_floor = 0.05
shrink_factor = 0.9


def copy_to(src, dst, send_sem, recv_sem, subj, vox):
    return pltpu.make_async_remote_copy(
        src_ref=src,
        dst_ref=dst,
        send_sem=send_sem,
        recv_sem=recv_sem,
        device_id={"subj": subj, "vox": vox},
        device_id_type=MESH,
    )


def await_bytes(ref, sem):
    pltpu.make_async_copy(ref, ref, sem).wait()


def fold(x):
    return x + pltpu.roll(x, 4, 0)


def exact_terms(x):
    first = x.astype(BF16)
    rest = x - first.astype(F32)
    second = rest.astype(BF16)
    return first, second, (rest - second.astype(F32)).astype(BF16)


def two_terms(x):
    first = x.astype(BF16)
    return first, (x - first.astype(F32)).astype(BF16)


def slot_of(group, taker):
    return jnp.where((group ^ taker) < 2, group ^ taker, 2 + (group & 1))


def line_of(slot, epoch, subject):
    return slot * (EP * LOCAL) + epoch * LOCAL + subject


def main_kernel(
    series_hbm,
    offsets_hbm,
    selected_hbm,
    out_ref,
    offsets,
    selected,
    series,
    choose,
    epochs,
    scale,
    slab_out,
    slab_in,
    slab_sum,
    slab,
    raw,
    lhs_hi,
    lhs_lo,
    std_hi,
    std_lo,
    corr_even,
    corr_odd,
    score,
    gram_a,
    gram_b,
    gram_c,
    z_parts_a,
    z_parts_b,
    z_parts_c,
    x_parts_a,
    x_parts_b,
    x_parts_c,
    y_parts,
    z_sums_a,
    z_sums_b,
    z_sums_c,
    x_sums_a,
    x_sums_b,
    x_sums_c,
    y_sums,
    z_last_a,
    z_last_b,
    z_last_c,
    x_last_a,
    x_last_b,
    x_last_c,
    y_last,
    total_a,
    total_b,
    total_c,
    final_a,
    final_b,
    final_c,
    pick_a,
    pick_b,
    pick_wide,
    pick_square,
    turn_a,
    turn_b,
    turn_c,
    put_columns,
    load_sem,
    slab_send,
    slab_recv,
    share_send,
    share_recv,
    near_send,
    near_recv,
    far_send,
    far_recv,
    relay_send,
    relay_recv,
    part_send,
    z_recv,
    x_recv,
    y_recv,
    sum_send,
    sum_recv,
    final_send,
    final_recv,
):
    corr = (corr_even, corr_odd)
    z_parts, x_parts = (z_parts_a, z_parts_b, z_parts_c), (x_parts_a, x_parts_b, x_parts_c)
    z_sums, x_sums = (z_sums_a, z_sums_b, z_sums_c), (x_sums_a, x_sums_b, x_sums_c)
    last = ((z_last_a, x_last_a), (z_last_b, x_last_b), (z_last_c, x_last_c, y_last))
    gram = (gram_a, gram_b, gram_c)
    total, final = (total_a, total_b, total_c), (final_a, final_b, final_c)
    j = lax.axis_index("subj")
    v = lax.axis_index("vox")
    near, far, core = j ^ 1, j ^ 2, j & 1
    z, x, y = v // 8, (v // 2) & 3, v & 1

    def ahead_of(place, step):
        return (place + step) & 3

    def shard_at(z, x, y):
        return z * 8 + x * 2 + y

    loads = [
        pltpu.make_async_copy(source, target, load_sem.at[i])
        for i, (source, target) in enumerate(
            ((offsets_hbm, offsets), (selected_hbm, selected), (series_hbm, series))
        )
    ]
    for load in loads:
        load.start()

    barrier = pltpu.get_barrier_semaphore()

    def greet(step, carry):
        for other in range(SUBJ):
            pl.semaphore_signal(
                barrier,
                inc=1,
                device_id={"subj": j ^ other, "vox": (v + step) & (SHARDS - 1)},
                device_id_type=MESH,
            )
        return carry

    with jax.named_scope("greet"):
        lax.fori_loop(1, SHARDS, greet, 0, unroll=4)
        for other in range(1, SUBJ):
            pl.semaphore_signal(barrier, inc=1, device_id={"subj": j ^ other, "vox": v}, device_id_type=MESH)

    loads[0].wait()
    loads[1].wait()

    with jax.named_scope("choose"):
        row16 = lax.broadcasted_iota(I32, (16, 128), 0)
        scan = lax.broadcasted_iota(I32, (16, LOCAL * RUN), 1)
        for q in range(QUADS):
            start = jnp.zeros((16, 128), I32)
            for r in range(16):
                first = offsets[j * LOCAL + r % 4, q * 4 + r // 4] + (r % 4) * RUN
                start = jnp.where(row16 == r, first, start)
            ahead = scan - jnp.concatenate([start] * (LOCAL * RUN // 128), axis=1)
            for t in range(TR):
                choose[pl.ds(q * 256 + t * 16, 16), :] = jnp.where(ahead == t, 1.0, 0.0).astype(BF16)

    id_rows = []
    row8 = lax.broadcasted_iota(I32, (8, 128), 0)
    for block in range(SEL // 8):
        ids = jnp.zeros((8, 128), I32)
        for r in range(8):
            place = block * 8 + r
            ids = jnp.where(row8 == r, selected[4 * (place % OWN) + place // OWN], ids)
        id_rows.append(ids)
    ids = jnp.concatenate(id_rows, axis=0)
    columns = lax.broadcasted_iota(I32, (SEL, VOX), 1) + v * VOX
    picker = jnp.where(columns == jnp.concatenate([ids] * (VOX // 128), axis=1), 1.0, 0.0).astype(BF16)

    with jax.named_scope("pick_epochs"):
        loads[2].wait()
        runs = series[...].reshape(LOCAL * RUN, VOX)
        all_chosen = jnp.dot(choose[...], runs, preferred_element_type=F32).astype(BF16)
        for q in range(QUADS):
            chosen = all_chosen[q * 256 : q * 256 + 256]
            for h in range(2):
                epochs[0, h, q] = chosen[:, h * 256 : h * 256 + 256]
            picked = lax.dot_general(picker, chosen, NT, preferred_element_type=F32)
            slab_out[:, :, pl.ds(q * 256, 256)] = picked.astype(BF16).reshape(SHARDS, 2, 256)

    with jax.named_scope("barrier"):
        pl.semaphore_wait(barrier, SUBJ * SHARDS - 1)

    def send_slab(step, carry):
        piece = (v + step) & (SHARDS - 1)
        to_j, to_v = piece // 8, j * 8 + (piece & 7)

        @pl.when(jnp.logical_or(to_j != j, to_v != v))
        def _():
            copy_to(slab_out.at[piece], slab_in.at[v], slab_send, slab_recv, to_j, to_v).start()

        return carry

    with jax.named_scope("send_slab"):
        lax.fori_loop(0, SHARDS, send_slab, 0)

    def near_copy(h):
        return copy_to(epochs.at[0, h], epochs.at[1, h], near_send.at[h], near_recv.at[h], near, v)

    def far_copy(g, q):
        at = g * QUADS + q
        source, target = epochs.at[core ^ g, core, q], epochs.at[2 + g, core, q]
        return copy_to(source, target, far_send.at[at], far_recv.at[at], far, v)

    def relay_copy(g, q):
        at = g * QUADS + q
        ref = epochs.at[2 + g, core, q]
        return copy_to(ref, ref, relay_send.at[at], relay_recv.at[at], near, v)

    def relay(g, q):
        with jax.named_scope("relay"):
            far_copy(g, q).wait_recv()
            relay_copy(g, q).start()

    for h in (1, 0):
        near_copy(h).start()

    @pl.when(core == 0)
    def _():
        far_copy(0, 0).start()

    def lanes_of(h):
        return pl.ds(h * 256 if isinstance(h, int) else pl.multiple_of(h * 256, 256), 256)

    def scales(r, h):
        lanes = lanes_of(h)
        for q in range(QUADS):
            seen = epochs[r, h, q].astype(F32).reshape(TR, 16, 256)
            centred = seen - (jnp.sum(seen, axis=0) * (1.0 / TR))[None]
            scale[r, q, :, lanes] = lax.rsqrt(jnp.sum(centred * centred, axis=0) + series_floor)

    for h in range(2):
        scales(0, h)

    with jax.named_scope("near_wait"):
        for h in range(2):
            near_copy(h).wait_recv()

    @pl.when(core == 1)
    def _():
        far_copy(0, 0).start()

    far_copy(0, 1).start()

    own_group = v // 8 == j

    with jax.named_scope("slab_wait"):

        @pl.when(own_group)
        def _():
            slab_in[v] = slab_out[j * 8 + (v & 7)]
            await_bytes(slab_in.at[pl.ds(0, SHARDS - 1)], slab_recv)

        @pl.when(jnp.logical_not(own_group))
        def _():
            await_bytes(slab_in, slab_recv)

    with jax.named_scope("slab_sum"):
        slab_sum[...] = jnp.sum(slab_in[...].astype(F32), axis=0).astype(BF16)

    def share_slab(step, carry):
        copy_to(slab_sum, slab.at[v], share_send, share_recv, j, (v + step) & (SHARDS - 1)).start()
        return carry

    with jax.named_scope("share_slab"):
        lax.fori_loop(1, SHARDS, share_slab, 0)
        slab[v] = slab_sum[...]

    far_copy(0, 2).start()
    for q in range(QUADS):
        far_copy(1, q).start()

    with jax.named_scope("places"):
        b = lax.broadcasted_iota(I32, (1, ROWS), 1)
        p = lax.broadcasted_iota(I32, (EP * LOCAL, 1), 0)
        for i in range(2):
            taker = y * 2 + i
            s = b // EP
            to = line_of(slot_of(s // LOCAL, taker), b - s * EP, s & 3)
            s = p // EP
            line = line_of(slot_of(j, taker), p - s * EP, s)

            def put(first, lines):
                put_columns[i, pl.ds(first, lines.shape[0]), :] = jnp.where(lines == to, 1.0, 0.0).astype(BF16)

            def hot(lines):
                return jnp.where(lines == line, 1.0, 0.0).astype(BF16)

            def down(count):
                return lax.broadcasted_iota(I32, (count, 1), 0)

            def across(count):
                return lax.broadcasted_iota(I32, (1, count), 1)

            c, r = down(128), down(64)
            around = (c & 63) + 64
            put(0, jnp.where(c < 64, c, c - 32))
            put(128, jnp.where(around < 96, around, around - 96))
            put(256, jnp.where(r < 32, r, jnp.where(r < 48, r + 32, -1)))
            put(320, jnp.where(r < 48, jnp.where(r < 32, r + 32, r + 48), -1))
            c, r = across(128), across(64)
            around = (c & 63) + 64
            apart = (c & 32) > 0
            for piece, (lines, columns) in enumerate(
                (
                    (jnp.where(r < 32, r, -1), jnp.where(apart & (c < 64), c, -1)),
                    (jnp.where(r < 32, r + 32, -1), jnp.where(apart & (c >= 64), c - 32, -1)),
                    (jnp.where((r >= 32) & (r < 48), r + 32, -1), jnp.where(apart & (c < 64), around - 96, -1)),
                    (jnp.where((r >= 32) & (r < 48), r + 48, -1), jnp.where(apart & (c >= 64), around - 96, -1)),
                )
            ):
                pick_a[i, pl.ds(piece * 48, 48), :] = hot(lines)
                turn_a[i, pl.ds(piece * 48, 48), :] = hot(columns)
            put(384, down(128))
            put(512, down(48) + 96)
            pick_b[i] = hot(across(48) + 96)
            turn_b[i, 0:48, :] = hot(jnp.where(c < 96, c, -1))
            turn_b[i, 48:96, :] = hot(jnp.where(c < 96, -1, c))
            put(560, down(128))
            put(688, (down(128) & 63) + 128)
            put(816, down(48) + 144)
            pick_wide[i] = hot(across(48) + 144)
            pick_square[i] = hot(r + 128)
            turn_c[i] = hot(c)
        for k in range(OWN):
            score[k, 96:128, :] = jnp.zeros((32, VOX), BF16)

    for h in range(2):
        scales(1, h)

    relay(0, 0)
    relay(0, 1)
    with jax.named_scope("share_wait"):
        await_bytes(slab.at[pl.ds(0, SHARDS - 1)], share_recv)
    relay(0, 2)

    with jax.named_scope("standard_slab"):
        for r in range(SUBJ):
            group = (j, near, far & 2, far | 1)[r]
            for kk in range(8):
                for q in range(QUADS):
                    raw[r * QUADS + q, pl.ds(kk * 2, 2), :] = slab[group * 8 + kk, :, pl.ds(q * 256, 256)].astype(F32)
        seen = raw[...].reshape(SUBJ * QUADS * OWN, 256)
        same = jnp.where(
            (lax.broadcasted_iota(I32, (256, 256), 0) & 15) == (lax.broadcasted_iota(I32, (256, 256), 1) & 15), 1.0, 0.0
        ).astype(BF16)
        centred = seen - jnp.dot(seen.astype(BF16), same, preferred_element_type=F32) * (1.0 / TR)
        terms = exact_terms(centred * centred)
        spread = [jnp.dot(t, same, preferred_element_type=F32) for t in terms]
        spread = spread[0] + spread[1] + spread[2]
        x_std = centred * lax.rsqrt(spread + series_floor) * shrink_factor
        x_hi = x_std.astype(BF16).astype(F32)
        std_hi[...] = x_hi.reshape(SUBJ * QUADS, OWN, 256)
        std_lo[...] = (x_std - x_hi).reshape(SUBJ * QUADS, OWN, 256)

    own_row = (lax.broadcasted_iota(I32, (16, 256), 1) & 15) == lax.broadcasted_iota(I32, (16, 256), 0)

    units = ((0, 0), (0, 1), (1, 0), (1, 1), (2, 0), (2, 1), (3, core), (3, 1 - core))

    def correlate(unit):
        r, h = units[unit]
        lanes = lanes_of(h)
        if r >= 2:
            scales(r, h)
        for q in range(QUADS):
            at = r * QUADS + q
            if unit % 2 == 0:
                for k in range(OWN):
                    for std, lhs in ((std_hi, lhs_hi), (std_lo, lhs_lo)):
                        line = jnp.broadcast_to(std[at, pl.ds(k, 1), :], (16, 256))
                        lhs[at, pl.ds(k * 16, 16), :] = jnp.where(own_row, line, 0.0).astype(BF16)
            seen = epochs[r, h, q]
            corr[unit % 2][q] = jnp.dot(lhs_hi[at], seen, preferred_element_type=F32) + jnp.dot(
                lhs_lo[at], seen, preferred_element_type=F32
            )

    def standard(unit, ids=range(OWN)):
        r, h = units[unit]
        lanes = lanes_of(h)
        for k in ids:
            rows = pl.ds(k * 16 if isinstance(k, int) else pl.multiple_of(k * 16, 16), 16)
            halves = []
            for q in range(QUADS):
                shrunk = corr[unit % 2][q, rows, :] * scale[r, q, :, lanes]
                twice = jnp.log(1.0 + shrunk) - jnp.log(1.0 - shrunk)
                halves += [twice[0:8], twice[8:16]]
            mean = fold(functools.reduce(jnp.add, halves)) * (1.0 / EP)
            halves = [f - mean for f in halves]
            spread = fold(functools.reduce(jnp.add, [f * f for f in halves])) * (1.0 / EP)
            gain = lax.rsqrt(spread + 4.0 * spread_floor)
            for q in range(QUADS):
                both = jnp.concatenate([halves[2 * q] * gain, halves[2 * q + 1] * gain], axis=0).astype(BF16)
                at = r * 48 + q * 16
                score[k, pl.ds(at, 16), lanes] = both

    split = ((32, 16, 0), (16, 32, 0), (32, 32, 16))
    lane = lax.broadcasted_iota(I32, (16, 128), 1)

    def against(m, first, count, columns=slice(0, 128)):
        return lax.dot_general(score[m, pl.ds(first, count), :], score[m, columns, :], NT, preferred_element_type=F32)

    def block_of(n, m):
        if n == 0:
            block = against(m, 0, 96)
            for top in (0, 16):
                beside = pltpu.roll(block[32 + top : 48 + top], 32, 1)
                gram[n][m, top : top + 16, :] = jnp.where(lane < 64, block[top : top + 16], beside)
            upper, lower = block[64:80], block[80:96]
            left = jnp.where(lane < 32, pltpu.roll(upper, 64, 1), pltpu.roll(upper, 32, 1))
            right = jnp.where(lane < 96, lower, pltpu.roll(lower, 96, 1))
            gram[n][m, 32:48, :] = jnp.where(lane < 64, left, right)
        elif n == 1:
            gram[n][m] = against(m, 96, 48)
        else:
            gram[n][m, 0:48, :] = against(m, 144, 48)
            square = against(m, 128, 64, slice(128, 192))
            gram[n][m, 48:80, :] = jnp.concatenate([square[0:32], square[32:64]], axis=1)

    def kernels(n, unfinished=None):
        z_rows, x_rows, y_rows = split[n]

        def offsets_at(step):
            slow, fast = (step // 4 + 1) & 3, (step + 1) & 3
            return slow ^ (slow >> 1), fast ^ (fast >> 1)

        def id_at(step):
            major, minor = offsets_at(step)
            return ahead_of(z, major) * 4 + ahead_of(x, minor)

        def four(index, carry):
            steps = [index * 4 + more for more in range(8)]
            for step in steps[:4]:
                block_of(n, id_at(step))
            if unfinished is not None:
                standard(unfinished, [id_at(step & 15) for step in steps[4:]])
            for step in steps[:4]:
                major, minor = offsets_at(step)
                m = ahead_of(z, major) * 4 + ahead_of(x, minor)

                @pl.when(major > 0)
                def _():
                    source = gram[n].at[m, pl.ds(0, z_rows)]
                    to_v = shard_at(ahead_of(z, major), x, y)
                    copy_to(source, z_parts[n].at[minor, major], part_send.at[n], z_recv.at[n, minor], j, to_v).start()

                @pl.when(minor > 0)
                def _():
                    source = gram[n].at[m, pl.ds(z_rows, x_rows)]
                    to_v = shard_at(z, ahead_of(x, minor), y)
                    copy_to(source, x_parts[n].at[major, minor], part_send.at[n], x_recv.at[n, major], j, to_v).start()

                if y_rows:
                    rows = pl.ds(pl.multiple_of(z_rows + x_rows + y_rows // 2 * (y ^ 1), 8), y_rows // 2)
                    copy_to(
                        gram[n].at[m, rows], y_parts.at[major * 4 + minor], part_send.at[n], y_recv.at[major], j, v ^ 1
                    ).start()
            return carry

        with jax.named_scope("kernels"):
            if unfinished is not None:
                standard(unfinished, [id_at(step) for step in range(4)])
            lax.fori_loop(0, OWN // 4, four, 0)

    def second_sums(n):
        z_rows, x_rows, y_rows = split[n]

        def along(step, block):
            parts, recv, sums = ((z_parts, z_recv, z_sums), (x_parts, x_recv, x_sums))[block]
            with jax.named_scope("part_wait"):
                await_bytes(parts[n].at[step, pl.ds(1, 3)], recv.at[n, step])
            own = (ahead_of(z, step) * 4 + x) if block else (z * 4 + ahead_of(x, step))
            own = gram[n][own, pl.ds(z_rows, x_rows) if block else pl.ds(0, z_rows), :]
            sums[n][step] = (own + parts[n][step, 1]) + (parts[n][step, 2] + parts[n][step, 3])
            for other in range(2):
                side = y ^ other
                count = (z_rows, x_rows)[block] // 2
                rows = pl.ds(pl.multiple_of(side * count, 8), count)
                slot = step * 2 + other
                to_v = shard_at(ahead_of(z, step), x, side) if block else shard_at(z, ahead_of(x, step), side)
                if slot:
                    copy_to(
                        sums[n].at[step, rows], last[n][block].at[slot], sum_send.at[n], sum_recv.at[n, block], j, to_v
                    ).start()
                else:
                    last[n][block][0] = sums[n][0, rows, :]

        def from_side(major):
            with jax.named_scope("part_wait"):
                await_bytes(y_parts.at[pl.ds(major * 4, 4)], y_recv.at[major])
            for minor in range(4):
                step = major * 4 + minor
                to_z, to_x = ahead_of(z, major), ahead_of(x, minor)
                rows = pl.ds(pl.multiple_of(z_rows + x_rows + y_rows // 2 * y, 8), y_rows // 2)
                added = y_parts[step] + gram[n][to_z * 4 + to_x, rows, :]
                if step:
                    y_sums[step] = added
                    copy_to(
                        y_sums.at[step], y_last.at[step], sum_send.at[n], sum_recv.at[n, 2], j, shard_at(to_z, to_x, y)
                    ).start()
                else:
                    y_last[0] = added

        if y_rows:
            for major in (1, 3, 2, 0):
                along(major, 1)
                from_side(major)
        else:
            for step in (1, 3, 2, 0):
                along(step, 1)
        for step in (1, 3, 2, 0):
            along(step, 0)

    owner_v = v - y + j // 2
    place = core * 2 + y

    def hand_over(n):
        with jax.named_scope("last_wait"):
            for block, ref in enumerate(last[n]):
                await_bytes(ref.at[pl.ds(0, ref.shape[0] - 1)], sum_recv.at[n, block])
        mean = 1.0 / (VOX * SHARDS)
        first = 0
        for ref in last[n]:
            rows = ref.shape[1]
            total[n][pl.ds(first, rows), :] = jnp.sum(ref[...], axis=0) * mean
            first += rows
        for other in range(SUBJ):
            copy = copy_to(
                total[n], final[n].at[place], final_send.at[n], final_recv.at[n], (j ^ other) if other else j, owner_v
            )
            if other:
                copy.start()
            else:

                @pl.when(owner_v != v)
                def _():
                    copy.start()

        @pl.when(owner_v == v)
        def _():
            final[n][place] = total[n][...]

    def await_final(n, sem):
        @pl.when(owner_v == v)
        def _():
            await_bytes(final[n].at[pl.ds(0, SUBJ - 1)], sem.at[n])

        @pl.when(owner_v != v)
        def _():
            await_bytes(final[n], sem.at[n])

    def scores_of(correlated, finished):
        with jax.named_scope("scores"):
            if correlated is not None:
                correlate(correlated)
            if finished is not None:
                standard(finished)

    def relayed(g):
        with jax.named_scope("relay_wait"):
            for q in range(QUADS):
                relay_copy(g, q).wait_recv()

    scores_of(0, None)
    scores_of(1, 0)
    scores_of(2, 1)
    scores_of(3, 2)
    relayed(0)
    scores_of(4, 3)
    relay(1, 0)
    kernels(0)
    scores_of(5, 4)
    kernels(1, 5)
    relay(1, 1)
    relay(1, 2)
    scores_of(6, None)
    scores_of(None, 6)
    second_sums(0)
    relayed(1)
    scores_of(7, None)
    kernels(2, 7)
    second_sums(1)
    second_sums(2)
    hand_over(0)
    hand_over(1)

    straight = (((1,), (0,)), ((), ()))
    left = lax.broadcasted_iota(I32, (EP * LOCAL, 128), 1) < 64
    upper = lax.broadcasted_iota(I32, (EP * LOCAL, 64), 1) < 32
    puts = (0, 384, 560, 864)
    corner = lax.broadcasted_iota(I32, (EP * LOCAL, 48), 1) >= 32

    def picked_by(pick, terms, dims):
        parts = [lax.dot_general(pick, t, dims, preferred_element_type=F32) for t in terms]
        return parts[0] + parts[1]

    def placed(n, i):
        pieces, first = [], 0
        for rows in split[n]:
            if rows:
                here = pl.ds(first, rows // 2)
                pieces += [final[n][2 * i, here, :], final[n][2 * i + 1, here, :]]
                first += rows // 2
        if n == 0:
            terms = two_terms(jnp.concatenate(pieces + [jnp.zeros((16, 128), F32)], axis=0))
            by_row = picked_by(pick_a[i], terms, straight)
            by_column = picked_by(turn_a[i], terms, NT)
            lines = [
                jnp.where(left, by_row[0:48], by_row[48:96]),
                jnp.where(left, by_row[96:144], by_row[144:192]),
                jnp.where(upper, by_column[0:48], by_column[96:144]),
                jnp.where(upper, by_column[48:96], by_column[144:192]),
            ]
        elif n == 1:
            terms = two_terms(jnp.concatenate(pieces, axis=0))
            by_column = picked_by(turn_b[i], terms, NT)
            turned = by_column[0:48] + jnp.where(corner, by_column[48:96], 0.0)
            lines = [picked_by(pick_b[i], terms, straight), turned]
        else:
            both = jnp.concatenate(pieces, axis=0)
            wide, square = two_terms(both[0:48]), two_terms(both[48:80])
            halves = [picked_by(pick_square[i, :, h * 32 : h * 32 + 32], square, straight) for h in range(2)]
            lines = [
                picked_by(pick_wide[i], wide, straight),
                jnp.where(left, halves[0], halves[1]),
                picked_by(turn_c[i], wide, NT),
            ]
        put = put_columns[i, puts[n] : puts[n + 1], :]
        terms = [jnp.dot(t, put, preferred_element_type=F32) for t in two_terms(jnp.concatenate(lines, axis=1))]
        return terms[0] + terms[1]

    with jax.named_scope("final"):
        await_final(0, final_recv)
    with jax.named_scope("place"):
        for i in range(2):
            out_ref[i] = placed(0, i)
    hand_over(2)
    with jax.named_scope("final"):
        await_final(1, final_recv)
    with jax.named_scope("place"):
        for i in range(2):
            out_ref[i] += placed(1, i)
    with jax.named_scope("final"):
        await_final(2, final_recv)
    with jax.named_scope("place"):
        for i in range(2):
            out_ref[i] += placed(2, i)

    with jax.named_scope("drain"):
        await_bytes(slab_in.at[pl.ds(0, SHARDS - 1)], share_send)

        @pl.when(own_group)
        def _():
            await_bytes(slab_in.at[pl.ds(0, SHARDS - 1)], slab_send)

        @pl.when(jnp.logical_not(own_group))
        def _():
            await_bytes(slab_in, slab_send)

        for n in range(3):
            await_bytes(z_parts[n].at[pl.ds(0, 3)], part_send.at[n])
            await_bytes(x_parts[n].at[pl.ds(0, 3)], part_send.at[n])
            for ref in last[n]:
                await_bytes(ref.at[pl.ds(0, ref.shape[0] - 1)], sum_send.at[n])
            await_final(n, final_send)
        await_bytes(y_parts, part_send.at[2])
        for h in range(2):
            near_copy(h).wait_send()
            for q in range(QUADS):
                far_copy(h, q).wait_send()
                relay_copy(h, q).wait_send()


def body(series, offsets, selected):
    vmem = pltpu.VMEM
    dma = pltpu.SemaphoreType.DMA
    return pl.pallas_call(
        main_kernel,
        out_shape=pltpu.VMEM((2, EP * LOCAL, ROWS), F32),
        in_specs=[
            pl.BlockSpec(memory_space=pl.ANY),
            pl.BlockSpec(memory_space=pl.ANY),
            pl.BlockSpec(memory_space=pl.ANY),
        ],
        out_specs=pl.BlockSpec(memory_space=pltpu.VMEM),
        scratch_shapes=[
            pltpu.SMEM((SUBJ * LOCAL, EP), I32),
            pltpu.SMEM((SEL,), I32),
            vmem((LOCAL, RUN, VOX), BF16),
            vmem((QUADS * 256, LOCAL * RUN), BF16),
            vmem((SUBJ, 2, QUADS, 256, 256), BF16),
            vmem((SUBJ, QUADS, 16, VOX), F32),
            vmem((SHARDS, 2, QUADS * 256), BF16),
            vmem((SHARDS, 2, QUADS * 256), BF16),
            vmem((2, QUADS * 256), BF16),
            vmem((SHARDS, 2, QUADS * 256), BF16),
            vmem((SUBJ * QUADS, OWN, 256), F32),
            vmem((SUBJ * QUADS, 256, 256), BF16),
            vmem((SUBJ * QUADS, 256, 256), BF16),
            vmem((SUBJ * QUADS, OWN, 256), F32),
            vmem((SUBJ * QUADS, OWN, 256), F32),
            vmem((QUADS, 256, 256), F32),
            vmem((QUADS, 256, 256), F32),
            vmem((OWN, ROWS, VOX), BF16),
            vmem((OWN, 48, 128), F32),
            vmem((OWN, 48, 128), F32),
            vmem((OWN, 80, 128), F32),
            vmem((4, 4, 32, 128), F32),
            vmem((4, 4, 16, 128), F32),
            vmem((4, 4, 32, 128), F32),
            vmem((4, 4, 16, 128), F32),
            vmem((4, 4, 32, 128), F32),
            vmem((4, 4, 32, 128), F32),
            vmem((OWN, 8, 128), F32),
            vmem((4, 32, 128), F32),
            vmem((4, 16, 128), F32),
            vmem((4, 32, 128), F32),
            vmem((4, 16, 128), F32),
            vmem((4, 32, 128), F32),
            vmem((4, 32, 128), F32),
            vmem((OWN, 8, 128), F32),
            vmem((8, 16, 128), F32),
            vmem((8, 8, 128), F32),
            vmem((8, 16, 128), F32),
            vmem((8, 8, 128), F32),
            vmem((8, 16, 128), F32),
            vmem((8, 16, 128), F32),
            vmem((OWN, 8, 128), F32),
            vmem((24, 128), F32),
            vmem((24, 128), F32),
            vmem((40, 128), F32),
            vmem((SUBJ, 24, 128), F32),
            vmem((SUBJ, 24, 128), F32),
            vmem((SUBJ, 40, 128), F32),
            vmem((2, 4 * EP * LOCAL, 64), BF16),
            vmem((2, EP * LOCAL, 48), BF16),
            vmem((2, EP * LOCAL, 48), BF16),
            vmem((2, EP * LOCAL, 64), BF16),
            vmem((2, 4 * EP * LOCAL, 128), BF16),
            vmem((2, 2 * EP * LOCAL, 128), BF16),
            vmem((2, EP * LOCAL, 128), BF16),
            vmem((2, 864, ROWS), BF16),
            dma((3,)),
            dma,
            dma,
            dma,
            dma,
            dma((2,)),
            dma((2,)),
            dma((2 * QUADS,)),
            dma((2 * QUADS,)),
            dma((2 * QUADS,)),
            dma((2 * QUADS,)),
            dma((3,)),
            dma((3, 4)),
            dma((3, 4)),
            dma((4,)),
            dma((3,)),
            dma((3, 3)),
            dma((3,)),
            dma((3,)),
        ],
        compiler_params=pltpu.CompilerParams(collective_id=0, has_side_effects=True),
    )(series, offsets, selected)


def solution(mesh):
    placed = (P("subj", None, "vox"), P(), P())
    return jax.shard_map(
        body, mesh=mesh, in_specs=placed, out_specs=P("vox", "subj", None), check_vma=False
    )
```

```python
import functools

import jax
import jax.numpy as jnp
from jax import lax
from jax.experimental import pallas as pl
from jax.experimental.pallas import tpu as pltpu
from jax.sharding import PartitionSpec as P

MESH = pl.DeviceIdType.MESH
F32, BF16, I32 = jnp.float32, jnp.bfloat16, jnp.int32
HIGH = lax.Precision.HIGHEST

SUBJ, SHARDS = 4, 32
TR, EP, RUN = 16, 12, 256
LOCAL = 4
QUADS = 3
SEL, OWN = 64, 16
VOX = 512
ROWS = SUBJ * EP * LOCAL
NT = (((1,), (1,)), ((), ()))
series_floor = 1.0
spread_floor = 0.05
shrink_factor = 0.9


def copy_to(src, dst, send_sem, recv_sem, subj, vox):
    return pltpu.make_async_remote_copy(
        src_ref=src,
        dst_ref=dst,
        send_sem=send_sem,
        recv_sem=recv_sem,
        device_id={"subj": subj, "vox": vox},
        device_id_type=MESH,
    )


def await_bytes(ref, sem):
    pltpu.make_async_copy(ref, ref, sem).wait()


def fold(x):
    return x + pltpu.roll(x, 4, 0)


def exact_terms(x):
    first = x.astype(BF16)
    rest = x - first.astype(F32)
    second = rest.astype(BF16)
    return first, second, (rest - second.astype(F32)).astype(BF16)


def two_terms(x):
    first = x.astype(BF16)
    return first, (x - first.astype(F32)).astype(BF16)


def slot_of(group, taker):
    return jnp.where((group ^ taker) < 2, group ^ taker, 2 + (group & 1))


def line_of(slot, epoch, subject):
    return slot * (EP * LOCAL) + epoch * LOCAL + subject


def main_kernel(
    series_hbm,
    offsets_hbm,
    selected_hbm,
    out_ref,
    offsets,
    selected,
    series,
    choose,
    epochs,
    scale,
    slab_out,
    slab_in,
    slab_sum,
    slab,
    raw,
    lhs_hi,
    lhs_lo,
    std_hi,
    std_lo,
    corr_even,
    corr_odd,
    score,
    gram_a,
    gram_b,
    gram_c,
    z_parts_a,
    z_parts_b,
    z_parts_c,
    x_parts_a,
    x_parts_b,
    x_parts_c,
    y_parts,
    z_sums_a,
    z_sums_b,
    z_sums_c,
    x_sums_a,
    x_sums_b,
    x_sums_c,
    y_sums,
    z_last_a,
    z_last_b,
    z_last_c,
    x_last_a,
    x_last_b,
    x_last_c,
    y_last,
    total_a,
    total_b,
    total_c,
    final_a,
    final_b,
    final_c,
    pick_a,
    pick_b,
    pick_wide,
    pick_square,
    turn_a,
    turn_b,
    turn_c,
    put_columns,
    load_sem,
    slab_send,
    slab_recv,
    share_send,
    share_recv,
    near_send,
    near_recv,
    far_send,
    far_recv,
    relay_send,
    relay_recv,
    part_send,
    z_recv,
    x_recv,
    y_recv,
    sum_send,
    sum_recv,
    final_send,
    final_recv,
):
    corr = (corr_even, corr_odd)
    z_parts, x_parts = (z_parts_a, z_parts_b, z_parts_c), (x_parts_a, x_parts_b, x_parts_c)
    z_sums, x_sums = (z_sums_a, z_sums_b, z_sums_c), (x_sums_a, x_sums_b, x_sums_c)
    last = ((z_last_a, x_last_a), (z_last_b, x_last_b), (z_last_c, x_last_c, y_last))
    gram = (gram_a, gram_b, gram_c)
    total, final = (total_a, total_b, total_c), (final_a, final_b, final_c)
    j = lax.axis_index("subj")
    v = lax.axis_index("vox")
    near, far, core = j ^ 1, j ^ 2, j & 1
    z, x, y = v // 8, (v // 2) & 3, v & 1

    def ahead_of(place, step):
        return (place + step) & 3

    def shard_at(z, x, y):
        return z * 8 + x * 2 + y

    loads = [
        pltpu.make_async_copy(source, target, load_sem.at[i])
        for i, (source, target) in enumerate(
            ((offsets_hbm, offsets), (selected_hbm, selected), (series_hbm, series))
        )
    ]
    for load in loads:
        load.start()

    barrier = pltpu.get_barrier_semaphore()

    def greet(step, carry):
        for other in range(SUBJ):
            pl.semaphore_signal(
                barrier,
                inc=1,
                device_id={"subj": j ^ other, "vox": (v + step) & (SHARDS - 1)},
                device_id_type=MESH,
            )
        return carry

    with jax.named_scope("greet"):
        lax.fori_loop(12, SHARDS, greet, 0, unroll=4)
        lax.fori_loop(1, 12, greet, 0, unroll=11)
        for other in range(1, SUBJ):
            pl.semaphore_signal(barrier, inc=1, device_id={"subj": j ^ other, "vox": v}, device_id_type=MESH)

    loads[0].wait()
    loads[1].wait()

    with jax.named_scope("choose"):
        row16 = lax.broadcasted_iota(I32, (16, 128), 0)
        scan = lax.broadcasted_iota(I32, (16, LOCAL * RUN), 1)
        for q in range(QUADS):
            start = jnp.zeros((16, 128), I32)
            for r in range(16):
                first = offsets[j * LOCAL + r % 4, q * 4 + r // 4] + (r % 4) * RUN
                start = jnp.where(row16 == r, first, start)
            ahead = scan - jnp.concatenate([start] * (LOCAL * RUN // 128), axis=1)
            for t in range(TR):
                choose[pl.ds(q * 256 + t * 16, 16), :] = jnp.where(ahead == t, 1.0, 0.0).astype(BF16)

    id_rows = []
    row8 = lax.broadcasted_iota(I32, (8, 128), 0)
    for block in range(SEL // 8):
        ids = jnp.zeros((8, 128), I32)
        for r in range(8):
            place = block * 8 + r
            ids = jnp.where(row8 == r, selected[4 * (place % OWN) + place // OWN], ids)
        id_rows.append(ids)
    ids = jnp.concatenate(id_rows, axis=0)
    columns = lax.broadcasted_iota(I32, (SEL, VOX), 1) + v * VOX
    picker = jnp.where(columns == jnp.concatenate([ids] * (VOX // 128), axis=1), 1.0, 0.0).astype(BF16)

    with jax.named_scope("pick_epochs"):
        loads[2].wait()
        runs = series[...].reshape(LOCAL * RUN, VOX)
        all_chosen = jnp.dot(choose[...], runs, preferred_element_type=F32).astype(BF16)
        for q in range(QUADS):
            chosen = all_chosen[q * 256 : q * 256 + 256]
            for h in range(2):
                epochs[0, h, q] = chosen[:, h * 256 : h * 256 + 256]
            picked = lax.dot_general(picker, chosen, NT, preferred_element_type=F32)
            slab_out[:, :, pl.ds(q * 256, 256)] = picked.astype(BF16).reshape(SHARDS, 2, 256)

    with jax.named_scope("barrier"):
        pl.semaphore_wait(barrier, SUBJ * SHARDS - 1)

    def send_slab(step, carry):
        piece = (v + step) & (SHARDS - 1)
        to_j, to_v = piece // 8, j * 8 + (piece & 7)

        @pl.when(jnp.logical_or(to_j != j, to_v != v))
        def _():
            copy_to(slab_out.at[piece], slab_in.at[v], slab_send, slab_recv, to_j, to_v).start()

        return carry

    with jax.named_scope("send_slab"):
        lax.fori_loop(0, SHARDS, send_slab, 0)

    def near_copy(h):
        return copy_to(epochs.at[0, h], epochs.at[1, h], near_send.at[h], near_recv.at[h], near, v)

    def far_copy(g, q):
        at = g * QUADS + q
        source, target = epochs.at[core ^ g, core, q], epochs.at[2 + g, core, q]
        return copy_to(source, target, far_send.at[at], far_recv.at[at], far, v)

    def relay_copy(g, q):
        at = g * QUADS + q
        ref = epochs.at[2 + g, core, q]
        return copy_to(ref, ref, relay_send.at[at], relay_recv.at[at], near, v)

    def relay(g, q):
        with jax.named_scope("relay"):
            far_copy(g, q).wait_recv()
            relay_copy(g, q).start()

    for h in (1, 0):
        near_copy(h).start()

    @pl.when(core == 0)
    def _():
        far_copy(0, 0).start()

    def lanes_of(h):
        return pl.ds(h * 256 if isinstance(h, int) else pl.multiple_of(h * 256, 256), 256)

    def scales(r, h):
        lanes = lanes_of(h)
        for q in range(QUADS):
            seen = epochs[r, h, q].astype(F32).reshape(TR, 16, 256)
            centred = seen - (jnp.sum(seen, axis=0) * (1.0 / TR))[None]
            scale[r, q, :, lanes] = lax.rsqrt(jnp.sum(centred * centred, axis=0) + series_floor)

    for h in range(2):
        scales(0, h)

    with jax.named_scope("near_wait"):
        for h in range(2):
            near_copy(h).wait_recv()

    @pl.when(core == 1)
    def _():
        far_copy(0, 0).start()

    far_copy(0, 1).start()

    own_group = v // 8 == j

    with jax.named_scope("slab_wait"):

        @pl.when(own_group)
        def _():
            slab_in[v] = slab_out[j * 8 + (v & 7)]
            await_bytes(slab_in.at[pl.ds(0, SHARDS - 1)], slab_recv)

        @pl.when(jnp.logical_not(own_group))
        def _():
            await_bytes(slab_in, slab_recv)

    with jax.named_scope("slab_sum"):
        slab_sum[...] = jnp.sum(slab_in[...].astype(F32), axis=0).astype(BF16)

    def share_slab(step, carry):
        copy_to(slab_sum, slab.at[v], share_send, share_recv, j, (v + step) & (SHARDS - 1)).start()
        return carry

    with jax.named_scope("share_slab"):
        lax.fori_loop(1, SHARDS, share_slab, 0)
        slab[v] = slab_sum[...]

    far_copy(0, 2).start()
    for q in range(QUADS):
        far_copy(1, q).start()

    with jax.named_scope("places"):
        b = lax.broadcasted_iota(I32, (1, ROWS), 1)
        p = lax.broadcasted_iota(I32, (EP * LOCAL, 1), 0)
        for i in range(2):
            taker = y * 2 + i
            s = b // EP
            to = line_of(slot_of(s // LOCAL, taker), b - s * EP, s & 3)
            s = p // EP
            line = line_of(slot_of(j, taker), p - s * EP, s)

            def put(first, lines):
                put_columns[i, pl.ds(first, lines.shape[0]), :] = jnp.where(lines == to, 1.0, 0.0).astype(BF16)

            def hot(lines):
                return jnp.where(lines == line, 1.0, 0.0).astype(BF16)

            def down(count):
                return lax.broadcasted_iota(I32, (count, 1), 0)

            def across(count):
                return lax.broadcasted_iota(I32, (1, count), 1)

            c, r = down(128), down(64)
            around = (c & 63) + 64
            put(0, jnp.where(c < 64, c, c - 32))
            put(128, jnp.where(around < 96, around, around - 96))
            put(256, jnp.where(r < 32, r, jnp.where(r < 48, r + 32, -1)))
            put(320, jnp.where(r < 48, jnp.where(r < 32, r + 32, r + 48), -1))
            c, r = across(128), across(64)
            around = (c & 63) + 64
            apart = (c & 32) > 0
            for piece, (lines, columns) in enumerate(
                (
                    (jnp.where(r < 32, r, -1), jnp.where(apart & (c < 64), c, -1)),
                    (jnp.where(r < 32, r + 32, -1), jnp.where(apart & (c >= 64), c - 32, -1)),
                    (jnp.where((r >= 32) & (r < 48), r + 32, -1), jnp.where(apart & (c < 64), around - 96, -1)),
                    (jnp.where((r >= 32) & (r < 48), r + 48, -1), jnp.where(apart & (c >= 64), around - 96, -1)),
                )
            ):
                pick_a[i, pl.ds(piece * 48, 48), :] = hot(lines)
                turn_a[i, pl.ds(piece * 48, 48), :] = hot(columns)
            put(384, down(128))
            put(512, down(48) + 96)
            pick_b[i] = hot(across(48) + 96)
            turn_b[i, 0:48, :] = hot(jnp.where(c < 96, c, -1))
            turn_b[i, 48:96, :] = hot(jnp.where(c < 96, -1, c))
            put(560, down(128))
            put(688, (down(128) & 63) + 128)
            put(816, down(48) + 144)
            pick_wide[i] = hot(across(48) + 144)
            pick_square[i] = hot(r + 128)
            turn_c[i] = hot(c)
        for k in range(OWN):
            score[k, 96:128, :] = jnp.zeros((32, VOX), BF16)

    for h in range(2):
        scales(1, h)

    relay(0, 0)
    relay(0, 1)
    with jax.named_scope("share_wait"):
        await_bytes(slab.at[pl.ds(0, SHARDS - 1)], share_recv)
    relay(0, 2)

    with jax.named_scope("standard_slab"):
        for r in range(SUBJ):
            group = (j, near, far & 2, far | 1)[r]
            for kk in range(8):
                for q in range(QUADS):
                    raw[r * QUADS + q, pl.ds(kk * 2, 2), :] = slab[group * 8 + kk, :, pl.ds(q * 256, 256)].astype(F32)
        seen = raw[...].reshape(SUBJ * QUADS * OWN, 256)
        same = jnp.where(
            (lax.broadcasted_iota(I32, (256, 256), 0) & 15) == (lax.broadcasted_iota(I32, (256, 256), 1) & 15), 1.0, 0.0
        ).astype(BF16)
        centred = seen - jnp.dot(seen.astype(BF16), same, preferred_element_type=F32) * (1.0 / TR)
        terms = exact_terms(centred * centred)
        spread = [jnp.dot(t, same, preferred_element_type=F32) for t in terms]
        spread = spread[0] + spread[1] + spread[2]
        x_std = centred * lax.rsqrt(spread + series_floor) * shrink_factor
        x_hi = x_std.astype(BF16).astype(F32)
        std_hi[...] = x_hi.reshape(SUBJ * QUADS, OWN, 256)
        std_lo[...] = (x_std - x_hi).reshape(SUBJ * QUADS, OWN, 256)

    own_row = (lax.broadcasted_iota(I32, (16, 256), 1) & 15) == lax.broadcasted_iota(I32, (16, 256), 0)

    units = ((0, 0), (0, 1), (1, 0), (1, 1), (2, 0), (2, 1), (3, core), (3, 1 - core))

    def correlate(unit):
        r, h = units[unit]
        lanes = lanes_of(h)
        if r >= 2:
            scales(r, h)
        for q in range(QUADS):
            at = r * QUADS + q
            if unit % 2 == 0:
                for k in range(OWN):
                    for std, lhs in ((std_hi, lhs_hi), (std_lo, lhs_lo)):
                        line = jnp.broadcast_to(std[at, pl.ds(k, 1), :], (16, 256))
                        lhs[at, pl.ds(k * 16, 16), :] = jnp.where(own_row, line, 0.0).astype(BF16)
            seen = epochs[r, h, q]
            corr[unit % 2][q] = jnp.dot(lhs_hi[at], seen, preferred_element_type=F32) + jnp.dot(
                lhs_lo[at], seen, preferred_element_type=F32
            )

    def standard(unit, ids=range(OWN)):
        r, h = units[unit]
        lanes = lanes_of(h)
        for k in ids:
            rows = pl.ds(k * 16 if isinstance(k, int) else pl.multiple_of(k * 16, 16), 16)
            halves = []
            for q in range(QUADS):
                shrunk = corr[unit % 2][q, rows, :] * scale[r, q, :, lanes]
                twice = jnp.log(1.0 + shrunk) - jnp.log(1.0 - shrunk)
                halves += [twice[0:8], twice[8:16]]
            mean = fold(functools.reduce(jnp.add, halves)) * (1.0 / EP)
            halves = [f - mean for f in halves]
            spread = fold(functools.reduce(jnp.add, [f * f for f in halves])) * (1.0 / EP)
            gain = lax.rsqrt(spread + 4.0 * spread_floor)
            for q in range(QUADS):
                both = jnp.concatenate([halves[2 * q] * gain, halves[2 * q + 1] * gain], axis=0).astype(BF16)
                at = r * 48 + q * 16
                score[k, pl.ds(at, 16), lanes] = both

    split = ((32, 16, 0), (16, 32, 0), (32, 32, 16))
    lane = lax.broadcasted_iota(I32, (16, 128), 1)

    def against(m, first, count, columns=slice(0, 128)):
        return lax.dot_general(score[m, pl.ds(first, count), :], score[m, columns, :], NT, preferred_element_type=F32)

    def block_of(n, m):
        if n == 0:
            block = against(m, 0, 96)
            for top in (0, 16):
                beside = pltpu.roll(block[32 + top : 48 + top], 32, 1)
                gram[n][m, top : top + 16, :] = jnp.where(lane < 64, block[top : top + 16], beside)
            upper, lower = block[64:80], block[80:96]
            left = jnp.where(lane < 32, pltpu.roll(upper, 64, 1), pltpu.roll(upper, 32, 1))
            right = jnp.where(lane < 96, lower, pltpu.roll(lower, 96, 1))
            gram[n][m, 32:48, :] = jnp.where(lane < 64, left, right)
        elif n == 1:
            gram[n][m] = against(m, 96, 48)
        else:
            gram[n][m, 0:48, :] = against(m, 144, 48)
            square = against(m, 128, 64, slice(128, 192))
            gram[n][m, 48:80, :] = jnp.concatenate([square[0:32], square[32:64]], axis=1)

    def kernels(n, unfinished=None):
        z_rows, x_rows, y_rows = split[n]

        def offsets_at(step):
            slow, fast = (step // 4 + 1) & 3, (step + 1) & 3
            return slow ^ (slow >> 1), fast ^ (fast >> 1)

        def id_at(step):
            major, minor = offsets_at(step)
            return ahead_of(z, major) * 4 + ahead_of(x, minor)

        def four(index, carry):
            steps = [index * 4 + more for more in range(8)]
            for step in steps[:4]:
                block_of(n, id_at(step))
            if unfinished is not None:
                standard(unfinished, [id_at(step & 15) for step in steps[4:]])
            for step in steps[:4]:
                major, minor = offsets_at(step)
                m = ahead_of(z, major) * 4 + ahead_of(x, minor)

                @pl.when(major > 0)
                def _():
                    source = gram[n].at[m, pl.ds(0, z_rows)]
                    to_v = shard_at(ahead_of(z, major), x, y)
                    copy_to(source, z_parts[n].at[minor, major], part_send.at[n], z_recv.at[n, minor], j, to_v).start()

                @pl.when(minor > 0)
                def _():
                    source = gram[n].at[m, pl.ds(z_rows, x_rows)]
                    to_v = shard_at(z, ahead_of(x, minor), y)
                    copy_to(source, x_parts[n].at[major, minor], part_send.at[n], x_recv.at[n, major], j, to_v).start()

                if y_rows:
                    rows = pl.ds(pl.multiple_of(z_rows + x_rows + y_rows // 2 * (y ^ 1), 8), y_rows // 2)
                    copy_to(
                        gram[n].at[m, rows], y_parts.at[major * 4 + minor], part_send.at[n], y_recv.at[major], j, v ^ 1
                    ).start()
            return carry

        with jax.named_scope("kernels"):
            if unfinished is not None:
                standard(unfinished, [id_at(step) for step in range(4)])
            lax.fori_loop(0, OWN // 4, four, 0)

    def second_sums(n):
        z_rows, x_rows, y_rows = split[n]

        def along(step, block):
            parts, recv, sums = ((z_parts, z_recv, z_sums), (x_parts, x_recv, x_sums))[block]
            with jax.named_scope("part_wait"):
                await_bytes(parts[n].at[step, pl.ds(1, 3)], recv.at[n, step])
            own = (ahead_of(z, step) * 4 + x) if block else (z * 4 + ahead_of(x, step))
            own = gram[n][own, pl.ds(z_rows, x_rows) if block else pl.ds(0, z_rows), :]
            sums[n][step] = (own + parts[n][step, 1]) + (parts[n][step, 2] + parts[n][step, 3])
            for other in range(2):
                side = y ^ other
                count = (z_rows, x_rows)[block] // 2
                rows = pl.ds(pl.multiple_of(side * count, 8), count)
                slot = step * 2 + other
                to_v = shard_at(ahead_of(z, step), x, side) if block else shard_at(z, ahead_of(x, step), side)
                if slot:
                    copy_to(
                        sums[n].at[step, rows], last[n][block].at[slot], sum_send.at[n], sum_recv.at[n, block], j, to_v
                    ).start()
                else:
                    last[n][block][0] = sums[n][0, rows, :]

        def from_side(major):
            with jax.named_scope("part_wait"):
                await_bytes(y_parts.at[pl.ds(major * 4, 4)], y_recv.at[major])
            for minor in range(4):
                step = major * 4 + minor
                to_z, to_x = ahead_of(z, major), ahead_of(x, minor)
                rows = pl.ds(pl.multiple_of(z_rows + x_rows + y_rows // 2 * y, 8), y_rows // 2)
                added = y_parts[step] + gram[n][to_z * 4 + to_x, rows, :]
                if step:
                    y_sums[step] = added
                    copy_to(
                        y_sums.at[step], y_last.at[step], sum_send.at[n], sum_recv.at[n, 2], j, shard_at(to_z, to_x, y)
                    ).start()
                else:
                    y_last[0] = added

        if y_rows:
            for major in (1, 3, 2, 0):
                along(major, 1)
                from_side(major)
        else:
            for step in (1, 3, 2, 0):
                along(step, 1)
        for step in (1, 3, 2, 0):
            along(step, 0)

    owner_v = v - y + j // 2
    place = core * 2 + y

    def hand_over(n):
        with jax.named_scope("last_wait"):
            for block, ref in enumerate(last[n]):
                await_bytes(ref.at[pl.ds(0, ref.shape[0] - 1)], sum_recv.at[n, block])
        mean = 1.0 / (VOX * SHARDS)
        first = 0
        for ref in last[n]:
            rows = ref.shape[1]
            total[n][pl.ds(first, rows), :] = jnp.sum(ref[...], axis=0) * mean
            first += rows
        for other in range(SUBJ):
            copy = copy_to(
                total[n], final[n].at[place], final_send.at[n], final_recv.at[n], (j ^ other) if other else j, owner_v
            )
            if other:
                copy.start()
            else:

                @pl.when(owner_v != v)
                def _():
                    copy.start()

        @pl.when(owner_v == v)
        def _():
            final[n][place] = total[n][...]

    def await_final(n, sem):
        @pl.when(owner_v == v)
        def _():
            await_bytes(final[n].at[pl.ds(0, SUBJ - 1)], sem.at[n])

        @pl.when(owner_v != v)
        def _():
            await_bytes(final[n], sem.at[n])

    def scores_of(correlated, finished):
        with jax.named_scope("scores"):
            if correlated is not None:
                correlate(correlated)
            if finished is not None:
                standard(finished)

    def relayed(g):
        with jax.named_scope("relay_wait"):
            for q in range(QUADS):
                relay_copy(g, q).wait_recv()

    scores_of(0, None)
    scores_of(1, 0)
    scores_of(2, 1)
    scores_of(3, 2)
    relayed(0)
    scores_of(4, 3)
    relay(1, 0)
    kernels(0)
    scores_of(5, 4)
    kernels(1, 5)
    relay(1, 1)
    relay(1, 2)
    scores_of(6, None)
    scores_of(None, 6)
    relayed(1)
    scores_of(7, None)
    kernels(2, 7)
    second_sums(0)
    second_sums(1)
    second_sums(2)
    hand_over(0)
    hand_over(1)
    hand_over(2)

    straight = (((1,), (0,)), ((), ()))
    left = lax.broadcasted_iota(I32, (EP * LOCAL, 128), 1) < 64
    upper = lax.broadcasted_iota(I32, (EP * LOCAL, 64), 1) < 32
    puts = (0, 384, 560, 864)
    corner = lax.broadcasted_iota(I32, (EP * LOCAL, 48), 1) >= 32

    def picked_by(pick, terms, dims):
        parts = [lax.dot_general(pick, t, dims, preferred_element_type=F32) for t in terms]
        return parts[0] + parts[1]

    def placed(n, i):
        pieces, first = [], 0
        for rows in split[n]:
            if rows:
                here = pl.ds(first, rows // 2)
                pieces += [final[n][2 * i, here, :], final[n][2 * i + 1, here, :]]
                first += rows // 2
        if n == 0:
            terms = two_terms(jnp.concatenate(pieces + [jnp.zeros((16, 128), F32)], axis=0))
            by_row = picked_by(pick_a[i], terms, straight)
            by_column = picked_by(turn_a[i], terms, NT)
            lines = [
                jnp.where(left, by_row[0:48], by_row[48:96]),
                jnp.where(left, by_row[96:144], by_row[144:192]),
                jnp.where(upper, by_column[0:48], by_column[96:144]),
                jnp.where(upper, by_column[48:96], by_column[144:192]),
            ]
        elif n == 1:
            terms = two_terms(jnp.concatenate(pieces, axis=0))
            by_column = picked_by(turn_b[i], terms, NT)
            turned = by_column[0:48] + jnp.where(corner, by_column[48:96], 0.0)
            lines = [picked_by(pick_b[i], terms, straight), turned]
        else:
            both = jnp.concatenate(pieces, axis=0)
            wide, square = two_terms(both[0:48]), two_terms(both[48:80])
            halves = [picked_by(pick_square[i, :, h * 32 : h * 32 + 32], square, straight) for h in range(2)]
            lines = [
                picked_by(pick_wide[i], wide, straight),
                jnp.where(left, halves[0], halves[1]),
                picked_by(turn_c[i], wide, NT),
            ]
        put = put_columns[i, puts[n] : puts[n + 1], :]
        terms = [jnp.dot(t, put, preferred_element_type=F32) for t in two_terms(jnp.concatenate(lines, axis=1))]
        return terms[0] + terms[1]

    with jax.named_scope("final"):
        await_final(0, final_recv)
    with jax.named_scope("place"):
        for i in range(2):
            out_ref[i] = placed(0, i)
    with jax.named_scope("final"):
        await_final(1, final_recv)
    with jax.named_scope("place"):
        for i in range(2):
            out_ref[i] += placed(1, i)
    with jax.named_scope("final"):
        await_final(2, final_recv)
    with jax.named_scope("place"):
        for i in range(2):
            out_ref[i] += placed(2, i)

    with jax.named_scope("drain"):
        await_bytes(slab_in.at[pl.ds(0, SHARDS - 1)], share_send)

        @pl.when(own_group)
        def _():
            await_bytes(slab_in.at[pl.ds(0, SHARDS - 1)], slab_send)

        @pl.when(jnp.logical_not(own_group))
        def _():
            await_bytes(slab_in, slab_send)

        for n in range(3):
            await_bytes(z_parts[n].at[pl.ds(0, 3)], part_send.at[n])
            await_bytes(x_parts[n].at[pl.ds(0, 3)], part_send.at[n])
            for ref in last[n]:
                await_bytes(ref.at[pl.ds(0, ref.shape[0] - 1)], sum_send.at[n])
            await_final(n, final_send)
        await_bytes(y_parts, part_send.at[2])
        for h in range(2):
            near_copy(h).wait_send()
            for q in range(QUADS):
                far_copy(h, q).wait_send()
                relay_copy(h, q).wait_send()


def body(series, offsets, selected):
    vmem = pltpu.VMEM
    dma = pltpu.SemaphoreType.DMA
    return pl.pallas_call(
        main_kernel,
        out_shape=pltpu.VMEM((2, EP * LOCAL, ROWS), F32),
        in_specs=[
            pl.BlockSpec(memory_space=pl.ANY),
            pl.BlockSpec(memory_space=pl.ANY),
            pl.BlockSpec(memory_space=pl.ANY),
        ],
        out_specs=pl.BlockSpec(memory_space=pltpu.VMEM),
        scratch_shapes=[
            pltpu.SMEM((SUBJ * LOCAL, EP), I32),
            pltpu.SMEM((SEL,), I32),
            vmem((LOCAL, RUN, VOX), BF16),
            vmem((QUADS * 256, LOCAL * RUN), BF16),
            vmem((SUBJ, 2, QUADS, 256, 256), BF16),
            vmem((SUBJ, QUADS, 16, VOX), F32),
            vmem((SHARDS, 2, QUADS * 256), BF16),
            vmem((SHARDS, 2, QUADS * 256), BF16),
            vmem((2, QUADS * 256), BF16),
            vmem((SHARDS, 2, QUADS * 256), BF16),
            vmem((SUBJ * QUADS, OWN, 256), F32),
            vmem((SUBJ * QUADS, 256, 256), BF16),
            vmem((SUBJ * QUADS, 256, 256), BF16),
            vmem((SUBJ * QUADS, OWN, 256), F32),
            vmem((SUBJ * QUADS, OWN, 256), F32),
            vmem((QUADS, 256, 256), F32),
            vmem((QUADS, 256, 256), F32),
            vmem((OWN, ROWS, VOX), BF16),
            vmem((OWN, 48, 128), F32),
            vmem((OWN, 48, 128), F32),
            vmem((OWN, 80, 128), F32),
            vmem((4, 4, 32, 128), F32),
            vmem((4, 4, 16, 128), F32),
            vmem((4, 4, 32, 128), F32),
            vmem((4, 4, 16, 128), F32),
            vmem((4, 4, 32, 128), F32),
            vmem((4, 4, 32, 128), F32),
            vmem((OWN, 8, 128), F32),
            vmem((4, 32, 128), F32),
            vmem((4, 16, 128), F32),
            vmem((4, 32, 128), F32),
            vmem((4, 16, 128), F32),
            vmem((4, 32, 128), F32),
            vmem((4, 32, 128), F32),
            vmem((OWN, 8, 128), F32),
            vmem((8, 16, 128), F32),
            vmem((8, 8, 128), F32),
            vmem((8, 16, 128), F32),
            vmem((8, 8, 128), F32),
            vmem((8, 16, 128), F32),
            vmem((8, 16, 128), F32),
            vmem((OWN, 8, 128), F32),
            vmem((24, 128), F32),
            vmem((24, 128), F32),
            vmem((40, 128), F32),
            vmem((SUBJ, 24, 128), F32),
            vmem((SUBJ, 24, 128), F32),
            vmem((SUBJ, 40, 128), F32),
            vmem((2, 4 * EP * LOCAL, 64), BF16),
            vmem((2, EP * LOCAL, 48), BF16),
            vmem((2, EP * LOCAL, 48), BF16),
            vmem((2, EP * LOCAL, 64), BF16),
            vmem((2, 4 * EP * LOCAL, 128), BF16),
            vmem((2, 2 * EP * LOCAL, 128), BF16),
            vmem((2, EP * LOCAL, 128), BF16),
            vmem((2, 864, ROWS), BF16),
            dma((3,)),
            dma,
            dma,
            dma,
            dma,
            dma((2,)),
            dma((2,)),
            dma((2 * QUADS,)),
            dma((2 * QUADS,)),
            dma((2 * QUADS,)),
            dma((2 * QUADS,)),
            dma((3,)),
            dma((3, 4)),
            dma((3, 4)),
            dma((4,)),
            dma((3,)),
            dma((3, 3)),
            dma((3,)),
            dma((3,)),
        ],
        compiler_params=pltpu.CompilerParams(collective_id=0, has_side_effects=True),
    )(series, offsets, selected)


def solution(mesh):
    placed = (P("subj", None, "vox"), P(), P())
    return jax.shard_map(
        body, mesh=mesh, in_specs=placed, out_specs=P("vox", "subj", None), check_vma=False
    )
```

```python
import functools

import jax
import jax.numpy as jnp
from jax import lax
from jax.experimental import pallas as pl
from jax.experimental.pallas import tpu as pltpu
from jax.sharding import PartitionSpec as P

MESH = pl.DeviceIdType.MESH
F32, BF16, I32 = jnp.float32, jnp.bfloat16, jnp.int32
HIGH = lax.Precision.HIGHEST

SUBJ, SHARDS = 4, 32
TR, EP, RUN = 16, 12, 256
LOCAL = 4
QUADS = 3
SEL, OWN = 64, 16
VOX = 512
ROWS = SUBJ * EP * LOCAL
NT = (((1,), (1,)), ((), ()))
series_floor = 1.0
spread_floor = 0.05
shrink_factor = 0.9


def copy_to(src, dst, send_sem, recv_sem, subj, vox):
    return pltpu.make_async_remote_copy(
        src_ref=src,
        dst_ref=dst,
        send_sem=send_sem,
        recv_sem=recv_sem,
        device_id={"subj": subj, "vox": vox},
        device_id_type=MESH,
    )


def await_bytes(ref, sem):
    pltpu.make_async_copy(ref, ref, sem).wait()


def fold(x):
    return x + pltpu.roll(x, 4, 0)


def exact_terms(x):
    first = x.astype(BF16)
    rest = x - first.astype(F32)
    second = rest.astype(BF16)
    return first, second, (rest - second.astype(F32)).astype(BF16)


def two_terms(x):
    first = x.astype(BF16)
    return first, (x - first.astype(F32)).astype(BF16)


def slot_of(group, taker):
    return jnp.where((group ^ taker) < 2, group ^ taker, 2 + (group & 1))


def line_of(slot, epoch, subject):
    return slot * (EP * LOCAL) + epoch * LOCAL + subject


def main_kernel(
    series_hbm,
    offsets_hbm,
    selected_hbm,
    out_ref,
    offsets,
    selected,
    series,
    choose,
    epochs,
    scale,
    slab_out,
    slab_in,
    slab_sum,
    slab,
    raw,
    lhs_hi,
    lhs_lo,
    std_hi,
    std_lo,
    corr_even,
    corr_odd,
    score,
    gram_a,
    gram_b,
    gram_c,
    z_parts_a,
    z_parts_b,
    z_parts_c,
    x_parts_a,
    x_parts_b,
    x_parts_c,
    y_parts,
    z_sums_a,
    z_sums_b,
    z_sums_c,
    x_sums_a,
    x_sums_b,
    x_sums_c,
    y_sums,
    z_last_a,
    z_last_b,
    z_last_c,
    x_last_a,
    x_last_b,
    x_last_c,
    y_last,
    total_a,
    total_b,
    total_c,
    final_a,
    final_b,
    final_c,
    pick_a,
    pick_b,
    pick_wide,
    pick_square,
    turn_a,
    turn_b,
    turn_c,
    put_columns,
    load_sem,
    slab_send,
    slab_recv,
    share_send,
    share_recv,
    partner_send,
    partner_recv,
    near_send,
    near_recv,
    far_send,
    far_recv,
    relay_send,
    relay_recv,
    part_send,
    z_recv,
    x_recv,
    y_recv,
    sum_send,
    sum_recv,
    final_send,
    final_recv,
):
    corr = (corr_even, corr_odd)
    z_parts, x_parts = (z_parts_a, z_parts_b, z_parts_c), (x_parts_a, x_parts_b, x_parts_c)
    z_sums, x_sums = (z_sums_a, z_sums_b, z_sums_c), (x_sums_a, x_sums_b, x_sums_c)
    last = ((z_last_a, x_last_a), (z_last_b, x_last_b), (z_last_c, x_last_c, y_last))
    gram = (gram_a, gram_b, gram_c)
    total, final = (total_a, total_b, total_c), (final_a, final_b, final_c)
    j = lax.axis_index("subj")
    v = lax.axis_index("vox")
    near, far, core = j ^ 1, j ^ 2, j & 1
    z, x, y = v // 8, (v // 2) & 3, v & 1

    def ahead_of(place, step):
        return (place + step) & 3

    def shard_at(z, x, y):
        return z * 8 + x * 2 + y

    loads = [
        pltpu.make_async_copy(source, target, load_sem.at[i])
        for i, (source, target) in enumerate(
            ((offsets_hbm, offsets), (selected_hbm, selected), (series_hbm, series))
        )
    ]
    for load in loads:
        load.start()

    barrier = pltpu.get_barrier_semaphore()

    def greet(step, carry):
        for other in range(SUBJ):
            pl.semaphore_signal(
                barrier,
                inc=1,
                device_id={"subj": j ^ other, "vox": (v + step) & (SHARDS - 1)},
                device_id_type=MESH,
            )
        return carry

    with jax.named_scope("greet"):
        for step in range(1, SHARDS):
            greet(step, 0)
        for other in range(1, SUBJ):
            pl.semaphore_signal(barrier, inc=1, device_id={"subj": j ^ other, "vox": v}, device_id_type=MESH)

    loads[0].wait()
    loads[1].wait()

    with jax.named_scope("choose"):
        row16 = lax.broadcasted_iota(I32, (16, 128), 0)
        scan = lax.broadcasted_iota(I32, (16, LOCAL * RUN), 1)
        for q in range(QUADS):
            start = jnp.zeros((16, 128), I32)
            for r in range(16):
                first = offsets[j * LOCAL + r % 4, q * 4 + r // 4] + (r % 4) * RUN
                start = jnp.where(row16 == r, first, start)
            ahead = scan - jnp.concatenate([start] * (LOCAL * RUN // 128), axis=1)
            for t in range(TR):
                choose[pl.ds(q * 256 + t * 16, 16), :] = jnp.where(ahead == t, 1.0, 0.0).astype(BF16)

    id_rows = []
    row8 = lax.broadcasted_iota(I32, (8, 128), 0)
    for block in range(SEL // 8):
        ids = jnp.zeros((8, 128), I32)
        for r in range(8):
            place = block * 8 + r
            ids = jnp.where(row8 == r, selected[4 * (place % OWN) + place // OWN], ids)
        id_rows.append(ids)
    ids = jnp.concatenate(id_rows, axis=0)
    columns = lax.broadcasted_iota(I32, (SEL, VOX), 1) + v * VOX
    picker = jnp.where(columns == jnp.concatenate([ids] * (VOX // 128), axis=1), 1.0, 0.0).astype(BF16)

    with jax.named_scope("pick_epochs"):
        loads[2].wait()
        runs = series[...].reshape(LOCAL * RUN, VOX)
        all_chosen = jnp.dot(choose[...], runs, preferred_element_type=F32).astype(BF16)
        for q in range(QUADS):
            chosen = all_chosen[q * 256 : q * 256 + 256]
            for h in range(2):
                epochs[0, h, q] = chosen[:, h * 256 : h * 256 + 256]
            picked = lax.dot_general(picker, chosen, NT, preferred_element_type=F32)
            slab_out[:, :, pl.ds(q * 256, 256)] = picked.astype(BF16).reshape(SHARDS, 2, 256)

    with jax.named_scope("barrier"):
        pl.semaphore_wait(barrier, SUBJ * SHARDS - 1)

    def send_slab(step, carry):
        piece = (v + step) & (SHARDS - 1)
        to_j, to_v = piece // 8, j * 8 + (piece & 7)

        @pl.when(jnp.logical_or(to_j != j, to_v != v))
        def _():
            copy_to(slab_out.at[piece], slab_in.at[v], slab_send, slab_recv, to_j, to_v).start()

        return carry

    with jax.named_scope("send_slab"):
        lax.fori_loop(0, SHARDS, send_slab, 0)

    def near_copy(h):
        return copy_to(epochs.at[0, h], epochs.at[1, h], near_send.at[h], near_recv.at[h], near, v)

    def far_copy(g, q):
        at = g * QUADS + q
        source, target = epochs.at[core ^ g, core, q], epochs.at[2 + g, core, q]
        return copy_to(source, target, far_send.at[at], far_recv.at[at], far, v)

    def relay_copy(g, q):
        at = g * QUADS + q
        ref = epochs.at[2 + g, core, q]
        return copy_to(ref, ref, relay_send.at[at], relay_recv.at[at], near, v)

    def relay(g, q):
        with jax.named_scope("relay"):
            far_copy(g, q).wait_recv()
            relay_copy(g, q).start()

    for h in (1, 0):
        near_copy(h).start()

    @pl.when(core == 0)
    def _():
        far_copy(0, 0).start()

    def lanes_of(h):
        return pl.ds(h * 256 if isinstance(h, int) else pl.multiple_of(h * 256, 256), 256)

    def scales(r, h):
        lanes = lanes_of(h)
        for q in range(QUADS):
            seen = epochs[r, h, q].astype(F32).reshape(TR, 16, 256)
            centred = seen - (jnp.sum(seen, axis=0) * (1.0 / TR))[None]
            scale[r, q, :, lanes] = lax.rsqrt(jnp.sum(centred * centred, axis=0) + series_floor)

    for h in range(2):
        scales(0, h)

    with jax.named_scope("near_wait"):
        for h in range(2):
            near_copy(h).wait_recv()

    @pl.when(core == 1)
    def _():
        far_copy(0, 0).start()

    far_copy(0, 1).start()

    own_group = v // 8 == j

    with jax.named_scope("slab_wait"):

        @pl.when(own_group)
        def _():
            slab_in[v] = slab_out[j * 8 + (v & 7)]
            await_bytes(slab_in.at[pl.ds(0, SHARDS - 1)], slab_recv)

        @pl.when(jnp.logical_not(own_group))
        def _():
            await_bytes(slab_in, slab_recv)

    with jax.named_scope("slab_sum"):
        slab_sum[...] = jnp.sum(slab_in[...].astype(F32), axis=0).astype(BF16)

    partner = copy_to(slab_sum, slab.at[v], partner_send, partner_recv, j, v ^ 1)

    def share_slab(source, slot):
        def send(step, carry):
            copy_to(source, slab.at[slot], share_send, share_recv, j, (v + 2 * step) & (SHARDS - 1)).start()
            return carry

        with jax.named_scope("share_slab"):
            lax.fori_loop(1, SHARDS // 2, send, 0)

    partner.start()
    share_slab(slab_sum, v)
    slab[v] = slab_sum[...]

    far_copy(0, 2).start()
    for q in range(QUADS):
        far_copy(1, q).start()

    with jax.named_scope("places"):
        b = lax.broadcasted_iota(I32, (1, ROWS), 1)
        p = lax.broadcasted_iota(I32, (EP * LOCAL, 1), 0)
        for i in range(2):
            taker = y * 2 + i
            s = b // EP
            to = line_of(slot_of(s // LOCAL, taker), b - s * EP, s & 3)
            s = p // EP
            line = line_of(slot_of(j, taker), p - s * EP, s)

            def put(first, lines):
                put_columns[i, pl.ds(first, lines.shape[0]), :] = jnp.where(lines == to, 1.0, 0.0).astype(BF16)

            def hot(lines):
                return jnp.where(lines == line, 1.0, 0.0).astype(BF16)

            def down(count):
                return lax.broadcasted_iota(I32, (count, 1), 0)

            def across(count):
                return lax.broadcasted_iota(I32, (1, count), 1)

            c, r = down(128), down(64)
            around = (c & 63) + 64
            put(0, jnp.where(c < 64, c, c - 32))
            put(128, jnp.where(around < 96, around, around - 96))
            put(256, jnp.where(r < 32, r, jnp.where(r < 48, r + 32, -1)))
            put(320, jnp.where(r < 48, jnp.where(r < 32, r + 32, r + 48), -1))
            c, r = across(128), across(64)
            around = (c & 63) + 64
            apart = (c & 32) > 0
            for piece, (lines, columns) in enumerate(
                (
                    (jnp.where(r < 32, r, -1), jnp.where(apart & (c < 64), c, -1)),
                    (jnp.where(r < 32, r + 32, -1), jnp.where(apart & (c >= 64), c - 32, -1)),
                    (jnp.where((r >= 32) & (r < 48), r + 32, -1), jnp.where(apart & (c < 64), around - 96, -1)),
                    (jnp.where((r >= 32) & (r < 48), r + 48, -1), jnp.where(apart & (c >= 64), around - 96, -1)),
                )
            ):
                pick_a[i, pl.ds(piece * 48, 48), :] = hot(lines)
                turn_a[i, pl.ds(piece * 48, 48), :] = hot(columns)
            put(384, down(128))
            put(512, down(48) + 96)
            pick_b[i] = hot(across(48) + 96)
            turn_b[i, 0:48, :] = hot(jnp.where(c < 96, c, -1))
            turn_b[i, 48:96, :] = hot(jnp.where(c < 96, -1, c))
            put(560, down(128))
            put(688, (down(128) & 63) + 128)
            put(816, down(48) + 144)
            pick_wide[i] = hot(across(48) + 144)
            pick_square[i] = hot(r + 128)
            turn_c[i] = hot(c)
        for k in range(OWN):
            score[k, 96:128, :] = jnp.zeros((32, VOX), BF16)

    for h in range(2):
        scales(1, h)

    with jax.named_scope("partner_wait"):
        partner.wait_recv()
    share_slab(slab.at[v ^ 1], v ^ 1)
    relay(0, 0)
    relay(0, 1)
    with jax.named_scope("share_wait"):
        await_bytes(slab.at[pl.ds(0, SHARDS - 2)], share_recv)
    relay(0, 2)

    with jax.named_scope("standard_slab"):
        for r in range(SUBJ):
            group = (j, near, far & 2, far | 1)[r]
            for kk in range(8):
                for q in range(QUADS):
                    raw[r * QUADS + q, pl.ds(kk * 2, 2), :] = slab[group * 8 + kk, :, pl.ds(q * 256, 256)].astype(F32)
        seen = raw[...].reshape(SUBJ * QUADS * OWN, 256)
        same = jnp.where(
            (lax.broadcasted_iota(I32, (256, 256), 0) & 15) == (lax.broadcasted_iota(I32, (256, 256), 1) & 15), 1.0, 0.0
        ).astype(BF16)
        centred = seen - jnp.dot(seen.astype(BF16), same, preferred_element_type=F32) * (1.0 / TR)
        terms = exact_terms(centred * centred)
        spread = [jnp.dot(t, same, preferred_element_type=F32) for t in terms]
        spread = spread[0] + spread[1] + spread[2]
        x_std = centred * lax.rsqrt(spread + series_floor) * shrink_factor
        x_hi = x_std.astype(BF16).astype(F32)
        std_hi[...] = x_hi.reshape(SUBJ * QUADS, OWN, 256)
        std_lo[...] = (x_std - x_hi).reshape(SUBJ * QUADS, OWN, 256)

    own_row = (lax.broadcasted_iota(I32, (16, 256), 1) & 15) == lax.broadcasted_iota(I32, (16, 256), 0)

    units = ((0, 0), (0, 1), (1, 0), (1, 1), (2, 0), (2, 1), (3, core), (3, 1 - core))

    def correlate(unit):
        r, h = units[unit]
        lanes = lanes_of(h)
        if r >= 2:
            scales(r, h)
        for q in range(QUADS):
            at = r * QUADS + q
            if unit % 2 == 0:
                for k in range(OWN):
                    for std, lhs in ((std_hi, lhs_hi), (std_lo, lhs_lo)):
                        line = jnp.broadcast_to(std[at, pl.ds(k, 1), :], (16, 256))
                        lhs[at, pl.ds(k * 16, 16), :] = jnp.where(own_row, line, 0.0).astype(BF16)
            seen = epochs[r, h, q]
            corr[unit % 2][q] = jnp.dot(lhs_hi[at], seen, preferred_element_type=F32) + jnp.dot(
                lhs_lo[at], seen, preferred_element_type=F32
            )

    def standard(unit, ids=range(OWN)):
        r, h = units[unit]
        lanes = lanes_of(h)
        for k in ids:
            rows = pl.ds(k * 16 if isinstance(k, int) else pl.multiple_of(k * 16, 16), 16)
            halves = []
            for q in range(QUADS):
                shrunk = corr[unit % 2][q, rows, :] * scale[r, q, :, lanes]
                twice = jnp.log(1.0 + shrunk) - jnp.log(1.0 - shrunk)
                halves += [twice[0:8], twice[8:16]]
            mean = fold(functools.reduce(jnp.add, halves)) * (1.0 / EP)
            halves = [f - mean for f in halves]
            spread = fold(functools.reduce(jnp.add, [f * f for f in halves])) * (1.0 / EP)
            gain = lax.rsqrt(spread + 4.0 * spread_floor)
            for q in range(QUADS):
                both = jnp.concatenate([halves[2 * q] * gain, halves[2 * q + 1] * gain], axis=0).astype(BF16)
                at = r * 48 + q * 16
                score[k, pl.ds(at, 16), lanes] = both

    split = ((32, 16, 0), (16, 32, 0), (32, 32, 16))
    lane = lax.broadcasted_iota(I32, (16, 128), 1)

    def against(m, first, count, columns=slice(0, 128)):
        return lax.dot_general(score[m, pl.ds(first, count), :], score[m, columns, :], NT, preferred_element_type=F32)

    def block_of(n, m):
        if n == 0:
            block = against(m, 0, 96)
            for top in (0, 16):
                beside = pltpu.roll(block[32 + top : 48 + top], 32, 1)
                gram[n][m, top : top + 16, :] = jnp.where(lane < 64, block[top : top + 16], beside)
            upper, lower = block[64:80], block[80:96]
            left = jnp.where(lane < 32, pltpu.roll(upper, 64, 1), pltpu.roll(upper, 32, 1))
            right = jnp.where(lane < 96, lower, pltpu.roll(lower, 96, 1))
            gram[n][m, 32:48, :] = jnp.where(lane < 64, left, right)
        elif n == 1:
            gram[n][m] = against(m, 96, 48)
        else:
            gram[n][m, 0:48, :] = against(m, 144, 48)
            square = against(m, 128, 64, slice(128, 192))
            gram[n][m, 48:80, :] = jnp.concatenate([square[0:32], square[32:64]], axis=1)

    def kernels(n, unfinished=None):
        z_rows, x_rows, y_rows = split[n]

        def offsets_at(step):
            slow, fast = (step // 4 + 1) & 3, (step + 1) & 3
            return slow ^ (slow >> 1), fast ^ (fast >> 1)

        def id_at(step):
            major, minor = offsets_at(step)
            return ahead_of(z, major) * 4 + ahead_of(x, minor)

        def four(index, carry):
            steps = [index * 4 + more for more in range(8)]
            for step in steps[:4]:
                block_of(n, id_at(step))
            if unfinished is not None:
                standard(unfinished, [id_at(step & 15) for step in steps[4:]])
            for step in steps[:4]:
                major, minor = offsets_at(step)
                m = ahead_of(z, major) * 4 + ahead_of(x, minor)

                @pl.when(major > 0)
                def _():
                    source = gram[n].at[m, pl.ds(0, z_rows)]
                    to_v = shard_at(ahead_of(z, major), x, y)
                    copy_to(source, z_parts[n].at[minor, major], part_send.at[n], z_recv.at[n, minor], j, to_v).start()

                @pl.when(minor > 0)
                def _():
                    source = gram[n].at[m, pl.ds(z_rows, x_rows)]
                    to_v = shard_at(z, ahead_of(x, minor), y)
                    copy_to(source, x_parts[n].at[major, minor], part_send.at[n], x_recv.at[n, major], j, to_v).start()

                if y_rows:
                    rows = pl.ds(pl.multiple_of(z_rows + x_rows + y_rows // 2 * (y ^ 1), 8), y_rows // 2)
                    copy_to(
                        gram[n].at[m, rows], y_parts.at[major * 4 + minor], part_send.at[n], y_recv.at[major], j, v ^ 1
                    ).start()
            return carry

        with jax.named_scope("kernels"):
            if unfinished is not None:
                standard(unfinished, [id_at(step) for step in range(4)])
            lax.fori_loop(0, OWN // 4, four, 0)

    def second_sums(n):
        z_rows, x_rows, y_rows = split[n]

        def along(step, block):
            parts, recv, sums = ((z_parts, z_recv, z_sums), (x_parts, x_recv, x_sums))[block]
            with jax.named_scope("part_wait"):
                await_bytes(parts[n].at[step, pl.ds(1, 3)], recv.at[n, step])
            own = (ahead_of(z, step) * 4 + x) if block else (z * 4 + ahead_of(x, step))
            own = gram[n][own, pl.ds(z_rows, x_rows) if block else pl.ds(0, z_rows), :]
            sums[n][step] = (own + parts[n][step, 1]) + (parts[n][step, 2] + parts[n][step, 3])
            for other in range(2):
                side = y ^ other
                count = (z_rows, x_rows)[block] // 2
                rows = pl.ds(pl.multiple_of(side * count, 8), count)
                slot = step * 2 + other
                to_v = shard_at(ahead_of(z, step), x, side) if block else shard_at(z, ahead_of(x, step), side)
                if slot:
                    copy_to(
                        sums[n].at[step, rows], last[n][block].at[slot], sum_send.at[n], sum_recv.at[n, block], j, to_v
                    ).start()
                else:
                    last[n][block][0] = sums[n][0, rows, :]

        def from_side(major):
            with jax.named_scope("part_wait"):
                await_bytes(y_parts.at[pl.ds(major * 4, 4)], y_recv.at[major])
            for minor in range(4):
                step = major * 4 + minor
                to_z, to_x = ahead_of(z, major), ahead_of(x, minor)
                rows = pl.ds(pl.multiple_of(z_rows + x_rows + y_rows // 2 * y, 8), y_rows // 2)
                added = y_parts[step] + gram[n][to_z * 4 + to_x, rows, :]
                if step:
                    y_sums[step] = added
                    copy_to(
                        y_sums.at[step], y_last.at[step], sum_send.at[n], sum_recv.at[n, 2], j, shard_at(to_z, to_x, y)
                    ).start()
                else:
                    y_last[0] = added

        if y_rows:
            for major in (1, 3, 2, 0):
                along(major, 1)
                from_side(major)
        else:
            for step in (1, 3, 2, 0):
                along(step, 1)
        for step in (1, 3, 2, 0):
            along(step, 0)

    owner_v = v - y + j // 2
    place = core * 2 + y

    def hand_over(n):
        with jax.named_scope("last_wait"):
            for block, ref in enumerate(last[n]):
                await_bytes(ref.at[pl.ds(0, ref.shape[0] - 1)], sum_recv.at[n, block])
        mean = 1.0 / (VOX * SHARDS)
        first = 0
        for ref in last[n]:
            rows = ref.shape[1]
            total[n][pl.ds(first, rows), :] = jnp.sum(ref[...], axis=0) * mean
            first += rows
        for other in range(SUBJ):
            copy = copy_to(
                total[n], final[n].at[place], final_send.at[n], final_recv.at[n], (j ^ other) if other else j, owner_v
            )
            if other:
                copy.start()
            else:

                @pl.when(owner_v != v)
                def _():
                    copy.start()

        @pl.when(owner_v == v)
        def _():
            final[n][place] = total[n][...]

    def await_final(n, sem):
        @pl.when(owner_v == v)
        def _():
            await_bytes(final[n].at[pl.ds(0, SUBJ - 1)], sem.at[n])

        @pl.when(owner_v != v)
        def _():
            await_bytes(final[n], sem.at[n])

    def scores_of(correlated, finished):
        with jax.named_scope("scores"):
            if correlated is not None:
                correlate(correlated)
            if finished is not None:
                standard(finished)

    def relayed(g):
        with jax.named_scope("relay_wait"):
            for q in range(QUADS):
                relay_copy(g, q).wait_recv()

    scores_of(0, None)
    scores_of(1, 0)
    scores_of(2, 1)
    scores_of(3, 2)
    relayed(0)
    scores_of(4, 3)
    relay(1, 0)
    kernels(0)
    scores_of(5, 4)
    kernels(1, 5)
    relay(1, 1)
    relay(1, 2)
    scores_of(6, None)
    scores_of(None, 6)
    relayed(1)
    scores_of(7, None)
    second_sums(0)
    kernels(2, 7)
    second_sums(1)
    second_sums(2)
    hand_over(0)
    hand_over(1)
    hand_over(2)

    straight = (((1,), (0,)), ((), ()))
    left = lax.broadcasted_iota(I32, (EP * LOCAL, 128), 1) < 64
    upper = lax.broadcasted_iota(I32, (EP * LOCAL, 64), 1) < 32
    puts = (0, 384, 560, 864)
    corner = lax.broadcasted_iota(I32, (EP * LOCAL, 48), 1) >= 32

    def picked_by(pick, terms, dims):
        parts = [lax.dot_general(pick, t, dims, preferred_element_type=F32) for t in terms]
        return parts[0] + parts[1]

    def placed(n, i):
        pieces, first = [], 0
        for rows in split[n]:
            if rows:
                here = pl.ds(first, rows // 2)
                pieces += [final[n][2 * i, here, :], final[n][2 * i + 1, here, :]]
                first += rows // 2
        if n == 0:
            terms = two_terms(jnp.concatenate(pieces + [jnp.zeros((16, 128), F32)], axis=0))
            by_row = picked_by(pick_a[i], terms, straight)
            by_column = picked_by(turn_a[i], terms, NT)
            lines = [
                jnp.where(left, by_row[0:48], by_row[48:96]),
                jnp.where(left, by_row[96:144], by_row[144:192]),
                jnp.where(upper, by_column[0:48], by_column[96:144]),
                jnp.where(upper, by_column[48:96], by_column[144:192]),
            ]
        elif n == 1:
            terms = two_terms(jnp.concatenate(pieces, axis=0))
            by_column = picked_by(turn_b[i], terms, NT)
            turned = by_column[0:48] + jnp.where(corner, by_column[48:96], 0.0)
            lines = [picked_by(pick_b[i], terms, straight), turned]
        else:
            both = jnp.concatenate(pieces, axis=0)
            wide, square = two_terms(both[0:48]), two_terms(both[48:80])
            halves = [picked_by(pick_square[i, :, h * 32 : h * 32 + 32], square, straight) for h in range(2)]
            lines = [
                picked_by(pick_wide[i], wide, straight),
                jnp.where(left, halves[0], halves[1]),
                picked_by(turn_c[i], wide, NT),
            ]
        put = put_columns[i, puts[n] : puts[n + 1], :]
        terms = [jnp.dot(t, put, preferred_element_type=F32) for t in two_terms(jnp.concatenate(lines, axis=1))]
        return terms[0] + terms[1]

    with jax.named_scope("final"):
        await_final(0, final_recv)
    with jax.named_scope("place"):
        for i in range(2):
            out_ref[i] = placed(0, i)
    with jax.named_scope("final"):
        await_final(1, final_recv)
    with jax.named_scope("place"):
        for i in range(2):
            out_ref[i] += placed(1, i)
    with jax.named_scope("final"):
        await_final(2, final_recv)
    with jax.named_scope("place"):
        for i in range(2):
            out_ref[i] += placed(2, i)

    with jax.named_scope("drain"):
        await_bytes(slab_in.at[pl.ds(0, SHARDS - 2)], share_send)
        partner.wait_send()

        @pl.when(own_group)
        def _():
            await_bytes(slab_in.at[pl.ds(0, SHARDS - 1)], slab_send)

        @pl.when(jnp.logical_not(own_group))
        def _():
            await_bytes(slab_in, slab_send)

        for n in range(3):
            await_bytes(z_parts[n].at[pl.ds(0, 3)], part_send.at[n])
            await_bytes(x_parts[n].at[pl.ds(0, 3)], part_send.at[n])
            for ref in last[n]:
                await_bytes(ref.at[pl.ds(0, ref.shape[0] - 1)], sum_send.at[n])
            await_final(n, final_send)
        await_bytes(y_parts, part_send.at[2])
        for h in range(2):
            near_copy(h).wait_send()
            for q in range(QUADS):
                far_copy(h, q).wait_send()
                relay_copy(h, q).wait_send()


def body(series, offsets, selected):
    vmem = pltpu.VMEM
    dma = pltpu.SemaphoreType.DMA
    return pl.pallas_call(
        main_kernel,
        out_shape=pltpu.VMEM((2, EP * LOCAL, ROWS), F32),
        in_specs=[
            pl.BlockSpec(memory_space=pl.ANY),
            pl.BlockSpec(memory_space=pl.ANY),
            pl.BlockSpec(memory_space=pl.ANY),
        ],
        out_specs=pl.BlockSpec(memory_space=pltpu.VMEM),
        scratch_shapes=[
            pltpu.SMEM((SUBJ * LOCAL, EP), I32),
            pltpu.SMEM((SEL,), I32),
            vmem((LOCAL, RUN, VOX), BF16),
            vmem((QUADS * 256, LOCAL * RUN), BF16),
            vmem((SUBJ, 2, QUADS, 256, 256), BF16),
            vmem((SUBJ, QUADS, 16, VOX), F32),
            vmem((SHARDS, 2, QUADS * 256), BF16),
            vmem((SHARDS, 2, QUADS * 256), BF16),
            vmem((2, QUADS * 256), BF16),
            vmem((SHARDS, 2, QUADS * 256), BF16),
            vmem((SUBJ * QUADS, OWN, 256), F32),
            vmem((SUBJ * QUADS, 256, 256), BF16),
            vmem((SUBJ * QUADS, 256, 256), BF16),
            vmem((SUBJ * QUADS, OWN, 256), F32),
            vmem((SUBJ * QUADS, OWN, 256), F32),
            vmem((QUADS, 256, 256), F32),
            vmem((QUADS, 256, 256), F32),
            vmem((OWN, ROWS, VOX), BF16),
            vmem((OWN, 48, 128), F32),
            vmem((OWN, 48, 128), F32),
            vmem((OWN, 80, 128), F32),
            vmem((4, 4, 32, 128), F32),
            vmem((4, 4, 16, 128), F32),
            vmem((4, 4, 32, 128), F32),
            vmem((4, 4, 16, 128), F32),
            vmem((4, 4, 32, 128), F32),
            vmem((4, 4, 32, 128), F32),
            vmem((OWN, 8, 128), F32),
            vmem((4, 32, 128), F32),
            vmem((4, 16, 128), F32),
            vmem((4, 32, 128), F32),
            vmem((4, 16, 128), F32),
            vmem((4, 32, 128), F32),
            vmem((4, 32, 128), F32),
            vmem((OWN, 8, 128), F32),
            vmem((8, 16, 128), F32),
            vmem((8, 8, 128), F32),
            vmem((8, 16, 128), F32),
            vmem((8, 8, 128), F32),
            vmem((8, 16, 128), F32),
            vmem((8, 16, 128), F32),
            vmem((OWN, 8, 128), F32),
            vmem((24, 128), F32),
            vmem((24, 128), F32),
            vmem((40, 128), F32),
            vmem((SUBJ, 24, 128), F32),
            vmem((SUBJ, 24, 128), F32),
            vmem((SUBJ, 40, 128), F32),
            vmem((2, 4 * EP * LOCAL, 64), BF16),
            vmem((2, EP * LOCAL, 48), BF16),
            vmem((2, EP * LOCAL, 48), BF16),
            vmem((2, EP * LOCAL, 64), BF16),
            vmem((2, 4 * EP * LOCAL, 128), BF16),
            vmem((2, 2 * EP * LOCAL, 128), BF16),
            vmem((2, EP * LOCAL, 128), BF16),
            vmem((2, 864, ROWS), BF16),
            dma((3,)),
            dma,
            dma,
            dma,
            dma,
            dma,
            dma,
            dma((2,)),
            dma((2,)),
            dma((2 * QUADS,)),
            dma((2 * QUADS,)),
            dma((2 * QUADS,)),
            dma((2 * QUADS,)),
            dma((3,)),
            dma((3, 4)),
            dma((3, 4)),
            dma((4,)),
            dma((3,)),
            dma((3, 3)),
            dma((3,)),
            dma((3,)),
        ],
        compiler_params=pltpu.CompilerParams(collective_id=0, has_side_effects=True),
    )(series, offsets, selected)


def solution(mesh):
    placed = (P("subj", None, "vox"), P(), P())
    return jax.shard_map(
        body, mesh=mesh, in_specs=placed, out_specs=P("vox", "subj", None), check_vma=False
    )
```

```python
import functools

import jax
import jax.numpy as jnp
from jax import lax
from jax.experimental import pallas as pl
from jax.experimental.pallas import tpu as pltpu
from jax.sharding import PartitionSpec as P

MESH = pl.DeviceIdType.MESH
F32, BF16, I32 = jnp.float32, jnp.bfloat16, jnp.int32
HIGH = lax.Precision.HIGHEST

SUBJ, SHARDS = 4, 32
TR, EP, RUN = 16, 12, 256
LOCAL = 4
QUADS = 3
SEL, OWN = 64, 16
VOX = 512
ROWS = SUBJ * EP * LOCAL
NT = (((1,), (1,)), ((), ()))
series_floor = 1.0
spread_floor = 0.05
shrink_factor = 0.9


def copy_to(src, dst, send_sem, recv_sem, subj, vox):
    return pltpu.make_async_remote_copy(
        src_ref=src,
        dst_ref=dst,
        send_sem=send_sem,
        recv_sem=recv_sem,
        device_id={"subj": subj, "vox": vox},
        device_id_type=MESH,
    )


def await_bytes(ref, sem):
    pltpu.make_async_copy(ref, ref, sem).wait()


def fold(x):
    return x + pltpu.roll(x, 4, 0)


def exact_terms(x):
    first = x.astype(BF16)
    rest = x - first.astype(F32)
    second = rest.astype(BF16)
    return first, second, (rest - second.astype(F32)).astype(BF16)


def two_terms(x):
    first = x.astype(BF16)
    return first, (x - first.astype(F32)).astype(BF16)


def slot_of(group, taker):
    return jnp.where((group ^ taker) < 2, group ^ taker, 2 + (group & 1))


def line_of(slot, epoch, subject):
    return slot * (EP * LOCAL) + epoch * LOCAL + subject


def main_kernel(
    series_hbm,
    offsets_hbm,
    selected_hbm,
    out_ref,
    offsets,
    selected,
    series,
    choose,
    epochs,
    scale,
    slab_out,
    slab_in,
    slab_sum,
    slab,
    raw,
    lhs_hi,
    lhs_lo,
    std_hi,
    std_lo,
    corr_even,
    corr_odd,
    score,
    gram_a,
    gram_b,
    gram_c,
    z_parts_a,
    z_parts_b,
    z_parts_c,
    x_parts_a,
    x_parts_b,
    x_parts_c,
    y_parts,
    z_sums_a,
    z_sums_b,
    z_sums_c,
    x_sums_a,
    x_sums_b,
    x_sums_c,
    y_sums,
    z_last_a,
    z_last_b,
    z_last_c,
    x_last_a,
    x_last_b,
    x_last_c,
    y_last,
    total_a,
    total_b,
    total_c,
    final_a,
    final_b,
    final_c,
    pick_a,
    pick_b,
    pick_wide,
    pick_square,
    turn_a,
    turn_b,
    turn_c,
    put_columns,
    load_sem,
    slab_send,
    slab_recv,
    share_send,
    share_recv,
    near_send,
    near_recv,
    far_send,
    far_recv,
    relay_send,
    relay_recv,
    part_send,
    z_recv,
    x_recv,
    y_recv,
    sum_send,
    sum_recv,
    final_send,
    final_recv,
):
    corr = (corr_even, corr_odd)
    z_parts, x_parts = (z_parts_a, z_parts_b, z_parts_c), (x_parts_a, x_parts_b, x_parts_c)
    z_sums, x_sums = (z_sums_a, z_sums_b, z_sums_c), (x_sums_a, x_sums_b, x_sums_c)
    last = ((z_last_a, x_last_a), (z_last_b, x_last_b), (z_last_c, x_last_c, y_last))
    gram = (gram_a, gram_b, gram_c)
    total, final = (total_a, total_b, total_c), (final_a, final_b, final_c)
    j = lax.axis_index("subj")
    v = lax.axis_index("vox")
    near, far, core = j ^ 1, j ^ 2, j & 1
    z, x, y = v // 8, (v // 2) & 3, v & 1

    def ahead_of(place, step):
        return (place + step) & 3

    def shard_at(z, x, y):
        return z * 8 + x * 2 + y

    loads = [
        pltpu.make_async_copy(source, target, load_sem.at[i])
        for i, (source, target) in enumerate(
            ((offsets_hbm, offsets), (selected_hbm, selected), (series_hbm, series))
        )
    ]
    for load in loads:
        load.start()

    barrier = pltpu.get_barrier_semaphore()

    def greet(step, carry):
        for other in range(SUBJ):
            pl.semaphore_signal(
                barrier,
                inc=1,
                device_id={"subj": j ^ other, "vox": (v + step) & (SHARDS - 1)},
                device_id_type=MESH,
            )
        return carry

    with jax.named_scope("greet"):
        lax.fori_loop(1, SHARDS, greet, 0, unroll=4)
        for other in range(1, SUBJ):
            pl.semaphore_signal(barrier, inc=1, device_id={"subj": j ^ other, "vox": v}, device_id_type=MESH)

    loads[0].wait()
    loads[1].wait()

    with jax.named_scope("choose"):
        row16 = lax.broadcasted_iota(I32, (16, 128), 0)
        scan = lax.broadcasted_iota(I32, (16, LOCAL * RUN), 1)
        for q in range(QUADS):
            start = jnp.zeros((16, 128), I32)
            for r in range(16):
                first = offsets[j * LOCAL + r % 4, q * 4 + r // 4] + (r % 4) * RUN
                start = jnp.where(row16 == r, first, start)
            ahead = scan - jnp.concatenate([start] * (LOCAL * RUN // 128), axis=1)
            for t in range(TR):
                choose[pl.ds(q * 256 + t * 16, 16), :] = jnp.where(ahead == t, 1.0, 0.0).astype(BF16)

    id_rows = []
    row8 = lax.broadcasted_iota(I32, (8, 128), 0)
    for block in range(SEL // 8):
        ids = jnp.zeros((8, 128), I32)
        for r in range(8):
            place = block * 8 + r
            ids = jnp.where(row8 == r, selected[4 * (place % OWN) + place // OWN], ids)
        id_rows.append(ids)
    ids = jnp.concatenate(id_rows, axis=0)
    columns = lax.broadcasted_iota(I32, (SEL, VOX), 1) + v * VOX
    picker = jnp.where(columns == jnp.concatenate([ids] * (VOX // 128), axis=1), 1.0, 0.0).astype(BF16)

    with jax.named_scope("pick_epochs"):
        loads[2].wait()
        runs = series[...].reshape(LOCAL * RUN, VOX)
        all_chosen = jnp.dot(choose[...], runs, preferred_element_type=F32).astype(BF16)
        for q in range(QUADS):
            chosen = all_chosen[q * 256 : q * 256 + 256]
            for h in range(2):
                epochs[0, h, q] = chosen[:, h * 256 : h * 256 + 256]
            picked = lax.dot_general(picker, chosen, NT, preferred_element_type=F32)
            slab_out[:, :, pl.ds(q * 256, 256)] = picked.astype(BF16).reshape(SHARDS, 2, 256)

    with jax.named_scope("barrier"):
        pl.semaphore_wait(barrier, SUBJ * SHARDS - 1)

    def send_slab(step, carry):
        piece = (v + step) & (SHARDS - 1)
        to_j, to_v = piece // 8, j * 8 + (piece & 7)

        @pl.when(jnp.logical_or(to_j != j, to_v != v))
        def _():
            copy_to(slab_out.at[piece], slab_in.at[v], slab_send, slab_recv, to_j, to_v).start()

        return carry

    with jax.named_scope("send_slab"):
        lax.fori_loop(0, SHARDS, send_slab, 0)

    def near_copy(h):
        return copy_to(epochs.at[0, h], epochs.at[1, h], near_send.at[h], near_recv.at[h], near, v)

    def far_copy(g, q):
        at = g * QUADS + q
        source, target = epochs.at[core ^ g, core, q], epochs.at[2 + g, core, q]
        return copy_to(source, target, far_send.at[at], far_recv.at[at], far, v)

    def relay_copy(g, q):
        at = g * QUADS + q
        ref = epochs.at[2 + g, core, q]
        return copy_to(ref, ref, relay_send.at[at], relay_recv.at[at], near, v)

    def relay(g, q):
        with jax.named_scope("relay"):
            far_copy(g, q).wait_recv()
            relay_copy(g, q).start()

    for h in (1, 0):
        near_copy(h).start()

    @pl.when(core == 0)
    def _():
        far_copy(0, 0).start()

    def lanes_of(h):
        return pl.ds(h * 256 if isinstance(h, int) else pl.multiple_of(h * 256, 256), 256)

    def scales(r, h):
        lanes = lanes_of(h)
        for q in range(QUADS):
            seen = epochs[r, h, q].astype(F32).reshape(TR, 16, 256)
            centred = seen - (jnp.sum(seen, axis=0) * (1.0 / TR))[None]
            scale[r, q, :, lanes] = lax.rsqrt(jnp.sum(centred * centred, axis=0) + series_floor)

    for h in range(2):
        scales(0, h)

    with jax.named_scope("near_wait"):
        for h in range(2):
            near_copy(h).wait_recv()

    @pl.when(core == 1)
    def _():
        far_copy(0, 0).start()

    far_copy(0, 1).start()

    own_group = v // 8 == j

    with jax.named_scope("slab_wait"):

        @pl.when(own_group)
        def _():
            slab_in[v] = slab_out[j * 8 + (v & 7)]
            await_bytes(slab_in.at[pl.ds(0, SHARDS - 1)], slab_recv)

        @pl.when(jnp.logical_not(own_group))
        def _():
            await_bytes(slab_in, slab_recv)

    with jax.named_scope("slab_sum"):
        slab_sum[...] = jnp.sum(slab_in[...].astype(F32), axis=0).astype(BF16)

    def share_slab(step, carry):
        copy_to(slab_sum, slab.at[v], share_send, share_recv, j, (v + step) & (SHARDS - 1)).start()
        return carry

    with jax.named_scope("share_slab"):
        lax.fori_loop(1, SHARDS, share_slab, 0)
        slab[v] = slab_sum[...]

    far_copy(0, 2).start()
    for q in range(QUADS):
        far_copy(1, q).start()

    with jax.named_scope("places"):
        b = lax.broadcasted_iota(I32, (1, ROWS), 1)
        p = lax.broadcasted_iota(I32, (EP * LOCAL, 1), 0)
        for i in range(2):
            taker = y * 2 + i
            s = b // EP
            to = line_of(slot_of(s // LOCAL, taker), b - s * EP, s & 3)
            s = p // EP
            line = line_of(slot_of(j, taker), p - s * EP, s)

            def put(first, lines):
                put_columns[i, pl.ds(first, lines.shape[0]), :] = jnp.where(lines == to, 1.0, 0.0).astype(BF16)

            def hot(lines):
                return jnp.where(lines == line, 1.0, 0.0).astype(BF16)

            def down(count):
                return lax.broadcasted_iota(I32, (count, 1), 0)

            def across(count):
                return lax.broadcasted_iota(I32, (1, count), 1)

            c, r = down(128), down(64)
            around = (c & 63) + 64
            put(0, jnp.where(c < 64, c, c - 32))
            put(128, jnp.where(around < 96, around, around - 96))
            put(256, jnp.where(r < 32, r, jnp.where(r < 48, r + 32, -1)))
            put(320, jnp.where(r < 48, jnp.where(r < 32, r + 32, r + 48), -1))
            c, r = across(128), across(64)
            around = (c & 63) + 64
            apart = (c & 32) > 0
            for piece, (lines, columns) in enumerate(
                (
                    (jnp.where(r < 32, r, -1), jnp.where(apart & (c < 64), c, -1)),
                    (jnp.where(r < 32, r + 32, -1), jnp.where(apart & (c >= 64), c - 32, -1)),
                    (jnp.where((r >= 32) & (r < 48), r + 32, -1), jnp.where(apart & (c < 64), around - 96, -1)),
                    (jnp.where((r >= 32) & (r < 48), r + 48, -1), jnp.where(apart & (c >= 64), around - 96, -1)),
                )
            ):
                pick_a[i, pl.ds(piece * 48, 48), :] = hot(lines)
                turn_a[i, pl.ds(piece * 48, 48), :] = hot(columns)
            put(384, down(128))
            put(512, down(48) + 96)
            pick_b[i] = hot(across(48) + 96)
            turn_b[i, 0:48, :] = hot(jnp.where(c < 96, c, -1))
            turn_b[i, 48:96, :] = hot(jnp.where(c < 96, -1, c))
            put(560, down(128))
            put(688, (down(128) & 63) + 128)
            put(816, down(48) + 144)
            pick_wide[i] = hot(across(48) + 144)
            pick_square[i] = hot(r + 128)
            turn_c[i] = hot(c)
        for k in range(OWN):
            score[k, 96:128, :] = jnp.zeros((32, VOX), BF16)

    for h in range(2):
        scales(1, h)

    relay(0, 0)
    relay(0, 1)
    with jax.named_scope("share_wait"):
        await_bytes(slab.at[pl.ds(0, SHARDS - 1)], share_recv)
    relay(0, 2)

    with jax.named_scope("standard_slab"):
        for r in range(SUBJ):
            group = (j, near, far & 2, far | 1)[r]
            for kk in range(8):
                for q in range(QUADS):
                    raw[r * QUADS + q, pl.ds(kk * 2, 2), :] = slab[group * 8 + kk, :, pl.ds(q * 256, 256)].astype(F32)
        seen = raw[...].reshape(SUBJ * QUADS * OWN, 256)
        same = jnp.where(
            (lax.broadcasted_iota(I32, (256, 256), 0) & 15) == (lax.broadcasted_iota(I32, (256, 256), 1) & 15), 1.0, 0.0
        ).astype(BF16)
        centred = seen - jnp.dot(seen.astype(BF16), same, preferred_element_type=F32) * (1.0 / TR)
        terms = exact_terms(centred * centred)
        spread = [jnp.dot(t, same, preferred_element_type=F32) for t in terms]
        spread = spread[0] + spread[1] + spread[2]
        x_std = centred * lax.rsqrt(spread + series_floor) * shrink_factor
        x_hi = x_std.astype(BF16).astype(F32)
        std_hi[...] = x_hi.reshape(SUBJ * QUADS, OWN, 256)
        std_lo[...] = (x_std - x_hi).reshape(SUBJ * QUADS, OWN, 256)

    own_row = (lax.broadcasted_iota(I32, (16, 256), 1) & 15) == lax.broadcasted_iota(I32, (16, 256), 0)

    units = ((0, 0), (0, 1), (1, 0), (1, 1), (2, 0), (2, 1), (3, core), (3, 1 - core))

    def correlate(unit):
        r, h = units[unit]
        lanes = lanes_of(h)
        if r >= 2:
            scales(r, h)
        for q in range(QUADS):
            at = r * QUADS + q
            if unit % 2 == 0:
                for k in range(OWN):
                    for std, lhs in ((std_hi, lhs_hi), (std_lo, lhs_lo)):
                        line = jnp.broadcast_to(std[at, pl.ds(k, 1), :], (16, 256))
                        lhs[at, pl.ds(k * 16, 16), :] = jnp.where(own_row, line, 0.0).astype(BF16)
            seen = epochs[r, h, q]
            corr[unit % 2][q] = jnp.dot(lhs_hi[at], seen, preferred_element_type=F32) + jnp.dot(
                lhs_lo[at], seen, preferred_element_type=F32
            )

    def standard(unit, ids=range(OWN)):
        r, h = units[unit]
        lanes = lanes_of(h)
        for k in ids:
            rows = pl.ds(k * 16 if isinstance(k, int) else pl.multiple_of(k * 16, 16), 16)
            halves = []
            for q in range(QUADS):
                shrunk = corr[unit % 2][q, rows, :] * scale[r, q, :, lanes]
                twice = jnp.log(1.0 + shrunk) - jnp.log(1.0 - shrunk)
                halves += [twice[0:8], twice[8:16]]
            mean = fold(functools.reduce(jnp.add, halves)) * (1.0 / EP)
            halves = [f - mean for f in halves]
            spread = fold(functools.reduce(jnp.add, [f * f for f in halves])) * (1.0 / EP)
            gain = lax.rsqrt(spread + 4.0 * spread_floor)
            for q in range(QUADS):
                both = jnp.concatenate([halves[2 * q] * gain, halves[2 * q + 1] * gain], axis=0).astype(BF16)
                at = r * 48 + q * 16
                score[k, pl.ds(at, 16), lanes] = both

    split = ((32, 16, 0), (16, 32, 0), (32, 32, 16))
    lane = lax.broadcasted_iota(I32, (16, 128), 1)

    def against(m, first, count, columns=slice(0, 128)):
        return lax.dot_general(score[m, pl.ds(first, count), :], score[m, columns, :], NT, preferred_element_type=F32)

    def block_of(n, m):
        if n == 0:
            block = against(m, 0, 96)
            for top in (0, 16):
                beside = pltpu.roll(block[32 + top : 48 + top], 32, 1)
                gram[n][m, top : top + 16, :] = jnp.where(lane < 64, block[top : top + 16], beside)
            upper, lower = block[64:80], block[80:96]
            left = jnp.where(lane < 32, pltpu.roll(upper, 64, 1), pltpu.roll(upper, 32, 1))
            right = jnp.where(lane < 96, lower, pltpu.roll(lower, 96, 1))
            gram[n][m, 32:48, :] = jnp.where(lane < 64, left, right)
        elif n == 1:
            gram[n][m] = against(m, 96, 48)
        else:
            gram[n][m, 0:48, :] = against(m, 144, 48)
            square = against(m, 128, 64, slice(128, 192))
            gram[n][m, 48:80, :] = jnp.concatenate([square[0:32], square[32:64]], axis=1)

    def kernels(n, unfinished=None):
        z_rows, x_rows, y_rows = split[n]

        def offsets_at(step):
            slow, fast = (step // 4 + 1) & 3, (step + 1) & 3
            return slow ^ (slow >> 1), fast ^ (fast >> 1)

        def id_at(step):
            major, minor = offsets_at(step)
            return ahead_of(z, major) * 4 + ahead_of(x, minor)

        def four(index, carry):
            steps = [index * 4 + more for more in range(8)]
            for step in steps[:4]:
                block_of(n, id_at(step))
            if unfinished is not None:
                standard(unfinished, [id_at(step & 15) for step in steps[4:]])
            for step in steps[:4]:
                major, minor = offsets_at(step)
                m = ahead_of(z, major) * 4 + ahead_of(x, minor)

                @pl.when(major > 0)
                def _():
                    source = gram[n].at[m, pl.ds(0, z_rows)]
                    to_v = shard_at(ahead_of(z, major), x, y)
                    copy_to(source, z_parts[n].at[minor, major], part_send.at[n], z_recv.at[n, minor], j, to_v).start()

                @pl.when(minor > 0)
                def _():
                    source = gram[n].at[m, pl.ds(z_rows, x_rows)]
                    to_v = shard_at(z, ahead_of(x, minor), y)
                    copy_to(source, x_parts[n].at[major, minor], part_send.at[n], x_recv.at[n, major], j, to_v).start()

                if y_rows:
                    rows = pl.ds(pl.multiple_of(z_rows + x_rows + y_rows // 2 * (y ^ 1), 8), y_rows // 2)
                    copy_to(
                        gram[n].at[m, rows], y_parts.at[major * 4 + minor], part_send.at[n], y_recv.at[major], j, v ^ 1
                    ).start()
            return carry

        with jax.named_scope("kernels"):
            if unfinished is not None:
                standard(unfinished, [id_at(step) for step in range(4)])
            lax.fori_loop(0, OWN // 4, four, 0)

    def second_sums(n):
        z_rows, x_rows, y_rows = split[n]

        def along(step, block):
            parts, recv, sums = ((z_parts, z_recv, z_sums), (x_parts, x_recv, x_sums))[block]
            with jax.named_scope("part_wait"):
                await_bytes(parts[n].at[step, pl.ds(1, 3)], recv.at[n, step])
            own = (ahead_of(z, step) * 4 + x) if block else (z * 4 + ahead_of(x, step))
            own = gram[n][own, pl.ds(z_rows, x_rows) if block else pl.ds(0, z_rows), :]
            sums[n][step] = (own + parts[n][step, 1]) + (parts[n][step, 2] + parts[n][step, 3])
            for other in range(2):
                side = y ^ other
                count = (z_rows, x_rows)[block] // 2
                rows = pl.ds(pl.multiple_of(side * count, 8), count)
                slot = step * 2 + other
                to_v = shard_at(ahead_of(z, step), x, side) if block else shard_at(z, ahead_of(x, step), side)
                if slot:
                    copy_to(
                        sums[n].at[step, rows], last[n][block].at[slot], sum_send.at[n], sum_recv.at[n, block], j, to_v
                    ).start()
                else:
                    last[n][block][0] = sums[n][0, rows, :]

        def from_side(major):
            with jax.named_scope("part_wait"):
                await_bytes(y_parts.at[pl.ds(major * 4, 4)], y_recv.at[major])
            for minor in range(4):
                step = major * 4 + minor
                to_z, to_x = ahead_of(z, major), ahead_of(x, minor)
                rows = pl.ds(pl.multiple_of(z_rows + x_rows + y_rows // 2 * y, 8), y_rows // 2)
                added = y_parts[step] + gram[n][to_z * 4 + to_x, rows, :]
                if step:
                    y_sums[step] = added
                    copy_to(
                        y_sums.at[step], y_last.at[step], sum_send.at[n], sum_recv.at[n, 2], j, shard_at(to_z, to_x, y)
                    ).start()
                else:
                    y_last[0] = added

        if y_rows:
            for major in (1, 3, 2, 0):
                along(major, 1)
                from_side(major)
        else:
            for step in (1, 3, 2, 0):
                along(step, 1)
        for step in (1, 3, 2, 0):
            along(step, 0)

    owner_v = v - y + j // 2
    place = core * 2 + y

    def hand_over(n):
        with jax.named_scope("last_wait"):
            for block, ref in enumerate(last[n]):
                await_bytes(ref.at[pl.ds(0, ref.shape[0] - 1)], sum_recv.at[n, block])
        mean = 1.0 / (VOX * SHARDS)
        first = 0
        for ref in last[n]:
            rows = ref.shape[1]
            total[n][pl.ds(first, rows), :] = jnp.sum(ref[...], axis=0) * mean
            first += rows
        for other in range(SUBJ):
            copy = copy_to(
                total[n], final[n].at[place], final_send.at[n], final_recv.at[n], (j ^ other) if other else j, owner_v
            )
            if other:
                copy.start()
            else:

                @pl.when(owner_v != v)
                def _():
                    copy.start()

        @pl.when(owner_v == v)
        def _():
            final[n][place] = total[n][...]

    def await_final(n, sem):
        @pl.when(owner_v == v)
        def _():
            await_bytes(final[n].at[pl.ds(0, SUBJ - 1)], sem.at[n])

        @pl.when(owner_v != v)
        def _():
            await_bytes(final[n], sem.at[n])

    def scores_of(correlated, finished):
        with jax.named_scope("scores"):
            if correlated is not None:
                correlate(correlated)
            if finished is not None:
                standard(finished)

    def relayed(g):
        with jax.named_scope("relay_wait"):
            for q in range(QUADS):
                relay_copy(g, q).wait_recv()

    scores_of(0, None)
    scores_of(1, 0)
    scores_of(2, 1)
    scores_of(3, 2)
    relayed(0)
    scores_of(4, 3)
    relay(1, 0)
    kernels(0, 4)
    scores_of(5, None)
    kernels(1, 5)
    relay(1, 1)
    relay(1, 2)
    scores_of(6, None)
    scores_of(None, 6)
    second_sums(0)
    relayed(1)
    scores_of(7, None)
    kernels(2, 7)
    second_sums(1)
    second_sums(2)
    hand_over(0)
    hand_over(1)
    hand_over(2)

    straight = (((1,), (0,)), ((), ()))
    left = lax.broadcasted_iota(I32, (EP * LOCAL, 128), 1) < 64
    upper = lax.broadcasted_iota(I32, (EP * LOCAL, 64), 1) < 32
    puts = (0, 384, 560, 864)
    corner = lax.broadcasted_iota(I32, (EP * LOCAL, 48), 1) >= 32

    def picked_by(pick, terms, dims):
        parts = [lax.dot_general(pick, t, dims, preferred_element_type=F32) for t in terms]
        return parts[0] + parts[1]

    def placed(n, i):
        pieces, first = [], 0
        for rows in split[n]:
            if rows:
                here = pl.ds(first, rows // 2)
                pieces += [final[n][2 * i, here, :], final[n][2 * i + 1, here, :]]
                first += rows // 2
        if n == 0:
            terms = two_terms(jnp.concatenate(pieces + [jnp.zeros((16, 128), F32)], axis=0))
            by_row = picked_by(pick_a[i], terms, straight)
            by_column = picked_by(turn_a[i], terms, NT)
            lines = [
                jnp.where(left, by_row[0:48], by_row[48:96]),
                jnp.where(left, by_row[96:144], by_row[144:192]),
                jnp.where(upper, by_column[0:48], by_column[96:144]),
                jnp.where(upper, by_column[48:96], by_column[144:192]),
            ]
        elif n == 1:
            terms = two_terms(jnp.concatenate(pieces, axis=0))
            by_column = picked_by(turn_b[i], terms, NT)
            turned = by_column[0:48] + jnp.where(corner, by_column[48:96], 0.0)
            lines = [picked_by(pick_b[i], terms, straight), turned]
        else:
            both = jnp.concatenate(pieces, axis=0)
            wide, square = two_terms(both[0:48]), two_terms(both[48:80])
            halves = [picked_by(pick_square[i, :, h * 32 : h * 32 + 32], square, straight) for h in range(2)]
            lines = [
                picked_by(pick_wide[i], wide, straight),
                jnp.where(left, halves[0], halves[1]),
                picked_by(turn_c[i], wide, NT),
            ]
        put = put_columns[i, puts[n] : puts[n + 1], :]
        terms = [jnp.dot(t, put, preferred_element_type=F32) for t in two_terms(jnp.concatenate(lines, axis=1))]
        return terms[0] + terms[1]

    with jax.named_scope("final"):
        await_final(0, final_recv)
    with jax.named_scope("place"):
        for i in range(2):
            out_ref[i] = placed(0, i)
    with jax.named_scope("final"):
        await_final(1, final_recv)
    with jax.named_scope("place"):
        for i in range(2):
            out_ref[i] += placed(1, i)
    with jax.named_scope("final"):
        await_final(2, final_recv)
    with jax.named_scope("place"):
        for i in range(2):
            out_ref[i] += placed(2, i)

    with jax.named_scope("drain"):
        await_bytes(slab_in.at[pl.ds(0, SHARDS - 1)], share_send)

        @pl.when(own_group)
        def _():
            await_bytes(slab_in.at[pl.ds(0, SHARDS - 1)], slab_send)

        @pl.when(jnp.logical_not(own_group))
        def _():
            await_bytes(slab_in, slab_send)

        for n in range(3):
            await_bytes(z_parts[n].at[pl.ds(0, 3)], part_send.at[n])
            await_bytes(x_parts[n].at[pl.ds(0, 3)], part_send.at[n])
            for ref in last[n]:
                await_bytes(ref.at[pl.ds(0, ref.shape[0] - 1)], sum_send.at[n])
            await_final(n, final_send)
        await_bytes(y_parts, part_send.at[2])
        for h in range(2):
            near_copy(h).wait_send()
            for q in range(QUADS):
                far_copy(h, q).wait_send()
                relay_copy(h, q).wait_send()


def body(series, offsets, selected):
    vmem = pltpu.VMEM
    dma = pltpu.SemaphoreType.DMA
    return pl.pallas_call(
        main_kernel,
        out_shape=pltpu.VMEM((2, EP * LOCAL, ROWS), F32),
        in_specs=[
            pl.BlockSpec(memory_space=pl.ANY),
            pl.BlockSpec(memory_space=pl.ANY),
            pl.BlockSpec(memory_space=pl.ANY),
        ],
        out_specs=pl.BlockSpec(memory_space=pltpu.VMEM),
        scratch_shapes=[
            pltpu.SMEM((SUBJ * LOCAL, EP), I32),
            pltpu.SMEM((SEL,), I32),
            vmem((LOCAL, RUN, VOX), BF16),
            vmem((QUADS * 256, LOCAL * RUN), BF16),
            vmem((SUBJ, 2, QUADS, 256, 256), BF16),
            vmem((SUBJ, QUADS, 16, VOX), F32),
            vmem((SHARDS, 2, QUADS * 256), BF16),
            vmem((SHARDS, 2, QUADS * 256), BF16),
            vmem((2, QUADS * 256), BF16),
            vmem((SHARDS, 2, QUADS * 256), BF16),
            vmem((SUBJ * QUADS, OWN, 256), F32),
            vmem((SUBJ * QUADS, 256, 256), BF16),
            vmem((SUBJ * QUADS, 256, 256), BF16),
            vmem((SUBJ * QUADS, OWN, 256), F32),
            vmem((SUBJ * QUADS, OWN, 256), F32),
            vmem((QUADS, 256, 256), F32),
            vmem((QUADS, 256, 256), F32),
            vmem((OWN, ROWS, VOX), BF16),
            vmem((OWN, 48, 128), F32),
            vmem((OWN, 48, 128), F32),
            vmem((OWN, 80, 128), F32),
            vmem((4, 4, 32, 128), F32),
            vmem((4, 4, 16, 128), F32),
            vmem((4, 4, 32, 128), F32),
            vmem((4, 4, 16, 128), F32),
            vmem((4, 4, 32, 128), F32),
            vmem((4, 4, 32, 128), F32),
            vmem((OWN, 8, 128), F32),
            vmem((4, 32, 128), F32),
            vmem((4, 16, 128), F32),
            vmem((4, 32, 128), F32),
            vmem((4, 16, 128), F32),
            vmem((4, 32, 128), F32),
            vmem((4, 32, 128), F32),
            vmem((OWN, 8, 128), F32),
            vmem((8, 16, 128), F32),
            vmem((8, 8, 128), F32),
            vmem((8, 16, 128), F32),
            vmem((8, 8, 128), F32),
            vmem((8, 16, 128), F32),
            vmem((8, 16, 128), F32),
            vmem((OWN, 8, 128), F32),
            vmem((24, 128), F32),
            vmem((24, 128), F32),
            vmem((40, 128), F32),
            vmem((SUBJ, 24, 128), F32),
            vmem((SUBJ, 24, 128), F32),
            vmem((SUBJ, 40, 128), F32),
            vmem((2, 4 * EP * LOCAL, 64), BF16),
            vmem((2, EP * LOCAL, 48), BF16),
            vmem((2, EP * LOCAL, 48), BF16),
            vmem((2, EP * LOCAL, 64), BF16),
            vmem((2, 4 * EP * LOCAL, 128), BF16),
            vmem((2, 2 * EP * LOCAL, 128), BF16),
            vmem((2, EP * LOCAL, 128), BF16),
            vmem((2, 864, ROWS), BF16),
            dma((3,)),
            dma,
            dma,
            dma,
            dma,
            dma((2,)),
            dma((2,)),
            dma((2 * QUADS,)),
            dma((2 * QUADS,)),
            dma((2 * QUADS,)),
            dma((2 * QUADS,)),
            dma((3,)),
            dma((3, 4)),
            dma((3, 4)),
            dma((4,)),
            dma((3,)),
            dma((3, 3)),
            dma((3,)),
            dma((3,)),
        ],
        compiler_params=pltpu.CompilerParams(collective_id=0, has_side_effects=True),
    )(series, offsets, selected)


def solution(mesh):
    placed = (P("subj", None, "vox"), P(), P())
    return jax.shard_map(
        body, mesh=mesh, in_specs=placed, out_specs=P("vox", "subj", None), check_vma=False
    )
```

```python
import functools

import jax
import jax.numpy as jnp
from jax import lax
from jax.experimental import pallas as pl
from jax.experimental.pallas import tpu as pltpu
from jax.sharding import PartitionSpec as P

MESH = pl.DeviceIdType.MESH
F32, BF16, I32 = jnp.float32, jnp.bfloat16, jnp.int32
HIGH = lax.Precision.HIGHEST

SUBJ, SHARDS = 4, 32
TR, EP, RUN = 16, 12, 256
LOCAL = 4
QUADS = 3
SEL, OWN = 64, 16
VOX = 512
ROWS = SUBJ * EP * LOCAL
NT = (((1,), (1,)), ((), ()))
series_floor = 1.0
spread_floor = 0.05
shrink_factor = 0.9


def copy_to(src, dst, send_sem, recv_sem, subj, vox):
    return pltpu.make_async_remote_copy(
        src_ref=src,
        dst_ref=dst,
        send_sem=send_sem,
        recv_sem=recv_sem,
        device_id={"subj": subj, "vox": vox},
        device_id_type=MESH,
    )


def await_bytes(ref, sem):
    pltpu.make_async_copy(ref, ref, sem).wait()


def fold(x):
    return x + pltpu.roll(x, 4, 0)


def exact_terms(x):
    first = x.astype(BF16)
    rest = x - first.astype(F32)
    second = rest.astype(BF16)
    return first, second, (rest - second.astype(F32)).astype(BF16)


def two_terms(x):
    first = x.astype(BF16)
    return first, (x - first.astype(F32)).astype(BF16)


def slot_of(group, taker):
    return jnp.where((group ^ taker) < 2, group ^ taker, 2 + (group & 1))


def line_of(slot, epoch, subject):
    return slot * (EP * LOCAL) + epoch * LOCAL + subject


def main_kernel(
    series_hbm,
    offsets_hbm,
    selected_hbm,
    out_ref,
    offsets,
    selected,
    series,
    choose,
    epochs,
    scale,
    slab_out,
    slab_in,
    slab_sum,
    slab,
    raw,
    lhs_hi,
    lhs_lo,
    std_hi,
    std_lo,
    corr_even,
    corr_odd,
    score,
    gram_a,
    gram_b,
    gram_c,
    z_parts_a,
    z_parts_b,
    z_parts_c,
    x_parts_a,
    x_parts_b,
    x_parts_c,
    y_parts,
    z_sums_a,
    z_sums_b,
    z_sums_c,
    x_sums_a,
    x_sums_b,
    x_sums_c,
    y_sums,
    z_last_a,
    z_last_b,
    z_last_c,
    x_last_a,
    x_last_b,
    x_last_c,
    y_last,
    total_a,
    total_b,
    total_c,
    final_a,
    final_b,
    final_c,
    pick_a,
    pick_b,
    pick_wide,
    pick_square,
    turn_a,
    turn_b,
    turn_c,
    put_columns,
    load_sem,
    slab_send,
    slab_recv,
    share_send,
    share_recv,
    near_send,
    near_recv,
    far_send,
    far_recv,
    relay_send,
    relay_recv,
    part_send,
    z_recv,
    x_recv,
    y_recv,
    sum_send,
    sum_recv,
    final_send,
    final_recv,
):
    corr = (corr_even, corr_odd)
    z_parts, x_parts = (z_parts_a, z_parts_b, z_parts_c), (x_parts_a, x_parts_b, x_parts_c)
    z_sums, x_sums = (z_sums_a, z_sums_b, z_sums_c), (x_sums_a, x_sums_b, x_sums_c)
    last = ((z_last_a, x_last_a), (z_last_b, x_last_b), (z_last_c, x_last_c, y_last))
    gram = (gram_a, gram_b, gram_c)
    total, final = (total_a, total_b, total_c), (final_a, final_b, final_c)
    j = lax.axis_index("subj")
    v = lax.axis_index("vox")
    near, far, core = j ^ 1, j ^ 2, j & 1
    z, x, y = v // 8, (v // 2) & 3, v & 1

    def ahead_of(place, step):
        return (place + step) & 3

    def shard_at(z, x, y):
        return z * 8 + x * 2 + y

    loads = [
        pltpu.make_async_copy(source, target, load_sem.at[i])
        for i, (source, target) in enumerate(
            ((offsets_hbm, offsets), (selected_hbm, selected), (series_hbm, series))
        )
    ]
    for load in loads:
        load.start()

    barrier = pltpu.get_barrier_semaphore()

    def greet(step, carry):
        for other in range(SUBJ):
            pl.semaphore_signal(
                barrier,
                inc=1,
                device_id={"subj": j ^ other, "vox": (v + step) & (SHARDS - 1)},
                device_id_type=MESH,
            )
        return carry

    with jax.named_scope("greet"):
        lax.fori_loop(1, SHARDS, greet, 0, unroll=4)
        for other in range(1, SUBJ):
            pl.semaphore_signal(barrier, inc=1, device_id={"subj": j ^ other, "vox": v}, device_id_type=MESH)

    loads[0].wait()
    loads[1].wait()

    with jax.named_scope("choose"):
        row16 = lax.broadcasted_iota(I32, (16, 128), 0)
        scan = lax.broadcasted_iota(I32, (16, LOCAL * RUN), 1)
        for q in range(QUADS):
            start = jnp.zeros((16, 128), I32)
            for r in range(16):
                first = offsets[j * LOCAL + r % 4, q * 4 + r // 4] + (r % 4) * RUN
                start = jnp.where(row16 == r, first, start)
            ahead = scan - jnp.concatenate([start] * (LOCAL * RUN // 128), axis=1)
            for t in range(TR):
                choose[pl.ds(q * 256 + t * 16, 16), :] = jnp.where(ahead == t, 1.0, 0.0).astype(BF16)

    id_rows = []
    row8 = lax.broadcasted_iota(I32, (8, 128), 0)
    for block in range(SEL // 8):
        ids = jnp.zeros((8, 128), I32)
        for r in range(8):
            place = block * 8 + r
            ids = jnp.where(row8 == r, selected[4 * (place % OWN) + place // OWN], ids)
        id_rows.append(ids)
    ids = jnp.concatenate(id_rows, axis=0)
    columns = lax.broadcasted_iota(I32, (SEL, VOX), 1) + v * VOX
    picker = jnp.where(columns == jnp.concatenate([ids] * (VOX // 128), axis=1), 1.0, 0.0).astype(BF16)

    with jax.named_scope("pick_epochs"):
        loads[2].wait()
        runs = series[...].reshape(LOCAL * RUN, VOX)
        all_chosen = jnp.dot(choose[...], runs, preferred_element_type=F32).astype(BF16)
        for q in range(QUADS):
            chosen = all_chosen[q * 256 : q * 256 + 256]
            for h in range(2):
                epochs[0, h, q] = chosen[:, h * 256 : h * 256 + 256]
            picked = lax.dot_general(picker, chosen, NT, preferred_element_type=F32)
            slab_out[:, :, pl.ds(q * 256, 256)] = picked.astype(BF16).reshape(SHARDS, 2, 256)

    with jax.named_scope("barrier"):
        pl.semaphore_wait(barrier, SUBJ * SHARDS - 1)

    def send_slab(step, carry):
        piece = (v + step) & (SHARDS - 1)
        to_j, to_v = piece // 8, j * 8 + (piece & 7)

        @pl.when(jnp.logical_or(to_j != j, to_v != v))
        def _():
            copy_to(slab_out.at[piece], slab_in.at[v], slab_send, slab_recv, to_j, to_v).start()

        return carry

    with jax.named_scope("send_slab"):
        lax.fori_loop(0, SHARDS, send_slab, 0)

    def near_copy(h):
        return copy_to(epochs.at[0, h], epochs.at[1, h], near_send.at[h], near_recv.at[h], near, v)

    def far_copy(g, q):
        at = g * QUADS + q
        source, target = epochs.at[core ^ g, core, q], epochs.at[2 + g, core, q]
        return copy_to(source, target, far_send.at[at], far_recv.at[at], far, v)

    def relay_copy(g, q):
        at = g * QUADS + q
        ref = epochs.at[2 + g, core, q]
        return copy_to(ref, ref, relay_send.at[at], relay_recv.at[at], near, v)

    def relay(g, q):
        with jax.named_scope("relay"):
            far_copy(g, q).wait_recv()
            relay_copy(g, q).start()

    for h in (1, 0):
        near_copy(h).start()

    def start_far(of_core_0, of_core_1):
        @pl.when(core == 0)
        def _():
            far_copy(*of_core_0).start()

        @pl.when(core == 1)
        def _():
            far_copy(*of_core_1).start()

    start_far((0, 0), (1, 0))

    def lanes_of(h):
        return pl.ds(h * 256 if isinstance(h, int) else pl.multiple_of(h * 256, 256), 256)

    def scales(r, h):
        lanes = lanes_of(h)
        for q in range(QUADS):
            seen = epochs[r, h, q].astype(F32).reshape(TR, 16, 256)
            centred = seen - (jnp.sum(seen, axis=0) * (1.0 / TR))[None]
            scale[r, q, :, lanes] = lax.rsqrt(jnp.sum(centred * centred, axis=0) + series_floor)

    for h in range(2):
        scales(0, h)

    with jax.named_scope("near_wait"):
        for h in range(2):
            near_copy(h).wait_recv()

    start_far((0, 1), (0, 0))

    own_group = v // 8 == j

    with jax.named_scope("slab_wait"):

        @pl.when(own_group)
        def _():
            slab_in[v] = slab_out[j * 8 + (v & 7)]
            await_bytes(slab_in.at[pl.ds(0, SHARDS - 1)], slab_recv)

        @pl.when(jnp.logical_not(own_group))
        def _():
            await_bytes(slab_in, slab_recv)

    with jax.named_scope("slab_sum"):
        slab_sum[...] = jnp.sum(slab_in[...].astype(F32), axis=0).astype(BF16)

    def share_slab(step, carry):
        copy_to(slab_sum, slab.at[v], share_send, share_recv, j, (v + step) & (SHARDS - 1)).start()
        return carry

    with jax.named_scope("share_slab"):
        lax.fori_loop(1, SHARDS, share_slab, 0)
        slab[v] = slab_sum[...]

    start_far((0, 2), (0, 1))
    start_far((1, 0), (0, 2))
    far_copy(1, 1).start()
    far_copy(1, 2).start()

    with jax.named_scope("places"):
        b = lax.broadcasted_iota(I32, (1, ROWS), 1)
        p = lax.broadcasted_iota(I32, (EP * LOCAL, 1), 0)
        for i in range(2):
            taker = y * 2 + i
            s = b // EP
            to = line_of(slot_of(s // LOCAL, taker), b - s * EP, s & 3)
            s = p // EP
            line = line_of(slot_of(j, taker), p - s * EP, s)

            def put(first, lines):
                put_columns[i, pl.ds(first, lines.shape[0]), :] = jnp.where(lines == to, 1.0, 0.0).astype(BF16)

            def hot(lines):
                return jnp.where(lines == line, 1.0, 0.0).astype(BF16)

            def down(count):
                return lax.broadcasted_iota(I32, (count, 1), 0)

            def across(count):
                return lax.broadcasted_iota(I32, (1, count), 1)

            c, r = down(128), down(64)
            around = (c & 63) + 64
            put(0, jnp.where(c < 64, c, c - 32))
            put(128, jnp.where(around < 96, around, around - 96))
            put(256, jnp.where(r < 32, r, jnp.where(r < 48, r + 32, -1)))
            put(320, jnp.where(r < 48, jnp.where(r < 32, r + 32, r + 48), -1))
            c, r = across(128), across(64)
            around = (c & 63) + 64
            apart = (c & 32) > 0
            for piece, (lines, columns) in enumerate(
                (
                    (jnp.where(r < 32, r, -1), jnp.where(apart & (c < 64), c, -1)),
                    (jnp.where(r < 32, r + 32, -1), jnp.where(apart & (c >= 64), c - 32, -1)),
                    (jnp.where((r >= 32) & (r < 48), r + 32, -1), jnp.where(apart & (c < 64), around - 96, -1)),
                    (jnp.where((r >= 32) & (r < 48), r + 48, -1), jnp.where(apart & (c >= 64), around - 96, -1)),
                )
            ):
                pick_a[i, pl.ds(piece * 48, 48), :] = hot(lines)
                turn_a[i, pl.ds(piece * 48, 48), :] = hot(columns)
            put(384, down(128))
            put(512, down(48) + 96)
            pick_b[i] = hot(across(48) + 96)
            turn_b[i, 0:48, :] = hot(jnp.where(c < 96, c, -1))
            turn_b[i, 48:96, :] = hot(jnp.where(c < 96, -1, c))
            put(560, down(128))
            put(688, (down(128) & 63) + 128)
            put(816, down(48) + 144)
            pick_wide[i] = hot(across(48) + 144)
            pick_square[i] = hot(r + 128)
            turn_c[i] = hot(c)
        for k in range(OWN):
            score[k, 96:128, :] = jnp.zeros((32, VOX), BF16)

    for h in range(2):
        scales(1, h)

    relay(0, 0)
    relay(0, 1)
    with jax.named_scope("share_wait"):
        await_bytes(slab.at[pl.ds(0, SHARDS - 1)], share_recv)
    relay(0, 2)

    with jax.named_scope("standard_slab"):
        for r in range(SUBJ):
            group = (j, near, far & 2, far | 1)[r]
            for kk in range(8):
                for q in range(QUADS):
                    raw[r * QUADS + q, pl.ds(kk * 2, 2), :] = slab[group * 8 + kk, :, pl.ds(q * 256, 256)].astype(F32)
        seen = raw[...].reshape(SUBJ * QUADS * OWN, 256)
        same = jnp.where(
            (lax.broadcasted_iota(I32, (256, 256), 0) & 15) == (lax.broadcasted_iota(I32, (256, 256), 1) & 15), 1.0, 0.0
        ).astype(BF16)
        centred = seen - jnp.dot(seen.astype(BF16), same, preferred_element_type=F32) * (1.0 / TR)
        terms = exact_terms(centred * centred)
        spread = [jnp.dot(t, same, preferred_element_type=F32) for t in terms]
        spread = spread[0] + spread[1] + spread[2]
        x_std = centred * lax.rsqrt(spread + series_floor) * shrink_factor
        x_hi = x_std.astype(BF16).astype(F32)
        std_hi[...] = x_hi.reshape(SUBJ * QUADS, OWN, 256)
        std_lo[...] = (x_std - x_hi).reshape(SUBJ * QUADS, OWN, 256)

    own_row = (lax.broadcasted_iota(I32, (16, 256), 1) & 15) == lax.broadcasted_iota(I32, (16, 256), 0)

    units = ((0, 0), (0, 1), (1, 0), (1, 1), (2, 0), (2, 1), (3, core), (3, 1 - core))

    def correlate(unit):
        r, h = units[unit]
        lanes = lanes_of(h)
        if r >= 2:
            scales(r, h)
        for q in range(QUADS):
            at = r * QUADS + q
            if unit % 2 == 0:
                for k in range(OWN):
                    for std, lhs in ((std_hi, lhs_hi), (std_lo, lhs_lo)):
                        line = jnp.broadcast_to(std[at, pl.ds(k, 1), :], (16, 256))
                        lhs[at, pl.ds(k * 16, 16), :] = jnp.where(own_row, line, 0.0).astype(BF16)
            seen = epochs[r, h, q]
            corr[unit % 2][q] = jnp.dot(lhs_hi[at], seen, preferred_element_type=F32) + jnp.dot(
                lhs_lo[at], seen, preferred_element_type=F32
            )

    def standard(unit, ids=range(OWN)):
        r, h = units[unit]
        lanes = lanes_of(h)
        for k in ids:
            rows = pl.ds(k * 16 if isinstance(k, int) else pl.multiple_of(k * 16, 16), 16)
            halves = []
            for q in range(QUADS):
                shrunk = corr[unit % 2][q, rows, :] * scale[r, q, :, lanes]
                twice = jnp.log(1.0 + shrunk) - jnp.log(1.0 - shrunk)
                halves += [twice[0:8], twice[8:16]]
            mean = fold(functools.reduce(jnp.add, halves)) * (1.0 / EP)
            halves = [f - mean for f in halves]
            spread = fold(functools.reduce(jnp.add, [f * f for f in halves])) * (1.0 / EP)
            gain = lax.rsqrt(spread + 4.0 * spread_floor)
            for q in range(QUADS):
                both = jnp.concatenate([halves[2 * q] * gain, halves[2 * q + 1] * gain], axis=0).astype(BF16)
                at = r * 48 + q * 16
                score[k, pl.ds(at, 16), lanes] = both

    split = ((32, 16, 0), (16, 32, 0), (32, 32, 16))
    lane = lax.broadcasted_iota(I32, (16, 128), 1)

    def against(m, first, count, columns=slice(0, 128)):
        return lax.dot_general(score[m, pl.ds(first, count), :], score[m, columns, :], NT, preferred_element_type=F32)

    def block_of(n, m):
        if n == 0:
            block = against(m, 0, 96)
            for top in (0, 16):
                beside = pltpu.roll(block[32 + top : 48 + top], 32, 1)
                gram[n][m, top : top + 16, :] = jnp.where(lane < 64, block[top : top + 16], beside)
            upper, lower = block[64:80], block[80:96]
            left = jnp.where(lane < 32, pltpu.roll(upper, 64, 1), pltpu.roll(upper, 32, 1))
            right = jnp.where(lane < 96, lower, pltpu.roll(lower, 96, 1))
            gram[n][m, 32:48, :] = jnp.where(lane < 64, left, right)
        elif n == 1:
            gram[n][m] = against(m, 96, 48)
        else:
            gram[n][m, 0:48, :] = against(m, 144, 48)
            square = against(m, 128, 64, slice(128, 192))
            gram[n][m, 48:80, :] = jnp.concatenate([square[0:32], square[32:64]], axis=1)

    def kernels(n, unfinished=None):
        z_rows, x_rows, y_rows = split[n]

        def offsets_at(step):
            slow, fast = (step // 4 + 1) & 3, (step + 1) & 3
            return slow ^ (slow >> 1), fast ^ (fast >> 1)

        def id_at(step):
            major, minor = offsets_at(step)
            return ahead_of(z, major) * 4 + ahead_of(x, minor)

        size = 2 if n == 2 else 4

        def some(index, carry):
            steps = [index * size + more for more in range(2 * size)]
            for step in steps[:size]:
                block_of(n, id_at(step))
            if unfinished is not None:
                standard(unfinished, [id_at(step & 15) for step in steps[size:]])
            for step in steps[:size]:
                major, minor = offsets_at(step)
                m = ahead_of(z, major) * 4 + ahead_of(x, minor)

                @pl.when(major > 0)
                def _():
                    source = gram[n].at[m, pl.ds(0, z_rows)]
                    to_v = shard_at(ahead_of(z, major), x, y)
                    copy_to(source, z_parts[n].at[minor, major], part_send.at[n], z_recv.at[n, minor], j, to_v).start()

                @pl.when(minor > 0)
                def _():
                    source = gram[n].at[m, pl.ds(z_rows, x_rows)]
                    to_v = shard_at(z, ahead_of(x, minor), y)
                    copy_to(source, x_parts[n].at[major, minor], part_send.at[n], x_recv.at[n, major], j, to_v).start()

                if y_rows:
                    rows = pl.ds(pl.multiple_of(z_rows + x_rows + y_rows // 2 * (y ^ 1), 8), y_rows // 2)
                    copy_to(
                        gram[n].at[m, rows], y_parts.at[major * 4 + minor], part_send.at[n], y_recv.at[major], j, v ^ 1
                    ).start()
            return carry

        with jax.named_scope("kernels"):
            if unfinished is not None:
                standard(unfinished, [id_at(step) for step in range(size)])
            lax.fori_loop(0, OWN // size, some, 0)

    def second_sums(n):
        z_rows, x_rows, y_rows = split[n]

        def along(step, block):
            parts, recv, sums = ((z_parts, z_recv, z_sums), (x_parts, x_recv, x_sums))[block]
            with jax.named_scope("part_wait"):
                await_bytes(parts[n].at[step, pl.ds(1, 3)], recv.at[n, step])
            own = (ahead_of(z, step) * 4 + x) if block else (z * 4 + ahead_of(x, step))
            own = gram[n][own, pl.ds(z_rows, x_rows) if block else pl.ds(0, z_rows), :]
            sums[n][step] = (own + parts[n][step, 1]) + (parts[n][step, 2] + parts[n][step, 3])
            for other in range(2):
                side = y ^ other
                count = (z_rows, x_rows)[block] // 2
                rows = pl.ds(pl.multiple_of(side * count, 8), count)
                slot = step * 2 + other
                to_v = shard_at(ahead_of(z, step), x, side) if block else shard_at(z, ahead_of(x, step), side)
                if slot:
                    copy_to(
                        sums[n].at[step, rows], last[n][block].at[slot], sum_send.at[n], sum_recv.at[n, block], j, to_v
                    ).start()
                else:
                    last[n][block][0] = sums[n][0, rows, :]

        def from_side(major):
            with jax.named_scope("part_wait"):
                await_bytes(y_parts.at[pl.ds(major * 4, 4)], y_recv.at[major])
            for minor in range(4):
                step = major * 4 + minor
                to_z, to_x = ahead_of(z, major), ahead_of(x, minor)
                rows = pl.ds(pl.multiple_of(z_rows + x_rows + y_rows // 2 * y, 8), y_rows // 2)
                added = y_parts[step] + gram[n][to_z * 4 + to_x, rows, :]
                if step:
                    y_sums[step] = added
                    copy_to(
                        y_sums.at[step], y_last.at[step], sum_send.at[n], sum_recv.at[n, 2], j, shard_at(to_z, to_x, y)
                    ).start()
                else:
                    y_last[0] = added

        if y_rows:
            for major in (1, 3, 2, 0):
                along(major, 1)
                from_side(major)
        else:
            for step in (1, 3, 2, 0):
                along(step, 1)
        for step in (1, 3, 2, 0):
            along(step, 0)

    owner_v = v - y + j // 2
    place = core * 2 + y

    def hand_over(n):
        with jax.named_scope("last_wait"):
            for block, ref in enumerate(last[n]):
                await_bytes(ref.at[pl.ds(0, ref.shape[0] - 1)], sum_recv.at[n, block])
        mean = 1.0 / (VOX * SHARDS)
        first = 0
        for ref in last[n]:
            rows = ref.shape[1]
            total[n][pl.ds(first, rows), :] = jnp.sum(ref[...], axis=0) * mean
            first += rows
        for other in range(SUBJ):
            copy = copy_to(
                total[n], final[n].at[place], final_send.at[n], final_recv.at[n], (j ^ other) if other else j, owner_v
            )
            if other:
                copy.start()
            else:

                @pl.when(owner_v != v)
                def _():
                    copy.start()

        @pl.when(owner_v == v)
        def _():
            final[n][place] = total[n][...]

    def await_final(n, sem):
        @pl.when(owner_v == v)
        def _():
            await_bytes(final[n].at[pl.ds(0, SUBJ - 1)], sem.at[n])

        @pl.when(owner_v != v)
        def _():
            await_bytes(final[n], sem.at[n])

    def scores_of(correlated, finished):
        with jax.named_scope("scores"):
            if correlated is not None:
                correlate(correlated)
            if finished is not None:
                standard(finished)

    def relayed(g):
        with jax.named_scope("relay_wait"):
            for q in range(QUADS):
                relay_copy(g, q).wait_recv()

    scores_of(0, None)
    scores_of(1, 0)
    scores_of(2, 1)
    scores_of(3, 2)
    relayed(0)
    scores_of(4, 3)
    relay(1, 0)
    kernels(0, 4)
    scores_of(5, None)
    kernels(1, 5)
    relay(1, 1)
    relay(1, 2)
    scores_of(6, None)
    scores_of(None, 6)
    second_sums(0)
    relayed(1)
    scores_of(7, None)
    kernels(2, 7)
    second_sums(1)
    second_sums(2)
    hand_over(0)
    hand_over(1)
    hand_over(2)

    straight = (((1,), (0,)), ((), ()))
    left = lax.broadcasted_iota(I32, (EP * LOCAL, 128), 1) < 64
    upper = lax.broadcasted_iota(I32, (EP * LOCAL, 64), 1) < 32
    puts = (0, 384, 560, 864)
    corner = lax.broadcasted_iota(I32, (EP * LOCAL, 48), 1) >= 32

    def picked_by(pick, terms, dims):
        parts = [lax.dot_general(pick, t, dims, preferred_element_type=F32) for t in terms]
        return parts[0] + parts[1]

    def placed(n, i):
        pieces, first = [], 0
        for rows in split[n]:
            if rows:
                here = pl.ds(first, rows // 2)
                pieces += [final[n][2 * i, here, :], final[n][2 * i + 1, here, :]]
                first += rows // 2
        if n == 0:
            terms = two_terms(jnp.concatenate(pieces + [jnp.zeros((16, 128), F32)], axis=0))
            by_row = picked_by(pick_a[i], terms, straight)
            by_column = picked_by(turn_a[i], terms, NT)
            lines = [
                jnp.where(left, by_row[0:48], by_row[48:96]),
                jnp.where(left, by_row[96:144], by_row[144:192]),
                jnp.where(upper, by_column[0:48], by_column[96:144]),
                jnp.where(upper, by_column[48:96], by_column[144:192]),
            ]
        elif n == 1:
            terms = two_terms(jnp.concatenate(pieces, axis=0))
            by_column = picked_by(turn_b[i], terms, NT)
            turned = by_column[0:48] + jnp.where(corner, by_column[48:96], 0.0)
            lines = [picked_by(pick_b[i], terms, straight), turned]
        else:
            both = jnp.concatenate(pieces, axis=0)
            wide, square = two_terms(both[0:48]), two_terms(both[48:80])
            halves = [picked_by(pick_square[i, :, h * 32 : h * 32 + 32], square, straight) for h in range(2)]
            lines = [
                picked_by(pick_wide[i], wide, straight),
                jnp.where(left, halves[0], halves[1]),
                picked_by(turn_c[i], wide, NT),
            ]
        put = put_columns[i, puts[n] : puts[n + 1], :]
        terms = [jnp.dot(t, put, preferred_element_type=F32) for t in two_terms(jnp.concatenate(lines, axis=1))]
        return terms[0] + terms[1]

    with jax.named_scope("final"):
        await_final(0, final_recv)
    with jax.named_scope("place"):
        for i in range(2):
            out_ref[i] = placed(0, i)
    with jax.named_scope("final"):
        await_final(1, final_recv)
    with jax.named_scope("place"):
        for i in range(2):
            out_ref[i] += placed(1, i)
    with jax.named_scope("final"):
        await_final(2, final_recv)
    with jax.named_scope("place"):
        for i in range(2):
            out_ref[i] += placed(2, i)

    with jax.named_scope("drain"):
        await_bytes(slab_in.at[pl.ds(0, SHARDS - 1)], share_send)

        @pl.when(own_group)
        def _():
            await_bytes(slab_in.at[pl.ds(0, SHARDS - 1)], slab_send)

        @pl.when(jnp.logical_not(own_group))
        def _():
            await_bytes(slab_in, slab_send)

        for n in range(3):
            await_bytes(z_parts[n].at[pl.ds(0, 3)], part_send.at[n])
            await_bytes(x_parts[n].at[pl.ds(0, 3)], part_send.at[n])
            for ref in last[n]:
                await_bytes(ref.at[pl.ds(0, ref.shape[0] - 1)], sum_send.at[n])
            await_final(n, final_send)
        await_bytes(y_parts, part_send.at[2])
        for h in range(2):
            near_copy(h).wait_send()
            for q in range(QUADS):
                far_copy(h, q).wait_send()
                relay_copy(h, q).wait_send()


def body(series, offsets, selected):
    vmem = pltpu.VMEM
    dma = pltpu.SemaphoreType.DMA
    return pl.pallas_call(
        main_kernel,
        out_shape=pltpu.VMEM((2, EP * LOCAL, ROWS), F32),
        in_specs=[
            pl.BlockSpec(memory_space=pl.ANY),
            pl.BlockSpec(memory_space=pl.ANY),
            pl.BlockSpec(memory_space=pl.ANY),
        ],
        out_specs=pl.BlockSpec(memory_space=pltpu.VMEM),
        scratch_shapes=[
            pltpu.SMEM((SUBJ * LOCAL, EP), I32),
            pltpu.SMEM((SEL,), I32),
            vmem((LOCAL, RUN, VOX), BF16),
            vmem((QUADS * 256, LOCAL * RUN), BF16),
            vmem((SUBJ, 2, QUADS, 256, 256), BF16),
            vmem((SUBJ, QUADS, 16, VOX), F32),
            vmem((SHARDS, 2, QUADS * 256), BF16),
            vmem((SHARDS, 2, QUADS * 256), BF16),
            vmem((2, QUADS * 256), BF16),
            vmem((SHARDS, 2, QUADS * 256), BF16),
            vmem((SUBJ * QUADS, OWN, 256), F32),
            vmem((SUBJ * QUADS, 256, 256), BF16),
            vmem((SUBJ * QUADS, 256, 256), BF16),
            vmem((SUBJ * QUADS, OWN, 256), F32),
            vmem((SUBJ * QUADS, OWN, 256), F32),
            vmem((QUADS, 256, 256), F32),
            vmem((QUADS, 256, 256), F32),
            vmem((OWN, ROWS, VOX), BF16),
            vmem((OWN, 48, 128), F32),
            vmem((OWN, 48, 128), F32),
            vmem((OWN, 80, 128), F32),
            vmem((4, 4, 32, 128), F32),
            vmem((4, 4, 16, 128), F32),
            vmem((4, 4, 32, 128), F32),
            vmem((4, 4, 16, 128), F32),
            vmem((4, 4, 32, 128), F32),
            vmem((4, 4, 32, 128), F32),
            vmem((OWN, 8, 128), F32),
            vmem((4, 32, 128), F32),
            vmem((4, 16, 128), F32),
            vmem((4, 32, 128), F32),
            vmem((4, 16, 128), F32),
            vmem((4, 32, 128), F32),
            vmem((4, 32, 128), F32),
            vmem((OWN, 8, 128), F32),
            vmem((8, 16, 128), F32),
            vmem((8, 8, 128), F32),
            vmem((8, 16, 128), F32),
            vmem((8, 8, 128), F32),
            vmem((8, 16, 128), F32),
            vmem((8, 16, 128), F32),
            vmem((OWN, 8, 128), F32),
            vmem((24, 128), F32),
            vmem((24, 128), F32),
            vmem((40, 128), F32),
            vmem((SUBJ, 24, 128), F32),
            vmem((SUBJ, 24, 128), F32),
            vmem((SUBJ, 40, 128), F32),
            vmem((2, 4 * EP * LOCAL, 64), BF16),
            vmem((2, EP * LOCAL, 48), BF16),
            vmem((2, EP * LOCAL, 48), BF16),
            vmem((2, EP * LOCAL, 64), BF16),
            vmem((2, 4 * EP * LOCAL, 128), BF16),
            vmem((2, 2 * EP * LOCAL, 128), BF16),
            vmem((2, EP * LOCAL, 128), BF16),
            vmem((2, 864, ROWS), BF16),
            dma((3,)),
            dma,
            dma,
            dma,
            dma,
            dma((2,)),
            dma((2,)),
            dma((2 * QUADS,)),
            dma((2 * QUADS,)),
            dma((2 * QUADS,)),
            dma((2 * QUADS,)),
            dma((3,)),
            dma((3, 4)),
            dma((3, 4)),
            dma((4,)),
            dma((3,)),
            dma((3, 3)),
            dma((3,)),
            dma((3,)),
        ],
        compiler_params=pltpu.CompilerParams(collective_id=0, has_side_effects=True),
    )(series, offsets, selected)


def solution(mesh):
    placed = (P("subj", None, "vox"), P(), P())
    return jax.shard_map(
        body, mesh=mesh, in_specs=placed, out_specs=P("vox", "subj", None), check_vma=False
    )
```

```python
import functools

import jax
import jax.numpy as jnp
from jax import lax
from jax.experimental import pallas as pl
from jax.experimental.pallas import tpu as pltpu
from jax.sharding import PartitionSpec as P

MESH = pl.DeviceIdType.MESH
F32, BF16, I32 = jnp.float32, jnp.bfloat16, jnp.int32
HIGH = lax.Precision.HIGHEST

SUBJ, SHARDS = 4, 32
TR, EP, RUN = 16, 12, 256
LOCAL = 4
QUADS = 3
SEL, OWN = 64, 16
VOX = 512
ROWS = SUBJ * EP * LOCAL
NT = (((1,), (1,)), ((), ()))
series_floor = 1.0
spread_floor = 0.05
shrink_factor = 0.9


def copy_to(src, dst, send_sem, recv_sem, subj, vox):
    return pltpu.make_async_remote_copy(
        src_ref=src,
        dst_ref=dst,
        send_sem=send_sem,
        recv_sem=recv_sem,
        device_id={"subj": subj, "vox": vox},
        device_id_type=MESH,
    )


def await_bytes(ref, sem):
    pltpu.make_async_copy(ref, ref, sem).wait()


def fold(x):
    return x + pltpu.roll(x, 4, 0)


def exact_terms(x):
    first = x.astype(BF16)
    rest = x - first.astype(F32)
    second = rest.astype(BF16)
    return first, second, (rest - second.astype(F32)).astype(BF16)


def two_terms(x):
    first = x.astype(BF16)
    return first, (x - first.astype(F32)).astype(BF16)


def slot_of(group, taker):
    return jnp.where((group ^ taker) < 2, group ^ taker, 2 + (group & 1))


def line_of(slot, epoch, subject):
    return slot * (EP * LOCAL) + epoch * LOCAL + subject


def main_kernel(
    series_hbm,
    offsets_hbm,
    selected_hbm,
    out_ref,
    offsets,
    selected,
    series,
    choose,
    epochs,
    scale,
    slab_out,
    slab_in,
    slab_sum,
    slab,
    raw,
    lhs_hi,
    lhs_lo,
    std_hi,
    std_lo,
    corr_even,
    corr_odd,
    score,
    gram_a,
    gram_b,
    gram_c,
    z_parts_a,
    z_parts_b,
    z_parts_c,
    x_parts_a,
    x_parts_b,
    x_parts_c,
    y_parts,
    z_sums_a,
    z_sums_b,
    z_sums_c,
    x_sums_a,
    x_sums_b,
    x_sums_c,
    y_sums,
    z_last_a,
    z_last_b,
    z_last_c,
    x_last_a,
    x_last_b,
    x_last_c,
    y_last,
    total_a,
    total_b,
    total_c,
    final_a,
    final_b,
    final_c,
    pick_a,
    pick_b,
    pick_wide,
    pick_square,
    turn_a,
    turn_b,
    turn_c,
    put_columns,
    load_sem,
    sent,
    slab_recv,
    share_recv,
    near_recv,
    far_recv,
    relay_recv,
    z_recv,
    x_recv,
    y_recv,
    sum_recv,
    final_recv,
):
    corr = (corr_even, corr_odd)
    z_parts, x_parts = (z_parts_a, z_parts_b, z_parts_c), (x_parts_a, x_parts_b, x_parts_c)
    z_sums, x_sums = (z_sums_a, z_sums_b, z_sums_c), (x_sums_a, x_sums_b, x_sums_c)
    last = ((z_last_a, x_last_a), (z_last_b, x_last_b), (z_last_c, x_last_c, y_last))
    gram = (gram_a, gram_b, gram_c)
    total, final = (total_a, total_b, total_c), (final_a, final_b, final_c)
    j = lax.axis_index("subj")
    v = lax.axis_index("vox")
    near, far, core = j ^ 1, j ^ 2, j & 1
    z, x, y = v // 8, (v // 2) & 3, v & 1

    def ahead_of(place, step):
        return (place + step) & 3

    def shard_at(z, x, y):
        return z * 8 + x * 2 + y

    loads = [
        pltpu.make_async_copy(source, target, load_sem.at[i])
        for i, (source, target) in enumerate(
            ((offsets_hbm, offsets), (selected_hbm, selected), (series_hbm, series))
        )
    ]
    for load in loads:
        load.start()

    barrier = pltpu.get_barrier_semaphore()

    def greet(step, carry):
        for other in range(SUBJ):
            pl.semaphore_signal(
                barrier,
                inc=1,
                device_id={"subj": j ^ other, "vox": (v + step) & (SHARDS - 1)},
                device_id_type=MESH,
            )
        return carry

    with jax.named_scope("greet"):
        lax.fori_loop(1, SHARDS, greet, 0, unroll=4)
        for other in range(1, SUBJ):
            pl.semaphore_signal(barrier, inc=1, device_id={"subj": j ^ other, "vox": v}, device_id_type=MESH)

    loads[0].wait()
    loads[1].wait()

    with jax.named_scope("choose"):
        row16 = lax.broadcasted_iota(I32, (16, 128), 0)
        scan = lax.broadcasted_iota(I32, (16, LOCAL * RUN), 1)
        for q in range(QUADS):
            start = jnp.zeros((16, 128), I32)
            for r in range(16):
                first = offsets[j * LOCAL + r % 4, q * 4 + r // 4] + (r % 4) * RUN
                start = jnp.where(row16 == r, first, start)
            ahead = scan - jnp.concatenate([start] * (LOCAL * RUN // 128), axis=1)
            for t in range(TR):
                choose[pl.ds(q * 256 + t * 16, 16), :] = jnp.where(ahead == t, 1.0, 0.0).astype(BF16)

    id_rows = []
    row8 = lax.broadcasted_iota(I32, (8, 128), 0)
    for block in range(SEL // 8):
        ids = jnp.zeros((8, 128), I32)
        for r in range(8):
            place = block * 8 + r
            ids = jnp.where(row8 == r, selected[4 * (place % OWN) + place // OWN], ids)
        id_rows.append(ids)
    ids = jnp.concatenate(id_rows, axis=0)
    columns = lax.broadcasted_iota(I32, (SEL, VOX), 1) + v * VOX
    picker = jnp.where(columns == jnp.concatenate([ids] * (VOX // 128), axis=1), 1.0, 0.0).astype(BF16)

    with jax.named_scope("pick_epochs"):
        loads[2].wait()
        runs = series[...].reshape(LOCAL * RUN, VOX)
        all_chosen = jnp.dot(choose[...], runs, preferred_element_type=F32).astype(BF16)
        for q in range(QUADS):
            chosen = all_chosen[q * 256 : q * 256 + 256]
            for h in range(2):
                epochs[0, h, q] = chosen[:, h * 256 : h * 256 + 256]
            picked = lax.dot_general(picker, chosen, NT, preferred_element_type=F32)
            slab_out[:, :, pl.ds(q * 256, 256)] = picked.astype(BF16).reshape(SHARDS, 2, 256)

    with jax.named_scope("barrier"):
        pl.semaphore_wait(barrier, SUBJ * SHARDS - 1)

    def send_slab(step, carry):
        piece = (v + step) & (SHARDS - 1)
        to_j, to_v = piece // 8, j * 8 + (piece & 7)

        @pl.when(jnp.logical_or(to_j != j, to_v != v))
        def _():
            copy_to(slab_out.at[piece], slab_in.at[v], sent, slab_recv, to_j, to_v).start()

        return carry

    with jax.named_scope("send_slab"):
        lax.fori_loop(0, SHARDS, send_slab, 0)

    def near_copy(h):
        return copy_to(epochs.at[0, h], epochs.at[1, h], sent, near_recv, near, v)

    def far_copy(g, q):
        at = g * QUADS + q
        source, target = epochs.at[core ^ g, core, q], epochs.at[2 + g, core, q]
        return copy_to(source, target, sent, far_recv.at[at], far, v)

    def relay_copy(g, q):
        ref = epochs.at[2 + g, core, q]
        return copy_to(ref, ref, sent, relay_recv.at[g], near, v)

    def relay(g, q):
        with jax.named_scope("relay"):
            far_copy(g, q).wait_recv()
            relay_copy(g, q).start()

    for h in (1, 0):
        near_copy(h).start()

    @pl.when(core == 0)
    def _():
        far_copy(0, 0).start()

    def lanes_of(h):
        return pl.ds(h * 256 if isinstance(h, int) else pl.multiple_of(h * 256, 256), 256)

    def scales(r, h):
        lanes = lanes_of(h)
        for q in range(QUADS):
            seen = epochs[r, h, q].astype(F32).reshape(TR, 16, 256)
            centred = seen - (jnp.sum(seen, axis=0) * (1.0 / TR))[None]
            scale[r, q, :, lanes] = lax.rsqrt(jnp.sum(centred * centred, axis=0) + series_floor)

    for h in range(2):
        scales(0, h)

    with jax.named_scope("near_wait"):
        await_bytes(epochs.at[1], near_recv)

    @pl.when(core == 1)
    def _():
        far_copy(0, 0).start()

    far_copy(0, 1).start()

    own_group = v // 8 == j

    with jax.named_scope("slab_wait"):

        @pl.when(own_group)
        def _():
            slab_in[v] = slab_out[j * 8 + (v & 7)]
            await_bytes(slab_in.at[pl.ds(0, SHARDS - 1)], slab_recv)

        @pl.when(jnp.logical_not(own_group))
        def _():
            await_bytes(slab_in, slab_recv)

    with jax.named_scope("slab_sum"):
        slab_sum[...] = jnp.sum(slab_in[...].astype(F32), axis=0).astype(BF16)

    def share_slab(step, carry):
        copy_to(slab_sum, slab.at[v], sent, share_recv, j, (v + step) & (SHARDS - 1)).start()
        return carry

    with jax.named_scope("share_slab"):
        lax.fori_loop(1, SHARDS, share_slab, 0)
        slab[v] = slab_sum[...]

    far_copy(0, 2).start()
    for q in range(QUADS):
        far_copy(1, q).start()

    with jax.named_scope("places"):
        b = lax.broadcasted_iota(I32, (1, ROWS), 1)
        p = lax.broadcasted_iota(I32, (EP * LOCAL, 1), 0)
        for i in range(2):
            taker = y * 2 + i
            s = b // EP
            to = line_of(slot_of(s // LOCAL, taker), b - s * EP, s & 3)
            s = p // EP
            line = line_of(slot_of(j, taker), p - s * EP, s)

            def put(first, lines):
                put_columns[i, pl.ds(first, lines.shape[0]), :] = jnp.where(lines == to, 1.0, 0.0).astype(BF16)

            def hot(lines):
                return jnp.where(lines == line, 1.0, 0.0).astype(BF16)

            def down(count):
                return lax.broadcasted_iota(I32, (count, 1), 0)

            def across(count):
                return lax.broadcasted_iota(I32, (1, count), 1)

            c, r = down(128), down(64)
            around = (c & 63) + 64
            put(0, jnp.where(c < 64, c, c - 32))
            put(128, jnp.where(around < 96, around, around - 96))
            put(256, jnp.where(r < 32, r, jnp.where(r < 48, r + 32, -1)))
            put(320, jnp.where(r < 48, jnp.where(r < 32, r + 32, r + 48), -1))
            c, r = across(128), across(64)
            around = (c & 63) + 64
            apart = (c & 32) > 0
            for piece, (lines, columns) in enumerate(
                (
                    (jnp.where(r < 32, r, -1), jnp.where(apart & (c < 64), c, -1)),
                    (jnp.where(r < 32, r + 32, -1), jnp.where(apart & (c >= 64), c - 32, -1)),
                    (jnp.where((r >= 32) & (r < 48), r + 32, -1), jnp.where(apart & (c < 64), around - 96, -1)),
                    (jnp.where((r >= 32) & (r < 48), r + 48, -1), jnp.where(apart & (c >= 64), around - 96, -1)),
                )
            ):
                pick_a[i, pl.ds(piece * 48, 48), :] = hot(lines)
                turn_a[i, pl.ds(piece * 48, 48), :] = hot(columns)
            put(384, down(128))
            put(512, down(48) + 96)
            pick_b[i] = hot(across(48) + 96)
            turn_b[i, 0:48, :] = hot(jnp.where(c < 96, c, -1))
            turn_b[i, 48:96, :] = hot(jnp.where(c < 96, -1, c))
            put(560, down(128))
            put(688, (down(128) & 63) + 128)
            put(816, down(48) + 144)
            pick_wide[i] = hot(across(48) + 144)
            pick_square[i] = hot(r + 128)
            turn_c[i] = hot(c)
        for k in range(OWN):
            score[k, 96:128, :] = jnp.zeros((32, VOX), BF16)

    for h in range(2):
        scales(1, h)

    relay(0, 0)
    relay(0, 1)
    with jax.named_scope("share_wait"):
        await_bytes(slab.at[pl.ds(0, SHARDS - 1)], share_recv)
    relay(0, 2)

    with jax.named_scope("standard_slab"):
        for r in range(SUBJ):
            group = (j, near, far & 2, far | 1)[r]
            for kk in range(8):
                for q in range(QUADS):
                    raw[r * QUADS + q, pl.ds(kk * 2, 2), :] = slab[group * 8 + kk, :, pl.ds(q * 256, 256)].astype(F32)
        seen = raw[...].reshape(SUBJ * QUADS * OWN, 256)
        same = jnp.where(
            (lax.broadcasted_iota(I32, (256, 256), 0) & 15) == (lax.broadcasted_iota(I32, (256, 256), 1) & 15), 1.0, 0.0
        ).astype(BF16)
        centred = seen - jnp.dot(seen.astype(BF16), same, preferred_element_type=F32) * (1.0 / TR)
        terms = exact_terms(centred * centred)
        spread = [jnp.dot(t, same, preferred_element_type=F32) for t in terms]
        spread = spread[0] + spread[1] + spread[2]
        x_std = centred * lax.rsqrt(spread + series_floor) * shrink_factor
        x_hi = x_std.astype(BF16).astype(F32)
        std_hi[...] = x_hi.reshape(SUBJ * QUADS, OWN, 256)
        std_lo[...] = (x_std - x_hi).reshape(SUBJ * QUADS, OWN, 256)

    own_row = (lax.broadcasted_iota(I32, (16, 256), 1) & 15) == lax.broadcasted_iota(I32, (16, 256), 0)

    units = ((0, 0), (0, 1), (1, 0), (1, 1), (2, 0), (2, 1), (3, core), (3, 1 - core))

    def correlate(unit):
        r, h = units[unit]
        lanes = lanes_of(h)
        if r >= 2:
            scales(r, h)
        for q in range(QUADS):
            at = r * QUADS + q
            if unit % 2 == 0:
                for k in range(OWN):
                    for std, lhs in ((std_hi, lhs_hi), (std_lo, lhs_lo)):
                        line = jnp.broadcast_to(std[at, pl.ds(k, 1), :], (16, 256))
                        lhs[at, pl.ds(k * 16, 16), :] = jnp.where(own_row, line, 0.0).astype(BF16)
            seen = epochs[r, h, q]
            corr[unit % 2][q] = jnp.dot(lhs_hi[at], seen, preferred_element_type=F32) + jnp.dot(
                lhs_lo[at], seen, preferred_element_type=F32
            )

    def standard(unit, ids=range(OWN)):
        r, h = units[unit]
        lanes = lanes_of(h)
        for k in ids:
            rows = pl.ds(k * 16 if isinstance(k, int) else pl.multiple_of(k * 16, 16), 16)
            halves = []
            for q in range(QUADS):
                shrunk = corr[unit % 2][q, rows, :] * scale[r, q, :, lanes]
                twice = jnp.log(1.0 + shrunk) - jnp.log(1.0 - shrunk)
                halves += [twice[0:8], twice[8:16]]
            mean = fold(functools.reduce(jnp.add, halves)) * (1.0 / EP)
            halves = [f - mean for f in halves]
            spread = fold(functools.reduce(jnp.add, [f * f for f in halves])) * (1.0 / EP)
            gain = lax.rsqrt(spread + 4.0 * spread_floor)
            for q in range(QUADS):
                both = jnp.concatenate([halves[2 * q] * gain, halves[2 * q + 1] * gain], axis=0).astype(BF16)
                at = r * 48 + q * 16
                score[k, pl.ds(at, 16), lanes] = both

    split = ((32, 16, 0), (16, 32, 0), (32, 32, 16))
    lane = lax.broadcasted_iota(I32, (16, 128), 1)

    def against(m, first, count, columns=slice(0, 128)):
        return lax.dot_general(score[m, pl.ds(first, count), :], score[m, columns, :], NT, preferred_element_type=F32)

    def block_of(n, m):
        if n == 0:
            block = against(m, 0, 96)
            for top in (0, 16):
                beside = pltpu.roll(block[32 + top : 48 + top], 32, 1)
                gram[n][m, top : top + 16, :] = jnp.where(lane < 64, block[top : top + 16], beside)
            upper, lower = block[64:80], block[80:96]
            left = jnp.where(lane < 32, pltpu.roll(upper, 64, 1), pltpu.roll(upper, 32, 1))
            right = jnp.where(lane < 96, lower, pltpu.roll(lower, 96, 1))
            gram[n][m, 32:48, :] = jnp.where(lane < 64, left, right)
        elif n == 1:
            gram[n][m] = against(m, 96, 48)
        else:
            gram[n][m, 0:48, :] = against(m, 144, 48)
            square = against(m, 128, 64, slice(128, 192))
            gram[n][m, 48:80, :] = jnp.concatenate([square[0:32], square[32:64]], axis=1)

    def kernels(n, unfinished=None):
        z_rows, x_rows, y_rows = split[n]

        def offsets_at(step):
            slow, fast = (step // 4 + 1) & 3, (step + 1) & 3
            return slow ^ (slow >> 1), fast ^ (fast >> 1)

        def id_at(step):
            major, minor = offsets_at(step)
            return ahead_of(z, major) * 4 + ahead_of(x, minor)

        def four(index, carry):
            steps = [index * 4 + more for more in range(8)]
            for step in steps[:4]:
                block_of(n, id_at(step))
            if unfinished is not None:
                standard(unfinished, [id_at(step & 15) for step in steps[4:]])
            for step in steps[:4]:
                major, minor = offsets_at(step)
                m = ahead_of(z, major) * 4 + ahead_of(x, minor)

                @pl.when(major > 0)
                def _():
                    source = gram[n].at[m, pl.ds(0, z_rows)]
                    to_v = shard_at(ahead_of(z, major), x, y)
                    copy_to(source, z_parts[n].at[minor, major], sent, z_recv.at[n * 4 + minor], j, to_v).start()

                @pl.when(minor > 0)
                def _():
                    source = gram[n].at[m, pl.ds(z_rows, x_rows)]
                    to_v = shard_at(z, ahead_of(x, minor), y)
                    copy_to(source, x_parts[n].at[major, minor], sent, x_recv.at[n * 4 + major], j, to_v).start()

                if y_rows:
                    rows = pl.ds(pl.multiple_of(z_rows + x_rows + y_rows // 2 * (y ^ 1), 8), y_rows // 2)
                    copy_to(
                        gram[n].at[m, rows], y_parts.at[major * 4 + minor], sent, y_recv.at[major], j, v ^ 1
                    ).start()
            return carry

        with jax.named_scope("kernels"):
            if unfinished is not None:
                standard(unfinished, [id_at(step) for step in range(4)])
            lax.fori_loop(0, OWN // 4, four, 0)

    def second_sums(n):
        z_rows, x_rows, y_rows = split[n]

        def along(step, block):
            parts, recv, sums = ((z_parts, z_recv, z_sums), (x_parts, x_recv, x_sums))[block]
            with jax.named_scope("part_wait"):
                await_bytes(parts[n].at[step, pl.ds(1, 3)], recv.at[n * 4 + step])
            own = (ahead_of(z, step) * 4 + x) if block else (z * 4 + ahead_of(x, step))
            own = gram[n][own, pl.ds(z_rows, x_rows) if block else pl.ds(0, z_rows), :]
            sums[n][step] = (own + parts[n][step, 1]) + (parts[n][step, 2] + parts[n][step, 3])
            for other in range(2):
                side = y ^ other
                count = (z_rows, x_rows)[block] // 2
                rows = pl.ds(pl.multiple_of(side * count, 8), count)
                slot = step * 2 + other
                to_v = shard_at(ahead_of(z, step), x, side) if block else shard_at(z, ahead_of(x, step), side)
                if slot:
                    copy_to(
                        sums[n].at[step, rows], last[n][block].at[slot], sent, sum_recv.at[n * 2 + block], j, to_v
                    ).start()
                else:
                    last[n][block][0] = sums[n][0, rows, :]

        def from_side(major):
            with jax.named_scope("part_wait"):
                await_bytes(y_parts.at[pl.ds(major * 4, 4)], y_recv.at[major])
            for minor in range(4):
                step = major * 4 + minor
                to_z, to_x = ahead_of(z, major), ahead_of(x, minor)
                rows = pl.ds(pl.multiple_of(z_rows + x_rows + y_rows // 2 * y, 8), y_rows // 2)
                added = y_parts[step] + gram[n][to_z * 4 + to_x, rows, :]
                if step:
                    y_sums[step] = added
                    copy_to(
                        y_sums.at[step], y_last.at[step], sent, sum_recv.at[n * 2 + 2], j, shard_at(to_z, to_x, y)
                    ).start()
                else:
                    y_last[0] = added

        if y_rows:
            for major in (1, 3, 2, 0):
                along(major, 1)
                from_side(major)
        else:
            for step in (1, 3, 2, 0):
                along(step, 1)
        for step in (1, 3, 2, 0):
            along(step, 0)

    owner_v = v - y + j // 2
    place = core * 2 + y

    def hand_over(n):
        with jax.named_scope("last_wait"):
            for block, ref in enumerate(last[n]):
                await_bytes(ref.at[pl.ds(0, ref.shape[0] - 1)], sum_recv.at[n * 2 + block])
        mean = 1.0 / (VOX * SHARDS)
        first = 0
        for ref in last[n]:
            rows = ref.shape[1]
            total[n][pl.ds(first, rows), :] = jnp.sum(ref[...], axis=0) * mean
            first += rows
        for other in range(SUBJ):
            copy = copy_to(
                total[n], final[n].at[place], sent, final_recv.at[n], (j ^ other) if other else j, owner_v
            )
            if other:
                copy.start()
            else:

                @pl.when(owner_v != v)
                def _():
                    copy.start()

        @pl.when(owner_v == v)
        def _():
            final[n][place] = total[n][...]

    def await_final(n, sem):
        @pl.when(owner_v == v)
        def _():
            await_bytes(final[n].at[pl.ds(0, SUBJ - 1)], sem)

        @pl.when(owner_v != v)
        def _():
            await_bytes(final[n], sem)

    def scores_of(correlated, finished):
        with jax.named_scope("scores"):
            if correlated is not None:
                correlate(correlated)
            if finished is not None:
                standard(finished)

    def relayed(g):
        with jax.named_scope("relay_wait"):
            await_bytes(epochs.at[2 + g, 1 - core], relay_recv.at[g])

    scores_of(0, None)
    scores_of(1, 0)
    scores_of(2, 1)
    scores_of(3, 2)
    relayed(0)
    scores_of(4, 3)
    relay(1, 0)
    kernels(0)
    scores_of(5, 4)
    kernels(1, 5)
    relay(1, 1)
    relay(1, 2)
    scores_of(6, None)
    scores_of(None, 6)
    second_sums(0)
    relayed(1)
    scores_of(7, None)
    kernels(2, 7)
    second_sums(1)
    second_sums(2)
    hand_over(0)
    hand_over(1)

    straight = (((1,), (0,)), ((), ()))
    left = lax.broadcasted_iota(I32, (EP * LOCAL, 128), 1) < 64
    upper = lax.broadcasted_iota(I32, (EP * LOCAL, 64), 1) < 32
    puts = (0, 384, 560, 864)
    corner = lax.broadcasted_iota(I32, (EP * LOCAL, 48), 1) >= 32

    def picked_by(pick, terms, dims):
        parts = [lax.dot_general(pick, t, dims, preferred_element_type=F32) for t in terms]
        return parts[0] + parts[1]

    def placed(n, i):
        pieces, first = [], 0
        for rows in split[n]:
            if rows:
                here = pl.ds(first, rows // 2)
                pieces += [final[n][2 * i, here, :], final[n][2 * i + 1, here, :]]
                first += rows // 2
        if n == 0:
            terms = two_terms(jnp.concatenate(pieces + [jnp.zeros((16, 128), F32)], axis=0))
            by_row = picked_by(pick_a[i], terms, straight)
            by_column = picked_by(turn_a[i], terms, NT)
            lines = [
                jnp.where(left, by_row[0:48], by_row[48:96]),
                jnp.where(left, by_row[96:144], by_row[144:192]),
                jnp.where(upper, by_column[0:48], by_column[96:144]),
                jnp.where(upper, by_column[48:96], by_column[144:192]),
            ]
        elif n == 1:
            terms = two_terms(jnp.concatenate(pieces, axis=0))
            by_column = picked_by(turn_b[i], terms, NT)
            turned = by_column[0:48] + jnp.where(corner, by_column[48:96], 0.0)
            lines = [picked_by(pick_b[i], terms, straight), turned]
        else:
            both = jnp.concatenate(pieces, axis=0)
            wide, square = two_terms(both[0:48]), two_terms(both[48:80])
            halves = [picked_by(pick_square[i, :, h * 32 : h * 32 + 32], square, straight) for h in range(2)]
            lines = [
                picked_by(pick_wide[i], wide, straight),
                jnp.where(left, halves[0], halves[1]),
                picked_by(turn_c[i], wide, NT),
            ]
        put = put_columns[i, puts[n] : puts[n + 1], :]
        terms = [jnp.dot(t, put, preferred_element_type=F32) for t in two_terms(jnp.concatenate(lines, axis=1))]
        return terms[0] + terms[1]

    with jax.named_scope("final"):
        await_final(0, final_recv.at[0])
    with jax.named_scope("place"):
        for i in range(2):
            out_ref[i] = placed(0, i)
    hand_over(2)
    with jax.named_scope("final"):
        await_final(1, final_recv.at[1])
    with jax.named_scope("place"):
        for i in range(2):
            out_ref[i] += placed(1, i)
    with jax.named_scope("final"):
        await_final(2, final_recv.at[2])
    with jax.named_scope("place"):
        for i in range(2):
            out_ref[i] += placed(2, i)

    with jax.named_scope("drain"):
        for ref in (slab_in.at[pl.ds(0, SHARDS - 1)], slab_in.at[pl.ds(0, SHARDS - 1)]):
            await_bytes(ref, sent)

        @pl.when(jnp.logical_not(own_group))
        def _():
            await_bytes(slab_sum, sent)

        for slot in range(2):
            await_bytes(epochs.at[slot], sent)
        await_bytes(epochs.at[2], sent)
        for n in range(3):
            await_bytes(z_parts[n].at[pl.ds(0, 3)], sent)
            await_bytes(x_parts[n].at[pl.ds(0, 3)], sent)
            for ref in last[n]:
                await_bytes(ref.at[pl.ds(0, ref.shape[0] - 1)], sent)
            await_final(n, sent)
        await_bytes(y_parts, sent)


def body(series, offsets, selected):
    vmem = pltpu.VMEM
    dma = pltpu.SemaphoreType.DMA
    return pl.pallas_call(
        main_kernel,
        out_shape=pltpu.VMEM((2, EP * LOCAL, ROWS), F32),
        in_specs=[
            pl.BlockSpec(memory_space=pl.ANY),
            pl.BlockSpec(memory_space=pl.ANY),
            pl.BlockSpec(memory_space=pl.ANY),
        ],
        out_specs=pl.BlockSpec(memory_space=pltpu.VMEM),
        scratch_shapes=[
            pltpu.SMEM((SUBJ * LOCAL, EP), I32),
            pltpu.SMEM((SEL,), I32),
            vmem((LOCAL, RUN, VOX), BF16),
            vmem((QUADS * 256, LOCAL * RUN), BF16),
            vmem((SUBJ, 2, QUADS, 256, 256), BF16),
            vmem((SUBJ, QUADS, 16, VOX), F32),
            vmem((SHARDS, 2, QUADS * 256), BF16),
            vmem((SHARDS, 2, QUADS * 256), BF16),
            vmem((2, QUADS * 256), BF16),
            vmem((SHARDS, 2, QUADS * 256), BF16),
            vmem((SUBJ * QUADS, OWN, 256), F32),
            vmem((SUBJ * QUADS, 256, 256), BF16),
            vmem((SUBJ * QUADS, 256, 256), BF16),
            vmem((SUBJ * QUADS, OWN, 256), F32),
            vmem((SUBJ * QUADS, OWN, 256), F32),
            vmem((QUADS, 256, 256), F32),
            vmem((QUADS, 256, 256), F32),
            vmem((OWN, ROWS, VOX), BF16),
            vmem((OWN, 48, 128), F32),
            vmem((OWN, 48, 128), F32),
            vmem((OWN, 80, 128), F32),
            vmem((4, 4, 32, 128), F32),
            vmem((4, 4, 16, 128), F32),
            vmem((4, 4, 32, 128), F32),
            vmem((4, 4, 16, 128), F32),
            vmem((4, 4, 32, 128), F32),
            vmem((4, 4, 32, 128), F32),
            vmem((OWN, 8, 128), F32),
            vmem((4, 32, 128), F32),
            vmem((4, 16, 128), F32),
            vmem((4, 32, 128), F32),
            vmem((4, 16, 128), F32),
            vmem((4, 32, 128), F32),
            vmem((4, 32, 128), F32),
            vmem((OWN, 8, 128), F32),
            vmem((8, 16, 128), F32),
            vmem((8, 8, 128), F32),
            vmem((8, 16, 128), F32),
            vmem((8, 8, 128), F32),
            vmem((8, 16, 128), F32),
            vmem((8, 16, 128), F32),
            vmem((OWN, 8, 128), F32),
            vmem((24, 128), F32),
            vmem((24, 128), F32),
            vmem((40, 128), F32),
            vmem((SUBJ, 24, 128), F32),
            vmem((SUBJ, 24, 128), F32),
            vmem((SUBJ, 40, 128), F32),
            vmem((2, 4 * EP * LOCAL, 64), BF16),
            vmem((2, EP * LOCAL, 48), BF16),
            vmem((2, EP * LOCAL, 48), BF16),
            vmem((2, EP * LOCAL, 64), BF16),
            vmem((2, 4 * EP * LOCAL, 128), BF16),
            vmem((2, 2 * EP * LOCAL, 128), BF16),
            vmem((2, EP * LOCAL, 128), BF16),
            vmem((2, 864, ROWS), BF16),
            dma((3,)),
            dma,
            dma,
            dma,
            dma,
            dma((2 * QUADS,)),
            dma((2,)),
            dma((12,)),
            dma((12,)),
            dma((4,)),
            dma((7,)),
            dma((3,)),
        ],
        compiler_params=pltpu.CompilerParams(collective_id=0, has_side_effects=True),
    )(series, offsets, selected)


def solution(mesh):
    placed = (P("subj", None, "vox"), P(), P())
    return jax.shard_map(
        body, mesh=mesh, in_specs=placed, out_specs=P("vox", "subj", None), check_vma=False
    )
```

```python
import functools

import jax
import jax.numpy as jnp
from jax import lax
from jax.experimental import pallas as pl
from jax.experimental.pallas import tpu as pltpu
from jax.sharding import PartitionSpec as P

MESH = pl.DeviceIdType.MESH
F32, BF16, I32 = jnp.float32, jnp.bfloat16, jnp.int32
HIGH = lax.Precision.HIGHEST

SUBJ, SHARDS = 4, 32
TR, EP, RUN = 16, 12, 256
LOCAL = 4
QUADS = 3
SEL, OWN = 64, 16
VOX = 512
ROWS = SUBJ * EP * LOCAL
NT = (((1,), (1,)), ((), ()))
series_floor = 1.0
spread_floor = 0.05
shrink_factor = 0.9


def copy_to(src, dst, send_sem, recv_sem, subj, vox):
    return pltpu.make_async_remote_copy(
        src_ref=src,
        dst_ref=dst,
        send_sem=send_sem,
        recv_sem=recv_sem,
        device_id={"subj": subj, "vox": vox},
        device_id_type=MESH,
    )


def await_bytes(ref, sem):
    pltpu.make_async_copy(ref, ref, sem).wait()


def fold(x):
    return x + pltpu.roll(x, 4, 0)


def exact_terms(x):
    first = x.astype(BF16)
    rest = x - first.astype(F32)
    second = rest.astype(BF16)
    return first, second, (rest - second.astype(F32)).astype(BF16)


def two_terms(x):
    first = x.astype(BF16)
    return first, (x - first.astype(F32)).astype(BF16)


def slot_of(group, taker):
    return jnp.where((group ^ taker) < 2, group ^ taker, 2 + (group & 1))


def line_of(slot, epoch, subject):
    return slot * (EP * LOCAL) + epoch * LOCAL + subject


def main_kernel(
    series_hbm,
    offsets_hbm,
    selected_hbm,
    out_ref,
    offsets,
    selected,
    series,
    choose,
    epochs,
    scale,
    slab_out,
    slab_in,
    slab_sum,
    slab,
    raw,
    lhs_hi,
    lhs_lo,
    std_hi,
    std_lo,
    corr_even,
    corr_odd,
    score,
    gram_a,
    gram_b,
    gram_c,
    z_parts_a,
    z_parts_b,
    z_parts_c,
    x_parts_a,
    x_parts_b,
    x_parts_c,
    y_parts,
    z_sums_a,
    z_sums_b,
    z_sums_c,
    x_sums_a,
    x_sums_b,
    x_sums_c,
    y_sums,
    z_last_a,
    z_last_b,
    z_last_c,
    x_last_a,
    x_last_b,
    x_last_c,
    y_last,
    total_a,
    total_b,
    total_c,
    final_a,
    final_b,
    final_c,
    pick_a,
    pick_b,
    pick_wide,
    pick_square,
    turn_a,
    turn_b,
    turn_c,
    put_columns,
    load_sem,
    sent,
    slab_recv,
    share_recv,
    near_recv,
    far_recv,
    relay_recv,
    z_recv,
    x_recv,
    y_recv,
    sum_recv,
    final_recv,
):
    corr = (corr_even, corr_odd)
    z_parts, x_parts = (z_parts_a, z_parts_b, z_parts_c), (x_parts_a, x_parts_b, x_parts_c)
    z_sums, x_sums = (z_sums_a, z_sums_b, z_sums_c), (x_sums_a, x_sums_b, x_sums_c)
    last = ((z_last_a, x_last_a), (z_last_b, x_last_b), (z_last_c, x_last_c, y_last))
    gram = (gram_a, gram_b, gram_c)
    total, final = (total_a, total_b, total_c), (final_a, final_b, final_c)
    j = lax.axis_index("subj")
    v = lax.axis_index("vox")
    near, far, core = j ^ 1, j ^ 2, j & 1
    z, x, y = v // 8, (v // 2) & 3, v & 1

    def ahead_of(place, step):
        return (place + step) & 3

    def shard_at(z, x, y):
        return z * 8 + x * 2 + y

    loads = [
        pltpu.make_async_copy(source, target, load_sem.at[i])
        for i, (source, target) in enumerate(
            ((offsets_hbm, offsets), (selected_hbm, selected), (series_hbm, series))
        )
    ]
    for load in loads:
        load.start()

    barrier = pltpu.get_barrier_semaphore()

    def greet(step, carry):
        for other in range(SUBJ):
            pl.semaphore_signal(
                barrier,
                inc=1,
                device_id={"subj": j ^ other, "vox": (v + step) & (SHARDS - 1)},
                device_id_type=MESH,
            )
        return carry

    with jax.named_scope("greet"):
        lax.fori_loop(1, SHARDS, greet, 0, unroll=4)
        for other in range(1, SUBJ):
            pl.semaphore_signal(barrier, inc=1, device_id={"subj": j ^ other, "vox": v}, device_id_type=MESH)

    loads[0].wait()
    loads[1].wait()

    with jax.named_scope("choose"):
        row16 = lax.broadcasted_iota(I32, (16, 128), 0)
        scan = lax.broadcasted_iota(I32, (16, LOCAL * RUN), 1)
        for q in range(QUADS):
            start = jnp.zeros((16, 128), I32)
            for r in range(16):
                first = offsets[j * LOCAL + r % 4, q * 4 + r // 4] + (r % 4) * RUN
                start = jnp.where(row16 == r, first, start)
            ahead = scan - jnp.concatenate([start] * (LOCAL * RUN // 128), axis=1)
            for t in range(TR):
                choose[pl.ds(q * 256 + t * 16, 16), :] = jnp.where(ahead == t, 1.0, 0.0).astype(BF16)

    id_rows = []
    row8 = lax.broadcasted_iota(I32, (8, 128), 0)
    for block in range(SEL // 8):
        ids = jnp.zeros((8, 128), I32)
        for r in range(8):
            place = block * 8 + r
            ids = jnp.where(row8 == r, selected[4 * (place % OWN) + place // OWN], ids)
        id_rows.append(ids)
    ids = jnp.concatenate(id_rows, axis=0)
    columns = lax.broadcasted_iota(I32, (SEL, VOX), 1) + v * VOX
    picker = jnp.where(columns == jnp.concatenate([ids] * (VOX // 128), axis=1), 1.0, 0.0).astype(BF16)

    with jax.named_scope("pick_epochs"):
        loads[2].wait()
        runs = series[...].reshape(LOCAL * RUN, VOX)
        all_chosen = jnp.dot(choose[...], runs, preferred_element_type=F32).astype(BF16)
        for q in range(QUADS):
            chosen = all_chosen[q * 256 : q * 256 + 256]
            for h in range(2):
                epochs[0, h, q] = chosen[:, h * 256 : h * 256 + 256]
            picked = lax.dot_general(picker, chosen, NT, preferred_element_type=F32)
            slab_out[:, :, pl.ds(q * 256, 256)] = picked.astype(BF16).reshape(SHARDS, 2, 256)

    with jax.named_scope("barrier"):
        pl.semaphore_wait(barrier, SUBJ * SHARDS - 1)

    def send_slab(step, carry):
        piece = (v + step) & (SHARDS - 1)
        to_j, to_v = piece // 8, j * 8 + (piece & 7)

        @pl.when(jnp.logical_or(to_j != j, to_v != v))
        def _():
            copy_to(slab_out.at[piece], slab_in.at[v], sent, slab_recv, to_j, to_v).start()

        return carry

    with jax.named_scope("send_slab"):
        lax.fori_loop(0, SHARDS, send_slab, 0)

    def near_copy(h):
        return copy_to(epochs.at[0, h], epochs.at[1, h], sent, near_recv, near, v)

    def far_copy(g, q):
        at = g * QUADS + q
        source, target = epochs.at[core ^ g, core, q], epochs.at[2 + g, core, q]
        return copy_to(source, target, sent, far_recv.at[at], far, v)

    def relay_copy(g, q):
        ref = epochs.at[2 + g, core, q]
        return copy_to(ref, ref, sent, relay_recv.at[g], near, v)

    def relay(g, q):
        with jax.named_scope("relay"):
            far_copy(g, q).wait_recv()
            relay_copy(g, q).start()

    for h in (1, 0):
        near_copy(h).start()

    @pl.when(core == 0)
    def _():
        far_copy(0, 0).start()

    def lanes_of(h):
        return pl.ds(h * 256 if isinstance(h, int) else pl.multiple_of(h * 256, 256), 256)

    def scales(r, h):
        lanes = lanes_of(h)
        for q in range(QUADS):
            seen = epochs[r, h, q].astype(F32).reshape(TR, 16, 256)
            centred = seen - (jnp.sum(seen, axis=0) * (1.0 / TR))[None]
            scale[r, q, :, lanes] = lax.rsqrt(jnp.sum(centred * centred, axis=0) + series_floor)

    for h in range(2):
        scales(0, h)

    with jax.named_scope("near_wait"):
        await_bytes(epochs.at[1], near_recv)

    @pl.when(core == 1)
    def _():
        far_copy(0, 0).start()

    far_copy(0, 1).start()

    own_group = v // 8 == j

    with jax.named_scope("slab_wait"):

        @pl.when(own_group)
        def _():
            slab_in[v] = slab_out[j * 8 + (v & 7)]
            await_bytes(slab_in.at[pl.ds(0, SHARDS - 1)], slab_recv)

        @pl.when(jnp.logical_not(own_group))
        def _():
            await_bytes(slab_in, slab_recv)

    with jax.named_scope("slab_sum"):
        slab_sum[...] = jnp.sum(slab_in[...].astype(F32), axis=0).astype(BF16)

    def share_slab(step, carry):
        copy_to(slab_sum, slab.at[v], sent, share_recv, j, (v + step) & (SHARDS - 1)).start()
        return carry

    with jax.named_scope("share_slab"):
        lax.fori_loop(1, SHARDS, share_slab, 0)
        slab[v] = slab_sum[...]

    far_copy(0, 2).start()
    for q in range(QUADS):
        far_copy(1, q).start()

    with jax.named_scope("places"):
        b = lax.broadcasted_iota(I32, (1, ROWS), 1)
        p = lax.broadcasted_iota(I32, (EP * LOCAL, 1), 0)
        for i in range(2):
            taker = y * 2 + i
            s = b // EP
            to = line_of(slot_of(s // LOCAL, taker), b - s * EP, s & 3)
            s = p // EP
            line = line_of(slot_of(j, taker), p - s * EP, s)

            def put(first, lines):
                put_columns[i, pl.ds(first, lines.shape[0]), :] = jnp.where(lines == to, 1.0, 0.0).astype(BF16)

            def hot(lines):
                return jnp.where(lines == line, 1.0, 0.0).astype(BF16)

            def down(count):
                return lax.broadcasted_iota(I32, (count, 1), 0)

            def across(count):
                return lax.broadcasted_iota(I32, (1, count), 1)

            c, r = down(128), down(64)
            around = (c & 63) + 64
            put(0, jnp.where(c < 64, c, c - 32))
            put(128, jnp.where(around < 96, around, around - 96))
            put(256, jnp.where(r < 32, r, jnp.where(r < 48, r + 32, -1)))
            put(320, jnp.where(r < 48, jnp.where(r < 32, r + 32, r + 48), -1))
            c, r = across(128), across(64)
            around = (c & 63) + 64
            apart = (c & 32) > 0
            for piece, (lines, columns) in enumerate(
                (
                    (jnp.where(r < 32, r, -1), jnp.where(apart & (c < 64), c, -1)),
                    (jnp.where(r < 32, r + 32, -1), jnp.where(apart & (c >= 64), c - 32, -1)),
                    (jnp.where((r >= 32) & (r < 48), r + 32, -1), jnp.where(apart & (c < 64), around - 96, -1)),
                    (jnp.where((r >= 32) & (r < 48), r + 48, -1), jnp.where(apart & (c >= 64), around - 96, -1)),
                )
            ):
                pick_a[i, pl.ds(piece * 48, 48), :] = hot(lines)
                turn_a[i, pl.ds(piece * 48, 48), :] = hot(columns)
            put(384, down(128))
            put(512, down(48) + 96)
            pick_b[i] = hot(across(48) + 96)
            turn_b[i, 0:48, :] = hot(jnp.where(c < 96, c, -1))
            turn_b[i, 48:96, :] = hot(jnp.where(c < 96, -1, c))
            put(560, down(128))
            put(688, (down(128) & 63) + 128)
            put(816, down(48) + 144)
            pick_wide[i] = hot(across(48) + 144)
            pick_square[i] = hot(r + 128)
            turn_c[i] = hot(c)
        for k in range(OWN):
            score[k, 96:128, :] = jnp.zeros((32, VOX), BF16)

    for h in range(2):
        scales(1, h)

    relay(0, 0)
    relay(0, 1)
    with jax.named_scope("share_wait"):
        await_bytes(slab.at[pl.ds(0, SHARDS - 1)], share_recv)
    relay(0, 2)

    with jax.named_scope("standard_slab"):
        for r in range(SUBJ):
            group = (j, near, far & 2, far | 1)[r]
            for kk in range(8):
                for q in range(QUADS):
                    raw[r * QUADS + q, pl.ds(kk * 2, 2), :] = slab[group * 8 + kk, :, pl.ds(q * 256, 256)].astype(F32)
        seen = raw[...].reshape(SUBJ * QUADS * OWN, 256)
        same = jnp.where(
            (lax.broadcasted_iota(I32, (256, 256), 0) & 15) == (lax.broadcasted_iota(I32, (256, 256), 1) & 15), 1.0, 0.0
        ).astype(BF16)
        centred = seen - jnp.dot(seen.astype(BF16), same, preferred_element_type=F32) * (1.0 / TR)
        terms = exact_terms(centred * centred)
        spread = [jnp.dot(t, same, preferred_element_type=F32) for t in terms]
        spread = spread[0] + spread[1] + spread[2]
        x_std = centred * lax.rsqrt(spread + series_floor) * shrink_factor
        x_hi = x_std.astype(BF16).astype(F32)
        std_hi[...] = x_hi.reshape(SUBJ * QUADS, OWN, 256)
        std_lo[...] = (x_std - x_hi).reshape(SUBJ * QUADS, OWN, 256)

    own_row = (lax.broadcasted_iota(I32, (16, 256), 1) & 15) == lax.broadcasted_iota(I32, (16, 256), 0)

    units = ((0, 0), (0, 1), (1, 0), (1, 1), (2, 0), (2, 1), (3, core), (3, 1 - core))

    def correlate(unit):
        r, h = units[unit]
        lanes = lanes_of(h)
        if r >= 2:
            scales(r, h)
        for q in range(QUADS):
            at = r * QUADS + q
            if unit % 2 == 0:
                for k in range(OWN):
                    for std, lhs in ((std_hi, lhs_hi), (std_lo, lhs_lo)):
                        line = jnp.broadcast_to(std[at, pl.ds(k, 1), :], (16, 256))
                        lhs[at, pl.ds(k * 16, 16), :] = jnp.where(own_row, line, 0.0).astype(BF16)
            seen = epochs[r, h, q]
            corr[unit % 2][q] = jnp.dot(lhs_hi[at], seen, preferred_element_type=F32) + jnp.dot(
                lhs_lo[at], seen, preferred_element_type=F32
            )

    def standard(unit, ids=range(OWN)):
        r, h = units[unit]
        lanes = lanes_of(h)
        for k in ids:
            rows = pl.ds(k * 16 if isinstance(k, int) else pl.multiple_of(k * 16, 16), 16)
            halves = []
            for q in range(QUADS):
                shrunk = corr[unit % 2][q, rows, :] * scale[r, q, :, lanes]
                twice = jnp.log(1.0 + shrunk) - jnp.log(1.0 - shrunk)
                halves += [twice[0:8], twice[8:16]]
            mean = fold(functools.reduce(jnp.add, halves)) * (1.0 / EP)
            halves = [f - mean for f in halves]
            spread = fold(functools.reduce(jnp.add, [f * f for f in halves])) * (1.0 / EP)
            gain = lax.rsqrt(spread + 4.0 * spread_floor)
            for q in range(QUADS):
                both = jnp.concatenate([halves[2 * q] * gain, halves[2 * q + 1] * gain], axis=0).astype(BF16)
                at = r * 48 + q * 16
                score[k, pl.ds(at, 16), lanes] = both

    split = ((32, 16, 0), (16, 32, 0), (32, 32, 16))
    lane = lax.broadcasted_iota(I32, (16, 128), 1)

    def against(m, first, count, columns=slice(0, 128)):
        return lax.dot_general(score[m, pl.ds(first, count), :], score[m, columns, :], NT, preferred_element_type=F32)

    def block_of(n, m):
        if n == 0:
            block = against(m, 0, 96)
            for top in (0, 16):
                beside = pltpu.roll(block[32 + top : 48 + top], 32, 1)
                gram[n][m, top : top + 16, :] = jnp.where(lane < 64, block[top : top + 16], beside)
            upper, lower = block[64:80], block[80:96]
            left = jnp.where(lane < 32, pltpu.roll(upper, 64, 1), pltpu.roll(upper, 32, 1))
            right = jnp.where(lane < 96, lower, pltpu.roll(lower, 96, 1))
            gram[n][m, 32:48, :] = jnp.where(lane < 64, left, right)
        elif n == 1:
            gram[n][m] = against(m, 96, 48)
        else:
            gram[n][m, 0:48, :] = against(m, 144, 48)
            square = against(m, 128, 64, slice(128, 192))
            gram[n][m, 48:80, :] = jnp.concatenate([square[0:32], square[32:64]], axis=1)

    def kernels(n, unfinished=None):
        z_rows, x_rows, y_rows = split[n]

        def offsets_at(step):
            slow, fast = (step // 4 + 1) & 3, (step + 1) & 3
            return slow ^ (slow >> 1), fast ^ (fast >> 1)

        def id_at(step):
            major, minor = offsets_at(step)
            return ahead_of(z, major) * 4 + ahead_of(x, minor)

        def four(index, carry):
            steps = [index * 4 + more for more in range(8)]
            for step in steps[:4]:
                block_of(n, id_at(step))
            if unfinished is not None:
                standard(unfinished, [id_at(step & 15) for step in steps[4:]])
            for step in steps[:4]:
                major, minor = offsets_at(step)
                m = ahead_of(z, major) * 4 + ahead_of(x, minor)

                @pl.when(major > 0)
                def _():
                    source = gram[n].at[m, pl.ds(0, z_rows)]
                    to_v = shard_at(ahead_of(z, major), x, y)
                    copy_to(source, z_parts[n].at[minor, major], sent, z_recv.at[minor + 2 if n == 2 else n], j, to_v).start()

                @pl.when(minor > 0)
                def _():
                    source = gram[n].at[m, pl.ds(z_rows, x_rows)]
                    to_v = shard_at(z, ahead_of(x, minor), y)
                    copy_to(source, x_parts[n].at[major, minor], sent, x_recv.at[major + 2 if n == 2 else n], j, to_v).start()

                if y_rows:
                    rows = pl.ds(pl.multiple_of(z_rows + x_rows + y_rows // 2 * (y ^ 1), 8), y_rows // 2)
                    copy_to(
                        gram[n].at[m, rows], y_parts.at[major * 4 + minor], sent, y_recv.at[major], j, v ^ 1
                    ).start()
            return carry

        with jax.named_scope("kernels"):
            if unfinished is not None:
                standard(unfinished, [id_at(step) for step in range(4)])
            lax.fori_loop(0, OWN // 4, four, 0)

    def second_sums(n):
        z_rows, x_rows, y_rows = split[n]

        def along(step, block):
            parts, recv, sums = ((z_parts, z_recv, z_sums), (x_parts, x_recv, x_sums))[block]
            if n == 2:
                with jax.named_scope("part_wait"):
                    await_bytes(parts[n].at[step, pl.ds(1, 3)], recv.at[step + 2])
            own = (ahead_of(z, step) * 4 + x) if block else (z * 4 + ahead_of(x, step))
            own = gram[n][own, pl.ds(z_rows, x_rows) if block else pl.ds(0, z_rows), :]
            sums[n][step] = (own + parts[n][step, 1]) + (parts[n][step, 2] + parts[n][step, 3])
            for other in range(2):
                side = y ^ other
                count = (z_rows, x_rows)[block] // 2
                rows = pl.ds(pl.multiple_of(side * count, 8), count)
                slot = step * 2 + other
                to_v = shard_at(ahead_of(z, step), x, side) if block else shard_at(z, ahead_of(x, step), side)
                if slot:
                    copy_to(
                        sums[n].at[step, rows], last[n][block].at[slot], sent, sum_recv.at[n * 2 + block], j, to_v
                    ).start()
                else:
                    last[n][block][0] = sums[n][0, rows, :]

        def from_side(major):
            with jax.named_scope("part_wait"):
                await_bytes(y_parts.at[pl.ds(major * 4, 4)], y_recv.at[major])
            for minor in range(4):
                step = major * 4 + minor
                to_z, to_x = ahead_of(z, major), ahead_of(x, minor)
                rows = pl.ds(pl.multiple_of(z_rows + x_rows + y_rows // 2 * y, 8), y_rows // 2)
                added = y_parts[step] + gram[n][to_z * 4 + to_x, rows, :]
                if step:
                    y_sums[step] = added
                    copy_to(
                        y_sums.at[step], y_last.at[step], sent, sum_recv.at[n * 2 + 2], j, shard_at(to_z, to_x, y)
                    ).start()
                else:
                    y_last[0] = added

        if y_rows:
            for major in (1, 3, 2, 0):
                along(major, 1)
                from_side(major)
        else:
            with jax.named_scope("part_wait"):
                await_bytes(x_parts[n].at[pl.ds(0, 3)], x_recv.at[n])
            for step in (1, 3, 2, 0):
                along(step, 1)
            with jax.named_scope("part_wait"):
                await_bytes(z_parts[n].at[pl.ds(0, 3)], z_recv.at[n])
        for step in (1, 3, 2, 0):
            along(step, 0)

    owner_v = v - y + j // 2
    place = core * 2 + y

    def hand_over(n):
        with jax.named_scope("last_wait"):
            for block, ref in enumerate(last[n]):
                await_bytes(ref.at[pl.ds(0, ref.shape[0] - 1)], sum_recv.at[n * 2 + block])
        mean = 1.0 / (VOX * SHARDS)
        first = 0
        for ref in last[n]:
            rows = ref.shape[1]
            total[n][pl.ds(first, rows), :] = jnp.sum(ref[...], axis=0) * mean
            first += rows
        for other in range(SUBJ):
            copy = copy_to(
                total[n], final[n].at[place], sent, final_recv.at[n], (j ^ other) if other else j, owner_v
            )
            if other:
                copy.start()
            else:

                @pl.when(owner_v != v)
                def _():
                    copy.start()

        @pl.when(owner_v == v)
        def _():
            final[n][place] = total[n][...]

    def await_final(n, sem):
        @pl.when(owner_v == v)
        def _():
            await_bytes(final[n].at[pl.ds(0, SUBJ - 1)], sem)

        @pl.when(owner_v != v)
        def _():
            await_bytes(final[n], sem)

    def scores_of(correlated, finished):
        with jax.named_scope("scores"):
            if correlated is not None:
                correlate(correlated)
            if finished is not None:
                standard(finished)

    def relayed(g):
        with jax.named_scope("relay_wait"):
            await_bytes(epochs.at[2 + g, 1 - core], relay_recv.at[g])

    scores_of(0, None)
    scores_of(1, 0)
    scores_of(2, 1)
    scores_of(3, 2)
    relayed(0)
    scores_of(4, 3)
    relay(1, 0)
    kernels(0)
    scores_of(5, 4)
    kernels(1, 5)
    relay(1, 1)
    relay(1, 2)
    scores_of(6, None)
    scores_of(None, 6)
    second_sums(0)
    relayed(1)
    scores_of(7, None)
    kernels(2, 7)
    second_sums(1)
    second_sums(2)
    hand_over(0)
    hand_over(1)

    straight = (((1,), (0,)), ((), ()))
    left = lax.broadcasted_iota(I32, (EP * LOCAL, 128), 1) < 64
    upper = lax.broadcasted_iota(I32, (EP * LOCAL, 64), 1) < 32
    puts = (0, 384, 560, 864)
    corner = lax.broadcasted_iota(I32, (EP * LOCAL, 48), 1) >= 32

    def picked_by(pick, terms, dims):
        parts = [lax.dot_general(pick, t, dims, preferred_element_type=F32) for t in terms]
        return parts[0] + parts[1]

    def placed(n, i):
        pieces, first = [], 0
        for rows in split[n]:
            if rows:
                here = pl.ds(first, rows // 2)
                pieces += [final[n][2 * i, here, :], final[n][2 * i + 1, here, :]]
                first += rows // 2
        if n == 0:
            terms = two_terms(jnp.concatenate(pieces + [jnp.zeros((16, 128), F32)], axis=0))
            by_row = picked_by(pick_a[i], terms, straight)
            by_column = picked_by(turn_a[i], terms, NT)
            lines = [
                jnp.where(left, by_row[0:48], by_row[48:96]),
                jnp.where(left, by_row[96:144], by_row[144:192]),
                jnp.where(upper, by_column[0:48], by_column[96:144]),
                jnp.where(upper, by_column[48:96], by_column[144:192]),
            ]
        elif n == 1:
            terms = two_terms(jnp.concatenate(pieces, axis=0))
            by_column = picked_by(turn_b[i], terms, NT)
            turned = by_column[0:48] + jnp.where(corner, by_column[48:96], 0.0)
            lines = [picked_by(pick_b[i], terms, straight), turned]
        else:
            both = jnp.concatenate(pieces, axis=0)
            wide, square = two_terms(both[0:48]), two_terms(both[48:80])
            halves = [picked_by(pick_square[i, :, h * 32 : h * 32 + 32], square, straight) for h in range(2)]
            lines = [
                picked_by(pick_wide[i], wide, straight),
                jnp.where(left, halves[0], halves[1]),
                picked_by(turn_c[i], wide, NT),
            ]
        put = put_columns[i, puts[n] : puts[n + 1], :]
        terms = [jnp.dot(t, put, preferred_element_type=F32) for t in two_terms(jnp.concatenate(lines, axis=1))]
        return terms[0] + terms[1]

    with jax.named_scope("final"):
        await_final(0, final_recv.at[0])
    with jax.named_scope("place"):
        for i in range(2):
            out_ref[i] = placed(0, i)
    hand_over(2)
    with jax.named_scope("final"):
        await_final(1, final_recv.at[1])
    with jax.named_scope("place"):
        for i in range(2):
            out_ref[i] += placed(1, i)
    with jax.named_scope("final"):
        await_final(2, final_recv.at[2])
    with jax.named_scope("place"):
        for i in range(2):
            out_ref[i] += placed(2, i)

    with jax.named_scope("drain"):
        for ref in (slab_in.at[pl.ds(0, SHARDS - 1)], slab_in.at[pl.ds(0, SHARDS - 1)]):
            await_bytes(ref, sent)

        @pl.when(jnp.logical_not(own_group))
        def _():
            await_bytes(slab_sum, sent)

        for slot in range(2):
            await_bytes(epochs.at[slot], sent)
        await_bytes(epochs.at[2], sent)
        for n in range(3):
            await_bytes(z_parts[n].at[pl.ds(0, 3)], sent)
            await_bytes(x_parts[n].at[pl.ds(0, 3)], sent)
            for ref in last[n]:
                await_bytes(ref.at[pl.ds(0, ref.shape[0] - 1)], sent)
            await_final(n, sent)
        await_bytes(y_parts, sent)


def body(series, offsets, selected):
    vmem = pltpu.VMEM
    dma = pltpu.SemaphoreType.DMA
    return pl.pallas_call(
        main_kernel,
        out_shape=pltpu.VMEM((2, EP * LOCAL, ROWS), F32),
        in_specs=[
            pl.BlockSpec(memory_space=pl.ANY),
            pl.BlockSpec(memory_space=pl.ANY),
            pl.BlockSpec(memory_space=pl.ANY),
        ],
        out_specs=pl.BlockSpec(memory_space=pltpu.VMEM),
        scratch_shapes=[
            pltpu.SMEM((SUBJ * LOCAL, EP), I32),
            pltpu.SMEM((SEL,), I32),
            vmem((LOCAL, RUN, VOX), BF16),
            vmem((QUADS * 256, LOCAL * RUN), BF16),
            vmem((SUBJ, 2, QUADS, 256, 256), BF16),
            vmem((SUBJ, QUADS, 16, VOX), F32),
            vmem((SHARDS, 2, QUADS * 256), BF16),
            vmem((SHARDS, 2, QUADS * 256), BF16),
            vmem((2, QUADS * 256), BF16),
            vmem((SHARDS, 2, QUADS * 256), BF16),
            vmem((SUBJ * QUADS, OWN, 256), F32),
            vmem((SUBJ * QUADS, 256, 256), BF16),
            vmem((SUBJ * QUADS, 256, 256), BF16),
            vmem((SUBJ * QUADS, OWN, 256), F32),
            vmem((SUBJ * QUADS, OWN, 256), F32),
            vmem((QUADS, 256, 256), F32),
            vmem((QUADS, 256, 256), F32),
            vmem((OWN, ROWS, VOX), BF16),
            vmem((OWN, 48, 128), F32),
            vmem((OWN, 48, 128), F32),
            vmem((OWN, 80, 128), F32),
            vmem((4, 4, 32, 128), F32),
            vmem((4, 4, 16, 128), F32),
            vmem((4, 4, 32, 128), F32),
            vmem((4, 4, 16, 128), F32),
            vmem((4, 4, 32, 128), F32),
            vmem((4, 4, 32, 128), F32),
            vmem((OWN, 8, 128), F32),
            vmem((4, 32, 128), F32),
            vmem((4, 16, 128), F32),
            vmem((4, 32, 128), F32),
            vmem((4, 16, 128), F32),
            vmem((4, 32, 128), F32),
            vmem((4, 32, 128), F32),
            vmem((OWN, 8, 128), F32),
            vmem((8, 16, 128), F32),
            vmem((8, 8, 128), F32),
            vmem((8, 16, 128), F32),
            vmem((8, 8, 128), F32),
            vmem((8, 16, 128), F32),
            vmem((8, 16, 128), F32),
            vmem((OWN, 8, 128), F32),
            vmem((24, 128), F32),
            vmem((24, 128), F32),
            vmem((40, 128), F32),
            vmem((SUBJ, 24, 128), F32),
            vmem((SUBJ, 24, 128), F32),
            vmem((SUBJ, 40, 128), F32),
            vmem((2, 4 * EP * LOCAL, 64), BF16),
            vmem((2, EP * LOCAL, 48), BF16),
            vmem((2, EP * LOCAL, 48), BF16),
            vmem((2, EP * LOCAL, 64), BF16),
            vmem((2, 4 * EP * LOCAL, 128), BF16),
            vmem((2, 2 * EP * LOCAL, 128), BF16),
            vmem((2, EP * LOCAL, 128), BF16),
            vmem((2, 864, ROWS), BF16),
            dma((3,)),
            dma,
            dma,
            dma,
            dma,
            dma((2 * QUADS,)),
            dma((2,)),
            dma((6,)),
            dma((6,)),
            dma((4,)),
            dma((7,)),
            dma((3,)),
        ],
        compiler_params=pltpu.CompilerParams(collective_id=0, has_side_effects=True),
    )(series, offsets, selected)


def solution(mesh):
    placed = (P("subj", None, "vox"), P(), P())
    return jax.shard_map(
        body, mesh=mesh, in_specs=placed, out_specs=P("vox", "subj", None), check_vma=False
    )
```

```python
import functools

import jax
import jax.numpy as jnp
from jax import lax
from jax.experimental import pallas as pl
from jax.experimental.pallas import tpu as pltpu
from jax.sharding import PartitionSpec as P

MESH = pl.DeviceIdType.MESH
F32, BF16, I32 = jnp.float32, jnp.bfloat16, jnp.int32
HIGH = lax.Precision.HIGHEST

SUBJ, SHARDS = 4, 32
TR, EP, RUN = 16, 12, 256
LOCAL = 4
QUADS = 3
SEL, OWN = 64, 16
VOX = 512
ROWS = SUBJ * EP * LOCAL
NT = (((1,), (1,)), ((), ()))
series_floor = 1.0
spread_floor = 0.05
shrink_factor = 0.9


def copy_to(src, dst, send_sem, recv_sem, subj, vox):
    return pltpu.make_async_remote_copy(
        src_ref=src,
        dst_ref=dst,
        send_sem=send_sem,
        recv_sem=recv_sem,
        device_id={"subj": subj, "vox": vox},
        device_id_type=MESH,
    )


def await_bytes(ref, sem):
    pltpu.make_async_copy(ref, ref, sem).wait()


def fold(x):
    return x + pltpu.roll(x, 4, 0)


def exact_terms(x):
    first = x.astype(BF16)
    rest = x - first.astype(F32)
    second = rest.astype(BF16)
    return first, second, (rest - second.astype(F32)).astype(BF16)


def two_terms(x):
    first = x.astype(BF16)
    return first, (x - first.astype(F32)).astype(BF16)


def slot_of(group, taker):
    return jnp.where((group ^ taker) < 2, group ^ taker, 2 + (group & 1))


def line_of(slot, epoch, subject):
    return slot * (EP * LOCAL) + epoch * LOCAL + subject


def main_kernel(
    series_hbm,
    offsets_hbm,
    selected_hbm,
    out_ref,
    offsets,
    selected,
    series,
    choose,
    epochs,
    scale,
    slab_out,
    slab_in,
    slab_sum,
    slab,
    raw,
    lhs_hi,
    lhs_lo,
    std_hi,
    std_lo,
    corr_even,
    corr_odd,
    score,
    gram_a,
    gram_b,
    gram_c,
    z_parts_a,
    z_parts_b,
    z_parts_c,
    x_parts_a,
    x_parts_b,
    x_parts_c,
    y_parts,
    z_sums_a,
    z_sums_b,
    z_sums_c,
    x_sums_a,
    x_sums_b,
    x_sums_c,
    y_sums,
    z_last_a,
    z_last_b,
    z_last_c,
    x_last_a,
    x_last_b,
    x_last_c,
    y_last,
    total_a,
    total_b,
    total_c,
    final_a,
    final_b,
    final_c,
    pick_a,
    pick_b,
    pick_wide,
    pick_square,
    turn_a,
    turn_b,
    turn_c,
    put_columns,
    load_sem,
    sent,
    slab_recv,
    share_recv,
    near_recv,
    far_recv,
    relay_recv,
    z_recv,
    x_recv,
    y_recv,
    sum_recv,
    final_recv,
):
    corr = (corr_even, corr_odd)
    z_parts, x_parts = (z_parts_a, z_parts_b, z_parts_c), (x_parts_a, x_parts_b, x_parts_c)
    z_sums, x_sums = (z_sums_a, z_sums_b, z_sums_c), (x_sums_a, x_sums_b, x_sums_c)
    last = ((z_last_a, x_last_a), (z_last_b, x_last_b), (z_last_c, x_last_c, y_last))
    gram = (gram_a, gram_b, gram_c)
    total, final = (total_a, total_b, total_c), (final_a, final_b, final_c)
    j = lax.axis_index("subj")
    v = lax.axis_index("vox")
    near, far, core = j ^ 1, j ^ 2, j & 1
    z, x, y = v // 8, (v // 2) & 3, v & 1

    def ahead_of(place, step):
        return (place + step) & 3

    def shard_at(z, x, y):
        return z * 8 + x * 2 + y

    loads = [
        pltpu.make_async_copy(source, target, load_sem.at[i])
        for i, (source, target) in enumerate(
            ((offsets_hbm, offsets), (selected_hbm, selected), (series_hbm, series))
        )
    ]
    for load in loads:
        load.start()

    barrier = pltpu.get_barrier_semaphore()

    def greet(step, carry):
        for other in range(SUBJ):
            pl.semaphore_signal(
                barrier,
                inc=1,
                device_id={"subj": j ^ other, "vox": (v + step) & (SHARDS - 1)},
                device_id_type=MESH,
            )
        return carry

    with jax.named_scope("greet"):
        lax.fori_loop(1, SHARDS, greet, 0, unroll=4)
        for other in range(1, SUBJ):
            pl.semaphore_signal(barrier, inc=1, device_id={"subj": j ^ other, "vox": v}, device_id_type=MESH)

    loads[0].wait()
    loads[1].wait()

    with jax.named_scope("choose"):
        row16 = lax.broadcasted_iota(I32, (16, 128), 0)
        scan = lax.broadcasted_iota(I32, (16, LOCAL * RUN), 1)
        for q in range(QUADS):
            start = jnp.zeros((16, 128), I32)
            for r in range(16):
                first = offsets[j * LOCAL + r % 4, q * 4 + r // 4] + (r % 4) * RUN
                start = jnp.where(row16 == r, first, start)
            ahead = scan - jnp.concatenate([start] * (LOCAL * RUN // 128), axis=1)
            for t in range(TR):
                choose[pl.ds(q * 256 + t * 16, 16), :] = jnp.where(ahead == t, 1.0, 0.0).astype(BF16)

    id_rows = []
    row8 = lax.broadcasted_iota(I32, (8, 128), 0)
    for block in range(SEL // 8):
        ids = jnp.zeros((8, 128), I32)
        for r in range(8):
            place = block * 8 + r
            ids = jnp.where(row8 == r, selected[4 * (place % OWN) + place // OWN], ids)
        id_rows.append(ids)
    ids = jnp.concatenate(id_rows, axis=0)
    columns = lax.broadcasted_iota(I32, (SEL, VOX), 1) + v * VOX
    picker = jnp.where(columns == jnp.concatenate([ids] * (VOX // 128), axis=1), 1.0, 0.0).astype(BF16)

    with jax.named_scope("pick_epochs"):
        loads[2].wait()
        runs = series[...].reshape(LOCAL * RUN, VOX)
        all_chosen = jnp.dot(choose[...], runs, preferred_element_type=F32).astype(BF16)
        for q in range(QUADS):
            chosen = all_chosen[q * 256 : q * 256 + 256]
            for h in range(2):
                epochs[0, h, q] = chosen[:, h * 256 : h * 256 + 256]
            picked = lax.dot_general(picker, chosen, NT, preferred_element_type=F32)
            slab_out[:, :, pl.ds(q * 256, 256)] = picked.astype(BF16).reshape(SHARDS, 2, 256)

    with jax.named_scope("barrier"):
        pl.semaphore_wait(barrier, SUBJ * SHARDS - 1)

    def send_slab(step, carry):
        piece = (v + step) & (SHARDS - 1)
        to_j, to_v = piece // 8, j * 8 + (piece & 7)

        @pl.when(jnp.logical_or(to_j != j, to_v != v))
        def _():
            copy_to(slab_out.at[piece], slab_in.at[v], sent, slab_recv, to_j, to_v).start()

        return carry

    with jax.named_scope("send_slab"):
        lax.fori_loop(0, SHARDS, send_slab, 0)

    def near_copy(h):
        return copy_to(epochs.at[0, h], epochs.at[1, h], sent, near_recv, near, v)

    def far_copy(g, q):
        at = g * QUADS + q
        source, target = epochs.at[core ^ g, core, q], epochs.at[2 + g, core, q]
        return copy_to(source, target, sent, far_recv.at[at], far, v)

    def relay_copy(g, q):
        ref = epochs.at[2 + g, core, q]
        return copy_to(ref, ref, sent, relay_recv.at[g], near, v)

    def relay(g, q):
        with jax.named_scope("relay"):
            far_copy(g, q).wait_recv()
            relay_copy(g, q).start()

    for h in (1, 0):
        near_copy(h).start()

    @pl.when(core == 0)
    def _():
        far_copy(0, 0).start()

    def lanes_of(h):
        return pl.ds(h * 256 if isinstance(h, int) else pl.multiple_of(h * 256, 256), 256)

    def scales(r, h):
        lanes = lanes_of(h)
        for q in range(QUADS):
            seen = epochs[r, h, q].astype(F32).reshape(TR, 16, 256)
            centred = seen - (jnp.sum(seen, axis=0) * (1.0 / TR))[None]
            scale[r, q, :, lanes] = lax.rsqrt(jnp.sum(centred * centred, axis=0) + series_floor)

    for h in range(2):
        scales(0, h)

    with jax.named_scope("near_wait"):
        await_bytes(epochs.at[1], near_recv)

    @pl.when(core == 1)
    def _():
        far_copy(0, 0).start()

    far_copy(0, 1).start()

    own_group = v // 8 == j

    with jax.named_scope("slab_wait"):

        @pl.when(own_group)
        def _():
            slab_in[v] = slab_out[j * 8 + (v & 7)]
            await_bytes(slab_in.at[pl.ds(0, SHARDS - 1)], slab_recv)

        @pl.when(jnp.logical_not(own_group))
        def _():
            await_bytes(slab_in, slab_recv)

    with jax.named_scope("slab_sum"):
        slab_sum[...] = jnp.sum(slab_in[...].astype(F32), axis=0).astype(BF16)

    def share_slab(step, carry):
        copy_to(slab_sum, slab.at[v], sent, share_recv, j, (v + step) & (SHARDS - 1)).start()
        return carry

    with jax.named_scope("share_slab"):
        lax.fori_loop(1, SHARDS, share_slab, 0)
        slab[v] = slab_sum[...]

    far_copy(0, 2).start()
    for q in range(QUADS):
        far_copy(1, q).start()

    with jax.named_scope("places"):
        b = lax.broadcasted_iota(I32, (1, ROWS), 1)
        p = lax.broadcasted_iota(I32, (EP * LOCAL, 1), 0)
        for i in range(2):
            taker = y * 2 + i
            s = b // EP
            to = line_of(slot_of(s // LOCAL, taker), b - s * EP, s & 3)
            s = p // EP
            line = line_of(slot_of(j, taker), p - s * EP, s)

            def put(first, lines):
                put_columns[i, pl.ds(first, lines.shape[0]), :] = jnp.where(lines == to, 1.0, 0.0).astype(BF16)

            def hot(lines):
                return jnp.where(lines == line, 1.0, 0.0).astype(BF16)

            def down(count):
                return lax.broadcasted_iota(I32, (count, 1), 0)

            def across(count):
                return lax.broadcasted_iota(I32, (1, count), 1)

            c, r = down(128), down(64)
            around = (c & 63) + 64
            put(0, jnp.where(c < 64, c, c - 32))
            put(128, jnp.where(around < 96, around, around - 96))
            put(256, jnp.where(r < 32, r, jnp.where(r < 48, r + 32, -1)))
            put(320, jnp.where(r < 48, jnp.where(r < 32, r + 32, r + 48), -1))
            c, r = across(128), across(64)
            around = (c & 63) + 64
            apart = (c & 32) > 0
            for piece, (lines, columns) in enumerate(
                (
                    (jnp.where(r < 32, r, -1), jnp.where(apart & (c < 64), c, -1)),
                    (jnp.where(r < 32, r + 32, -1), jnp.where(apart & (c >= 64), c - 32, -1)),
                    (jnp.where((r >= 32) & (r < 48), r + 32, -1), jnp.where(apart & (c < 64), around - 96, -1)),
                    (jnp.where((r >= 32) & (r < 48), r + 48, -1), jnp.where(apart & (c >= 64), around - 96, -1)),
                )
            ):
                pick_a[i, pl.ds(piece * 48, 48), :] = hot(lines)
                turn_a[i, pl.ds(piece * 48, 48), :] = hot(columns)
            put(384, down(128))
            put(512, down(48) + 96)
            pick_b[i] = hot(across(48) + 96)
            turn_b[i, 0:48, :] = hot(jnp.where(c < 96, c, -1))
            turn_b[i, 48:96, :] = hot(jnp.where(c < 96, -1, c))
            put(560, down(128))
            put(688, (down(128) & 63) + 128)
            put(816, down(48) + 144)
            pick_wide[i] = hot(across(48) + 144)
            pick_square[i] = hot(r + 128)
            turn_c[i] = hot(c)
        for k in range(OWN):
            score[k, 96:128, :] = jnp.zeros((32, VOX), BF16)

    for h in range(2):
        scales(1, h)

    relay(0, 0)
    relay(0, 1)
    with jax.named_scope("share_wait"):
        await_bytes(slab.at[pl.ds(0, SHARDS - 1)], share_recv)
    relay(0, 2)

    with jax.named_scope("standard_slab"):
        for r in range(SUBJ):
            group = (j, near, far & 2, far | 1)[r]
            for kk in range(8):
                for q in range(QUADS):
                    raw[r * QUADS + q, pl.ds(kk * 2, 2), :] = slab[group * 8 + kk, :, pl.ds(q * 256, 256)].astype(F32)
        seen = raw[...].reshape(SUBJ * QUADS * OWN, 256)
        same = jnp.where(
            (lax.broadcasted_iota(I32, (256, 256), 0) & 15) == (lax.broadcasted_iota(I32, (256, 256), 1) & 15), 1.0, 0.0
        ).astype(BF16)
        centred = seen - jnp.dot(seen.astype(BF16), same, preferred_element_type=F32) * (1.0 / TR)
        terms = exact_terms(centred * centred)
        spread = [jnp.dot(t, same, preferred_element_type=F32) for t in terms]
        spread = spread[0] + spread[1] + spread[2]
        x_std = centred * lax.rsqrt(spread + series_floor) * shrink_factor
        x_hi = x_std.astype(BF16).astype(F32)
        std_hi[...] = x_hi.reshape(SUBJ * QUADS, OWN, 256)
        std_lo[...] = (x_std - x_hi).reshape(SUBJ * QUADS, OWN, 256)

    own_row = (lax.broadcasted_iota(I32, (16, 256), 1) & 15) == lax.broadcasted_iota(I32, (16, 256), 0)

    units = ((0, 0), (0, 1), (1, 0), (1, 1), (2, 0), (2, 1), (3, core), (3, 1 - core))

    def correlate(unit):
        r, h = units[unit]
        lanes = lanes_of(h)
        if r >= 2:
            scales(r, h)
        for q in range(QUADS):
            at = r * QUADS + q
            if unit % 2 == 0:
                for k in range(OWN):
                    for std, lhs in ((std_hi, lhs_hi), (std_lo, lhs_lo)):
                        line = jnp.broadcast_to(std[at, pl.ds(k, 1), :], (16, 256))
                        lhs[at, pl.ds(k * 16, 16), :] = jnp.where(own_row, line, 0.0).astype(BF16)
            seen = epochs[r, h, q]
            corr[unit % 2][q] = jnp.dot(lhs_hi[at], seen, preferred_element_type=F32) + jnp.dot(
                lhs_lo[at], seen, preferred_element_type=F32
            )

    def standard(unit, ids=range(OWN)):
        r, h = units[unit]
        lanes = lanes_of(h)
        for k in ids:
            rows = pl.ds(k * 16 if isinstance(k, int) else pl.multiple_of(k * 16, 16), 16)
            halves = []
            for q in range(QUADS):
                shrunk = corr[unit % 2][q, rows, :] * scale[r, q, :, lanes]
                twice = jnp.log(1.0 + shrunk) - jnp.log(1.0 - shrunk)
                halves += [twice[0:8], twice[8:16]]
            mean = fold(functools.reduce(jnp.add, halves)) * (1.0 / EP)
            halves = [f - mean for f in halves]
            spread = fold(functools.reduce(jnp.add, [f * f for f in halves])) * (1.0 / EP)
            gain = lax.rsqrt(spread + 4.0 * spread_floor)
            for q in range(QUADS):
                both = jnp.concatenate([halves[2 * q] * gain, halves[2 * q + 1] * gain], axis=0).astype(BF16)
                at = r * 48 + q * 16
                score[k, pl.ds(at, 16), lanes] = both

    split = ((32, 16, 0), (16, 32, 0), (32, 32, 16))
    lane = lax.broadcasted_iota(I32, (16, 128), 1)

    def against(m, first, count, columns=slice(0, 128)):
        return lax.dot_general(score[m, pl.ds(first, count), :], score[m, columns, :], NT, preferred_element_type=F32)

    def block_of(n, m):
        if n == 0:
            block = against(m, 0, 96)
            for top in (0, 16):
                beside = pltpu.roll(block[32 + top : 48 + top], 32, 1)
                gram[n][m, top : top + 16, :] = jnp.where(lane < 64, block[top : top + 16], beside)
            upper, lower = block[64:80], block[80:96]
            left = jnp.where(lane < 32, pltpu.roll(upper, 64, 1), pltpu.roll(upper, 32, 1))
            right = jnp.where(lane < 96, lower, pltpu.roll(lower, 96, 1))
            gram[n][m, 32:48, :] = jnp.where(lane < 64, left, right)
        elif n == 1:
            gram[n][m] = against(m, 96, 48)
        else:
            gram[n][m, 0:48, :] = against(m, 144, 48)
            square = against(m, 128, 64, slice(128, 192))
            gram[n][m, 48:80, :] = jnp.concatenate([square[0:32], square[32:64]], axis=1)

    def kernels(n, unfinished=None):
        z_rows, x_rows, y_rows = split[n]

        def offsets_at(step):
            slow, fast = (step // 4 + 1) & 3, (step + 1) & 3
            return slow ^ (slow >> 1), fast ^ (fast >> 1)

        def id_at(step):
            major, minor = offsets_at(step)
            return ahead_of(z, major) * 4 + ahead_of(x, minor)

        def four(index, carry):
            steps = [index * 4 + more for more in range(8)]
            for step in steps[:4]:
                block_of(n, id_at(step))
            if unfinished is not None:
                standard(unfinished, [id_at(step & 15) for step in steps[4:]])
            for step in steps[:4]:
                major, minor = offsets_at(step)
                m = ahead_of(z, major) * 4 + ahead_of(x, minor)

                @pl.when(major > 0)
                def _():
                    source = gram[n].at[m, pl.ds(0, z_rows)]
                    to_v = shard_at(ahead_of(z, major), x, y)
                    copy_to(source, z_parts[n].at[minor, major], sent, z_recv.at[minor + 2 if n == 2 else n], j, to_v).start()

                @pl.when(minor > 0)
                def _():
                    source = gram[n].at[m, pl.ds(z_rows, x_rows)]
                    to_v = shard_at(z, ahead_of(x, minor), y)
                    copy_to(source, x_parts[n].at[major, minor], sent, x_recv.at[major + 2 if n == 2 else n], j, to_v).start()

                if y_rows:
                    rows = pl.ds(pl.multiple_of(z_rows + x_rows + y_rows // 2 * (y ^ 1), 8), y_rows // 2)
                    copy_to(
                        gram[n].at[m, rows], y_parts.at[major * 4 + minor], sent, y_recv.at[major], j, v ^ 1
                    ).start()
            return carry

        with jax.named_scope("kernels"):
            if unfinished is not None:
                standard(unfinished, [id_at(step) for step in range(4)])
            lax.fori_loop(0, OWN // 4, four, 0)

    def second_sums(n):
        z_rows, x_rows, y_rows = split[n]

        def along(step, block):
            parts, recv, sums = ((z_parts, z_recv, z_sums), (x_parts, x_recv, x_sums))[block]
            if n == 2:
                with jax.named_scope("part_wait"):
                    await_bytes(parts[n].at[step, pl.ds(1, 3)], recv.at[step + 2])
            own = (ahead_of(z, step) * 4 + x) if block else (z * 4 + ahead_of(x, step))
            own = gram[n][own, pl.ds(z_rows, x_rows) if block else pl.ds(0, z_rows), :]
            sums[n][step] = (own + parts[n][step, 1]) + (parts[n][step, 2] + parts[n][step, 3])
            for other in range(2):
                side = y ^ other
                count = (z_rows, x_rows)[block] // 2
                rows = pl.ds(pl.multiple_of(side * count, 8), count)
                slot = step * 2 + other
                to_v = shard_at(ahead_of(z, step), x, side) if block else shard_at(z, ahead_of(x, step), side)
                if slot:
                    copy_to(
                        sums[n].at[step, rows], last[n][block].at[slot], sent, sum_recv.at[n * 2 + block], j, to_v
                    ).start()
                else:
                    last[n][block][0] = sums[n][0, rows, :]

        def from_side(major):
            with jax.named_scope("part_wait"):
                await_bytes(y_parts.at[pl.ds(major * 4, 4)], y_recv.at[major])
            for minor in range(4):
                step = major * 4 + minor
                to_z, to_x = ahead_of(z, major), ahead_of(x, minor)
                rows = pl.ds(pl.multiple_of(z_rows + x_rows + y_rows // 2 * y, 8), y_rows // 2)
                added = y_parts[step] + gram[n][to_z * 4 + to_x, rows, :]
                if step:
                    y_sums[step] = added
                    copy_to(
                        y_sums.at[step], y_last.at[step], sent, sum_recv.at[n * 2 + 2], j, shard_at(to_z, to_x, y)
                    ).start()
                else:
                    y_last[0] = added

        if y_rows:
            for major in (1, 3, 2, 0):
                along(major, 1)
                from_side(major)
        else:
            with jax.named_scope("part_wait"):
                await_bytes(x_parts[n].at[pl.ds(0, 3)], x_recv.at[n])
            for step in (1, 3, 2, 0):
                along(step, 1)
            with jax.named_scope("part_wait"):
                await_bytes(z_parts[n].at[pl.ds(0, 3)], z_recv.at[n])
        for step in (1, 3, 2, 0):
            along(step, 0)

    owner_v = v - y + j // 2
    place = core * 2 + y

    def hand_over(n):
        with jax.named_scope("last_wait"):
            for block, ref in enumerate(last[n]):
                await_bytes(ref.at[pl.ds(0, ref.shape[0] - 1)], sum_recv.at[n * 2 + block])
        mean = 1.0 / (VOX * SHARDS)
        first = 0
        for ref in last[n]:
            rows = ref.shape[1]
            total[n][pl.ds(first, rows), :] = jnp.sum(ref[...], axis=0) * mean
            first += rows
        for other in range(SUBJ):
            copy = copy_to(
                total[n], final[n].at[place], sent, final_recv.at[n], (j ^ other) if other else j, owner_v
            )
            if other:
                copy.start()
            else:

                @pl.when(owner_v != v)
                def _():
                    copy.start()

        @pl.when(owner_v == v)
        def _():
            final[n][place] = total[n][...]

    def await_final(n, sem):
        @pl.when(owner_v == v)
        def _():
            await_bytes(final[n].at[pl.ds(0, SUBJ - 1)], sem)

        @pl.when(owner_v != v)
        def _():
            await_bytes(final[n], sem)

    def scores_of(correlated, finished):
        with jax.named_scope("scores"):
            if correlated is not None:
                correlate(correlated)
            if finished is not None:
                standard(finished)

    def relayed(g):
        with jax.named_scope("relay_wait"):
            await_bytes(epochs.at[2 + g, 1 - core], relay_recv.at[g])

    scores_of(0, None)
    scores_of(1, 0)
    scores_of(2, 1)
    scores_of(3, 2)
    relayed(0)
    scores_of(4, 3)
    relay(1, 0)
    kernels(0, 4)
    scores_of(5, None)
    kernels(1, 5)
    relay(1, 1)
    relay(1, 2)
    scores_of(6, None)
    scores_of(None, 6)
    second_sums(0)
    relayed(1)
    scores_of(7, None)
    kernels(2, 7)
    second_sums(1)
    second_sums(2)
    hand_over(0)
    hand_over(1)
    hand_over(2)

    straight = (((1,), (0,)), ((), ()))
    left = lax.broadcasted_iota(I32, (EP * LOCAL, 128), 1) < 64
    upper = lax.broadcasted_iota(I32, (EP * LOCAL, 64), 1) < 32
    puts = (0, 384, 560, 864)
    corner = lax.broadcasted_iota(I32, (EP * LOCAL, 48), 1) >= 32

    def picked_by(pick, terms, dims):
        parts = [lax.dot_general(pick, t, dims, preferred_element_type=F32) for t in terms]
        return parts[0] + parts[1]

    def placed(n, i):
        pieces, first = [], 0
        for rows in split[n]:
            if rows:
                here = pl.ds(first, rows // 2)
                pieces += [final[n][2 * i, here, :], final[n][2 * i + 1, here, :]]
                first += rows // 2
        if n == 0:
            terms = two_terms(jnp.concatenate(pieces + [jnp.zeros((16, 128), F32)], axis=0))
            by_row = picked_by(pick_a[i], terms, straight)
            by_column = picked_by(turn_a[i], terms, NT)
            lines = [
                jnp.where(left, by_row[0:48], by_row[48:96]),
                jnp.where(left, by_row[96:144], by_row[144:192]),
                jnp.where(upper, by_column[0:48], by_column[96:144]),
                jnp.where(upper, by_column[48:96], by_column[144:192]),
            ]
        elif n == 1:
            terms = two_terms(jnp.concatenate(pieces, axis=0))
            by_column = picked_by(turn_b[i], terms, NT)
            turned = by_column[0:48] + jnp.where(corner, by_column[48:96], 0.0)
            lines = [picked_by(pick_b[i], terms, straight), turned]
        else:
            both = jnp.concatenate(pieces, axis=0)
            wide, square = two_terms(both[0:48]), two_terms(both[48:80])
            halves = [picked_by(pick_square[i, :, h * 32 : h * 32 + 32], square, straight) for h in range(2)]
            lines = [
                picked_by(pick_wide[i], wide, straight),
                jnp.where(left, halves[0], halves[1]),
                picked_by(turn_c[i], wide, NT),
            ]
        put = put_columns[i, puts[n] : puts[n + 1], :]
        terms = [jnp.dot(t, put, preferred_element_type=F32) for t in two_terms(jnp.concatenate(lines, axis=1))]
        return terms[0] + terms[1]

    with jax.named_scope("final"):
        await_final(0, final_recv.at[0])
    with jax.named_scope("place"):
        for i in range(2):
            out_ref[i] = placed(0, i)
    with jax.named_scope("final"):
        await_final(1, final_recv.at[1])
    with jax.named_scope("place"):
        for i in range(2):
            out_ref[i] += placed(1, i)
    with jax.named_scope("final"):
        await_final(2, final_recv.at[2])
    with jax.named_scope("place"):
        for i in range(2):
            out_ref[i] += placed(2, i)

    with jax.named_scope("drain"):
        for ref in (slab_in.at[pl.ds(0, SHARDS - 1)], slab_in.at[pl.ds(0, SHARDS - 1)]):
            await_bytes(ref, sent)

        @pl.when(jnp.logical_not(own_group))
        def _():
            await_bytes(slab_sum, sent)

        for slot in range(2):
            await_bytes(epochs.at[slot], sent)
        await_bytes(epochs.at[2], sent)
        for n in range(3):
            await_bytes(z_parts[n].at[pl.ds(0, 3)], sent)
            await_bytes(x_parts[n].at[pl.ds(0, 3)], sent)
            for ref in last[n]:
                await_bytes(ref.at[pl.ds(0, ref.shape[0] - 1)], sent)
            await_final(n, sent)
        await_bytes(y_parts, sent)


def body(series, offsets, selected):
    vmem = pltpu.VMEM
    dma = pltpu.SemaphoreType.DMA
    return pl.pallas_call(
        main_kernel,
        out_shape=pltpu.VMEM((2, EP * LOCAL, ROWS), F32),
        in_specs=[
            pl.BlockSpec(memory_space=pl.ANY),
            pl.BlockSpec(memory_space=pl.ANY),
            pl.BlockSpec(memory_space=pl.ANY),
        ],
        out_specs=pl.BlockSpec(memory_space=pltpu.VMEM),
        scratch_shapes=[
            pltpu.SMEM((SUBJ * LOCAL, EP), I32),
            pltpu.SMEM((SEL,), I32),
            vmem((LOCAL, RUN, VOX), BF16),
            vmem((QUADS * 256, LOCAL * RUN), BF16),
            vmem((SUBJ, 2, QUADS, 256, 256), BF16),
            vmem((SUBJ, QUADS, 16, VOX), F32),
            vmem((SHARDS, 2, QUADS * 256), BF16),
            vmem((SHARDS, 2, QUADS * 256), BF16),
            vmem((2, QUADS * 256), BF16),
            vmem((SHARDS, 2, QUADS * 256), BF16),
            vmem((SUBJ * QUADS, OWN, 256), F32),
            vmem((SUBJ * QUADS, 256, 256), BF16),
            vmem((SUBJ * QUADS, 256, 256), BF16),
            vmem((SUBJ * QUADS, OWN, 256), F32),
            vmem((SUBJ * QUADS, OWN, 256), F32),
            vmem((QUADS, 256, 256), F32),
            vmem((QUADS, 256, 256), F32),
            vmem((OWN, ROWS, VOX), BF16),
            vmem((OWN, 48, 128), F32),
            vmem((OWN, 48, 128), F32),
            vmem((OWN, 80, 128), F32),
            vmem((4, 4, 32, 128), F32),
            vmem((4, 4, 16, 128), F32),
            vmem((4, 4, 32, 128), F32),
            vmem((4, 4, 16, 128), F32),
            vmem((4, 4, 32, 128), F32),
            vmem((4, 4, 32, 128), F32),
            vmem((OWN, 8, 128), F32),
            vmem((4, 32, 128), F32),
            vmem((4, 16, 128), F32),
            vmem((4, 32, 128), F32),
            vmem((4, 16, 128), F32),
            vmem((4, 32, 128), F32),
            vmem((4, 32, 128), F32),
            vmem((OWN, 8, 128), F32),
            vmem((8, 16, 128), F32),
            vmem((8, 8, 128), F32),
            vmem((8, 16, 128), F32),
            vmem((8, 8, 128), F32),
            vmem((8, 16, 128), F32),
            vmem((8, 16, 128), F32),
            vmem((OWN, 8, 128), F32),
            vmem((24, 128), F32),
            vmem((24, 128), F32),
            vmem((40, 128), F32),
            vmem((SUBJ, 24, 128), F32),
            vmem((SUBJ, 24, 128), F32),
            vmem((SUBJ, 40, 128), F32),
            vmem((2, 4 * EP * LOCAL, 64), BF16),
            vmem((2, EP * LOCAL, 48), BF16),
            vmem((2, EP * LOCAL, 48), BF16),
            vmem((2, EP * LOCAL, 64), BF16),
            vmem((2, 4 * EP * LOCAL, 128), BF16),
            vmem((2, 2 * EP * LOCAL, 128), BF16),
            vmem((2, EP * LOCAL, 128), BF16),
            vmem((2, 864, ROWS), BF16),
            dma((3,)),
            dma,
            dma,
            dma,
            dma,
            dma((2 * QUADS,)),
            dma((2,)),
            dma((6,)),
            dma((6,)),
            dma((4,)),
            dma((7,)),
            dma((3,)),
        ],
        compiler_params=pltpu.CompilerParams(collective_id=0, has_side_effects=True),
    )(series, offsets, selected)


def solution(mesh):
    placed = (P("subj", None, "vox"), P(), P())
    return jax.shard_map(
        body, mesh=mesh, in_specs=placed, out_specs=P("vox", "subj", None), check_vma=False
    )
```
